32 devices in a mesh: dp: 8 (over y, x, core), tensor: 4 (over z).
Axes of the slice: x: 2, y: 2, z: 4, core: 2. Of those that a mesh axis runs over, the one named last changes fastest.
Arguments:
- tokens: bfloat16 [2048, 2048], P('dp'), may hold values from -6 to 6
- w_query: bfloat16 [2048, 2048], P('dp', 'tensor'), may hold values from -0.125 to 0.125
- w_key: bfloat16 [2048, 2048], P('dp', 'tensor'), may hold values from -0.125 to 0.125
- w_value: bfloat16 [2048, 2048], P('dp', 'tensor'), may hold values from -0.125 to 0.125
- w_out: bfloat16 [2048, 2048], P('tensor', 'dp'), may hold values from -0.5 to 0.5
- gain_attn: bfloat16 [2048], P('dp'), may hold values from 0.5 to 1.5
- gain_ffn: bfloat16 [2048], P('dp'), may hold values from 0.5 to 1.5
- w_router: bfloat16 [2048, 16], P('dp'), may hold values from -0.25 to 0.25
- shared_gate: bfloat16 [2048, 5632], P('dp', 'tensor'), may hold values from -0.125 to 0.125
- shared_up: bfloat16 [2048, 5632], P('dp', 'tensor'), may hold values from -0.125 to 0.125
- shared_down: bfloat16 [5632, 2048], P('tensor', 'dp'), may hold values from -0.15625 to 0.15625
- shared_switch: bfloat16 [2048], P('dp'), may hold values from -0.125 to 0.125
- expert_gate: bfloat16 [16, 2048, 1408], P('dp', None, 'tensor'), may hold values from -0.125 to 0.125
- expert_up_weight: bfloat16 [16, 2048, 1408], P('dp', None, 'tensor'), may hold values from -0.125 to 0.125
- expert_down: bfloat16 [16, 1408, 2048], P('dp', 'tensor'), may hold values from -1.25 to 1.25
- routes: int32 [2048, 4], P('dp'), may hold values from 0 to 15, all different within a row; in each aligned block of 256 rows (0 to 255, 256 to 511, ...) at most 96 rows name the same one
- segments: int32 [8, 256], P('dp'), may hold values from 0 to 3, never falling along the last dimension, each value on 1 to 128 neighbouring positions
- cotangent: bfloat16 [2048, 2048], P('dp'), may hold values from -6 to 6
Outputs:
- output: bfloat16 [2048, 2048], P('dp')
- grad_input: float32 [2048, 2048], P('dp')
- grad_query: float32 [2048, 2048], P('dp', 'tensor')
- grad_key: float32 [2048, 2048], P('dp', 'tensor')
- grad_value: float32 [2048, 2048], P('dp', 'tensor')
- grad_out_proj: float32 [2048, 2048], P('tensor', 'dp')
- grad_gain_attn: float32 [2048], P('dp')
- grad_gain_ffn: float32 [2048], P('dp')
- grad_router: float32 [2048, 16], P('dp')
- grad_shared_gate: float32 [2048, 5632], P('dp', 'tensor')
- grad_shared_up: float32 [2048, 5632], P('dp', 'tensor')
- grad_shared_down: float32 [5632, 2048], P('tensor', 'dp')
- grad_shared_switch: float32 [2048], P('dp')
- grad_expert_gate: float32 [16, 2048, 1408], P('dp', None, 'tensor')
- grad_expert_up: float32 [16, 2048, 1408], P('dp', None, 'tensor')
- grad_expert_down: float32 [16, 1408, 2048], P('dp', 'tensor')
The draws below stay inside these ranges and needn't reach their ends.
Inputs may be any that keep to these rules, and one draw needn't show every extreme that they name: `routes`: A token names 4 different experts. Within the tokens of one device (aligned blocks of 256 tokens) no expert is named by more than 96 tokens, and in every draw some expert is named by exactly 96. `segments`: within a packed row segment numbers never fall; each segment holds 1 to 128 positions, and one holds exactly 128.
All inputs are finite; a program needn't handle non-finite values.
Results may differ from the reference program's by a relative error of at most 0.025.
Values may be sent and summed in bfloat16 or wider, within the bound.
A program may use at most 256 MiB of HBM per device.

```python
import math
import jax
import jax.numpy as jnp
import numpy as np
from jax import lax

D = 2048
HEADS = 16
HEAD_DIM = 128
FE = 1408
FS = 5632
TOP = 4
SEQ = 256
TOK_DEV = 256
ROWS = 8
TOKENS = 2048
EXPERTS = 16
CAP = 96
N_DP = 8
N_TENSOR = 4


def level_of(key, extent, pieces, low, high):
    level, own = 1.0, jax.random.fold_in(key, 6)
    for axis_at, blocks in pieces:
        draws = jnp.exp(jax.random.uniform(jax.random.fold_in(own, axis_at), (blocks,), jnp.float32, low / len(pieces), high / len(pieces)))
        level = level * jnp.repeat(draws, extent[axis_at] // blocks).reshape([-1 if axis == axis_at else 1 for axis in range(len(extent))])
    return level


def length_profile(amount, total, bound, skew):
    weights = [(1 << 20) // math.isqrt(standing ** skew) + 1 for standing in range(2, amount + 1)]
    rest, given = total - bound - (amount - 1), [1] * (amount - 1)
    while rest > 0:
        movable = [i for i in range(amount - 1) if given[i] < bound]
        pool, budget = sum([weights[i] for i in movable]), rest
        for i in movable:
            more = min(bound - given[i], max(1, budget * weights[i] // pool), rest)
            given[i] = given[i] + more
            rest = rest - more
    return np.array([bound] + given)


def ragged_sizes(key, number_of, total, bound, slope):
    if number_of == 2:
        one = jax.random.randint(key, (), max(1, total - bound), min(bound, total - 1) + 1)
        return jnp.stack([one, total - one])
    tallies = jnp.asarray(length_profile(number_of, total, bound, slope), jnp.int32)
    twos = (number_of - 1) // 2
    donor, taker = tallies[1:1 + 2 * twos:2], tallies[2:2 + 2 * twos:2]
    room = jnp.minimum(donor - 1, bound - taker)
    passed = jax.random.randint(jax.random.fold_in(key, 1), (twos,), 0, 1 << 20) % (room + 1)
    tallies = tallies.at[1:1 + 2 * twos:2].set(donor - passed).at[2:2 + 2 * twos:2].set(taker + passed)
    return tallies[jax.random.permutation(jax.random.fold_in(key, 2), number_of)]


def routed_block(own_key, own, number, rows, amount, top, most, skew):
    sequence = jax.random.permutation(own_key, amount)
    crowded, usual = portions_of(amount, rows * top, most, skew, True), portions_of(amount, rows * top, most, skew, False)
    places = jnp.arange(amount)

    def named(sizes, rotation):
        used = int((sizes > 0).sum())
        fixed = max(1, used // 4)
        passed = fixed + (places - fixed + rotation * (used - fixed)) % max(1, amount - fixed)
        return jnp.zeros((amount,), jnp.int32).at[sequence[jnp.where(places < fixed, places, passed)]].set(jnp.asarray(sizes, jnp.int32))

    sizes = jnp.where(number % 4 == 0, named(crowded, number // 4), named(usual, number - number // 4 - 1))
    mixed = jax.random.permutation(jax.random.fold_in(own, 3), amount)
    giver, receiver = mixed[0:amount // 2 * 2:2], mixed[1:amount // 2 * 2:2]
    slack = jnp.minimum(sizes[giver] - 1, most - sizes[receiver]) // 2
    slack = jnp.where((giver == sequence[0]) | (receiver == sequence[0]) | (sizes[receiver] == 0), 0, jnp.maximum(slack, 0))
    passed = jax.random.randint(jax.random.fold_in(own, 4), (amount // 2,), 0, 1 << 20) % (slack + 1)
    sizes = sizes.at[giver].add(-passed).at[receiver].add(passed)
    items = jnp.searchsorted(jnp.cumsum(sizes), jnp.arange(rows * top), side="right").astype(jnp.int32)
    table = items.reshape(top, rows).T
    table = table[jax.random.permutation(jax.random.fold_in(own, 1), rows)]
    rotation = jax.random.randint(jax.random.fold_in(own, 2), (rows, 1), 0, top)
    return jnp.take_along_axis(table, (jnp.arange(top)[None, :] + rotation) % top, axis=1)


def portions_of(amount, total, limit, lean, full):
    loads = [(1 << 20) // math.isqrt(standing ** lean) + 1 for standing in range(1, amount + 1)]
    largest = limit if full else min(limit, max(-(-total // amount), total * loads[0] // sum(loads)))
    least = 1 if total - largest >= amount - 1 else 0
    counts, spare = [largest] + [least] * (amount - 1), total - largest - least * (amount - 1)
    while spare > 0:
        movable = [i for i in range(1, amount) if counts[i] < largest] or [i for i in range(1, amount) if counts[i] < limit]
        whole, budget = sum([loads[i] for i in movable]), spare
        for i in movable:
            addition = min(limit - counts[i], max(1, budget * loads[i] // whole), spare)
            counts[i] = counts[i] + addition
            spare = spare - addition
    return np.array(counts)


def normal_values(rng, dims, width, bound, split=(), kind=jnp.bfloat16):
    level = level_of(rng, dims, split, -0.22, 0.18) if split else 1.0
    array = jax.random.normal(rng, dims, jnp.float32) * width * level
    return jnp.minimum(jnp.maximum(array, -bound), bound).astype(kind)


def setup_inputs(seed: int = 0) -> dict:
    keys = jax.random.split(jax.random.key(seed), 19)
    tokens = normal_values(keys[0], (TOKENS, D), 1.0, 6.0, ((0, 8),))
    w_query = normal_values(keys[1], (D, D), D ** -0.5, 0.125, ((0, 8), (1, 4)))
    w_key = normal_values(keys[2], (D, D), D ** -0.5, 0.125, ((0, 8), (1, 4)))
    w_value = normal_values(keys[3], (D, D), D ** -0.5, 0.125, ((0, 8), (1, 4)))
    w_out = normal_values(keys[4], (D, D), (D // 16) ** -0.5, 0.5, ((0, 4), (1, 8)))
    gain_attn = jnp.clip(1.0 + 0.1 * jax.random.normal(keys[5], (D,), jnp.float32), 0.5, 1.5).astype(jnp.bfloat16)
    gain_ffn = jnp.clip(1.0 + 0.1 * jax.random.normal(keys[6], (D,), jnp.float32), 0.5, 1.5).astype(jnp.bfloat16)
    w_router = normal_values(keys[7], (D, EXPERTS), (D // 4) ** -0.5, 0.25, ((0, 8),))
    shared_gate = normal_values(keys[8], (D, FS), D ** -0.5, 0.125, ((0, 8), (1, 4)))
    shared_up = normal_values(keys[9], (D, FS), D ** -0.5, 0.125, ((0, 8), (1, 4)))
    shared_down = normal_values(keys[10], (FS, D), (FS // 4) ** -0.5, 0.15625, ((0, 4), (1, 8)))
    shared_switch = normal_values(keys[11], (D,), D ** -0.5, 0.125, ((0, 8),))
    expert_gate = normal_values(keys[12], (EXPERTS, D, FE), D ** -0.5, 0.125, ((0, 8), (2, 4)))
    expert_up_weight = normal_values(keys[13], (EXPERTS, D, FE), D ** -0.5, 0.125, ((0, 8), (2, 4)))
    expert_down = normal_values(keys[14], (EXPERTS, FE, D), (max(FE // 64, 2)) ** -0.5, 1.25, ((0, 8), (1, 4)))
    routes_keys = jax.random.split(jax.random.fold_in(keys[15], 1), TOKENS // TOK_DEV)
    routes_turns = jax.random.permutation(jax.random.fold_in(keys[15], 3), TOKENS // TOK_DEV)
    routes = jax.vmap(lambda own, number: routed_block(jax.random.fold_in(keys[15], 2), own, number, TOK_DEV, EXPERTS, TOP, CAP, 1))(routes_keys, routes_turns).reshape((TOKENS, TOP))
    segments = jax.vmap(lambda own: jnp.searchsorted(jnp.cumsum(ragged_sizes(own, 4, SEQ, SEQ // 2, 0)), jnp.arange(SEQ), side="right"))(jax.random.split(keys[16], ROWS)).reshape((ROWS, SEQ)).astype(jnp.int32)
    cotangent = normal_values(keys[17], (TOKENS, D), 1.0, 6.0, ((0, 8),))
    return dict(tokens=tokens, w_query=w_query, w_key=w_key, w_value=w_value, w_out=w_out, gain_attn=gain_attn, gain_ffn=gain_ffn, w_router=w_router, shared_gate=shared_gate, shared_up=shared_up, shared_down=shared_down, shared_switch=shared_switch, expert_gate=expert_gate, expert_up_weight=expert_up_weight, expert_down=expert_down, routes=routes, segments=segments, cotangent=cotangent)


@jax.custom_vjp
def low(v):
    return lax.optimization_barrier(v.astype(jnp.bfloat16)).astype(jnp.float32)

@jax.custom_vjp
def low_back(v):
    return v

def low_keep(v):
    return (low(v), None)

def low_pass(kept, grad):
    return (grad,)

def back_keep(v):
    return (v, None)

def back_low(kept, grad):
    return (low(grad),)
low.defvjp(low_keep, low_pass)
low_back.defvjp(back_keep, back_low)
EPSILON = 1e-06
HIGHEST = lax.Precision.HIGHEST

def matmul(left, right):
    return jnp.dot(left, right, preferred_element_type=jnp.float32, precision=HIGHEST)

def rms_norm(values, gain):
    inverse = lax.rsqrt(lax.optimization_barrier(jnp.mean(values * values, axis=-1, keepdims=True)) + EPSILON)
    return values * inverse * gain

def softmax_last(scores):
    exponent = jnp.exp(scores)
    return exponent / lax.optimization_barrier(jnp.sum(exponent, axis=-1, keepdims=True))

def rope_tables():
    half_dim = HEAD_DIM // 2
    exponent = jnp.arange(half_dim, dtype=jnp.float32) * (2.0 / HEAD_DIM)
    inverse_freq = jnp.exp(-exponent * jnp.log(jnp.float32(1000000.0)))
    angles = jnp.arange(SEQ, dtype=jnp.float32)[:, None] * inverse_freq[None, :]
    return (jnp.cos(angles), jnp.sin(angles))

def rotate(values, cosine, sine, sign):
    half_dim = values.shape[-1] // 2
    first = values[..., :half_dim]
    second = values[..., half_dim:]
    cos_table = cosine[:, None, :]
    sin_table = sine[:, None, :] * sign
    return jnp.concatenate([first * cos_table - second * sin_table, second * cos_table + first * sin_table], axis=-1)

def allowed_mask(segment_row):
    spots = jnp.arange(segment_row.shape[0], dtype=jnp.int32)
    return (spots[None, :] <= spots[:, None]) & (segment_row[None, :] == segment_row[:, None])

def attend_row(inputs):
    queries, key_rows, value_rows, segment_row = inputs
    scores = jnp.einsum('qhd,khd->hqk', queries, key_rows, precision=HIGHEST) * HEAD_DIM ** (-0.5)
    scores = low_back(scores)
    scores = jnp.where(allowed_mask(segment_row)[None], scores, -1e+30)
    weights = low(softmax_last(scores))
    return jnp.einsum('hqk,khd->qhd', weights, value_rows, precision=HIGHEST)

def slot_table(routes):
    blocks = routes.reshape(N_DP, TOK_DEV * TOP)
    onehot = (blocks[:, :, None] == jnp.arange(EXPERTS, dtype=jnp.int32)[None, None, :]).astype(jnp.int32)
    ranking = lax.optimization_barrier(jnp.sum((jnp.cumsum(onehot, axis=1) - 1) * onehot, axis=-1))
    column = jnp.arange(N_DP, dtype=jnp.int32)[:, None] * CAP + ranking
    entries = jnp.arange(TOKENS * TOP, dtype=jnp.int32).reshape(N_DP, TOK_DEV * TOP)
    return jnp.full((EXPERTS, N_DP * CAP), -1, jnp.int32).at[blocks, column].set(entries)

def reference(tokens, w_query, w_key, w_value, w_out, gain_attn, gain_ffn, w_router, shared_gate, shared_up, shared_down, shared_switch, expert_gate, expert_up_weight, expert_down, routes, segments, cotangent):
    table = slot_table(routes)
    hits = routes[:, :, None] == jnp.arange(EXPERTS, dtype=jnp.int32)[None, None, :]
    cosine, sine = rope_tables()

    def forward(params):
        inputs, query_w, key_w, value_w, out_w, attn_gain, ffn_gain, router_w, gate_w, up_w, down_w, switch_w, expert_gates, expert_ups, expert_downs = params
        attn_in = low(rms_norm(inputs, attn_gain))
        shape_four = (TOKENS // SEQ, SEQ, HEADS, HEAD_DIM)
        queries = low(rotate(low_back(matmul(attn_in, query_w)).reshape(shape_four), cosine, sine, 1.0))
        key_rows = low(rotate(low_back(matmul(attn_in, key_w)).reshape(shape_four), cosine, sine, 1.0))
        value_rows = low(low_back(matmul(attn_in, value_w))).reshape(shape_four)
        context = lax.map(jax.checkpoint(attend_row), (queries, key_rows, value_rows, segments))
        context = low_back(low(context.reshape(TOKENS, D)))
        middle = inputs + low_back(matmul(context, out_w))
        ffn_in = low(rms_norm(middle, ffn_gain))
        router_probs = softmax_last(low_back(matmul(ffn_in, router_w)))
        route_weight = lax.optimization_barrier(jnp.sum(jnp.where(hits, router_probs[:, None, :], 0.0), axis=-1))
        shared_hidden = low(jax.nn.silu(low_back(matmul(ffn_in, gate_w))) * low_back(matmul(ffn_in, up_w)))
        shared_out = low_back(matmul(shared_hidden, down_w))
        switch = jax.nn.sigmoid(lax.optimization_barrier(jnp.sum(ffn_in * switch_w, axis=-1, keepdims=True)))
        flat_weight = route_weight.reshape(-1)

        def expert_rows(slots, gates_one, ups_one, downs_one):
            valid = (slots >= 0).astype(jnp.float32)
            safe_slots = jnp.where(slots >= 0, slots, 0)
            owners = safe_slots // TOP
            rows_in = ffn_in[owners] * valid[:, None]
            hidden = low(jax.nn.silu(low_back(matmul(rows_in, gates_one))) * low_back(matmul(rows_in, ups_one)))
            grouped = hidden.reshape(hidden.shape[0], N_TENSOR, FE // N_TENSOR)
            partial_out = jnp.einsum('rnf,nfd->nrd', grouped, downs_one.reshape(N_TENSOR, FE // N_TENSOR, D), precision=HIGHEST)
            summed = lax.optimization_barrier(jnp.sum(low_back(low(partial_out)), axis=0))
            return summed * (flat_weight[safe_slots] * valid)[:, None]
        checked_rows = jax.checkpoint(expert_rows)

        def expert_step(total, items):
            slots, gates_one, ups_one, downs_one = items
            owners = jnp.where(slots >= 0, slots, 0) // TOP
            return (total.at[owners].add(checked_rows(slots, gates_one, ups_one, downs_one)), None)
        routed, unused = lax.scan(expert_step, jnp.zeros((TOKENS, D), jnp.float32), (table, expert_gates, expert_ups, expert_downs))
        return middle + routed + switch * shared_out
    params = (tokens.astype(jnp.float32), w_query.astype(jnp.float32), w_key.astype(jnp.float32), w_value.astype(jnp.float32), w_out.astype(jnp.float32), gain_attn.astype(jnp.float32), gain_ffn.astype(jnp.float32), w_router.astype(jnp.float32), shared_gate.astype(jnp.float32), shared_up.astype(jnp.float32), shared_down.astype(jnp.float32), shared_switch.astype(jnp.float32), expert_gate.astype(jnp.float32), expert_up_weight.astype(jnp.float32), expert_down.astype(jnp.float32))
    result, pullback = jax.vjp(forward, params)
    grads = pullback(cotangent.astype(jnp.float32))[0]
    return (result.astype(jnp.bfloat16), grads[0], grads[1], grads[2], grads[3], grads[4], grads[5], grads[6], grads[7], grads[8], grads[9], grads[10], grads[11], grads[12], grads[13], grads[14])
```

```python
import functools

import jax
import jax.numpy as jnp
from jax import lax
from jax.experimental import pallas as pl
from jax.experimental.pallas import tpu as pltpu
from jax.sharding import PartitionSpec as P

HEAD_DIM = 128
TOP = 4
SEQ = 256


EPSILON = 1e-06
MESH = pl.DeviceIdType.MESH


def ring_chip(position, chips):
    half = chips // 2
    upper = position // half
    return position + upper * (chips - 1 + half - 2 * position)


def ring_spot(chip, chips):
    return ring_chip(chip, chips)


def greet(partners):
    barrier = pltpu.get_barrier_semaphore()
    for partner in partners:
        pl.semaphore_signal(barrier, inc=1, device_id=partner, device_id_type=MESH)
    pl.semaphore_wait(barrier, len(partners))


def remote(source, target, axis, device, sends, recvs, slot):
    return pltpu.make_async_remote_copy(
        src_ref=source,
        dst_ref=target,
        send_sem=sends.at[slot],
        recv_sem=recvs.at[slot],
        device_id={axis: device},
        device_id_type=MESH,
    )


class Ring:
    def __init__(self, ranks):
        self.ranks = ranks
        self.chips = ranks // 2
        self.half = self.chips // 2
        self.me = lax.axis_index("dp")
        self.core = self.me % 2
        self.position = ring_spot(self.me // 2, self.chips)
        self.sibling = self.me + 1 - 2 * self.core
        self.ahead = self.device(1)
        self.behind = self.device(-1)

    def chip(self, offset):
        return ring_chip((self.position + offset + self.chips) % self.chips, self.chips)

    def device(self, offset):
        return self.chip(offset) * 2 + self.core

    def other(self, offset):
        return self.chip(offset) * 2 + 1 - self.core

    def partners(self):
        return [{"dp": self.ahead}, {"dp": self.behind}, {"dp": self.sibling}]


def gather_slots(half):
    return 2 * half


def side_slots(half):
    return 2 * half + 1


class RingGather:
    def __init__(self, ring, place, rows, sends, recvs, side_sends, side_recvs, base, side_base):
        self.ring, self.place, self.rows, self.cut = ring, place, rows, rows // 2
        self.sends, self.recvs = sends, recvs
        self.side_sends, self.side_recvs = side_sends, side_recvs
        self.base, self.side_base = base, side_base
        self.started, self.side_sizes = [], []

    def hop(self, source, target, device, slot):
        copy = remote(source, target, "dp", device, self.sends, self.recvs, self.base + slot)
        copy.start()
        self.started.append(copy)
        return copy

    def share(self, source, target, size):
        slot = self.side_base + len(self.side_sizes)
        copy = remote(source, target, "dp", self.ring.sibling, self.side_sends, self.side_recvs, slot)
        copy.start()
        self.started.append(copy)
        self.side_sizes.append(size)

    def begin(self, source):
        ring = self.ring
        target = self.place(ring.me, 0, self.rows)
        ahead = self.hop(source, target, ring.ahead, 0)
        behind = self.hop(source, target, ring.behind, ring.half)
        self.share(source, target, self.rows)
        self.last = (ahead, behind)

    def step(self, number):
        ring = self.ring
        following = []
        for which, sign in enumerate((-1, 1)):
            owner = ring.device(sign * number)
            onward = (ring.ahead, ring.behind)[which]
            self.last[which].wait_recv()
            if number < ring.half:
                block = self.place(owner, 0, self.rows)
                if number == ring.half - 1:
                    part = self.place(owner, (0, self.cut)[which], self.cut)
                else:
                    part = block
                following.append(self.hop(part, part, onward, which * ring.half + number))
                self.share(block, block, self.rows)
            else:
                part = self.place(owner, (0, self.cut)[which], self.cut)
                self.share(part, part, self.cut)
        self.last = following

    def finish(self):
        ring = self.ring
        for copy in self.started:
            copy.wait_send()
        for index, size in enumerate(self.side_sizes):
            block = self.place(ring.me, 0, size)
            remote(
                block, block, "dp", ring.sibling, self.side_sends, self.side_recvs, self.side_base + index
            ).wait_recv()


def gather_kernel(ranks, counts, *refs):
    amount = len(counts)
    sources, all_ref = refs[:amount], refs[amount]
    stage, local_sem, sends, recvs, side_sends, side_recvs = refs[amount + 1 :]
    rows = stage.shape[0]
    ring = Ring(ranks)
    loads, start = [], 0
    for index, count in enumerate(counts):
        load = pltpu.make_async_copy(
            sources[index], stage.at[:, pl.ds(start, count)], local_sem.at[index]
        )
        load.start()
        loads.append(load)
        start += count

    def place(device, first, size):
        return all_ref.at[pl.ds(device * rows + first, size)]

    greet(ring.partners())
    for load in loads:
        load.wait()
    work = RingGather(ring, place, rows, sends, recvs, side_sends, side_recvs, 0, 0)
    work.begin(stage)
    store = pltpu.make_async_copy(stage, place(ring.me, 0, rows), local_sem.at[amount])
    store.start()
    for number in range(1, ring.half + 1):
        work.step(number)
    store.wait()
    work.finish()


def gather_dp(values, ranks, identity):
    half = ranks // 4
    rows = values[0].shape[0]
    counts = [value.shape[1] for value in values]
    return pl.pallas_call(
        functools.partial(gather_kernel, ranks, counts),
        out_shape=jax.ShapeDtypeStruct((ranks * rows, sum(counts)), values[0].dtype),
        in_specs=[pl.BlockSpec(memory_space=pl.ANY)] * len(values),
        out_specs=pl.BlockSpec(memory_space=pl.ANY),
        scratch_shapes=[
            pltpu.VMEM((rows, sum(counts)), values[0].dtype),
            pltpu.SemaphoreType.DMA((len(counts) + 1,)),
            pltpu.SemaphoreType.DMA((gather_slots(half),)),
            pltpu.SemaphoreType.DMA((gather_slots(half),)),
            pltpu.SemaphoreType.DMA((side_slots(half),)),
            pltpu.SemaphoreType.DMA((side_slots(half),)),
        ],
        compiler_params=pltpu.CompilerParams(collective_id=identity, has_side_effects=True),
        name="gather_dp",
    )(*values)


def near_first(peers):
    order = [0]
    for step in range(1, peers // 2 + 1):
        order.append(step)
        if peers - step != step:
            order.append(peers - step)
    return order


STRIP = 16


def strips(rows, body):
    strip = min(STRIP, rows)

    def step(index, carry):
        body(pl.ds(pl.multiple_of(index * strip, strip), strip), index * strip, strip)
        return carry

    lax.fori_loop(0, rows // strip, step, 0)


def middle_kernel(
    ranks,
    peers,
    part_ref,
    tokens_ref,
    gain_ref,
    all_ref,
    middle_ref,
    own,
    got,
    local_sem,
    z_sends,
    z_recvs,
    x_sends,
    x_recvs,
    sends,
    recvs,
    side_sends,
    side_recvs,
):
    ring = Ring(ranks)
    here = lax.axis_index("tensor")
    block = part_ref.shape[0]
    rows = block // peers
    away = [(here + k) % peers for k in range(peers)]
    greet(ring.partners() + [{"tensor": away[k]} for k in range(1, peers)])
    order = near_first(peers)
    exchanged = []
    for k in reversed(order[1:]):
        copy = remote(
            part_ref.at[pl.ds(away[k] * rows, rows)],
            got.at[peers - k - 1],
            "tensor",
            away[k],
            z_sends,
            z_recvs,
            peers - k - 1,
        )
        copy.start()
        exchanged.append(copy)
    for copy in exchanged:
        copy.wait()
    first = here * rows

    def norm(spot, start, size):
        mine = pl.ds(pl.multiple_of(first + start, size), size)
        total = part_ref[mine, :].astype(jnp.float32)
        for k in range(peers - 1):
            total = total + got[k, spot, :].astype(jnp.float32)
        middle = tokens_ref[mine, :].astype(jnp.float32) + total
        middle_ref[spot, :] = middle
        inverse = lax.rsqrt(jnp.mean(middle * middle, axis=-1, keepdims=True) + EPSILON)
        own[spot, :] = ((middle * inverse) * gain_ref[...]).astype(own.dtype)

    strips(rows, norm)

    def place_of(k):
        def place(device, start, size):
            return all_ref.at[pl.ds(device * block + away[k] * rows + start, size)]

        return place

    mine = place_of(0)(ring.me, 0, rows)
    forwards = []
    for k in order[1:]:
        copy = remote(own, mine, "tensor", away[k], x_sends, x_recvs, peers - k - 1)
        copy.start()
        forwards.append(copy)
    half = ring.half
    works = []
    for k in range(peers):
        works.append(
            RingGather(
                ring,
                place_of(k),
                rows,
                sends,
                recvs,
                side_sends,
                side_recvs,
                k * gather_slots(half),
                k * side_slots(half),
            )
        )
    works[0].begin(own)
    store = pltpu.make_async_copy(own, mine, local_sem)
    store.start()
    for index in range(len(order) + half):
        if 0 < index < len(order):
            k = order[index]
            spot = place_of(k)(ring.me, 0, rows)
            remote(own, spot, "tensor", away[k], x_sends, x_recvs, k - 1).wait_recv()
            works[k].begin(spot)
        for number in range(1, half + 1):
            if 0 <= index - number < len(order):
                works[order[index - number]].step(number)
    store.wait()
    for copy in forwards:
        copy.wait_send()
    for work in works:
        work.finish()


def middle_and_gather(part, tokens, gain, ranks, peers, identity):
    half = ranks // 4
    block, width = part.shape
    rows = block // peers
    vmem = pl.BlockSpec(memory_space=pltpu.VMEM)
    return pl.pallas_call(
        functools.partial(middle_kernel, ranks, peers),
        out_shape=(
            jax.ShapeDtypeStruct((ranks * block, width), part.dtype),
            jax.ShapeDtypeStruct((rows, width), jnp.float32),
        ),
        in_specs=[vmem, vmem, vmem],
        out_specs=(pl.BlockSpec(memory_space=pl.ANY), vmem),
        scratch_shapes=[
            pltpu.VMEM((rows, width), part.dtype),
            pltpu.VMEM((peers - 1, rows, width), part.dtype),
            pltpu.SemaphoreType.DMA,
            pltpu.SemaphoreType.DMA((peers - 1,)),
            pltpu.SemaphoreType.DMA((peers - 1,)),
            pltpu.SemaphoreType.DMA((peers - 1,)),
            pltpu.SemaphoreType.DMA((peers - 1,)),
            pltpu.SemaphoreType.DMA((peers * gather_slots(half),)),
            pltpu.SemaphoreType.DMA((peers * gather_slots(half),)),
            pltpu.SemaphoreType.DMA((peers * side_slots(half),)),
            pltpu.SemaphoreType.DMA((peers * side_slots(half),)),
        ],
        compiler_params=pltpu.CompilerParams(collective_id=identity, has_side_effects=True),
        name="middle_and_gather",
    )(part, tokens, gain)


class RingReduce:
    def __init__(self, ring, part_at, rows, side, stage, got, sends, recvs, side_sends, side_recvs, base, side_base):
        self.ring, self.part_at, self.rows, self.cut = ring, part_at, rows, rows // 2
        self.side, self.stage, self.got = side, stage, got
        self.sends, self.recvs = sends, recvs
        self.side_sends, self.side_recvs = side_sends, side_recvs
        self.base, self.side_base = base, side_base
        self.started = []
        self.arrivals = {}

    def order(self):
        half = self.ring.half
        offsets = [half]
        for distance in range(half - 1, 0, -1):
            offsets += [distance, self.ring.chips - distance]
        return offsets + [0]

    def hand_over(self, offset):
        ring = self.ring
        copy = remote(
            self.part_at(ring.other(offset)),
            self.side.at[offset],
            "dp",
            ring.sibling,
            self.side_sends,
            self.side_recvs,
            self.side_base + offset,
        )
        copy.start()
        self.started.append(copy)
        self.arrivals[offset] = copy

    def hop(self, source, target, device, slot):
        copy = remote(source, target, "dp", device, self.sends, self.recvs, self.base + slot)
        copy.start()
        self.started.append(copy)
        return copy

    def add(self, offset, extra, first, size):
        mine = self.part_at(self.ring.device(offset))

        def whole(spot, start, count):
            total = mine[spot, :].astype(jnp.float32) + self.side[offset, spot, :].astype(jnp.float32)
            self.stage[offset, spot, :] = total.astype(self.stage.dtype)

        def more(spot, start, count):
            here = pl.ds(pl.multiple_of(first + start, count), count)
            total = mine[here, :].astype(jnp.float32) + self.side[offset, here, :].astype(jnp.float32)
            total = total + extra[here, :].astype(jnp.float32)
            self.stage[offset, here, :] = total.astype(self.stage.dtype)

        if extra is None:
            strips(self.rows, whole)
            return
        strips(size, more)
        if size < self.rows:
            rest = self.rows - size
            begin = 0 if first else size

            def plain(spot, start, count):
                here = pl.ds(pl.multiple_of(begin + start, count), count)
                total = mine[here, :].astype(jnp.float32) + self.side[offset, here, :].astype(jnp.float32)
                self.stage[offset, here, :] = total.astype(self.stage.dtype)

            strips(rest, plain)

    def step(self, number):
        ring, half, cut = self.ring, self.ring.half, self.cut
        if number == 0:
            self.arrivals[half].wait_recv()
            self.add(half, None, 0, self.rows)
            self.last = []
            for which, device in enumerate((ring.ahead, ring.behind)):
                part = pl.ds((0, cut)[which], cut)
                self.last.append(
                    self.hop(
                        self.stage.at[half, part], self.got.at[which * half, part], device, which * half
                    )
                )
            return
        following = []
        for which, device in enumerate((ring.ahead, ring.behind)):
            distance = half - number
            offset = distance if which == 0 else ring.chips - distance
            self.arrivals[offset].wait_recv()
            self.last[which].wait_recv()
            extra = self.got.at[which * half + number - 1]
            if number == 1:
                self.add(offset, extra, (0, cut)[which], cut)
            else:
                self.add(offset, extra, 0, self.rows)
            following.append(
                self.hop(
                    self.stage.at[offset],
                    self.got.at[which * half + number],
                    device,
                    which * half + number,
                )
            )
        self.last = following

    def total(self, emit):
        half = self.ring.half
        self.arrivals[0].wait_recv()
        for copy in self.last:
            copy.wait_recv()
        mine = self.part_at(self.ring.me)

        def body(spot, start, size):
            value = mine[spot, :].astype(jnp.float32) + self.side[0, spot, :].astype(jnp.float32)
            value = value + self.got[half - 1, spot, :].astype(jnp.float32)
            value = value + self.got[2 * half - 1, spot, :].astype(jnp.float32)
            emit(spot, start, size, value)

        strips(self.rows, body)

    def finish(self):
        for copy in self.started:
            copy.wait_send()


def back_kernel(
    ranks,
    peers,
    part_ref,
    middle_ref,
    cot_ref,
    gain_ref,
    out_ref,
    grad_ref,
    gain_grad_ref,
    side,
    stage,
    got,
    z_stage,
    z_got,
    low_ref,
    sends,
    recvs,
    side_sends,
    side_recvs,
    z_sends,
    z_recvs,
    x_sends,
    x_recvs,
    local_sem,
):
    ring = Ring(ranks)
    here = lax.axis_index("tensor")
    block = cot_ref.shape[0]
    rows = block // peers
    half, chips = ring.half, ring.chips
    away = [(here + k) % peers for k in range(peers)]
    greet(ring.partners() + [{"tensor": away[k]} for k in range(1, peers)])
    order = list(reversed(near_first(peers)))
    works = {}
    for k in order:

        def part_at(device, k=k):
            return part_ref.at[pl.ds(device * block + away[k] * rows, rows)]

        works[k] = RingReduce(
            ring,
            part_at,
            rows,
            side.at[k],
            stage.at[k],
            got.at[k],
            sends,
            recvs,
            side_sends,
            side_recvs,
            k * 2 * half,
            k * chips,
        )
    for offset in works[order[0]].order():
        for k in order:
            works[k].hand_over(offset)
    reduced = []
    for index in range(len(order) + half):
        for number in range(0, half):
            if 0 <= index - number < len(order):
                works[order[index - number]].step(number)
        if 0 <= index - half < len(order):
            k = order[index - half]

            def emit(spot, start, size, value, k=k):
                z_stage[k, spot, :] = value.astype(z_stage.dtype)

            if k:
                works[k].total(emit)
                copy = remote(
                    z_stage.at[k], z_got.at[peers - k - 1], "tensor", away[k], z_sends, z_recvs, peers - k - 1
                )
                copy.start()
                reduced.append(copy)
    for copy in reduced:
        copy.wait_recv()
    first = here * rows
    gain_grad_ref[...] = jnp.zeros_like(gain_grad_ref)

    def norm(spot, start, size, value):
        for k in range(peers - 1):
            value = value + z_got[k, spot, :].astype(jnp.float32)
        middle = middle_ref[spot, :]
        inverse = lax.rsqrt(jnp.mean(middle * middle, axis=-1, keepdims=True) + EPSILON)
        normed = middle * inverse
        scaled = value * gain_ref[...]
        back = inverse * (scaled - normed * jnp.mean(scaled * normed, axis=-1, keepdims=True))
        mine = pl.ds(pl.multiple_of(first + start, size), size)
        grad = cot_ref[mine, :].astype(jnp.float32) + back
        grad_ref[spot, :] = grad
        low_ref[spot, :] = grad.astype(low_ref.dtype)
        gain_grad_ref[...] += jnp.sum(value * normed, axis=0, keepdims=True)

    works[0].total(norm)
    mine = out_ref.at[pl.ds(here * rows, rows)]
    spread = []
    for k in near_first(peers)[:0:-1]:
        copy = remote(low_ref, mine, "tensor", away[k], x_sends, x_recvs, peers - k - 1)
        copy.start()
        spread.append(copy)
    store = pltpu.make_async_copy(low_ref, mine, local_sem)
    store.start()
    store.wait()
    for copy in reduced:
        copy.wait_send()
    for copy in spread:
        copy.wait()
    for k in order:
        works[k].finish()


def reduce_and_norm(part, middle, cotangent, gain, ranks, peers, identity):
    half = ranks // 4
    chips = ranks // 2
    block, width = cotangent.shape
    rows = block // peers
    vmem = pl.BlockSpec(memory_space=pltpu.VMEM)
    low = part.dtype
    return pl.pallas_call(
        functools.partial(back_kernel, ranks, peers),
        out_shape=(
            jax.ShapeDtypeStruct((block, width), low),
            jax.ShapeDtypeStruct((rows, width), jnp.float32),
            jax.ShapeDtypeStruct((1, width), jnp.float32),
        ),
        in_specs=[vmem] * 4,
        out_specs=(pl.BlockSpec(memory_space=pl.ANY), vmem, vmem),
        scratch_shapes=[
            pltpu.VMEM((peers, chips, rows, width), low),
            pltpu.VMEM((peers, chips, rows, width), low),
            pltpu.VMEM((peers, 2 * half, rows, width), low),
            pltpu.VMEM((peers, rows, width), low),
            pltpu.VMEM((peers - 1, rows, width), low),
            pltpu.VMEM((rows, width), low),
            pltpu.SemaphoreType.DMA((peers * 2 * half,)),
            pltpu.SemaphoreType.DMA((peers * 2 * half,)),
            pltpu.SemaphoreType.DMA((peers * chips,)),
            pltpu.SemaphoreType.DMA((peers * chips,)),
            pltpu.SemaphoreType.DMA((peers - 1,)),
            pltpu.SemaphoreType.DMA((peers - 1,)),
            pltpu.SemaphoreType.DMA((peers - 1,)),
            pltpu.SemaphoreType.DMA((peers - 1,)),
            pltpu.SemaphoreType.DMA,
        ],
        compiler_params=pltpu.CompilerParams(
            collective_id=identity, has_side_effects=True, vmem_limit_bytes=50 << 20
        ),
        name="reduce_and_norm",
    )(part, middle, cotangent, gain)


def final_kernel(
    ranks,
    peers,
    part_ref,
    tokens_ref,
    gain_ref,
    grad_ref,
    gain_grad_ref,
    weights_ref,
    out_ref,
    sum_ref,
    small_ref,
    gains_ref,
    side,
    stage,
    got,
    z_got,
    low_ref,
    small_own,
    small_got,
    gains_own,
    gains_got,
    gains_part,
    gains_z,
    sends,
    recvs,
    side_sends,
    side_recvs,
    z_sends,
    z_recvs,
    x_sends,
    x_recvs,
    s_sends,
    s_recvs,
    g_sends,
    g_recvs,
    h_sends,
    h_recvs,
    local_sem,
):
    ring = Ring(ranks)
    here = lax.axis_index("tensor")
    block, width = part_ref.shape
    rows = block // peers
    half, chips = ring.half, ring.chips
    lot = weights_ref.shape[0] // ranks
    pieces = side.shape[0]
    size = lot // pieces
    wide = sum_ref.shape[1]
    columns = width // ranks
    away = [(here + k) % peers for k in range(peers)]
    others = [(ring.me + k) % ranks for k in range(ranks)]
    greet(
        [{"dp": others[k]} for k in range(1, ranks)] + [{"tensor": away[k]} for k in range(1, peers)]
    )
    far_first = near_first(peers)[:0:-1]
    exchanged = []
    for k in far_first:
        copy = remote(
            part_ref.at[pl.ds(away[k] * rows, rows)],
            z_got.at[peers - k - 1],
            "tensor",
            away[k],
            z_sends,
            z_recvs,
            peers - k - 1,
        )
        copy.start()
        exchanged.append(copy)
    works = []
    for piece in range(pieces):

        def part_at(device, piece=piece):
            return weights_ref.at[pl.ds(device * lot + piece * size, size)]

        works.append(
            RingReduce(
                ring,
                part_at,
                size,
                side.at[piece],
                stage.at[piece],
                got.at[piece],
                sends,
                recvs,
                side_sends,
                side_recvs,
                piece * 2 * half,
                piece * chips,
            )
        )
    for offset in works[0].order():
        for work in works:
            work.hand_over(offset)

    first = here * rows
    gains_own[...] = jnp.zeros_like(gains_own)
    gains_own[1:2, :] = gain_grad_ref[...]

    def norm(spot, start, count):
        mine = pl.ds(pl.multiple_of(first + start, count), count)
        value = part_ref[mine, :].astype(jnp.float32)
        for k in range(peers - 1):
            value = value + z_got[k, spot, :].astype(jnp.float32)
        inputs = tokens_ref[mine, :].astype(jnp.float32)
        inverse = lax.rsqrt(jnp.mean(inputs * inputs, axis=-1, keepdims=True) + EPSILON)
        normed = inputs * inverse
        scaled = value * gain_ref[...]
        back = inverse * (scaled - normed * jnp.mean(scaled * normed, axis=-1, keepdims=True))
        low_ref[spot, :] = (grad_ref[spot, :] + back).astype(low_ref.dtype)
        gains_own[0:1, :] += jnp.sum(value * normed, axis=0, keepdims=True)

    spread, handed = [], []
    mine = out_ref.at[pl.ds(here * rows, rows)]
    store = pltpu.make_async_copy(low_ref, mine, local_sem)

    def after_norm():
        for copy in exchanged:
            copy.wait()
        strips(rows, norm)
        for k in range(1, ranks):
            copy = remote(
                gains_own.at[:, pl.ds(pl.multiple_of(others[k] * columns, columns), columns)],
                gains_got.at[ranks - k - 1],
                "dp",
                others[k],
                g_sends,
                g_recvs,
                ranks - k - 1,
            )
            copy.start()
            handed.append(copy)
        for k in far_first:
            copy = remote(low_ref, mine, "tensor", away[k], x_sends, x_recvs, peers - k - 1)
            copy.start()
            spread.append(copy)
        store.start()

    for index in range(pieces + half):
        if index == half:
            after_norm()
        for number in range(0, half):
            if 0 <= index - number < pieces:
                works[index - number].step(number)
        if 0 <= index - half < pieces:
            piece = index - half

            def emit(spot, start, count, value, piece=piece):
                place = pl.ds(pl.multiple_of(piece * size + start, count), count)
                sum_ref[place, :] = value[:, :wide]
                small_own[place, :] = value[:, wide:]

            works[piece].total(emit)
    for copy in handed:
        copy.wait_recv()
    gains = gains_own[:, pl.ds(pl.multiple_of(ring.me * columns, columns), columns)]
    for k in range(ranks - 1):
        gains = gains + gains_got[k]
    gains_part[...] = gains
    last = []
    for k in far_first:
        for source, target, out_sems, in_sems in (
            (gains_part, gains_z, h_sends, h_recvs),
            (small_own, small_got, s_sends, s_recvs),
        ):
            copy = remote(
                source, target.at[peers - k - 1], "tensor", away[k], out_sems, in_sems, peers - k - 1
            )
            copy.start()
            last.append(copy)
    store.wait()
    for copy in handed:
        copy.wait_send()
    for copy in spread + last:
        copy.wait()
    gains = gains_part[...]
    small = small_own[...]
    for k in range(peers - 1):
        gains = gains + gains_z[k]
        small = small + small_got[k]
    gains_ref[...] = gains
    small_ref[...] = small
    for work in works:
        work.finish()


def finish_grads(part, tokens, gain, grad, gain_grad, weights, ranks, peers, identity):
    half = ranks // 4
    chips = ranks // 2
    block, width = part.shape
    rows = block // peers
    lot = weights.shape[0] // ranks
    total = weights.shape[1]
    tail = 128
    pieces = 4
    size = lot // pieces
    columns = width // ranks
    vmem = pl.BlockSpec(memory_space=pltpu.VMEM)
    low = part.dtype
    dma = pltpu.SemaphoreType.DMA
    return pl.pallas_call(
        functools.partial(final_kernel, ranks, peers),
        out_shape=(
            jax.ShapeDtypeStruct((block, width), low),
            jax.ShapeDtypeStruct((lot, total - tail), jnp.float32),
            jax.ShapeDtypeStruct((lot, tail), jnp.float32),
            jax.ShapeDtypeStruct((8, columns), jnp.float32),
        ),
        in_specs=[vmem] * 6,
        out_specs=(pl.BlockSpec(memory_space=pl.ANY), vmem, vmem, vmem),
        scratch_shapes=[
            pltpu.VMEM((pieces, chips, size, total), low),
            pltpu.VMEM((pieces, chips, size, total), low),
            pltpu.VMEM((pieces, 2 * half, size, total), low),
            pltpu.VMEM((peers - 1, rows, width), low),
            pltpu.VMEM((rows, width), low),
            pltpu.VMEM((lot, tail), jnp.float32),
            pltpu.VMEM((peers - 1, lot, tail), jnp.float32),
            pltpu.VMEM((8, width), jnp.float32),
            pltpu.VMEM((ranks - 1, 8, columns), jnp.float32),
            pltpu.VMEM((8, columns), jnp.float32),
            pltpu.VMEM((peers - 1, 8, columns), jnp.float32),
            dma((pieces * 2 * half,)),
            dma((pieces * 2 * half,)),
            dma((pieces * chips,)),
            dma((pieces * chips,)),
            dma((peers - 1,)),
            dma((peers - 1,)),
            dma((peers - 1,)),
            dma((peers - 1,)),
            dma((peers - 1,)),
            dma((peers - 1,)),
            dma((ranks - 1,)),
            dma((ranks - 1,)),
            dma((peers - 1,)),
            dma((peers - 1,)),
            dma,
        ],
        compiler_params=pltpu.CompilerParams(
            collective_id=identity, has_side_effects=True, vmem_limit_bytes=50 << 20
        ),
        name="finish_grads",
    )(part, tokens, gain, grad, gain_grad, weights)


def dot_rows(left, right):
    return lax.dot_general(
        left, right, (((0,), (0,)), ((), ())), preferred_element_type=jnp.float32
    )


def dot_last(left, right):
    return lax.dot_general(
        left, right, (((1,), (1,)), ((), ())), preferred_element_type=jnp.float32
    )


def forward_rms_norm(values, gain):
    inverse = lax.rsqrt(jnp.mean(values * values, axis=-1, keepdims=True) + EPSILON)
    normed = values * inverse
    return (normed * gain, normed, inverse)


def rope_tables():
    half_dim = HEAD_DIM // 2
    exponent = jnp.arange(half_dim, dtype=jnp.float32) * (2.0 / HEAD_DIM)
    inverse_freq = jnp.exp(-exponent * jnp.log(jnp.float32(1000000.0)))
    angles = jnp.arange(SEQ, dtype=jnp.float32)[:, None] * inverse_freq[None, :]
    return (jnp.cos(angles), jnp.sin(angles))


def rotate(values, cosine, sine, sign):
    half_dim = values.shape[-1] // 2
    first = values[..., :half_dim]
    second = values[..., half_dim:]
    cos_table = cosine[:, None, :]
    sin_table = sine[:, None, :] * sign
    return jnp.concatenate(
        [first * cos_table - second * sin_table, second * cos_table + first * sin_table], axis=-1
    )


def masked_scores(queries, key_rows, segment_row):
    raw = jnp.einsum(
        "qhd,khd->hqk", queries, key_rows, preferred_element_type=jnp.float32
    ) * HEAD_DIM ** (-0.5)
    spots = jnp.arange(segment_row.shape[0], dtype=jnp.int32)
    allowed = (spots[None, :] <= spots[:, None]) & (segment_row[None, :] == segment_row[:, None])
    return jnp.where(allowed[None], raw, -1e30)


def attend_forward(inputs):
    queries, key_rows, value_rows, segment_row = inputs
    scores = masked_scores(queries, key_rows, segment_row)
    exponent = jnp.exp(scores)
    totals = jnp.sum(exponent, axis=-1, keepdims=True)
    probs = (exponent / totals).astype(jnp.bfloat16)
    context = jnp.einsum(
        "hqk,khd->qhd", probs, value_rows, preferred_element_type=jnp.float32
    ).astype(jnp.bfloat16)
    return (context, jnp.log(totals[..., 0]))


def attend_backward(inputs):
    queries, key_rows, value_rows, segment_row, log_total, grad_context = inputs
    scores = masked_scores(queries, key_rows, segment_row)
    probs = jnp.exp(scores - log_total[..., None])
    probs_low = probs.astype(jnp.bfloat16)
    grad_probs = jnp.einsum(
        "qhd,khd->hqk", grad_context, value_rows, preferred_element_type=jnp.float32
    )
    inner = jnp.sum(probs * grad_probs, axis=-1, keepdims=True)
    grad_scores = (probs * (grad_probs - inner)).astype(jnp.bfloat16)
    grad_queries = jnp.einsum(
        "hqk,khd->qhd", grad_scores, key_rows, preferred_element_type=jnp.float32
    ) * HEAD_DIM ** (-0.5)
    grad_keys = jnp.einsum(
        "hqk,qhd->khd", grad_scores, queries, preferred_element_type=jnp.float32
    ) * HEAD_DIM ** (-0.5)
    grad_values = jnp.einsum(
        "hqk,qhd->khd", probs_low, grad_context, preferred_element_type=jnp.float32
    )
    return (grad_queries, grad_keys, grad_values)


def pad_columns(parts, width):
    rows = parts[0].shape[0]
    used = sum(part.shape[1] for part in parts)
    if used < width:
        parts = list(parts) + [jnp.zeros((rows, width - used), parts[0].dtype)]
    return jnp.concatenate(parts, axis=1)


def lanes(count):
    return -(-count // 128) * 128


def gather_rows(values):
    return lax.all_gather(values, "dp", axis=0, tiled=True)


def scatter_rows(values):
    return lax.psum_scatter(values, "dp", scatter_dimension=0, tiled=True)


def spread_columns(values, ranks):
    rows, columns = values.shape
    blocks = values.reshape(rows, ranks, columns // ranks).transpose(1, 0, 2)
    return blocks


def shards(
    tokens,
    w_query,
    w_key,
    w_value,
    w_out,
    gain_attn,
    gain_ffn,
    w_router,
    shared_gate,
    shared_up,
    shared_down,
    shared_switch,
    expert_gate,
    expert_up_weight,
    expert_down,
    routes,
    segments,
    cotangent,
):
    low = jnp.bfloat16
    ranks = lax.axis_size("dp")
    peers = lax.axis_size("tensor")
    me = lax.axis_index("dp")
    token_count, width = tokens.shape
    local_experts, _, expert_hidden = expert_gate.shape
    expert_count = local_experts * ranks
    block = width // ranks
    head_width = w_query.shape[1]
    head_count = head_width // HEAD_DIM
    row_count = token_count // SEQ
    shared_width = shared_gate.shape[1]
    shared_own = shared_width // ranks
    hidden = local_experts * expert_hidden + shared_own
    hidden_pad = lanes(hidden)
    small_pad = 128
    shape_four = (row_count, SEQ, head_count, HEAD_DIM)

    small = pad_columns(
        [w_router, shared_switch[:, None], gain_attn[:, None], gain_ffn[:, None]], small_pad
    )
    gathered = gather_dp([w_query, w_key, w_value, small, w_out.T], ranks, 0)
    qkv_full = gathered[:, : 3 * head_width]
    small_full = gathered[:, 3 * head_width : 3 * head_width + small_pad]
    out_rows = gathered[:, 3 * head_width + small_pad :]
    attn_gain = small_full[:, expert_count + 1].astype(jnp.float32)
    ffn_gain = small_full[:, expert_count + 2].astype(jnp.float32)
    router_columns = jnp.where(
        jnp.arange(small_pad)[None, :] <= expert_count, small_full, jnp.zeros_like(small_full)
    )

    packed = jnp.concatenate(
        [
            spread_columns(shared_gate, ranks),
            spread_columns(shared_up, ranks),
            spread_columns(shared_down.T, ranks),
        ],
        axis=2,
    )
    shared_mine = lax.all_to_all(packed, "dp", split_axis=0, concat_axis=0, tiled=True)
    shared_mine = shared_mine.reshape(width, 3 * shared_own)
    gate_own = shared_mine[:, :shared_own]
    up_own = shared_mine[:, shared_own : 2 * shared_own]
    down_own = shared_mine[:, 2 * shared_own :].T

    gates = pad_columns([expert_gate[j] for j in range(local_experts)] + [gate_own], hidden_pad)
    ups = pad_columns([expert_up_weight[j] for j in range(local_experts)] + [up_own], hidden_pad)
    wide = jnp.concatenate([gates, ups, router_columns], axis=1)
    downs = jnp.concatenate(
        [expert_down[j] for j in range(local_experts)]
        + [down_own, jnp.zeros((hidden_pad - hidden, width), low)],
        axis=0,
    )

    chosen = jnp.sum(
        (routes[:, :, None] == jnp.arange(small_pad, dtype=jnp.int32)[None, None, :]).astype(jnp.float32),
        axis=1,
    ).astype(low)
    cot_chosen = gather_rows(jnp.concatenate([cotangent, chosen], axis=1))
    cot_all = cot_chosen[:, :width]
    chosen_all = cot_chosen[:, width:].astype(jnp.float32)

    cosine, sine = rope_tables()
    inputs = tokens.astype(jnp.float32)
    attn_pre, _, _ = forward_rms_norm(inputs, attn_gain)
    attn_in = attn_pre.astype(low)
    qkv = jnp.dot(attn_in, qkv_full, preferred_element_type=jnp.float32)
    queries = rotate(qkv[:, :head_width].reshape(shape_four), cosine, sine, 1.0).astype(low)
    key_rows = rotate(
        qkv[:, head_width : 2 * head_width].reshape(shape_four), cosine, sine, 1.0
    ).astype(low)
    value_rows = qkv[:, 2 * head_width :].astype(low).reshape(shape_four)
    contexts, log_totals = jax.vmap(attend_forward)((queries, key_rows, value_rows, segments))
    context_flat = contexts.reshape(token_count, head_width)
    attn_part = dot_last(context_flat, out_rows)
    x_all, middle = middle_and_gather(
        attn_part.astype(low), tokens, ffn_gain[None, :], ranks, peers, 1
    )

    pre = jnp.dot(x_all, wide, preferred_element_type=jnp.float32)
    pre_gate = pre[:, :hidden_pad]
    pre_up = pre[:, hidden_pad : 2 * hidden_pad]
    pre_small = pre[:, 2 * hidden_pad :]
    column = jnp.arange(small_pad, dtype=jnp.int32)[None, :]
    exponent = jnp.where(column < expert_count, jnp.exp(jnp.where(column < expert_count, pre_small, 0.0)), 0.0)
    router_probs = exponent / jnp.sum(exponent, axis=-1, keepdims=True)
    switch = lax.logistic(jnp.sum(jnp.where(column == expert_count, pre_small, 0.0), axis=-1, keepdims=True))
    weights, spots = [], []
    for j in range(local_experts):
        spot = column == me * local_experts + j
        spots.append(spot)
        weights.append(jnp.sum(jnp.where(spot, router_probs * chosen_all, 0.0), axis=-1, keepdims=True))
    unit = jnp.arange(hidden_pad, dtype=jnp.int32)[None, :]
    scale = switch
    for j in reversed(range(local_experts)):
        scale = jnp.where(unit < (j + 1) * expert_hidden, weights[j], scale)
    sig = lax.logistic(pre_gate)
    act = pre_gate * sig
    hidden_state = (act * pre_up).astype(low)
    scaled_hidden = (scale * (act * pre_up)).astype(low)
    out_part = jnp.dot(scaled_hidden, downs, preferred_element_type=jnp.float32).astype(low)
    moe = lax.psum_scatter(scatter_rows(out_part), "tensor", scatter_dimension=0, tiled=True)
    output = (middle + moe.astype(jnp.float32)).astype(low)
    output = lax.all_gather(output, "tensor", axis=0, tiled=True)

    cot_hidden = dot_last(cot_all, downs)
    products = hidden_state.astype(jnp.float32) * cot_hidden
    grad_hidden = scale * cot_hidden
    grad_gate = (grad_hidden * pre_up * sig * (1.0 + pre_gate * (1.0 - sig))).astype(low)
    grad_up = (grad_hidden * act).astype(low)
    grad_choice = jnp.zeros_like(router_probs)
    for j in range(local_experts):
        inside = (unit >= j * expert_hidden) & (unit < (j + 1) * expert_hidden)
        total = jnp.sum(jnp.where(inside, products, 0.0), axis=-1, keepdims=True)
        grad_choice = grad_choice + jnp.where(spots[j], chosen_all * total, 0.0)
    switch_total = jnp.sum(
        jnp.where(unit >= local_experts * expert_hidden, products, 0.0), axis=-1, keepdims=True
    )
    grad_logits = router_probs * (
        grad_choice - jnp.sum(router_probs * grad_choice, axis=-1, keepdims=True)
    )
    grad_small = jnp.where(
        column == expert_count, switch_total * switch * (1.0 - switch), grad_logits
    ).astype(low)
    grads_wide = jnp.concatenate([grad_gate, grad_up, grad_small], axis=1)
    back_part = dot_last(grads_wide, wide).astype(low)
    grad_attn_out, grad_middle, grad_gain_ffn = reduce_and_norm(
        back_part, middle, cotangent, ffn_gain[None, :], ranks, peers, 2
    )

    grad_wide = dot_rows(x_all, grads_wide)
    grad_downs = dot_rows(scaled_hidden, cot_all)
    grad_expert_gate = jnp.stack(
        [grad_wide[:, j * expert_hidden : (j + 1) * expert_hidden] for j in range(local_experts)]
    )
    grad_expert_up = jnp.stack(
        [
            grad_wide[:, hidden_pad + j * expert_hidden : hidden_pad + (j + 1) * expert_hidden]
            for j in range(local_experts)
        ]
    )
    grad_expert_down = grad_downs[: local_experts * expert_hidden].reshape(
        local_experts, expert_hidden, width
    )
    first = local_experts * expert_hidden
    grad_shared = jnp.concatenate(
        [
            grad_wide[:, first : first + shared_own].astype(low),
            grad_wide[:, hidden_pad + first : hidden_pad + first + shared_own].astype(low),
            grad_downs[first : first + shared_own].astype(low).T,
        ],
        axis=1,
    ).reshape(ranks, block, 3 * shared_own)
    grad_shared = lax.all_to_all(grad_shared, "dp", split_axis=0, concat_axis=0, tiled=True)

    def whole_columns(part):
        return part.transpose(1, 0, 2).reshape(block, shared_width)

    grad_shared_gate = whole_columns(grad_shared[:, :, :shared_own]).astype(jnp.float32)
    grad_shared_up = whole_columns(grad_shared[:, :, shared_own : 2 * shared_own]).astype(jnp.float32)
    grad_shared_down = whole_columns(grad_shared[:, :, 2 * shared_own :]).T.astype(jnp.float32)

    grad_out_rows = dot_rows(grad_attn_out, context_flat)
    grad_context = jnp.dot(grad_attn_out, out_rows, preferred_element_type=jnp.float32)
    grad_context = grad_context.astype(low).reshape(shape_four)
    grad_queries, grad_keys, grad_values = jax.vmap(attend_backward)(
        (queries, key_rows, value_rows, segments, log_totals, grad_context)
    )
    flat_shape = (token_count, head_width)
    grad_qkv_rows = jnp.concatenate(
        [
            rotate(grad_queries, cosine, sine, -1.0).reshape(flat_shape).astype(low),
            rotate(grad_keys, cosine, sine, -1.0).reshape(flat_shape).astype(low),
            grad_values.reshape(flat_shape).astype(low),
        ],
        axis=1,
    )
    grad_qkv = dot_rows(attn_in, grad_qkv_rows)
    attn_back_part = dot_last(grad_qkv_rows, qkv_full)
    grad_weights = jnp.concatenate(
        [grad_qkv.astype(low), grad_out_rows.astype(low), grad_wide[:, 2 * hidden_pad :].astype(low)],
        axis=1,
    )
    grad_input, grad_four, grad_tail, grad_gains = finish_grads(
        attn_back_part.astype(low),
        tokens,
        attn_gain[None, :],
        grad_middle,
        grad_gain_ffn,
        grad_weights,
        ranks,
        peers,
        3,
    )
    grad_input = grad_input.astype(jnp.float32)
    grad_query = grad_four[:, :head_width]
    grad_key = grad_four[:, head_width : 2 * head_width]
    grad_value = grad_four[:, 2 * head_width : 3 * head_width]
    grad_out_proj = grad_four[:, 3 * head_width :].T
    return (
        output,
        grad_input,
        grad_query,
        grad_key,
        grad_value,
        grad_out_proj,
        grad_gains[0],
        grad_gains[1],
        grad_tail[:, :expert_count],
        grad_shared_gate,
        grad_shared_up,
        grad_shared_down,
        grad_tail[:, expert_count],
        grad_expert_gate,
        grad_expert_up,
        grad_expert_down,
    )


def solution(mesh):
    in_specs = (
        P("dp", None),
        P("dp", "tensor"),
        P("dp", "tensor"),
        P("dp", "tensor"),
        P("tensor", "dp"),
        P("dp"),
        P("dp"),
        P("dp", None),
        P("dp", "tensor"),
        P("dp", "tensor"),
        P("tensor", "dp"),
        P("dp"),
        P("dp", None, "tensor"),
        P("dp", None, "tensor"),
        P("dp", "tensor", None),
        P("dp", None),
        P("dp", None),
        P("dp", None),
    )
    out_specs = (
        P("dp", None),
        P("dp", None),
        P("dp", "tensor"),
        P("dp", "tensor"),
        P("dp", "tensor"),
        P("tensor", "dp"),
        P("dp"),
        P("dp"),
        P("dp", None),
        P("dp", "tensor"),
        P("dp", "tensor"),
        P("tensor", "dp"),
        P("dp"),
        P("dp", None, "tensor"),
        P("dp", None, "tensor"),
        P("dp", "tensor", None),
    )
    return jax.shard_map(shards, mesh=mesh, in_specs=in_specs, out_specs=out_specs, check_vma=False)
```

```python
import functools

import jax
import jax.numpy as jnp
from jax import lax
from jax.experimental import pallas as pl
from jax.experimental.pallas import tpu as pltpu
from jax.sharding import PartitionSpec as P

HEAD_DIM = 128
TOP = 4
SEQ = 256


EPSILON = 1e-06
MESH = pl.DeviceIdType.MESH


def ring_chip(position, chips):
    half = chips // 2
    upper = position // half
    return position + upper * (chips - 1 + half - 2 * position)


def ring_spot(chip, chips):
    return ring_chip(chip, chips)


def greet(partners):
    barrier = pltpu.get_barrier_semaphore()
    for partner in partners:
        pl.semaphore_signal(barrier, inc=1, device_id=partner, device_id_type=MESH)
    pl.semaphore_wait(barrier, len(partners))


def remote(source, target, axis, device, sends, recvs, slot):
    return pltpu.make_async_remote_copy(
        src_ref=source,
        dst_ref=target,
        send_sem=sends.at[slot],
        recv_sem=recvs.at[slot],
        device_id={axis: device},
        device_id_type=MESH,
    )


class Ring:
    def __init__(self, ranks):
        self.ranks = ranks
        self.chips = ranks // 2
        self.half = self.chips // 2
        self.me = lax.axis_index("dp")
        self.core = self.me % 2
        self.position = ring_spot(self.me // 2, self.chips)
        self.sibling = self.me + 1 - 2 * self.core
        self.ahead = self.device(1)
        self.behind = self.device(-1)

    def chip(self, offset):
        return ring_chip((self.position + offset + self.chips) % self.chips, self.chips)

    def device(self, offset):
        return self.chip(offset) * 2 + self.core

    def other(self, offset):
        return self.chip(offset) * 2 + 1 - self.core

    def partners(self):
        return [{"dp": self.ahead}, {"dp": self.behind}, {"dp": self.sibling}]


def gather_slots(half):
    return 2 * half


def side_slots(half):
    return 2 * half


class RingGather:
    def __init__(self, ring, place, rows, sends, recvs, side_sends, side_recvs, base, side_base):
        self.ring, self.place, self.rows, self.cut = ring, place, rows, rows // 2
        self.sends, self.recvs = sends, recvs
        self.side_sends, self.side_recvs = side_sends, side_recvs
        self.base, self.side_base = base, side_base
        self.hops, self.sides = {}, 0

    def hop_copy(self, source, target, device, slot):
        return remote(source, target, "dp", device, self.sends, self.recvs, self.base + slot)

    def side_copy(self, source, target, slot):
        return remote(
            source,
            target,
            "dp",
            self.ring.sibling,
            self.side_sends,
            self.side_recvs,
            self.side_base + slot,
        )

    def hop(self, source, target, device, slot, size):
        self.hop_copy(source, target, device, slot).start()
        self.hops[slot] = size

    def share(self, source, target):
        self.side_copy(source, target, self.sides).start()
        self.sides += 1

    def begin(self, source):
        ring = self.ring
        target = self.place(ring.me, 0, self.rows)
        self.hop(source, target, ring.ahead, 0, self.rows)
        self.hop(source, target, ring.behind, ring.half, self.rows)
        self.share(source, target)

    def wait_hop(self, slot):
        block = self.place(self.ring.me, 0, self.hops[slot])
        self.hop_copy(block, block, self.ring.ahead, slot).wait_recv()

    def step(self, number):
        ring = self.ring
        for which, sign in enumerate((-1, 1)):
            owner = ring.device(sign * number)
            onward = (ring.ahead, ring.behind)[which]
            self.wait_hop(which * ring.half + number - 1)
            if number < ring.half:
                block = self.place(owner, 0, self.rows)
                size = self.rows
                part = block
                if number == ring.half - 1:
                    size = self.cut
                    part = self.place(owner, (0, self.cut)[which], size)
                self.hop(part, part, onward, which * ring.half + number, size)
                self.share(block, block)
        if number == ring.half:
            block = self.place(ring.device(number), 0, self.rows)
            self.share(block, block)

    def wait_side(self, index):
        block = self.place(self.ring.me, 0, self.rows)
        self.side_copy(block, block, index).wait_recv()

    def sent(self):
        for slot, size in self.hops.items():
            block = self.place(self.ring.me, 0, size)
            self.hop_copy(block, block, self.ring.ahead, slot).wait_send()
        for index in range(self.sides):
            block = self.place(self.ring.me, 0, self.rows)
            self.side_copy(block, block, index).wait_send()

    def finish(self):
        self.sent()
        for index in range(self.sides):
            self.wait_side(index)


def gather_kernel(ranks, counts, *refs):
    amount = len(counts)
    sources, all_ref = refs[:amount], refs[amount]
    stage, local_sem, sends, recvs, side_sends, side_recvs = refs[amount + 1 :]
    rows = stage.shape[0]
    ring = Ring(ranks)
    loads, start = [], 0
    for index, count in enumerate(counts):
        load = pltpu.make_async_copy(
            sources[index], stage.at[:, pl.ds(start, count)], local_sem.at[index]
        )
        load.start()
        loads.append(load)
        start += count

    def place(device, first, size):
        return all_ref.at[pl.ds(device * rows + first, size)]

    greet(ring.partners())
    for load in loads:
        load.wait()
    work = RingGather(ring, place, rows, sends, recvs, side_sends, side_recvs, 0, 0)
    work.begin(stage)
    store = pltpu.make_async_copy(stage, place(ring.me, 0, rows), local_sem.at[amount])
    store.start()
    for number in range(1, ring.half + 1):
        work.step(number)
    store.wait()
    work.finish()


def gather_dp(values, ranks, identity):
    half = ranks // 4
    rows = values[0].shape[0]
    counts = [value.shape[1] for value in values]
    return pl.pallas_call(
        functools.partial(gather_kernel, ranks, counts),
        out_shape=jax.ShapeDtypeStruct((ranks * rows, sum(counts)), values[0].dtype),
        in_specs=[pl.BlockSpec(memory_space=pl.ANY)] * len(values),
        out_specs=pl.BlockSpec(memory_space=pl.ANY),
        scratch_shapes=[
            pltpu.VMEM((rows, sum(counts)), values[0].dtype),
            pltpu.SemaphoreType.DMA((len(counts) + 1,)),
            pltpu.SemaphoreType.DMA((gather_slots(half),)),
            pltpu.SemaphoreType.DMA((gather_slots(half),)),
            pltpu.SemaphoreType.DMA((side_slots(half),)),
            pltpu.SemaphoreType.DMA((side_slots(half),)),
        ],
        compiler_params=pltpu.CompilerParams(collective_id=identity, has_side_effects=True),
        name="gather_dp",
    )(*values)


def near_first(peers):
    order = [0]
    for step in range(1, peers // 2 + 1):
        order.append(step)
        if peers - step != step:
            order.append(peers - step)
    return order


STRIP = 16


def strips(rows, body):
    strip = min(STRIP, rows)

    def step(index, carry):
        body(pl.ds(pl.multiple_of(index * strip, strip), strip), index * strip, strip)
        return carry

    lax.fori_loop(0, rows // strip, step, 0)


def matmul(left, right):
    return lax.dot_general(
        left, right, (((1,), (0,)), ((), ())), preferred_element_type=jnp.float32
    )


def matmul_last(left, right):
    return lax.dot_general(
        left, right, (((1,), (1,)), ((), ())), preferred_element_type=jnp.float32
    )


def tiles(width, tile, body):
    def step(index, carry):
        body(pl.ds(pl.multiple_of(index * tile, tile), tile))
        return carry

    lax.fori_loop(0, width // tile, step, 0)


class Layout:
    def __init__(self, local_experts, expert_hidden, shared_own, expert_count):
        self.local_experts = local_experts
        self.expert_hidden = expert_hidden
        self.shared_own = shared_own
        self.expert_count = expert_count
        self.part = -(-expert_hidden // 128) * 128
        self.shared_at = local_experts * self.part
        self.router_at = self.shared_at + shared_own
        self.last = -(-(shared_own + expert_count + 1) // 128) * 128
        self.hidden = self.shared_at + self.last
        self.router_tile = self.router_at // 128 * 128
        self.router_lane = self.router_at - self.router_tile
        self.tile = 256 if self.hidden % 256 == 0 else 128


def hidden_tiles(layout, x_ref, gates, ups, pre_gate, pre_up):
    def body(spot):
        pre_gate[:, spot] = matmul(x_ref[...], gates[:, spot])
        pre_up[:, spot] = matmul(x_ref[...], ups[:, spot])

    tiles(layout.hidden, layout.tile, body)


def cot_tiles(layout, cot_ref, downs, cot_hidden):
    def body(spot):
        cot_hidden[:, spot] = matmul_last(cot_ref[...], downs[spot, :])

    tiles(layout.hidden, layout.tile, body)


def gate_strips(layout, first_expert, chosen, pre_gate, pre_up, cot_hidden, scaled, grads):
    rows = pre_gate.shape[0]
    count, lane0 = layout.expert_count, layout.router_lane
    router = slice(layout.router_tile, layout.router_tile + 128)
    bounds = [(j * layout.part, (j + 1) * layout.part) for j in range(layout.local_experts)]
    bounds.append((layout.shared_at, layout.hidden))
    low = scaled.dtype

    def body(spot, start, size):
        lane = lax.broadcasted_iota(jnp.int32, (size, 128), 1)
        logits = pre_gate[spot, router]
        is_router = (lane >= lane0) & (lane < lane0 + count)
        is_switch = lane == lane0 + count
        power = jnp.where(is_router, jnp.exp(jnp.where(is_router, logits, 0.0)), 0.0)
        probs = power / jnp.sum(power, axis=-1, keepdims=True)
        raw = jnp.sum(jnp.where(is_switch, logits, 0.0), axis=-1, keepdims=True)
        switch = 1.0 / (1.0 + jnp.exp(-raw))
        mask = chosen[spot, :].astype(jnp.float32)
        scales = []
        for j in range(layout.local_experts):
            spotted = lane == lane0 + first_expert + j
            scales.append(jnp.sum(jnp.where(spotted, probs * mask, 0.0), axis=-1, keepdims=True))
        scales.append(switch)
        totals = []
        for (begin, end), scale in zip(bounds, scales):
            shared = begin == layout.shared_at
            columns = slice(begin, end)
            gate, up = pre_gate[spot, columns], pre_up[spot, columns]
            through = cot_hidden[spot, columns].astype(jnp.float32)
            sig = 1.0 / (1.0 + jnp.exp(-gate))
            act = gate * sig
            state = act * up
            grad = scale * through
            totals.append(jnp.sum(state * through, axis=-1, keepdims=True))
            scaled[spot, columns] = (scale * state).astype(low)
            grad_gate = grad * up * sig * (1.0 + gate * (1.0 - sig))
            grads[spot, columns] = grad_gate.astype(low)
            grads[spot, layout.hidden + begin : layout.hidden + end] = (grad * act).astype(low)
        choice = jnp.zeros_like(probs)
        for j in range(layout.local_experts):
            spotted = lane == lane0 + first_expert + j
            choice = choice + jnp.where(spotted, mask * totals[j], 0.0)
        small = probs * (choice - jnp.sum(probs * choice, axis=-1, keepdims=True))
        small = jnp.where(is_switch, totals[-1] * switch * (1.0 - switch), small)
        kept = grads[spot, router].astype(jnp.float32)
        kept = jnp.where(is_router | is_switch, small, kept)
        grads[spot, router] = kept.astype(low)

    strips(rows, body)


def out_tiles(width, scaled, downs, out):
    def body(spot):
        out[:, spot] = matmul(scaled[...], downs[:, spot]).astype(out.dtype)

    tiles(width, 256, body)


def back_tiles(layout, width, grads, gates, ups, back):
    hidden = layout.hidden

    def body(spot):
        total = matmul_last(grads[:, :hidden], gates[spot, :])
        total = total + matmul_last(grads[:, hidden:], ups[spot, :])
        back[:, spot] = total.astype(back.dtype)

    tiles(width, 256, body)


def layer_kernel(
    layout,
    ranks,
    peers,
    part_ref,
    tokens_ref,
    gain_ref,
    cot_ref,
    chosen_ref,
    small_ref,
    expert_gate_ref,
    expert_up_ref,
    expert_down_ref,
    shared_in_ref,
    shared_out_ref,
    x_all,
    cot_all,
    middle_ref,
    scaled_ref,
    grads_ref,
    out_ref,
    back_ref,
    gates,
    ups,
    downs,
    stage,
    pair_got,
    down_got,
    own,
    got,
    x_block,
    cot_block,
    pre_gate,
    pre_up,
    cot_hidden,
    scaled,
    grads,
    out,
    back,
    local_sem,
    stage_sem,
    block_sem,
    store_sem,
    pair_sends,
    pair_recvs,
    down_sends,
    down_recvs,
    z_sends,
    z_recvs,
    x_sends,
    x_recvs,
    sends,
    recvs,
    side_sends,
    side_recvs,
    c_sends,
    c_recvs,
    c_side_sends,
    c_side_recvs,
):
    ring = Ring(ranks)
    here = lax.axis_index("tensor")
    block, width = part_ref.shape
    rows = block // peers
    depth = width // ranks
    half = ring.half
    away = [(here + k) % peers for k in range(peers)]
    others = [(ring.me + k) % ranks for k in range(ranks)]
    greet(
        [{"dp": others[k]} for k in range(1, ranks)] + [{"tensor": away[k]} for k in range(1, peers)]
    )
    order = near_first(peers)

    exchanged = []
    for k in reversed(order[1:]):
        copy = remote(
            part_ref.at[pl.ds(away[k] * rows, rows)],
            got.at[peers - k - 1],
            "tensor",
            away[k],
            z_sends,
            z_recvs,
            peers - k - 1,
        )
        copy.start()
        exchanged.append(copy)

    handed = []
    for k in range(1, ranks):
        for source, target, out_sems, in_sems in (
            (shared_in_ref, pair_got, pair_sends, pair_recvs),
            (shared_out_ref, down_got, down_sends, down_recvs),
        ):
            copy = remote(
                source.at[others[k]], target.at[ring.me], "dp", others[k], out_sems, in_sems, ranks - k - 1
            )
            copy.start()
            handed.append(copy)
    kept = [
        pltpu.make_async_copy(shared_in_ref.at[ring.me], pair_got.at[ring.me], local_sem.at[0]),
        pltpu.make_async_copy(shared_out_ref.at[ring.me], down_got.at[ring.me], local_sem.at[1]),
    ]
    for copy in kept:
        copy.start()

    def cot_place(device, start, size):
        return cot_all.at[pl.ds(device * block + start, size)]

    cots = RingGather(
        ring, cot_place, block, c_sends, c_recvs, c_side_sends, c_side_recvs, 0, 0
    )
    cots.begin(cot_ref)
    kept_cot = pltpu.make_async_copy(cot_ref, cot_place(ring.me, 0, block), local_sem.at[2])
    kept_cot.start()

    low = gates.dtype
    experts, hid = layout.local_experts, layout.expert_hidden
    last = layout.hidden - layout.shared_at
    loads = []
    for j in range(experts):
        load = pltpu.make_async_copy(
            expert_down_ref.at[j], downs.at[pl.ds(j * layout.part, hid)], local_sem.at[4 + j]
        )
        load.start()
        loads.append(load)
        if layout.part > hid:
            downs[j * layout.part + hid : (j + 1) * layout.part, :] = jnp.zeros(
                (layout.part - hid, width), low
            )
    columns = [(gates, expert_gate_ref, j) for j in range(experts)]
    columns += [(ups, expert_up_ref, j) for j in range(experts)]

    def fetch(index):
        return pltpu.make_async_copy(
            columns[index][1].at[columns[index][2]], stage.at[index % 2], stage_sem.at[index % 2]
        )

    fetch(0).start()
    for index, (target, _, j) in enumerate(columns):
        fetch(index).wait()
        if index + 1 < len(columns):
            fetch(index + 1).start()

        def lay(spot, start, size, index=index, target=target, j=j):
            fill = jnp.zeros((size, layout.part - layout.part // 128 * 128 + 128), low)
            if layout.part > hid:
                target[spot, (j + 1) * layout.part - 128 : (j + 1) * layout.part] = fill[:, :128]
            target[spot, j * layout.part : j * layout.part + hid] = stage[index % 2, spot, :]

        strips(width, lay)
    for load in loads:
        load.wait()

    for copy in exchanged:
        copy.wait()
    first = here * rows

    def norm(spot, start, size):
        mine = pl.ds(pl.multiple_of(first + start, size), size)
        total = part_ref[mine, :].astype(jnp.float32)
        for k in range(peers - 1):
            total = total + got[k, spot, :].astype(jnp.float32)
        middle = tokens_ref[mine, :].astype(jnp.float32) + total
        middle_ref[spot, :] = middle
        inverse = lax.rsqrt(jnp.mean(middle * middle, axis=-1, keepdims=True) + EPSILON)
        own[spot, :] = ((middle * inverse) * gain_ref[...]).astype(own.dtype)

    strips(rows, norm)

    def place_of(k):
        def place(device, start, size):
            return x_all.at[pl.ds(device * block + away[k] * rows + start, size)]

        return place

    mine = place_of(0)(ring.me, 0, rows)
    forwards = []
    for k in order[1:]:
        copy = remote(own, mine, "tensor", away[k], x_sends, x_recvs, peers - k - 1)
        copy.start()
        forwards.append(copy)
    works = [
        RingGather(
            ring,
            place_of(k),
            rows,
            sends,
            recvs,
            side_sends,
            side_recvs,
            k * gather_slots(half),
            k * side_slots(half),
        )
        for k in range(peers)
    ]
    works[0].begin(own)
    store = pltpu.make_async_copy(own, mine, local_sem.at[3])
    store.start()

    for copy in kept:
        copy.wait()
    for copy in handed:
        copy.wait_recv()
    count, lane0 = layout.expert_count, layout.router_lane
    units = layout.shared_own
    for source in range(ranks):

        def lay_own(spot, start, size, source=source):
            there = pl.ds(pl.multiple_of(source * depth + start, size), size)
            pair = pair_got[source, spot, :].astype(jnp.float32)
            zero = jnp.zeros((size, last), low)
            gates[there, layout.shared_at :] = zero
            ups[there, layout.shared_at :] = zero
            gates[there, layout.shared_at : layout.router_at] = pair[:, :units].astype(low)
            ups[there, layout.shared_at : layout.router_at] = pair[:, units:].astype(low)
            lane = lax.broadcasted_iota(jnp.int32, (size, 128), 1)
            inside = (lane >= lane0) & (lane <= lane0 + count)
            tile = slice(layout.router_tile, layout.router_tile + 128)
            mixed = jnp.where(
                inside, small_ref[there, :].astype(jnp.float32), gates[there, tile].astype(jnp.float32)
            )
            gates[there, tile] = mixed.astype(low)

        strips(depth, lay_own)
        downs[layout.shared_at : layout.router_at, source * depth : (source + 1) * depth] = down_got[source]
    downs[layout.router_at :, :] = jnp.zeros((layout.hidden - layout.router_at, width), low)

    events, ready = [], 0

    def begin(k):
        spot = place_of(k)(ring.me, 0, rows)
        remote(own, spot, "tensor", away[k], x_sends, x_recvs, k - 1).wait_recv()
        works[k].begin(spot)

    for index in range(1, peers + half):
        if index < peers:
            events.append(functools.partial(begin, order[index]))
            ready = len(events)
        for number in range(1, half + 1):
            if 0 <= index - number < peers:
                events.append(functools.partial(works[order[index - number]].step, number))
        if index <= half:
            events.append(functools.partial(cots.step, index))
    for event in events[:ready]:
        event()
    late = events[ready:]
    cuts = [len(late) * part // 4 for part in range(5)]
    store.wait()
    kept_cot.wait()
    chip_rows = 2 * block
    first_expert = ring.me * experts

    def stores(spot):
        return [
            pltpu.make_async_copy(source, target.at[spot], store_sem.at[slot])
            for slot, (source, target) in enumerate(
                ((scaled, scaled_ref), (grads, grads_ref), (out, out_ref), (back, back_ref))
            )
        ]

    def chip_step(turn, carry):
        offset = (1 - 2 * (turn % 2)) * ((turn + 1) // 2)
        spot = pl.ds(pl.multiple_of(ring.chip(offset) * chip_rows, chip_rows), chip_rows)

        def run_late(part):
            @pl.when(turn == 0)
            def _():
                for event in late[cuts[part] : cuts[part + 1]]:
                    event()

        cots.wait_side(turn)
        load_cot = pltpu.make_async_copy(cot_all.at[spot], cot_block, block_sem.at[0])
        load_cot.start()
        for work in works:
            work.wait_side(turn)
        load_x = pltpu.make_async_copy(x_all.at[spot], x_block, block_sem.at[1])
        load_x.start()
        load_cot.wait()
        cot_tiles(layout, cot_block, downs, cot_hidden)
        load_x.wait()
        run_late(0)
        hidden_tiles(layout, x_block, gates, ups, pre_gate, pre_up)
        run_late(1)
        pending = stores(spot)

        @pl.when(turn > 0)
        def _():
            pending[0].wait()
            pending[1].wait()

        gate_strips(
            layout, first_expert, chosen_ref.at[spot], pre_gate, pre_up, cot_hidden, scaled, grads
        )
        pending[0].start()
        pending[1].start()
        run_late(2)

        @pl.when(turn > 0)
        def _():
            pending[2].wait()
            pending[3].wait()

        out_tiles(width, scaled, downs, out)
        pending[2].start()
        run_late(3)
        back_tiles(layout, width, grads, gates, ups, back)
        pending[3].start()
        return carry

    lax.fori_loop(0, ring.chips, chip_step, 0)
    for copy in stores(pl.ds(0, chip_rows)):
        copy.wait()
    for copy in forwards + handed:
        copy.wait_send()
    cots.sent()
    for work in works:
        work.sent()


def layer_forward_back(
    layout,
    part,
    tokens,
    gain,
    cot,
    chosen,
    small,
    expert_gate,
    expert_up,
    expert_down,
    shared_in,
    shared_out,
    ranks,
    peers,
    identity,
):
    half = ranks // 4
    block, width = part.shape
    rows = block // peers
    total = ranks * block
    depth = width // ranks
    hidden = layout.hidden
    chip = 2 * block
    low = part.dtype
    vmem = pl.BlockSpec(memory_space=pltpu.VMEM)
    hbm = pl.BlockSpec(memory_space=pl.ANY)
    dma = pltpu.SemaphoreType.DMA
    f32 = jnp.float32
    return pl.pallas_call(
        functools.partial(layer_kernel, layout, ranks, peers),
        out_shape=(
            jax.ShapeDtypeStruct((total, width), low),
            jax.ShapeDtypeStruct((total, width), low),
            jax.ShapeDtypeStruct((rows, width), f32),
            jax.ShapeDtypeStruct((total, hidden), low),
            jax.ShapeDtypeStruct((total, 2 * hidden), low),
            jax.ShapeDtypeStruct((total, width), low),
            jax.ShapeDtypeStruct((total, width), low),
        ),
        in_specs=[vmem] * 6 + [hbm] * 5,
        out_specs=(hbm, hbm, vmem, hbm, hbm, hbm, hbm),
        scratch_shapes=[
            pltpu.VMEM((width, hidden), low),
            pltpu.VMEM((width, hidden), low),
            pltpu.VMEM((hidden, width), low),
            pltpu.VMEM((2, width, layout.expert_hidden), low),
            pltpu.VMEM((ranks, depth, 2 * layout.shared_own), low),
            pltpu.VMEM((ranks, layout.shared_own, depth), low),
            pltpu.VMEM((rows, width), low),
            pltpu.VMEM((peers - 1, rows, width), low),
            pltpu.VMEM((chip, width), low),
            pltpu.VMEM((chip, width), low),
            pltpu.VMEM((chip, hidden), f32),
            pltpu.VMEM((chip, hidden), f32),
            pltpu.VMEM((chip, hidden), f32),
            pltpu.VMEM((chip, hidden), low),
            pltpu.VMEM((chip, 2 * hidden), low),
            pltpu.VMEM((chip, width), low),
            pltpu.VMEM((chip, width), low),
            dma((4 + layout.local_experts,)),
            dma((2,)),
            dma((2,)),
            dma((4,)),
            dma((ranks - 1,)),
            dma((ranks - 1,)),
            dma((ranks - 1,)),
            dma((ranks - 1,)),
            dma((peers - 1,)),
            dma((peers - 1,)),
            dma((peers - 1,)),
            dma((peers - 1,)),
            dma((peers * gather_slots(half),)),
            dma((peers * gather_slots(half),)),
            dma((peers * side_slots(half),)),
            dma((peers * side_slots(half),)),
            dma((gather_slots(half),)),
            dma((gather_slots(half),)),
            dma((side_slots(half),)),
            dma((side_slots(half),)),
        ],
        compiler_params=pltpu.CompilerParams(
            collective_id=identity, has_side_effects=True, vmem_limit_bytes=60 << 20
        ),
        name="layer_forward_back",
    )(part, tokens, gain, cot, chosen, small, expert_gate, expert_up, expert_down, shared_in, shared_out)


class RingReduce:
    def __init__(self, ring, part_at, rows, side, stage, got, sends, recvs, side_sends, side_recvs, base, side_base):
        self.ring, self.part_at, self.rows, self.cut = ring, part_at, rows, rows // 2
        self.side, self.stage, self.got = side, stage, got
        self.sends, self.recvs = sends, recvs
        self.side_sends, self.side_recvs = side_sends, side_recvs
        self.base, self.side_base = base, side_base
        self.started = []
        self.arrivals = {}

    def order(self):
        half = self.ring.half
        offsets = [half]
        for distance in range(half - 1, 0, -1):
            offsets += [distance, self.ring.chips - distance]
        return offsets + [0]

    def hand_over(self, offset):
        ring = self.ring
        copy = remote(
            self.part_at(ring.other(offset)),
            self.side.at[offset],
            "dp",
            ring.sibling,
            self.side_sends,
            self.side_recvs,
            self.side_base + offset,
        )
        copy.start()
        self.started.append(copy)
        self.arrivals[offset] = copy

    def hop(self, source, target, device, slot):
        copy = remote(source, target, "dp", device, self.sends, self.recvs, self.base + slot)
        copy.start()
        self.started.append(copy)
        return copy

    def add(self, offset, extra, first, size):
        mine = self.part_at(self.ring.device(offset))

        def whole(spot, start, count):
            total = mine[spot, :].astype(jnp.float32) + self.side[offset, spot, :].astype(jnp.float32)
            self.stage[offset, spot, :] = total.astype(self.stage.dtype)

        def more(spot, start, count):
            here = pl.ds(pl.multiple_of(first + start, count), count)
            total = mine[here, :].astype(jnp.float32) + self.side[offset, here, :].astype(jnp.float32)
            total = total + extra[here, :].astype(jnp.float32)
            self.stage[offset, here, :] = total.astype(self.stage.dtype)

        if extra is None:
            strips(self.rows, whole)
            return
        strips(size, more)
        if size < self.rows:
            rest = self.rows - size
            begin = 0 if first else size

            def plain(spot, start, count):
                here = pl.ds(pl.multiple_of(begin + start, count), count)
                total = mine[here, :].astype(jnp.float32) + self.side[offset, here, :].astype(jnp.float32)
                self.stage[offset, here, :] = total.astype(self.stage.dtype)

            strips(rest, plain)

    def step(self, number):
        ring, half, cut = self.ring, self.ring.half, self.cut
        if number == 0:
            self.arrivals[half].wait_recv()
            self.add(half, None, 0, self.rows)
            self.last = []
            for which, device in enumerate((ring.ahead, ring.behind)):
                part = pl.ds((0, cut)[which], cut)
                self.last.append(
                    self.hop(
                        self.stage.at[half, part], self.got.at[which * half, part], device, which * half
                    )
                )
            return
        following = []
        for which, device in enumerate((ring.ahead, ring.behind)):
            distance = half - number
            offset = distance if which == 0 else ring.chips - distance
            self.arrivals[offset].wait_recv()
            self.last[which].wait_recv()
            extra = self.got.at[which * half + number - 1]
            if number == 1:
                self.add(offset, extra, (0, cut)[which], cut)
            else:
                self.add(offset, extra, 0, self.rows)
            following.append(
                self.hop(
                    self.stage.at[offset],
                    self.got.at[which * half + number],
                    device,
                    which * half + number,
                )
            )
        self.last = following

    def total(self, emit):
        half = self.ring.half
        self.arrivals[0].wait_recv()
        for copy in self.last:
            copy.wait_recv()
        mine = self.part_at(self.ring.me)

        def body(spot, start, size):
            value = mine[spot, :].astype(jnp.float32) + self.side[0, spot, :].astype(jnp.float32)
            value = value + self.got[half - 1, spot, :].astype(jnp.float32)
            value = value + self.got[2 * half - 1, spot, :].astype(jnp.float32)
            emit(spot, start, size, value)

        strips(self.rows, body)

    def finish(self):
        for copy in self.started:
            copy.wait_send()


def back_kernel(
    ranks,
    peers,
    part_ref,
    middle_ref,
    cot_ref,
    gain_ref,
    out_ref,
    grad_ref,
    gain_grad_ref,
    side,
    stage,
    got,
    z_stage,
    z_got,
    low_ref,
    sends,
    recvs,
    side_sends,
    side_recvs,
    z_sends,
    z_recvs,
    x_sends,
    x_recvs,
    local_sem,
):
    ring = Ring(ranks)
    here = lax.axis_index("tensor")
    block = cot_ref.shape[0]
    rows = block // peers
    half, chips = ring.half, ring.chips
    away = [(here + k) % peers for k in range(peers)]
    greet(ring.partners() + [{"tensor": away[k]} for k in range(1, peers)])
    order = list(reversed(near_first(peers)))
    works = {}
    for k in order:

        def part_at(device, k=k):
            return part_ref.at[pl.ds(device * block + away[k] * rows, rows)]

        works[k] = RingReduce(
            ring,
            part_at,
            rows,
            side.at[k],
            stage.at[k],
            got.at[k],
            sends,
            recvs,
            side_sends,
            side_recvs,
            k * 2 * half,
            k * chips,
        )
    for offset in works[order[0]].order():
        for k in order:
            works[k].hand_over(offset)
    reduced = []
    for index in range(len(order) + half):
        for number in range(0, half):
            if 0 <= index - number < len(order):
                works[order[index - number]].step(number)
        if 0 <= index - half < len(order):
            k = order[index - half]

            def emit(spot, start, size, value, k=k):
                z_stage[k, spot, :] = value.astype(z_stage.dtype)

            if k:
                works[k].total(emit)
                copy = remote(
                    z_stage.at[k], z_got.at[peers - k - 1], "tensor", away[k], z_sends, z_recvs, peers - k - 1
                )
                copy.start()
                reduced.append(copy)
    for copy in reduced:
        copy.wait_recv()
    first = here * rows
    gain_grad_ref[...] = jnp.zeros_like(gain_grad_ref)

    def norm(spot, start, size, value):
        for k in range(peers - 1):
            value = value + z_got[k, spot, :].astype(jnp.float32)
        middle = middle_ref[spot, :]
        inverse = lax.rsqrt(jnp.mean(middle * middle, axis=-1, keepdims=True) + EPSILON)
        normed = middle * inverse
        scaled = value * gain_ref[...]
        back = inverse * (scaled - normed * jnp.mean(scaled * normed, axis=-1, keepdims=True))
        mine = pl.ds(pl.multiple_of(first + start, size), size)
        grad = cot_ref[mine, :].astype(jnp.float32) + back
        grad_ref[spot, :] = grad
        low_ref[spot, :] = grad.astype(low_ref.dtype)
        gain_grad_ref[...] += jnp.sum(value * normed, axis=0, keepdims=True)

    works[0].total(norm)
    mine = out_ref.at[pl.ds(here * rows, rows)]
    spread = []
    for k in near_first(peers)[:0:-1]:
        copy = remote(low_ref, mine, "tensor", away[k], x_sends, x_recvs, peers - k - 1)
        copy.start()
        spread.append(copy)
    store = pltpu.make_async_copy(low_ref, mine, local_sem)
    store.start()
    store.wait()
    for copy in reduced:
        copy.wait_send()
    for copy in spread:
        copy.wait()
    for k in order:
        works[k].finish()


def reduce_and_norm(part, middle, cotangent, gain, ranks, peers, identity):
    half = ranks // 4
    chips = ranks // 2
    block, width = cotangent.shape
    rows = block // peers
    vmem = pl.BlockSpec(memory_space=pltpu.VMEM)
    low = part.dtype
    return pl.pallas_call(
        functools.partial(back_kernel, ranks, peers),
        out_shape=(
            jax.ShapeDtypeStruct((block, width), low),
            jax.ShapeDtypeStruct((rows, width), jnp.float32),
            jax.ShapeDtypeStruct((1, width), jnp.float32),
        ),
        in_specs=[vmem] * 4,
        out_specs=(pl.BlockSpec(memory_space=pl.ANY), vmem, vmem),
        scratch_shapes=[
            pltpu.VMEM((peers, chips, rows, width), low),
            pltpu.VMEM((peers, chips, rows, width), low),
            pltpu.VMEM((peers, 2 * half, rows, width), low),
            pltpu.VMEM((peers, rows, width), low),
            pltpu.VMEM((peers - 1, rows, width), low),
            pltpu.VMEM((rows, width), low),
            pltpu.SemaphoreType.DMA((peers * 2 * half,)),
            pltpu.SemaphoreType.DMA((peers * 2 * half,)),
            pltpu.SemaphoreType.DMA((peers * chips,)),
            pltpu.SemaphoreType.DMA((peers * chips,)),
            pltpu.SemaphoreType.DMA((peers - 1,)),
            pltpu.SemaphoreType.DMA((peers - 1,)),
            pltpu.SemaphoreType.DMA((peers - 1,)),
            pltpu.SemaphoreType.DMA((peers - 1,)),
            pltpu.SemaphoreType.DMA,
        ],
        compiler_params=pltpu.CompilerParams(
            collective_id=identity, has_side_effects=True, vmem_limit_bytes=50 << 20
        ),
        name="reduce_and_norm",
    )(part, middle, cotangent, gain)


def final_kernel(
    ranks,
    peers,
    part_ref,
    tokens_ref,
    gain_ref,
    grad_ref,
    gain_grad_ref,
    weights_ref,
    out_ref,
    sum_ref,
    small_ref,
    gains_ref,
    side,
    stage,
    got,
    z_got,
    low_ref,
    small_own,
    small_got,
    gains_own,
    gains_got,
    gains_part,
    gains_z,
    sends,
    recvs,
    side_sends,
    side_recvs,
    z_sends,
    z_recvs,
    x_sends,
    x_recvs,
    s_sends,
    s_recvs,
    g_sends,
    g_recvs,
    h_sends,
    h_recvs,
    local_sem,
):
    ring = Ring(ranks)
    here = lax.axis_index("tensor")
    block, width = part_ref.shape
    rows = block // peers
    half, chips = ring.half, ring.chips
    lot = weights_ref.shape[0] // ranks
    pieces = side.shape[0]
    size = lot // pieces
    wide = sum_ref.shape[1]
    columns = width // ranks
    away = [(here + k) % peers for k in range(peers)]
    others = [(ring.me + k) % ranks for k in range(ranks)]
    greet(
        [{"dp": others[k]} for k in range(1, ranks)] + [{"tensor": away[k]} for k in range(1, peers)]
    )
    far_first = near_first(peers)[:0:-1]
    exchanged = []
    for k in far_first:
        copy = remote(
            part_ref.at[pl.ds(away[k] * rows, rows)],
            z_got.at[peers - k - 1],
            "tensor",
            away[k],
            z_sends,
            z_recvs,
            peers - k - 1,
        )
        copy.start()
        exchanged.append(copy)
    works = []
    for piece in range(pieces):

        def part_at(device, piece=piece):
            return weights_ref.at[pl.ds(device * lot + piece * size, size)]

        works.append(
            RingReduce(
                ring,
                part_at,
                size,
                side.at[piece],
                stage.at[piece],
                got.at[piece],
                sends,
                recvs,
                side_sends,
                side_recvs,
                piece * 2 * half,
                piece * chips,
            )
        )
    for offset in works[0].order():
        for work in works:
            work.hand_over(offset)

    first = here * rows
    gains_own[...] = jnp.zeros_like(gains_own)
    gains_own[1:2, :] = gain_grad_ref[...]

    def norm(spot, start, count):
        mine = pl.ds(pl.multiple_of(first + start, count), count)
        value = part_ref[mine, :].astype(jnp.float32)
        for k in range(peers - 1):
            value = value + z_got[k, spot, :].astype(jnp.float32)
        inputs = tokens_ref[mine, :].astype(jnp.float32)
        inverse = lax.rsqrt(jnp.mean(inputs * inputs, axis=-1, keepdims=True) + EPSILON)
        normed = inputs * inverse
        scaled = value * gain_ref[...]
        back = inverse * (scaled - normed * jnp.mean(scaled * normed, axis=-1, keepdims=True))
        low_ref[spot, :] = (grad_ref[spot, :] + back).astype(low_ref.dtype)
        gains_own[0:1, :] += jnp.sum(value * normed, axis=0, keepdims=True)

    spread, handed = [], []
    mine = out_ref.at[pl.ds(here * rows, rows)]
    store = pltpu.make_async_copy(low_ref, mine, local_sem)

    def after_norm():
        for copy in exchanged:
            copy.wait()
        strips(rows, norm)
        for k in range(1, ranks):
            copy = remote(
                gains_own.at[:, pl.ds(pl.multiple_of(others[k] * columns, columns), columns)],
                gains_got.at[ranks - k - 1],
                "dp",
                others[k],
                g_sends,
                g_recvs,
                ranks - k - 1,
            )
            copy.start()
            handed.append(copy)
        for k in far_first:
            copy = remote(low_ref, mine, "tensor", away[k], x_sends, x_recvs, peers - k - 1)
            copy.start()
            spread.append(copy)
        store.start()

    for index in range(pieces + half):
        if index == half:
            after_norm()
        for number in range(0, half):
            if 0 <= index - number < pieces:
                works[index - number].step(number)
        if 0 <= index - half < pieces:
            piece = index - half

            def emit(spot, start, count, value, piece=piece):
                place = pl.ds(pl.multiple_of(piece * size + start, count), count)
                sum_ref[place, :] = value[:, :wide]
                small_own[place, :] = value[:, wide:]

            works[piece].total(emit)
    for copy in handed:
        copy.wait_recv()
    gains = gains_own[:, pl.ds(pl.multiple_of(ring.me * columns, columns), columns)]
    for k in range(ranks - 1):
        gains = gains + gains_got[k]
    gains_part[...] = gains
    last = []
    for k in far_first:
        for source, target, out_sems, in_sems in (
            (gains_part, gains_z, h_sends, h_recvs),
            (small_own, small_got, s_sends, s_recvs),
        ):
            copy = remote(
                source, target.at[peers - k - 1], "tensor", away[k], out_sems, in_sems, peers - k - 1
            )
            copy.start()
            last.append(copy)
    store.wait()
    for copy in handed:
        copy.wait_send()
    for copy in spread + last:
        copy.wait()
    gains = gains_part[...]
    small = small_own[...]
    for k in range(peers - 1):
        gains = gains + gains_z[k]
        small = small + small_got[k]
    gains_ref[...] = gains
    small_ref[...] = small
    for work in works:
        work.finish()


def finish_grads(part, tokens, gain, grad, gain_grad, weights, ranks, peers, identity):
    half = ranks // 4
    chips = ranks // 2
    block, width = part.shape
    rows = block // peers
    lot = weights.shape[0] // ranks
    total = weights.shape[1]
    tail = 128
    pieces = 4
    size = lot // pieces
    columns = width // ranks
    vmem = pl.BlockSpec(memory_space=pltpu.VMEM)
    low = part.dtype
    dma = pltpu.SemaphoreType.DMA
    return pl.pallas_call(
        functools.partial(final_kernel, ranks, peers),
        out_shape=(
            jax.ShapeDtypeStruct((block, width), low),
            jax.ShapeDtypeStruct((lot, total - tail), jnp.float32),
            jax.ShapeDtypeStruct((lot, tail), jnp.float32),
            jax.ShapeDtypeStruct((8, columns), jnp.float32),
        ),
        in_specs=[vmem] * 6,
        out_specs=(pl.BlockSpec(memory_space=pl.ANY), vmem, vmem, vmem),
        scratch_shapes=[
            pltpu.VMEM((pieces, chips, size, total), low),
            pltpu.VMEM((pieces, chips, size, total), low),
            pltpu.VMEM((pieces, 2 * half, size, total), low),
            pltpu.VMEM((peers - 1, rows, width), low),
            pltpu.VMEM((rows, width), low),
            pltpu.VMEM((lot, tail), jnp.float32),
            pltpu.VMEM((peers - 1, lot, tail), jnp.float32),
            pltpu.VMEM((8, width), jnp.float32),
            pltpu.VMEM((ranks - 1, 8, columns), jnp.float32),
            pltpu.VMEM((8, columns), jnp.float32),
            pltpu.VMEM((peers - 1, 8, columns), jnp.float32),
            dma((pieces * 2 * half,)),
            dma((pieces * 2 * half,)),
            dma((pieces * chips,)),
            dma((pieces * chips,)),
            dma((peers - 1,)),
            dma((peers - 1,)),
            dma((peers - 1,)),
            dma((peers - 1,)),
            dma((peers - 1,)),
            dma((peers - 1,)),
            dma((ranks - 1,)),
            dma((ranks - 1,)),
            dma((peers - 1,)),
            dma((peers - 1,)),
            dma,
        ],
        compiler_params=pltpu.CompilerParams(
            collective_id=identity, has_side_effects=True, vmem_limit_bytes=50 << 20
        ),
        name="finish_grads",
    )(part, tokens, gain, grad, gain_grad, weights)


def dot_rows(left, right):
    return lax.dot_general(
        left, right, (((0,), (0,)), ((), ())), preferred_element_type=jnp.float32
    )


def dot_last(left, right):
    return lax.dot_general(
        left, right, (((1,), (1,)), ((), ())), preferred_element_type=jnp.float32
    )


def forward_rms_norm(values, gain):
    inverse = lax.rsqrt(jnp.mean(values * values, axis=-1, keepdims=True) + EPSILON)
    normed = values * inverse
    return (normed * gain, normed, inverse)


def rope_tables():
    half_dim = HEAD_DIM // 2
    exponent = jnp.arange(half_dim, dtype=jnp.float32) * (2.0 / HEAD_DIM)
    inverse_freq = jnp.exp(-exponent * jnp.log(jnp.float32(1000000.0)))
    angles = jnp.arange(SEQ, dtype=jnp.float32)[:, None] * inverse_freq[None, :]
    return (jnp.cos(angles), jnp.sin(angles))


def rotate(values, cosine, sine, sign):
    half_dim = values.shape[-1] // 2
    first = values[..., :half_dim]
    second = values[..., half_dim:]
    cos_table = cosine[:, None, :]
    sin_table = sine[:, None, :] * sign
    return jnp.concatenate(
        [first * cos_table - second * sin_table, second * cos_table + first * sin_table], axis=-1
    )


def masked_scores(queries, key_rows, segment_row):
    raw = jnp.einsum(
        "qhd,khd->hqk", queries, key_rows, preferred_element_type=jnp.float32
    ) * HEAD_DIM ** (-0.5)
    spots = jnp.arange(segment_row.shape[0], dtype=jnp.int32)
    allowed = (spots[None, :] <= spots[:, None]) & (segment_row[None, :] == segment_row[:, None])
    return jnp.where(allowed[None], raw, -1e30)


def attend_forward(inputs):
    queries, key_rows, value_rows, segment_row = inputs
    scores = masked_scores(queries, key_rows, segment_row)
    exponent = jnp.exp(scores)
    totals = jnp.sum(exponent, axis=-1, keepdims=True)
    probs = (exponent / totals).astype(jnp.bfloat16)
    context = jnp.einsum(
        "hqk,khd->qhd", probs, value_rows, preferred_element_type=jnp.float32
    ).astype(jnp.bfloat16)
    return (context, jnp.log(totals[..., 0]))


def attend_backward(inputs):
    queries, key_rows, value_rows, segment_row, log_total, grad_context = inputs
    scores = masked_scores(queries, key_rows, segment_row)
    probs = jnp.exp(scores - log_total[..., None])
    probs_low = probs.astype(jnp.bfloat16)
    grad_probs = jnp.einsum(
        "qhd,khd->hqk", grad_context, value_rows, preferred_element_type=jnp.float32
    )
    inner = jnp.sum(probs * grad_probs, axis=-1, keepdims=True)
    grad_scores = (probs * (grad_probs - inner)).astype(jnp.bfloat16)
    grad_queries = jnp.einsum(
        "hqk,khd->qhd", grad_scores, key_rows, preferred_element_type=jnp.float32
    ) * HEAD_DIM ** (-0.5)
    grad_keys = jnp.einsum(
        "hqk,qhd->khd", grad_scores, queries, preferred_element_type=jnp.float32
    ) * HEAD_DIM ** (-0.5)
    grad_values = jnp.einsum(
        "hqk,qhd->khd", probs_low, grad_context, preferred_element_type=jnp.float32
    )
    return (grad_queries, grad_keys, grad_values)


def pad_columns(parts, width):
    rows = parts[0].shape[0]
    used = sum(part.shape[1] for part in parts)
    if used < width:
        parts = list(parts) + [jnp.zeros((rows, width - used), parts[0].dtype)]
    return jnp.concatenate(parts, axis=1)


def scatter_rows(values):
    return lax.psum_scatter(values, "dp", scatter_dimension=0, tiled=True)


def spread_columns(values, ranks):
    rows, columns = values.shape
    blocks = values.reshape(rows, ranks, columns // ranks).transpose(1, 0, 2)
    return blocks


def shards(
    tokens,
    w_query,
    w_key,
    w_value,
    w_out,
    gain_attn,
    gain_ffn,
    w_router,
    shared_gate,
    shared_up,
    shared_down,
    shared_switch,
    expert_gate,
    expert_up_weight,
    expert_down,
    routes,
    segments,
    cotangent,
):
    low = jnp.bfloat16
    ranks = lax.axis_size("dp")
    peers = lax.axis_size("tensor")
    me = lax.axis_index("dp")
    token_count, width = tokens.shape
    local_experts, _, expert_hidden = expert_gate.shape
    expert_count = local_experts * ranks
    block = width // ranks
    head_width = w_query.shape[1]
    head_count = head_width // HEAD_DIM
    row_count = token_count // SEQ
    shared_width = shared_gate.shape[1]
    shared_own = shared_width // ranks
    small_pad = 128
    layout = Layout(local_experts, expert_hidden, shared_own, expert_count)
    part_pad, shared_at, router_at = layout.part, layout.shared_at, layout.router_at
    hidden_pad, lane0 = layout.hidden, layout.router_lane
    shape_four = (row_count, SEQ, head_count, HEAD_DIM)

    rest = jnp.zeros((block, small_pad - 2 - lane0 - expert_count - 1), low)
    small = jnp.concatenate(
        [
            jnp.zeros((block, lane0), low),
            w_router,
            shared_switch[:, None],
            rest,
            gain_attn[:, None],
            gain_ffn[:, None],
        ],
        axis=1,
    )
    spots = jnp.arange(small_pad, dtype=jnp.int32)[None, None, :] - lane0
    chosen = jnp.sum((routes[:, :, None] == spots).astype(jnp.float32), axis=1).astype(low)
    fold = token_count // block
    chosen = chosen.reshape(fold, block, small_pad).transpose(1, 0, 2).reshape(block, fold * small_pad)
    gathered = gather_dp([w_query, w_key, w_value, small, w_out.T, chosen], ranks, 0)
    qkv_full = gathered[:, : 3 * head_width]
    small_full = gathered[:, 3 * head_width : 3 * head_width + small_pad]
    out_rows = gathered[:, 3 * head_width + small_pad : 3 * head_width + small_pad + head_width]
    chosen_all = gathered[:, 3 * head_width + small_pad + head_width :]
    chosen_all = chosen_all.reshape(ranks, block, fold, small_pad).transpose(0, 2, 1, 3)
    chosen_all = chosen_all.reshape(ranks * token_count, small_pad)
    attn_gain = small_full[:, small_pad - 2].astype(jnp.float32)
    ffn_gain = small_full[:, small_pad - 1].astype(jnp.float32)

    shared_in = jnp.concatenate(
        [spread_columns(shared_gate, ranks), spread_columns(shared_up, ranks)], axis=2
    )
    shared_out = shared_down.reshape(ranks, shared_own, block)

    cosine, sine = rope_tables()
    inputs = tokens.astype(jnp.float32)
    attn_pre, _, _ = forward_rms_norm(inputs, attn_gain)
    attn_in = attn_pre.astype(low)
    qkv = jnp.dot(attn_in, qkv_full, preferred_element_type=jnp.float32)
    queries = rotate(qkv[:, :head_width].reshape(shape_four), cosine, sine, 1.0).astype(low)
    key_rows = rotate(
        qkv[:, head_width : 2 * head_width].reshape(shape_four), cosine, sine, 1.0
    ).astype(low)
    value_rows = qkv[:, 2 * head_width :].astype(low).reshape(shape_four)
    contexts, log_totals = jax.vmap(attend_forward)((queries, key_rows, value_rows, segments))
    context_flat = contexts.reshape(token_count, head_width)
    attn_part = dot_last(context_flat, out_rows)
    x_all, cot_all, middle, scaled_hidden, grads_wide, out_part, back_part = layer_forward_back(
        layout,
        attn_part.astype(low),
        tokens,
        ffn_gain[None, :],
        cotangent,
        chosen_all,
        small_full,
        expert_gate,
        expert_up_weight,
        expert_down,
        shared_in,
        shared_out,
        ranks,
        peers,
        1,
    )
    grad_attn_out, grad_middle, grad_gain_ffn = reduce_and_norm(
        back_part, middle, cotangent, ffn_gain[None, :], ranks, peers, 2
    )

    out_part, grad_attn_out = lax.optimization_barrier((out_part, grad_attn_out))
    moe = lax.psum_scatter(scatter_rows(out_part), "tensor", scatter_dimension=0, tiled=True)
    output = (middle + moe.astype(jnp.float32)).astype(low)
    output = lax.all_gather(output, "tensor", axis=0, tiled=True)

    grad_wide = dot_rows(x_all, grads_wide)
    grad_downs = dot_rows(scaled_hidden, cot_all)
    grad_expert_gate = jnp.stack(
        [grad_wide[:, j * part_pad : j * part_pad + expert_hidden] for j in range(local_experts)]
    )
    grad_expert_up = jnp.stack(
        [
            grad_wide[:, hidden_pad + j * part_pad : hidden_pad + j * part_pad + expert_hidden]
            for j in range(local_experts)
        ]
    )
    grad_expert_down = jnp.stack(
        [grad_downs[j * part_pad : j * part_pad + expert_hidden] for j in range(local_experts)]
    )
    grad_shared = jnp.concatenate(
        [
            grad_wide[:, shared_at : shared_at + shared_own].astype(low),
            grad_wide[:, hidden_pad + shared_at : hidden_pad + shared_at + shared_own].astype(low),
            grad_downs[shared_at : shared_at + shared_own].astype(low).T,
        ],
        axis=1,
    ).reshape(ranks, block, 3 * shared_own)
    grad_shared = lax.all_to_all(grad_shared, "dp", split_axis=0, concat_axis=0, tiled=True)

    def whole_columns(part):
        return part.transpose(1, 0, 2).reshape(block, shared_width)

    grad_shared_gate = whole_columns(grad_shared[:, :, :shared_own]).astype(jnp.float32)
    grad_shared_up = whole_columns(grad_shared[:, :, shared_own : 2 * shared_own]).astype(jnp.float32)
    grad_shared_down = whole_columns(grad_shared[:, :, 2 * shared_own :]).T.astype(jnp.float32)

    grad_out_rows = dot_rows(grad_attn_out, context_flat)
    grad_context = jnp.dot(grad_attn_out, out_rows, preferred_element_type=jnp.float32)
    grad_context = grad_context.astype(low).reshape(shape_four)
    grad_queries, grad_keys, grad_values = jax.vmap(attend_backward)(
        (queries, key_rows, value_rows, segments, log_totals, grad_context)
    )
    flat_shape = (token_count, head_width)
    grad_qkv_rows = jnp.concatenate(
        [
            rotate(grad_queries, cosine, sine, -1.0).reshape(flat_shape).astype(low),
            rotate(grad_keys, cosine, sine, -1.0).reshape(flat_shape).astype(low),
            grad_values.reshape(flat_shape).astype(low),
        ],
        axis=1,
    )
    grad_qkv = dot_rows(attn_in, grad_qkv_rows)
    attn_back_part = dot_last(grad_qkv_rows, qkv_full)
    grad_weights = jnp.concatenate(
        [grad_qkv.astype(low), grad_out_rows.astype(low), pad_columns([grad_wide[:, router_at : router_at + expert_count + 1].astype(low)], small_pad)],
        axis=1,
    )
    grad_input, grad_four, grad_tail, grad_gains = finish_grads(
        attn_back_part.astype(low),
        tokens,
        attn_gain[None, :],
        grad_middle,
        grad_gain_ffn,
        grad_weights,
        ranks,
        peers,
        3,
    )
    grad_input = grad_input.astype(jnp.float32)
    grad_query = grad_four[:, :head_width]
    grad_key = grad_four[:, head_width : 2 * head_width]
    grad_value = grad_four[:, 2 * head_width : 3 * head_width]
    grad_out_proj = grad_four[:, 3 * head_width :].T
    return (
        output,
        grad_input,
        grad_query,
        grad_key,
        grad_value,
        grad_out_proj,
        grad_gains[0],
        grad_gains[1],
        grad_tail[:, :expert_count],
        grad_shared_gate,
        grad_shared_up,
        grad_shared_down,
        grad_tail[:, expert_count],
        grad_expert_gate,
        grad_expert_up,
        grad_expert_down,
    )


def solution(mesh):
    in_specs = (
        P("dp", None),
        P("dp", "tensor"),
        P("dp", "tensor"),
        P("dp", "tensor"),
        P("tensor", "dp"),
        P("dp"),
        P("dp"),
        P("dp", None),
        P("dp", "tensor"),
        P("dp", "tensor"),
        P("tensor", "dp"),
        P("dp"),
        P("dp", None, "tensor"),
        P("dp", None, "tensor"),
        P("dp", "tensor", None),
        P("dp", None),
        P("dp", None),
        P("dp", None),
    )
    out_specs = (
        P("dp", None),
        P("dp", None),
        P("dp", "tensor"),
        P("dp", "tensor"),
        P("dp", "tensor"),
        P("tensor", "dp"),
        P("dp"),
        P("dp"),
        P("dp", None),
        P("dp", "tensor"),
        P("dp", "tensor"),
        P("tensor", "dp"),
        P("dp"),
        P("dp", None, "tensor"),
        P("dp", None, "tensor"),
        P("dp", "tensor", None),
    )
    return jax.shard_map(shards, mesh=mesh, in_specs=in_specs, out_specs=out_specs, check_vma=False)
```

```python
import functools

import jax
import jax.numpy as jnp
import numpy as np
from jax import lax
from jax.experimental import pallas as pl
from jax.experimental.pallas import tpu as pltpu
from jax.sharding import PartitionSpec as P

HEAD_DIM = 128
TOP = 4
SEQ = 256


EPSILON = 1e-06
MESH = pl.DeviceIdType.MESH


def ring_chip(position, chips):
    half = chips // 2
    upper = position // half
    return position + upper * (chips - 1 + half - 2 * position)


def ring_spot(chip, chips):
    return ring_chip(chip, chips)


def greet(partners):
    barrier = pltpu.get_barrier_semaphore()
    for partner in partners:
        pl.semaphore_signal(barrier, inc=1, device_id=partner, device_id_type=MESH)
    pl.semaphore_wait(barrier, len(partners))


def remote(source, target, axis, device, sends, recvs, slot):
    return pltpu.make_async_remote_copy(
        src_ref=source,
        dst_ref=target,
        send_sem=sends.at[slot],
        recv_sem=recvs.at[slot],
        device_id={axis: device},
        device_id_type=MESH,
    )


class Ring:
    def __init__(self, ranks):
        self.ranks = ranks
        self.chips = ranks // 2
        self.half = self.chips // 2
        self.me = lax.axis_index("dp")
        self.core = self.me % 2
        self.position = ring_spot(self.me // 2, self.chips)
        self.sibling = self.me + 1 - 2 * self.core
        self.ahead = self.device(1)
        self.behind = self.device(-1)

    def chip(self, offset):
        return ring_chip((self.position + offset + self.chips) % self.chips, self.chips)

    def device(self, offset):
        return self.chip(offset) * 2 + self.core

    def other(self, offset):
        return self.chip(offset) * 2 + 1 - self.core

    def partners(self):
        return [{"dp": self.ahead}, {"dp": self.behind}, {"dp": self.sibling}]


def gather_slots(half):
    return 2 * half


def side_slots(half):
    return 2 * half


class RingGather:
    def __init__(self, ring, place, rows, sends, recvs, side_sends, side_recvs, base, side_base):
        self.ring, self.place, self.rows, self.cut = ring, place, rows, rows // 2
        self.sends, self.recvs = sends, recvs
        self.side_sends, self.side_recvs = side_sends, side_recvs
        self.base, self.side_base = base, side_base
        self.hops, self.sides = {}, 0

    def hop_copy(self, source, target, device, slot):
        return remote(source, target, "dp", device, self.sends, self.recvs, self.base + slot)

    def side_copy(self, source, target, slot):
        return remote(
            source,
            target,
            "dp",
            self.ring.sibling,
            self.side_sends,
            self.side_recvs,
            self.side_base + slot,
        )

    def hop(self, source, target, device, slot, size):
        self.hop_copy(source, target, device, slot).start()
        self.hops[slot] = size

    def share(self, source, target):
        self.side_copy(source, target, self.sides).start()
        self.sides += 1

    def begin(self, source):
        ring = self.ring
        target = self.place(ring.me, 0, self.rows)
        self.hop(source, target, ring.ahead, 0, self.rows)
        self.hop(source, target, ring.behind, ring.half, self.rows)
        self.share(source, target)

    def wait_hop(self, slot):
        block = self.place(self.ring.me, 0, self.hops[slot])
        self.hop_copy(block, block, self.ring.ahead, slot).wait_recv()

    def step(self, number):
        ring = self.ring
        for which, sign in enumerate((-1, 1)):
            owner = ring.device(sign * number)
            onward = (ring.ahead, ring.behind)[which]
            self.wait_hop(which * ring.half + number - 1)
            if number < ring.half:
                block = self.place(owner, 0, self.rows)
                size = self.rows
                part = block
                if number == ring.half - 1:
                    size = self.cut
                    part = self.place(owner, (0, self.cut)[which], size)
                self.hop(part, part, onward, which * ring.half + number, size)
                self.share(block, block)
        if number == ring.half:
            block = self.place(ring.device(number), 0, self.rows)
            self.share(block, block)

    def wait_side(self, index):
        block = self.place(self.ring.me, 0, self.rows)
        self.side_copy(block, block, index).wait_recv()

    def sent(self):
        for slot, size in self.hops.items():
            block = self.place(self.ring.me, 0, size)
            self.hop_copy(block, block, self.ring.ahead, slot).wait_send()
        for index in range(self.sides):
            block = self.place(self.ring.me, 0, self.rows)
            self.side_copy(block, block, index).wait_send()

    def finish(self):
        self.sent()
        for index in range(self.sides):
            self.wait_side(index)


def near_first(peers):
    order = [0]
    for step in range(1, peers // 2 + 1):
        order.append(step)
        if peers - step != step:
            order.append(peers - step)
    return order


STRIP = 64
OUT_FIRST, OUT_NEXT, NORM_DUE = 10, 13, 15


def strips(rows, body):
    strip = min(STRIP, rows)

    def step(index, carry):
        body(pl.ds(pl.multiple_of(index * strip, strip), strip), index * strip, strip)
        return carry

    lax.fori_loop(0, rows // strip, step, 0)


def matmul(left, right):
    return lax.dot_general(
        left, right, (((1,), (0,)), ((), ())), preferred_element_type=jnp.float32
    )


def matmul_last(left, right):
    return lax.dot_general(
        left, right, (((1,), (1,)), ((), ())), preferred_element_type=jnp.float32
    )


def tiles(width, tile, body):
    def step(index, carry):
        body(pl.ds(pl.multiple_of(index * tile, tile), tile))
        return carry

    lax.fori_loop(0, width // tile, step, 0)


class Layout:
    def __init__(self, local_experts, expert_hidden, shared_own, expert_count):
        self.local_experts = local_experts
        self.expert_hidden = expert_hidden
        self.shared_own = shared_own
        self.expert_count = expert_count
        self.part = -(-expert_hidden // 128) * 128
        self.shared_at = local_experts * self.part
        self.router_at = self.shared_at + shared_own
        self.last = -(-(shared_own + expert_count + 1) // 128) * 128
        self.hidden = self.shared_at + self.last
        self.router_tile = self.router_at // 128 * 128
        self.router_lane = self.router_at - self.router_tile
        self.tile = 256 if self.hidden % 256 == 0 else 128


def hidden_tiles(layout, x_ref, gates, ups, pre_gate, pre_up):
    def body(spot):
        pre_gate[:, spot] = matmul_last(x_ref[...], gates[spot, :])
        pre_up[:, spot] = matmul_last(x_ref[...], ups[spot, :])

    tiles(layout.hidden, layout.tile, body)


def cot_tiles(layout, cot_ref, downs, cot_hidden):
    def body(spot):
        cot_hidden[:, spot] = matmul_last(cot_ref[...], downs[spot, :])

    tiles(layout.hidden, layout.tile, body)


def gate_strips(layout, first_expert, chosen, pre_gate, pre_up, cot_hidden, scaled, grads):
    rows = pre_gate.shape[0]
    count, lane0 = layout.expert_count, layout.router_lane
    router = slice(layout.router_tile, layout.router_tile + 128)
    bounds = [(j * layout.part, (j + 1) * layout.part) for j in range(layout.local_experts)]
    bounds.append((layout.shared_at, layout.hidden))
    low = scaled.dtype

    def body(spot, start, size):
        lane = lax.broadcasted_iota(jnp.int32, (size, 128), 1)
        logits = pre_gate[spot, router]
        is_router = (lane >= lane0) & (lane < lane0 + count)
        is_switch = lane == lane0 + count
        power = jnp.where(is_router, jnp.exp(jnp.where(is_router, logits, 0.0)), 0.0)
        probs = power / jnp.sum(power, axis=-1, keepdims=True)
        raw = jnp.sum(jnp.where(is_switch, logits, 0.0), axis=-1, keepdims=True)
        switch = 1.0 / (1.0 + jnp.exp(-raw))
        mask = chosen[spot, :].astype(jnp.float32)
        scales = []
        for j in range(layout.local_experts):
            spotted = lane == lane0 + first_expert + j
            scales.append(jnp.sum(jnp.where(spotted, probs * mask, 0.0), axis=-1, keepdims=True))
        scales.append(switch)
        totals = []
        for (begin, end), scale in zip(bounds, scales):
            shared = begin == layout.shared_at
            columns = slice(begin, end)
            gate, up = pre_gate[spot, columns], pre_up[spot, columns]
            through = cot_hidden[spot, columns].astype(jnp.float32)
            sig = 1.0 / (1.0 + jnp.exp(-gate))
            act = gate * sig
            state = act * up
            grad = scale * through
            totals.append(jnp.sum(state * through, axis=-1, keepdims=True))
            scaled[spot, columns] = (scale * state).astype(low)
            grad_gate = grad * up * sig * (1.0 + gate * (1.0 - sig))
            grads[spot, columns] = grad_gate.astype(low)
            grads[spot, layout.hidden + begin : layout.hidden + end] = (grad * act).astype(low)
        choice = jnp.zeros_like(probs)
        for j in range(layout.local_experts):
            spotted = lane == lane0 + first_expert + j
            choice = choice + jnp.where(spotted, mask * totals[j], 0.0)
        small = probs * (choice - jnp.sum(probs * choice, axis=-1, keepdims=True))
        small = jnp.where(is_switch, totals[-1] * switch * (1.0 - switch), small)
        kept = grads[spot, router].astype(jnp.float32)
        kept = jnp.where(is_router | is_switch, small, kept)
        grads[spot, router] = kept.astype(low)

    strips(rows, body)


def out_tiles(width, scaled, downs, out):
    def body(spot):
        out[:, spot] = matmul(scaled[...], downs[:, spot]).astype(out.dtype)

    tiles(width, 256, body)


def back_tiles(layout, width, grads, gates, ups, back):
    hidden = layout.hidden

    def body(spot):
        total = matmul(grads[:, :hidden], gates[:, spot])
        total = total + matmul(grads[:, hidden:], ups[:, spot])
        back[:, spot] = total.astype(back.dtype)

    tiles(width, 256, body)


def rope(values, cosine, sine, sign):
    return values * cosine + pltpu.roll(values, HEAD_DIM // 2, 1) * (sine * sign)


def attend(heads, qkv, allowed_ref, cos_ref, sin_ref, queries, keys, values, probs_ref, context):
    cosine, sine = cos_ref[...], sin_ref[...]
    allowed = allowed_ref[...] > 0.5
    low = queries.dtype
    for head in range(heads):
        columns = slice(head * HEAD_DIM, (head + 1) * HEAD_DIM)
        query = rope(qkv(head), cosine, sine, 1.0).astype(low)
        key = rope(qkv(heads + head), cosine, sine, 1.0).astype(low)
        value = qkv(2 * heads + head).astype(low)
        queries[:, columns], keys[:, columns], values[:, columns] = query, key, value
        scores = matmul_last(query, key) * HEAD_DIM ** (-0.5)
        power = jnp.where(allowed, jnp.exp(jnp.where(allowed, scores, 0.0)), 0.0)
        probs = power / jnp.sum(power, axis=-1, keepdims=True)
        probs_ref[head] = probs
        context[:, columns] = matmul(probs.astype(low), value).astype(low)


def layer_kernel(
    layout,
    ranks,
    peers,
    query_ref,
    key_ref,
    value_ref,
    chosen_own_ref,
    proj_ref,
    router_ref,
    vectors_ref,
    tokens_ref,
    cot_ref,
    allowed_ref,
    cos_ref,
    sin_ref,
    expert_gate_ref,
    expert_up_ref,
    expert_down_ref,
    shared_gate_ref,
    shared_up_ref,
    shared_down_ref,
    rows_all,
    columns_all,
    attn_in,
    queries,
    keys,
    values,
    context,
    probs_ref,
    x_all,
    cot_all,
    middle_ref,
    scaled_ref,
    grads_ref,
    out_ref,
    back_ref,
    row_stage,
    column_stage,
    rows_full,
    columns_full,
    qkv_raw,
    part_ref,
    gates,
    ups,
    downs,
    shared_got,
    own,
    got,
    x_block,
    cot_block,
    pre_gate,
    pre_up,
    cot_hidden,
    scaled,
    grads,
    out,
    back,
    chosen,
    local_sem,
    gather_sem,
    a_sends,
    a_recvs,
    a_side_sends,
    a_side_recvs,
    block_sem,
    store_sem,
    shared_sends,
    shared_recvs,
    z_sends,
    z_recvs,
    x_sends,
    x_recvs,
    sends,
    recvs,
    side_sends,
    side_recvs,
    c_sends,
    c_recvs,
    c_side_sends,
    c_side_recvs,
):
    ring = Ring(ranks)
    here = lax.axis_index("tensor")
    block, width = tokens_ref.shape
    rows = block // peers
    depth = width // ranks
    half = ring.half
    away = [(here + k) % peers for k in range(peers)]
    others = [(ring.me + k) % ranks for k in range(ranks)]

    count, lane0 = layout.expert_count, layout.router_lane
    head_width = query_ref.shape[1]
    heads = head_width // HEAD_DIM
    lot, wide = row_stage.shape
    height = column_stage.shape[0]
    small_rows = height - head_width
    low = gates.dtype
    loads, start = [], 0
    for index, source in enumerate((query_ref, key_ref, value_ref, chosen_own_ref)):
        size = source.shape[1]
        loads.append(
            pltpu.make_async_copy(source, row_stage.at[:, pl.ds(start, size)], gather_sem.at[index])
        )
        start += size
    loads.append(
        pltpu.make_async_copy(
            proj_ref, column_stage.at[pl.ds(small_rows, head_width)], gather_sem.at[4]
        )
    )
    for load in loads:
        load.start()
    small = jnp.concatenate(
        [
            router_ref[...].astype(jnp.float32),
            vectors_ref[...].astype(jnp.float32),
            jnp.zeros((small_rows - count - vectors_ref.shape[0], depth), jnp.float32),
        ],
        axis=0,
    )
    column_stage[:small_rows, :] = small.astype(low)
    greet(
        [{"dp": others[k]} for k in range(1, ranks)] + [{"tensor": away[k]} for k in range(1, peers)]
    )
    order = near_first(peers)

    def row_place(device, first, size):
        return rows_all.at[pl.ds(device * lot + first, size)]

    def column_place(device, first, size):
        place = pl.ds(pl.multiple_of(device * depth, depth), depth)
        return columns_all.at[pl.ds(first, size), place]

    for load in loads:
        load.wait()
    gathers = [
        RingGather(ring, row_place, lot, a_sends, a_recvs, a_side_sends, a_side_recvs, 0, 0),
        RingGather(
            ring,
            column_place,
            height,
            a_sends,
            a_recvs,
            a_side_sends,
            a_side_recvs,
            gather_slots(half),
            side_slots(half),
        ),
    ]
    stores_own = []
    for index, (gather, stage) in enumerate(zip(gathers, (row_stage, column_stage))):
        gather.begin(stage)
        store = pltpu.make_async_copy(
            stage, gather.place(ring.me, 0, gather.rows), gather_sem.at[5 + index]
        )
        store.start()
        stores_own.append(store)
    for number in range(1, half):
        for gather in gathers:
            gather.step(number)

    shared_refs = (shared_gate_ref, shared_up_ref, shared_down_ref)
    handed, kept = [], []
    for k in range(1, ranks):
        for which, source in enumerate(shared_refs):
            copy = remote(
                source.at[others[k]],
                shared_got.at[which, ring.me],
                "dp",
                others[k],
                shared_sends,
                shared_recvs,
                which * (ranks - 1) + ranks - k - 1,
            )
            copy.start()
            handed.append(copy)
    for which, source in enumerate(shared_refs):
        copy = pltpu.make_async_copy(
            source.at[ring.me], shared_got.at[which, ring.me], local_sem.at[which]
        )
        copy.start()
        kept.append(copy)

    def cot_place(device, start, size):
        return cot_all.at[pl.ds(device * block + start, size)]

    cots = RingGather(
        ring, cot_place, block, c_sends, c_recvs, c_side_sends, c_side_recvs, 0, 0
    )
    cots.begin(cot_ref)
    kept_cot = pltpu.make_async_copy(cot_ref, cot_place(ring.me, 0, block), local_sem.at[3])
    kept_cot.start()

    experts, hid = layout.local_experts, layout.expert_hidden
    wides = (gates, ups, downs)
    loads = []
    for which, (target, source) in enumerate(
        zip(wides, (expert_gate_ref, expert_up_ref, expert_down_ref))
    ):
        for j in range(experts):
            load = pltpu.make_async_copy(
                source.at[j],
                target.at[pl.ds(j * layout.part, hid)],
                local_sem.at[5 + which * experts + j],
            )
            load.start()
            loads.append(load)
            if layout.part > hid:
                target[j * layout.part + hid : (j + 1) * layout.part, :] = jnp.zeros(
                    (layout.part - hid, width), low
                )
        target[layout.router_at :, :] = jnp.zeros((layout.hidden - layout.router_at, width), low)

    for gather in gathers:
        gather.step(half)
    for store in stores_own:
        store.wait()
    for gather in gathers:
        for index in range(gather.sides):
            gather.wait_side(index)
    fetches = [
        pltpu.make_async_copy(rows_all, rows_full, gather_sem.at[7]),
        pltpu.make_async_copy(columns_all, columns_full, gather_sem.at[8]),
    ]
    for fetch in fetches:
        fetch.start()
    fetches[1].wait()
    gates[layout.router_at : layout.router_at + count + 1, :] = columns_full[: count + 1, :]
    vectors = columns_full[:small_rows, :].astype(jnp.float32)
    attn_gain = vectors[count + 1 : count + 2, :]
    ffn_gain = vectors[count + 2 : count + 3, :]

    def norm_in(spot, start, size):
        value = tokens_ref[spot, :].astype(jnp.float32)
        inverse = lax.rsqrt(jnp.mean(value * value, axis=-1, keepdims=True) + EPSILON)
        attn_in[spot, :] = ((value * inverse) * attn_gain).astype(low)

    strips(block, norm_in)
    fetches[0].wait()

    def project(spot):
        qkv_raw[:, spot] = matmul(attn_in[...], rows_full[:, spot])

    tiles(3 * head_width, 256, project)

    def qkv(index):
        return qkv_raw[:, index * HEAD_DIM : (index + 1) * HEAD_DIM]

    attend(heads, qkv, allowed_ref, cos_ref, sin_ref, queries, keys, values, probs_ref, context)

    def project_out(spot):
        part_ref[:, spot] = matmul(context[...], columns_full[small_rows:, spot]).astype(low)

    tiles(width, 256, project_out)

    exchanged = []
    for k in reversed(order[1:]):
        copy = remote(
            part_ref.at[pl.ds(away[k] * rows, rows)],
            got.at[peers - k - 1],
            "tensor",
            away[k],
            z_sends,
            z_recvs,
            peers - k - 1,
        )
        copy.start()
        exchanged.append(copy)

    for copy in exchanged:
        copy.wait()
    first = here * rows

    def norm(spot, start, size):
        mine = pl.ds(pl.multiple_of(first + start, size), size)
        total = part_ref[mine, :].astype(jnp.float32)
        for k in range(peers - 1):
            total = total + got[k, spot, :].astype(jnp.float32)
        middle = tokens_ref[mine, :].astype(jnp.float32) + total
        middle_ref[spot, :] = middle
        inverse = lax.rsqrt(jnp.mean(middle * middle, axis=-1, keepdims=True) + EPSILON)
        own[spot, :] = ((middle * inverse) * ffn_gain).astype(own.dtype)

    strips(rows, norm)

    def place_of(k):
        def place(device, start, size):
            return x_all.at[pl.ds(device * block + away[k] * rows + start, size)]

        return place

    mine = place_of(0)(ring.me, 0, rows)
    forwards = []
    for k in order[1:]:
        copy = remote(own, mine, "tensor", away[k], x_sends, x_recvs, peers - k - 1)
        copy.start()
        forwards.append(copy)
    works = [
        RingGather(
            ring,
            place_of(k),
            rows,
            sends,
            recvs,
            side_sends,
            side_recvs,
            k * gather_slots(half),
            k * side_slots(half),
        )
        for k in range(peers)
    ]
    works[0].begin(own)
    store = pltpu.make_async_copy(own, mine, local_sem.at[4])
    store.start()

    for copy in kept + loads:
        copy.wait()
    for copy in handed:
        copy.wait_recv()
    for which, target in enumerate(wides):
        for source in range(ranks):
            columns = slice(source * depth, (source + 1) * depth)
            target[layout.shared_at : layout.router_at, columns] = shared_got[which, source]

    for k in order[1:]:
        spot = place_of(k)(ring.me, 0, rows)
        remote(own, spot, "tensor", away[k], x_sends, x_recvs, k - 1).wait_recv()
        works[k].begin(spot)
    store.wait()
    kept_cot.wait()
    passing = [cots] + [works[k] for k in order]
    cuts = [part * len(passing) // 5 for part in range(6)]
    chip_rows = 2 * block
    first_expert = ring.me * experts

    def stores(spot):
        return [
            pltpu.make_async_copy(source, target.at[spot], store_sem.at[slot])
            for slot, (source, target) in enumerate(
                ((scaled, scaled_ref), (grads, grads_ref), (out, out_ref), (back, back_ref))
            )
        ]

    def chip_step(turn, carry):
        offset = (1 - 2 * (turn % 2)) * ((turn + 1) // 2)
        spot = pl.ds(pl.multiple_of(ring.chip(offset) * chip_rows, chip_rows), chip_rows)

        def pass_on(part):
            for number in range(1, half + 1):

                @pl.when(turn == 2 * number - 2)
                def _(number=number):
                    for work in passing[cuts[part] : cuts[part + 1]]:
                        work.step(number)

        cots.wait_side(turn)
        load_cot = pltpu.make_async_copy(cot_all.at[spot], cot_block, block_sem.at[0])
        load_cot.start()
        for device in range(2):
            for fold in range(block // lot):
                there = ring.chip(offset) * 2 * lot + device * lot
                first_lane = 3 * head_width + fold * 128
                chosen[device * block + fold * lot : device * block + (fold + 1) * lot, :] = rows_full[
                    pl.ds(pl.multiple_of(there, lot), lot), first_lane : first_lane + 128
                ]
        for work in works:
            work.wait_side(turn)
        load_x = pltpu.make_async_copy(x_all.at[spot], x_block, block_sem.at[1])
        load_x.start()
        load_cot.wait()
        cot_tiles(layout, cot_block, downs, cot_hidden)
        pass_on(0)
        load_x.wait()
        hidden_tiles(layout, x_block, gates, ups, pre_gate, pre_up)
        pass_on(1)
        pending = stores(spot)

        @pl.when(turn > 0)
        def _():
            pending[0].wait()
            pending[1].wait()

        gate_strips(
            layout,
            first_expert,
            chosen,
            pre_gate,
            pre_up,
            cot_hidden,
            scaled,
            grads,
        )
        pending[0].start()
        pending[1].start()
        pass_on(2)

        @pl.when(turn > 0)
        def _():
            pending[2].wait()
            pending[3].wait()

        out_tiles(width, scaled, downs, out)
        pending[2].start()
        pass_on(3)
        back_tiles(layout, width, grads, gates, ups, back)
        pending[3].start()
        pass_on(4)
        return carry

    lax.fori_loop(0, ring.chips, chip_step, 0)
    for copy in stores(pl.ds(0, chip_rows)):
        copy.wait()
    for copy in forwards + handed:
        copy.wait_send()
    for gather in gathers:
        gather.sent()
    cots.sent()
    for work in works:
        work.sent()


def layer_forward_back(
    layout,
    query,
    key,
    value,
    chosen,
    proj,
    router,
    vectors,
    tokens,
    cot,
    allowed,
    cosine,
    sine,
    expert_gate,
    expert_up,
    expert_down,
    shared_gate,
    shared_up,
    shared_down,
    small_rows,
    ranks,
    peers,
    identity,
):
    half = ranks // 4
    block, width = tokens.shape
    rows = block // peers
    total = ranks * block
    depth = width // ranks
    hidden = layout.hidden
    chip = 2 * block
    head_width = query.shape[1]
    wide = 3 * head_width + chosen.shape[1]
    height = small_rows + head_width
    low = tokens.dtype
    vmem = pl.BlockSpec(memory_space=pltpu.VMEM)
    hbm = pl.BlockSpec(memory_space=pl.ANY)
    dma = pltpu.SemaphoreType.DMA
    f32 = jnp.float32
    heads = head_width // HEAD_DIM
    small_ones = [jax.ShapeDtypeStruct((block, head_width), low)] * 4
    return pl.pallas_call(
        functools.partial(layer_kernel, layout, ranks, peers),
        out_shape=(
            jax.ShapeDtypeStruct((width, wide), low),
            jax.ShapeDtypeStruct((height, width), low),
            jax.ShapeDtypeStruct((block, width), low),
            *small_ones,
            jax.ShapeDtypeStruct((heads, block, block), f32),
            jax.ShapeDtypeStruct((total, width), low),
            jax.ShapeDtypeStruct((total, width), low),
            jax.ShapeDtypeStruct((rows, width), f32),
            jax.ShapeDtypeStruct((total, hidden), low),
            jax.ShapeDtypeStruct((total, 2 * hidden), low),
            jax.ShapeDtypeStruct((total, width), low),
            jax.ShapeDtypeStruct((total, width), low),
        ),
        in_specs=[hbm] * 5 + [vmem] * 7 + [hbm] * 6,
        out_specs=(hbm, hbm, *[vmem] * 6, hbm, hbm, vmem, hbm, hbm, hbm, hbm),
        scratch_shapes=[
            pltpu.VMEM((depth, wide), low),
            pltpu.VMEM((height, depth), low),
            pltpu.VMEM((width, wide), low),
            pltpu.VMEM((height, width), low),
            pltpu.VMEM((block, 3 * head_width), f32),
            pltpu.VMEM((block, width), low),
            pltpu.VMEM((hidden, width), low),
            pltpu.VMEM((hidden, width), low),
            pltpu.VMEM((hidden, width), low),
            pltpu.VMEM((3, ranks, layout.shared_own, depth), low),
            pltpu.VMEM((rows, width), low),
            pltpu.VMEM((peers - 1, rows, width), low),
            pltpu.VMEM((chip, width), low),
            pltpu.VMEM((chip, width), low),
            pltpu.VMEM((chip, hidden), f32),
            pltpu.VMEM((chip, hidden), f32),
            pltpu.VMEM((chip, hidden), f32),
            pltpu.VMEM((chip, hidden), low),
            pltpu.VMEM((chip, 2 * hidden), low),
            pltpu.VMEM((chip, width), low),
            pltpu.VMEM((chip, width), low),
            pltpu.VMEM((chip, 128), low),
            dma((5 + 3 * layout.local_experts,)),
            dma((9,)),
            dma((2 * gather_slots(half),)),
            dma((2 * gather_slots(half),)),
            dma((2 * side_slots(half),)),
            dma((2 * side_slots(half),)),
            dma((2,)),
            dma((4,)),
            dma((3 * (ranks - 1),)),
            dma((3 * (ranks - 1),)),
            dma((peers - 1,)),
            dma((peers - 1,)),
            dma((peers - 1,)),
            dma((peers - 1,)),
            dma((peers * gather_slots(half),)),
            dma((peers * gather_slots(half),)),
            dma((peers * side_slots(half),)),
            dma((peers * side_slots(half),)),
            dma((gather_slots(half),)),
            dma((gather_slots(half),)),
            dma((side_slots(half),)),
            dma((side_slots(half),)),
        ],
        compiler_params=pltpu.CompilerParams(
            collective_id=identity, has_side_effects=True, vmem_limit_bytes=62 << 20
        ),
        name="layer_forward_back",
    )(
        query,
        key,
        value,
        chosen,
        proj,
        router,
        vectors,
        tokens,
        cot,
        allowed,
        cosine,
        sine,
        expert_gate,
        expert_up,
        expert_down,
        shared_gate,
        shared_up,
        shared_down,
    )


class RingReduce:
    def __init__(self, ring, source_at, rows, buffers, sems, slot):
        self.ring, self.source_at, self.rows, self.cut = ring, source_at, rows, rows // 2
        self.mine, self.side, self.got = [buffer.at[slot] for buffer in buffers]
        self.loads, self.sends, self.recvs, self.side_sends, self.side_recvs = sems
        self.base, self.side_base = slot * 2 * ring.half, slot * ring.chips
        half = ring.half
        self.order = [half]
        for distance in range(half - 1, 0, -1):
            self.order += [distance, ring.chips - distance]
        self.order.append(0)

    def load(self, offset):
        return pltpu.make_async_copy(
            self.source_at(self.ring.device(offset)),
            self.mine.at[offset],
            self.loads.at[self.side_base + offset],
        )

    def side_copy(self, offset):
        return remote(
            self.source_at(self.ring.other(offset)),
            self.side.at[offset],
            "dp",
            self.ring.sibling,
            self.side_sends,
            self.side_recvs,
            self.side_base + offset,
        )

    def hand_over(self, offset):
        self.side_copy(offset).start()
        self.load(offset).start()

    def ready(self, offset):
        self.load(offset).wait()
        self.side_copy(offset).wait_recv()

    def hop(self, which, number):
        ring, half, cut = self.ring, self.ring.half, self.cut
        distance = half - number
        offset = distance if which == 0 else ring.chips - distance
        place = pl.ds((0, cut)[which], cut) if number == 0 else pl.ds(0, self.rows)
        return remote(
            self.mine.at[offset, place],
            self.got.at[which * half + number, place],
            "dp",
            (ring.ahead, ring.behind)[which],
            self.sends,
            self.recvs,
            self.base + which * half + number,
        )

    def add(self, offset, extra, first, size):
        def total(spot):
            mine = self.mine[offset, spot, :].astype(jnp.float32)
            return mine + self.side[offset, spot, :].astype(jnp.float32)

        def more(spot, start, count):
            here = pl.ds(pl.multiple_of(first + start, count), count)
            value = total(here) + extra[here, :].astype(jnp.float32)
            self.mine[offset, here, :] = value.astype(self.mine.dtype)

        rest, begin = self.rows - size, 0 if first else size

        def plain(spot, start, count):
            here = pl.ds(pl.multiple_of(begin + start, count), count)
            self.mine[offset, here, :] = total(here).astype(self.mine.dtype)

        if size:
            strips(size, more)
        if rest:
            strips(rest, plain)

    def step(self, number):
        ring, half, cut = self.ring, self.ring.half, self.cut
        if number == 0:
            self.ready(half)
            self.add(half, None, 0, 0)
            self.hop(0, 0).start()
            self.hop(1, 0).start()
            return
        for which in range(2):
            distance = half - number
            offset = distance if which == 0 else ring.chips - distance
            self.ready(offset)
            self.hop(which, number - 1).wait_recv()
            extra = self.got.at[which * half + number - 1]
            if number == 1:
                self.add(offset, extra, (0, cut)[which], cut)
            else:
                self.add(offset, extra, 0, self.rows)
            self.hop(which, number).start()

    def total(self, emit):
        half = self.ring.half
        self.ready(0)
        self.hop(0, half - 1).wait_recv()
        self.hop(1, half - 1).wait_recv()

        def body(spot, start, size):
            value = self.mine[0, spot, :].astype(jnp.float32) + self.side[0, spot, :].astype(jnp.float32)
            value = value + self.got[half - 1, spot, :].astype(jnp.float32)
            value = value + self.got[2 * half - 1, spot, :].astype(jnp.float32)
            emit(spot, start, size, value)

        strips(self.rows, body)

    def finish(self):
        for offset in range(self.ring.chips):
            self.side_copy(offset).wait_send()
        for number in range(self.ring.half):
            for which in range(2):
                self.hop(which, number).wait_send()


def reduce_buffers(pieces, chips, rows, width, low):
    return [pltpu.VMEM((pieces, chips, rows, width), low)] * 3


def reduce_sems(pieces, chips):
    dma = pltpu.SemaphoreType.DMA
    return [dma((pieces * chips,))] * 5


def back_kernel(
    layout,
    ranks,
    peers,
    with_out,
    part_ref,
    out_part_ref,
    middle_ref,
    cot_ref,
    gain_ref,
    x_ref,
    cots_ref,
    grads_ref,
    scaled_ref,
    low_all_ref,
    grad_ref,
    small_ref,
    out_sum_ref,
    gate_grads_ref,
    up_grads_ref,
    down_grads_ref,
    shared_grads_ref,
    *refs,
):
    z_stage, z_got, low_ref, right, left, turned, product, experts_low, gain_grad = refs[:9]
    z_sends, z_recvs, x_sends, x_recvs, local_sem, right_sem, left_sem, product_sem = refs[9:17]
    back_buffers, back_sems = refs[17:20], refs[20:25]
    out_buffers, out_sems = refs[25:28], refs[28:]
    ring = Ring(ranks)
    here = lax.axis_index("tensor")
    block, width = cot_ref.shape
    rows = block // peers
    half = ring.half
    away = [(here + k) % peers for k in range(peers)]
    greet(ring.partners() + [{"tensor": away[k]} for k in range(1, peers)])
    order = list(reversed(near_first(peers)))
    hidden = layout.hidden

    def reducer(source, buffers, sems, k):
        def source_at(device):
            return source.at[pl.ds(device * block + away[k] * rows, rows)]

        return RingReduce(ring, source_at, rows, buffers, sems, k)

    backs = {k: reducer(part_ref, back_buffers, back_sems, k) for k in order}
    outs = {}
    if with_out:
        outs = {k: reducer(out_part_ref, out_buffers, out_sems, k) for k in order}
    for offset in backs[0].order:
        for k in order:
            backs[k].hand_over(offset)

    def fetch_right(source, slot):
        return pltpu.make_async_copy(source, right, right_sem)

    def fetch_left(wide):
        source = scaled_ref if wide == 2 else grads_ref.at[:, pl.ds(wide * hidden, hidden)]
        return pltpu.make_async_copy(source, left, left_sem)

    fetch_right(x_ref, 0).start()
    fetch_left(0).start()
    for number in range(half):
        for k in order:
            backs[k].step(number)
    for offset in backs[0].order:
        for k in outs:
            outs[k].hand_over(offset)

    def pass_z(k):
        def emit(spot, start, size, value):
            z_stage[k, spot, :] = value.astype(z_stage.dtype)

        backs[k].total(emit)
        z_copy(k).start()

    def z_copy(k):
        return remote(
            z_stage.at[k], z_got.at[peers - k - 1], "tensor", away[k], z_sends, z_recvs, peers - k - 1
        )

    tile = 256
    blocks = width // tile
    steps = 3 * blocks

    def results(step, wide):
        slot = step % 2
        columns = pl.ds(pl.multiple_of(step % blocks * tile, tile), tile)
        copies = [
            pltpu.make_async_copy(
                product.at[slot, pl.ds(j * layout.part, layout.expert_hidden)],
                (gate_grads_ref, up_grads_ref, down_grads_ref)[wide].at[j, :, columns],
                product_sem.at[slot * (layout.local_experts + 1) + j],
            )
            for j in range(layout.local_experts)
        ]
        copies.append(
            pltpu.make_async_copy(
                experts_low.at[slot],
                shared_grads_ref.at[wide, :, columns],
                product_sem.at[slot * (layout.local_experts + 1) + layout.local_experts],
            )
        )
        return copies

    def grad_step(step, carry):
        wide, turn, slot = step // blocks, step % blocks, step % 2
        for number in range(3):

            @pl.when(step == number * blocks)
            def _(number=number):
                fetch_left(number).wait()
                if number == 0:
                    fetch_right(x_ref, 0).wait()

                def turn_over(index, carry):
                    spot = pl.ds(pl.multiple_of(index * tile, tile), tile)
                    turned[:, spot] = left[spot, :].T
                    return carry

                lax.fori_loop(0, left.shape[0] // tile, turn_over, 0)
                if number < 2:
                    fetch_left(number + 1).start()
                else:
                    fetch_right(cots_ref, 0).start()
                    fetch_right(cots_ref, 0).wait()

        @pl.when(step > 1)
        def _():
            for copy in results(step, 0):
                copy.wait()

        columns = pl.ds(pl.multiple_of(turn * tile, tile), tile)
        value = matmul(turned[...], right[:, columns])
        product[slot] = value[: layout.shared_at].astype(product.dtype)
        experts_low[slot] = value[layout.shared_at : layout.router_at].astype(product.dtype)

        @pl.when(wide == 0)
        def _():
            small = small_ref.shape[0]
            small_ref[:, columns] = value[layout.router_at : layout.router_at + small]

        for number in range(3):

            @pl.when(wide == number)
            def _(number=number):
                for copy in results(step, number):
                    copy.start()

        for due, event in events:

            @pl.when(step == due)
            def _(event=event):
                event()

        return carry

    first = here * rows
    spare = layout.expert_count + 2
    gain_grad[...] = jnp.zeros_like(gain_grad)

    def norm(spot, start, size, value):
        for k in range(peers - 1):
            value = value + z_got[k, spot, :].astype(jnp.float32)
        middle = middle_ref[spot, :]
        inverse = lax.rsqrt(jnp.mean(middle * middle, axis=-1, keepdims=True) + EPSILON)
        normed = middle * inverse
        scaled = value * gain_ref[...]
        back = inverse * (scaled - normed * jnp.mean(scaled * normed, axis=-1, keepdims=True))
        mine = pl.ds(pl.multiple_of(first + start, size), size)
        grad = cot_ref[mine, :].astype(jnp.float32) + back
        grad_ref[spot, :] = grad
        low_ref[spot, :] = grad.astype(low_ref.dtype)
        gain_grad[...] += jnp.sum(value * normed, axis=0, keepdims=True)

    mine = low_all_ref.at[pl.ds(here * rows, rows)]
    store = pltpu.make_async_copy(low_ref, mine, local_sem)

    def spread():
        return [
            remote(low_ref, mine, "tensor", away[k], x_sends, x_recvs, peers - k - 1)
            for k in near_first(peers)[:0:-1]
        ]

    def finish_norm():
        for k in order[:-1]:
            z_copy(k).wait_recv()
        backs[0].total(norm)
        for copy in spread():
            copy.start()
        store.start()

    gap = 12 // (peers - 1)
    events = [(3 + gap * index, functools.partial(pass_z, k)) for index, k in enumerate(order[:-1])]
    for k in outs:
        events.append((OUT_FIRST, functools.partial(outs[k].step, 0)))
    for number in range(1, half):
        for index, k in enumerate(outs):
            events.append((OUT_NEXT + number, functools.partial(outs[k].step, number)))
    events.append((NORM_DUE, finish_norm))
    lax.fori_loop(0, steps, grad_step, 0)
    for step in (steps - 2, steps - 1):
        for copy in results(step, 0):
            copy.wait()
    small_ref[spare - 1 : spare, :] = jnp.zeros((1, width), jnp.float32)
    small_ref[spare : spare + 1, :] = gain_grad[...]
    if not with_out:
        out_sum_ref[...] = jnp.zeros_like(out_sum_ref)
    for k in outs:

        def emit_out(spot, start, size, value, k=k):
            there = pl.ds(pl.multiple_of(away[k] * rows + start, size), size)
            out_sum_ref[there, :] = value.astype(out_sum_ref.dtype)

        outs[k].total(emit_out)
    store.wait()
    for k in order[:-1]:
        z_copy(k).wait_send()
    for copy in spread():
        copy.wait()
    for k in order:
        backs[k].finish()
    for k in outs:
        outs[k].finish()


def reduce_and_norm(
    layout,
    part,
    out_part,
    middle,
    cotangent,
    gain,
    x_all,
    cot_all,
    grads,
    scaled,
    small_rows,
    ranks,
    peers,
    identity,
):
    chips = ranks // 2
    block, width = cotangent.shape
    total = x_all.shape[0]
    rows = block // peers
    hidden = layout.hidden
    experts = layout.local_experts
    vmem = pl.BlockSpec(memory_space=pltpu.VMEM)
    hbm = pl.BlockSpec(memory_space=pl.ANY)
    dma = pltpu.SemaphoreType.DMA
    low, f32 = part.dtype, jnp.float32
    with_out = chips == 4
    return pl.pallas_call(
        functools.partial(back_kernel, layout, ranks, peers, with_out),
        out_shape=(
            jax.ShapeDtypeStruct((block, width), low),
            jax.ShapeDtypeStruct((rows, width), f32),
            jax.ShapeDtypeStruct((small_rows, width), f32),
            jax.ShapeDtypeStruct((block, width), low),
            jax.ShapeDtypeStruct((experts, layout.expert_hidden, width), low),
            jax.ShapeDtypeStruct((experts, layout.expert_hidden, width), low),
            jax.ShapeDtypeStruct((experts, layout.expert_hidden, width), low),
            jax.ShapeDtypeStruct((3, layout.shared_own, width), low),
        ),
        in_specs=[hbm, hbm] + [vmem] * 3 + [hbm] * 4,
        out_specs=(hbm, vmem, vmem, vmem, hbm, hbm, hbm, hbm),
        scratch_shapes=[
            pltpu.VMEM((peers, rows, width), low),
            pltpu.VMEM((peers - 1, rows, width), low),
            pltpu.VMEM((rows, width), low),
            pltpu.VMEM((total, width), low),
            pltpu.VMEM((total, hidden), low),
            pltpu.VMEM((hidden, total), low),
            pltpu.VMEM((2, layout.shared_at, 256), low),
            pltpu.VMEM((2, layout.shared_own, 256), low),
            pltpu.VMEM((1, width), f32),
            dma((peers - 1,)),
            dma((peers - 1,)),
            dma((peers - 1,)),
            dma((peers - 1,)),
            dma,
            dma,
            dma,
            dma((2 * (experts + 1),)),
        ]
        + (reduce_buffers(peers, chips, rows, width, low) + reduce_sems(peers, chips))
        * (1 + with_out),
        compiler_params=pltpu.CompilerParams(
            collective_id=identity, has_side_effects=True, vmem_limit_bytes=62 << 20
        ),
        name="reduce_and_norm",
    )(part, out_part, middle, cotangent, gain, x_all, cot_all, grads, scaled)


def final_kernel(
    layout,
    ranks,
    peers,
    part_ref,
    out_sum_ref,
    middle_ref,
    tokens_ref,
    gain_ref,
    grad_ref,
    small_ref,
    qkv_ref,
    proj_ref,
    shared_ref,
    input_ref,
    output_ref,
    qkv_sum_ref,
    proj_sum_ref,
    small_sum_ref,
    shared_got_ref,
    z_got,
    o_got,
    low_ref,
    out_low,
    small_own,
    small_got,
    small_part,
    small_z,
    kept,
    z_sends,
    z_recvs,
    o_sends,
    o_recvs,
    x_sends,
    x_recvs,
    y_sends,
    y_recvs,
    g_sends,
    g_recvs,
    h_sends,
    h_recvs,
    s_sends,
    s_recvs,
    local_sem,
    *refs,
):
    ring = Ring(ranks)
    here = lax.axis_index("tensor")
    block, width = part_ref.shape
    rows = block // peers
    half = ring.half
    pieces = refs[0].shape[0]
    lot, size = qkv_sum_ref.shape[0], refs[0].shape[2]
    proj_size = refs[8].shape[2]
    columns = width // ranks
    away = [(here + k) % peers for k in range(peers)]
    others = [(ring.me + k) % ranks for k in range(ranks)]
    greet(
        [{"dp": others[k]} for k in range(1, ranks)] + [{"tensor": away[k]} for k in range(1, peers)]
    )
    far_first = near_first(peers)[:0:-1]

    def to_peers(source_of, target_of, sends, recvs):
        copies = []
        for k in far_first:
            slot = peers - k - 1
            copy = remote(source_of(k), target_of(slot), "tensor", away[k], sends, recvs, slot)
            copy.start()
            copies.append(copy)
        return copies

    exchanged = to_peers(
        lambda k: part_ref.at[pl.ds(away[k] * rows, rows)], lambda slot: z_got.at[slot], z_sends, z_recvs
    )
    summed = to_peers(
        lambda k: out_sum_ref.at[pl.ds(away[k] * rows, rows)],
        lambda slot: o_got.at[slot],
        o_sends,
        o_recvs,
    )

    def slice_of(device):
        return pl.ds(pl.multiple_of(device * columns, columns), columns)

    works = []
    for piece in range(pieces):

        def qkv_at(device, piece=piece):
            return qkv_ref.at[pl.ds(device * lot + piece * size, size)]

        def proj_at(device, piece=piece):
            return proj_ref.at[pl.ds(piece * proj_size, proj_size), slice_of(device)]

        works.append(RingReduce(ring, qkv_at, size, refs[0:3], refs[3:8], piece))
        works.append(RingReduce(ring, proj_at, proj_size, refs[8:11], refs[11:16], piece))
    for offset in works[0].order:
        for work in works:
            work.hand_over(offset)
    shared = []
    for k in range(1, ranks):
        copy = remote(
            shared_ref.at[:, :, slice_of(others[k])],
            shared_got_ref.at[ring.me],
            "dp",
            others[k],
            s_sends,
            s_recvs,
            ranks - k - 1,
        )
        copy.start()
        shared.append(copy)
    keep = pltpu.make_async_copy(shared_ref.at[:, :, slice_of(ring.me)], kept, local_sem.at[0])
    keep.start()
    for number in range(half):
        for work in works:
            work.step(number)
    keep.wait()
    keep = pltpu.make_async_copy(kept, shared_got_ref.at[ring.me], local_sem.at[0])
    keep.start()

    first = here * rows
    small_own[...] = small_ref[...]
    spot_row = layout.expert_count + 1

    def norm(spot, start, count):
        mine = pl.ds(pl.multiple_of(first + start, count), count)
        value = part_ref[mine, :].astype(jnp.float32)
        for k in range(peers - 1):
            value = value + z_got[k, spot, :].astype(jnp.float32)
        inputs = tokens_ref[mine, :].astype(jnp.float32)
        inverse = lax.rsqrt(jnp.mean(inputs * inputs, axis=-1, keepdims=True) + EPSILON)
        normed = inputs * inverse
        scaled = value * gain_ref[...]
        back = inverse * (scaled - normed * jnp.mean(scaled * normed, axis=-1, keepdims=True))
        low_ref[spot, :] = (grad_ref[spot, :] + back).astype(low_ref.dtype)
        small_own[spot_row : spot_row + 1, :] += jnp.sum(value * normed, axis=0, keepdims=True)

    for copy in exchanged:
        copy.wait_recv()
    strips(rows, norm)
    mine = input_ref.at[pl.ds(here * rows, rows)]
    spread = to_peers(lambda k: low_ref, lambda slot: mine, x_sends, x_recvs)
    stores = [pltpu.make_async_copy(low_ref, mine, local_sem.at[1])]
    stores[0].start()
    handed = []
    for k in range(1, ranks):
        copy = remote(
            small_own.at[:, slice_of(others[k])],
            small_got.at[ranks - k - 1],
            "dp",
            others[k],
            g_sends,
            g_recvs,
            ranks - k - 1,
        )
        copy.start()
        handed.append(copy)

    def finish_rows(spot, start, count):
        there = pl.ds(pl.multiple_of(first + start, count), count)
        value = out_sum_ref[there, :].astype(jnp.float32)
        for k in range(peers - 1):
            value = value + o_got[k, spot, :].astype(jnp.float32)
        out_low[spot, :] = (middle_ref[spot, :] + value).astype(out_low.dtype)

    for copy in summed:
        copy.wait_recv()
    strips(rows, finish_rows)
    out_mine = output_ref.at[pl.ds(here * rows, rows)]
    spread += to_peers(lambda k: out_low, lambda slot: out_mine, y_sends, y_recvs)
    stores.append(pltpu.make_async_copy(out_low, out_mine, local_sem.at[2]))
    stores[1].start()
    for piece in range(pieces):

        def emit_qkv(spot, start, count, value, piece=piece):
            qkv_sum_ref[pl.ds(pl.multiple_of(piece * size + start, count), count), :] = value

        def emit_proj(spot, start, count, value, piece=piece):
            proj_sum_ref[pl.ds(pl.multiple_of(piece * proj_size + start, count), count), :] = value

        works[2 * piece].total(emit_qkv)
        works[2 * piece + 1].total(emit_proj)
    for copy in handed:
        copy.wait_recv()
    value = small_own[:, slice_of(ring.me)]
    for k in range(ranks - 1):
        value = value + small_got[k]
    small_part[...] = value
    last = to_peers(lambda k: small_part, lambda slot: small_z.at[slot], h_sends, h_recvs)
    for copy in last:
        copy.wait_recv()
    value = small_part[...]
    for k in range(peers - 1):
        value = value + small_z[k]
    small_sum_ref[...] = value
    keep.wait()
    for copy in stores:
        copy.wait()
    for copy in exchanged + summed + handed + last:
        copy.wait_send()
    for copy in shared + spread:
        copy.wait()
    for work in works:
        work.finish()


def finish_grads(
    layout,
    part,
    out_sum,
    middle,
    tokens,
    gain,
    grad,
    small,
    grad_qkv,
    grad_proj,
    shared_grads,
    ranks,
    peers,
    identity,
):
    chips = ranks // 2
    block, width = part.shape
    rows = block // peers
    lot, wide = grad_qkv.shape[0] // ranks, grad_qkv.shape[1]
    columns = width // ranks
    height = grad_proj.shape[0]
    pieces = 4
    small_rows = small.shape[0]
    own = layout.shared_own
    vmem = pl.BlockSpec(memory_space=pltpu.VMEM)
    hbm = pl.BlockSpec(memory_space=pl.ANY)
    low, f32 = part.dtype, jnp.float32
    dma = pltpu.SemaphoreType.DMA
    return pl.pallas_call(
        functools.partial(final_kernel, layout, ranks, peers),
        out_shape=(
            jax.ShapeDtypeStruct((block, width), low),
            jax.ShapeDtypeStruct((block, width), low),
            jax.ShapeDtypeStruct((lot, wide), f32),
            jax.ShapeDtypeStruct((height, columns), f32),
            jax.ShapeDtypeStruct((small_rows, columns), f32),
            jax.ShapeDtypeStruct((ranks, 3, own, columns), low),
        ),
        in_specs=[vmem] * 7 + [hbm] * 3,
        out_specs=(hbm, hbm, vmem, vmem, vmem, hbm),
        scratch_shapes=[
            pltpu.VMEM((peers - 1, rows, width), low),
            pltpu.VMEM((peers - 1, rows, width), low),
            pltpu.VMEM((rows, width), low),
            pltpu.VMEM((rows, width), low),
            pltpu.VMEM((small_rows, width), f32),
            pltpu.VMEM((ranks - 1, small_rows, columns), f32),
            pltpu.VMEM((small_rows, columns), f32),
            pltpu.VMEM((peers - 1, small_rows, columns), f32),
            pltpu.VMEM((3, own, columns), low),
        ]
        + [dma((peers - 1,))] * 8
        + [dma((ranks - 1,))] * 2
        + [dma((peers - 1,))] * 2
        + [dma((ranks - 1,))] * 2
        + [dma((3,))]
        + reduce_buffers(pieces, chips, lot // pieces, wide, low)
        + reduce_sems(pieces, chips)
        + reduce_buffers(pieces, chips, height // pieces, columns, low)
        + reduce_sems(pieces, chips),
        compiler_params=pltpu.CompilerParams(
            collective_id=identity, has_side_effects=True, vmem_limit_bytes=60 << 20
        ),
        name="finish_grads",
    )(part, out_sum, middle, tokens, gain, grad, small, grad_qkv, grad_proj, shared_grads)


def dot_rows(left, right):
    return lax.dot_general(
        left, right, (((0,), (0,)), ((), ())), preferred_element_type=jnp.float32
    )


def dot_last(left, right):
    return lax.dot_general(
        left, right, (((1,), (1,)), ((), ())), preferred_element_type=jnp.float32
    )


def rope_tables():
    half_dim = HEAD_DIM // 2
    exponent = np.arange(half_dim, dtype=np.float32) * np.float32(2.0 / HEAD_DIM)
    inverse_freq = np.exp(-exponent * np.log(np.float32(1000000.0)))
    angles = np.arange(SEQ, dtype=np.float32)[:, None] * inverse_freq[None, :]
    cosine, sine = np.cos(angles), np.sin(angles)
    return (
        jnp.asarray(np.concatenate([cosine, cosine], axis=1)),
        jnp.asarray(np.concatenate([-sine, sine], axis=1)),
    )


def rotate_back(values, cosine, sine):
    swapped = jnp.roll(values, HEAD_DIM // 2, axis=-1)
    return values * cosine[:, None, :] - swapped * sine[:, None, :]


def attend_backward(queries, key_rows, value_rows, probs, grad_context):
    probs_low = probs.astype(jnp.bfloat16)
    grad_probs = jnp.einsum(
        "qhd,khd->hqk", grad_context, value_rows, preferred_element_type=jnp.float32
    )
    inner = jnp.sum(probs * grad_probs, axis=-1, keepdims=True)
    grad_scores = (probs * (grad_probs - inner)).astype(jnp.bfloat16)
    grad_queries = jnp.einsum(
        "hqk,khd->qhd", grad_scores, key_rows, preferred_element_type=jnp.float32
    ) * HEAD_DIM ** (-0.5)
    grad_keys = jnp.einsum(
        "hqk,qhd->khd", grad_scores, queries, preferred_element_type=jnp.float32
    ) * HEAD_DIM ** (-0.5)
    grad_values = jnp.einsum(
        "hqk,qhd->khd", probs_low, grad_context, preferred_element_type=jnp.float32
    )
    return (grad_queries, grad_keys, grad_values)


def scatter_rows(values):
    return lax.psum_scatter(values, "dp", scatter_dimension=0, tiled=True)


def shards(
    tokens,
    w_query,
    w_key,
    w_value,
    w_out,
    gain_attn,
    gain_ffn,
    w_router,
    shared_gate,
    shared_up,
    shared_down,
    shared_switch,
    expert_gate,
    expert_up_weight,
    expert_down,
    routes,
    segments,
    cotangent,
):
    low = jnp.bfloat16
    ranks = lax.axis_size("dp")
    peers = lax.axis_size("tensor")
    me = lax.axis_index("dp")
    token_count, width = tokens.shape
    local_experts, _, expert_hidden = expert_gate.shape
    expert_count = local_experts * ranks
    block = width // ranks
    head_width = w_query.shape[1]
    head_count = head_width // HEAD_DIM
    shared_width = shared_gate.shape[1]
    shared_own = shared_width // ranks
    small_pad = 128
    layout = Layout(local_experts, expert_hidden, shared_own, expert_count)
    lane0 = layout.router_lane

    small_rows = -(-(expert_count + 3) // 16) * 16
    spots = jnp.arange(small_pad, dtype=jnp.int32)[None, None, :] - lane0
    chosen = jnp.sum((routes[:, :, None] == spots).astype(jnp.float32), axis=1).astype(low)
    fold = token_count // block
    chosen = chosen.reshape(fold, block, small_pad).transpose(1, 0, 2).reshape(block, fold * small_pad)
    vectors = jnp.stack([shared_switch, gain_attn, gain_ffn])
    cosine, sine = rope_tables()
    spots = jnp.arange(SEQ, dtype=jnp.int32)
    allowed = (spots[None, :] <= spots[:, None]) & (segments[0][None, :] == segments[0][:, None])

    (
        qkv_full,
        columns_full,
        attn_in,
        queries,
        key_rows,
        value_rows,
        context_flat,
        probs,
        x_all,
        cot_all,
        middle,
        scaled_hidden,
        grads_wide,
        out_part,
        back_part,
    ) = layer_forward_back(
        layout,
        w_query,
        w_key,
        w_value,
        chosen,
        w_out,
        w_router.T,
        vectors,
        tokens,
        cotangent,
        allowed.astype(jnp.float32),
        cosine,
        sine,
        expert_gate.swapaxes(1, 2),
        expert_up_weight.swapaxes(1, 2),
        expert_down,
        shared_gate.T.reshape(ranks, shared_own, block),
        shared_up.T.reshape(ranks, shared_own, block),
        shared_down.reshape(ranks, shared_own, block),
        small_rows,
        ranks,
        peers,
        1,
    )
    qkv_full = qkv_full[:, : 3 * head_width]
    out_full = columns_full[small_rows:]
    attn_gain = columns_full[expert_count + 1].astype(jnp.float32)
    ffn_gain = columns_full[expert_count + 2].astype(jnp.float32)
    grad_attn_out, grad_middle, grad_small, out_sum, *grad_experts, grad_shared = reduce_and_norm(
        layout,
        back_part,
        out_part,
        middle,
        cotangent,
        ffn_gain[None, :],
        x_all,
        cot_all,
        grads_wide,
        scaled_hidden,
        small_rows,
        ranks,
        peers,
        2,
    )
    if ranks != 8:
        out_sum = scatter_rows(out_part)
    grad_experts = [grads.astype(jnp.float32) for grads in grad_experts]

    grad_proj = dot_rows(context_flat, grad_attn_out).astype(low)
    grad_context = dot_last(grad_attn_out, out_full)
    shape_three = (SEQ, head_count, HEAD_DIM)
    grad_queries, grad_keys, grad_values = attend_backward(
        queries.reshape(shape_three),
        key_rows.reshape(shape_three),
        value_rows.reshape(shape_three),
        probs,
        grad_context.astype(low).reshape(shape_three),
    )
    flat_shape = (token_count, head_width)
    grad_qkv_rows = jnp.concatenate(
        [
            rotate_back(grad_queries, cosine, sine).reshape(flat_shape).astype(low),
            rotate_back(grad_keys, cosine, sine).reshape(flat_shape).astype(low),
            grad_values.reshape(flat_shape).astype(low),
        ],
        axis=1,
    )
    grad_qkv = dot_rows(attn_in, grad_qkv_rows)
    attn_back_part = dot_last(grad_qkv_rows, qkv_full)
    grad_input, output, grad_qkv, grad_proj, grad_small, grad_shared = finish_grads(
        layout,
        attn_back_part.astype(low),
        out_sum,
        middle,
        tokens,
        attn_gain[None, :],
        grad_middle,
        grad_small,
        grad_qkv.astype(low),
        grad_proj,
        grad_shared,
        ranks,
        peers,
        3,
    )
    grad_shared = grad_shared.astype(jnp.float32)
    return (
        output,
        grad_input.astype(jnp.float32),
        grad_qkv[:, :head_width],
        grad_qkv[:, head_width : 2 * head_width],
        grad_qkv[:, 2 * head_width :],
        grad_proj,
        grad_small[expert_count + 1],
        grad_small[expert_count + 2],
        grad_small[:expert_count].T,
        grad_shared[:, 0].reshape(shared_width, block).T,
        grad_shared[:, 1].reshape(shared_width, block).T,
        grad_shared[:, 2].reshape(shared_width, block),
        grad_small[expert_count],
        grad_experts[0].swapaxes(1, 2),
        grad_experts[1].swapaxes(1, 2),
        grad_experts[2],
    )


def solution(mesh):
    in_specs = (
        P("dp", None),
        P("dp", "tensor"),
        P("dp", "tensor"),
        P("dp", "tensor"),
        P("tensor", "dp"),
        P("dp"),
        P("dp"),
        P("dp", None),
        P("dp", "tensor"),
        P("dp", "tensor"),
        P("tensor", "dp"),
        P("dp"),
        P("dp", None, "tensor"),
        P("dp", None, "tensor"),
        P("dp", "tensor", None),
        P("dp", None),
        P("dp", None),
        P("dp", None),
    )
    out_specs = (
        P("dp", None),
        P("dp", None),
        P("dp", "tensor"),
        P("dp", "tensor"),
        P("dp", "tensor"),
        P("tensor", "dp"),
        P("dp"),
        P("dp"),
        P("dp", None),
        P("dp", "tensor"),
        P("dp", "tensor"),
        P("tensor", "dp"),
        P("dp"),
        P("dp", None, "tensor"),
        P("dp", None, "tensor"),
        P("dp", "tensor", None),
    )
    return jax.shard_map(shards, mesh=mesh, in_specs=in_specs, out_specs=out_specs, check_vma=False)
```

```python
import functools

import jax
import jax.numpy as jnp
import numpy as np
from jax import lax
from jax.experimental import pallas as pl
from jax.experimental.pallas import tpu as pltpu
from jax.sharding import PartitionSpec as P

HEAD_DIM = 128
TOP = 4
SEQ = 256


EPSILON = 1e-06
MESH = pl.DeviceIdType.MESH


def ring_chip(position, chips):
    half = chips // 2
    upper = position // half
    return position + upper * (chips - 1 + half - 2 * position)


def ring_spot(chip, chips):
    return ring_chip(chip, chips)


def greet(partners):
    barrier = pltpu.get_barrier_semaphore()
    for partner in partners:
        pl.semaphore_signal(barrier, inc=1, device_id=partner, device_id_type=MESH)
    pl.semaphore_wait(barrier, len(partners))


def remote(source, target, axis, device, sends, recvs, slot):
    return pltpu.make_async_remote_copy(
        src_ref=source,
        dst_ref=target,
        send_sem=sends.at[slot],
        recv_sem=recvs.at[slot],
        device_id={axis: device},
        device_id_type=MESH,
    )


class Ring:
    def __init__(self, ranks):
        self.ranks = ranks
        self.chips = ranks // 2
        self.half = self.chips // 2
        self.me = lax.axis_index("dp")
        self.core = self.me % 2
        self.position = ring_spot(self.me // 2, self.chips)
        self.sibling = self.me + 1 - 2 * self.core
        self.ahead = self.device(1)
        self.behind = self.device(-1)

    def chip(self, offset):
        return ring_chip((self.position + offset + self.chips) % self.chips, self.chips)

    def device(self, offset):
        return self.chip(offset) * 2 + self.core

    def other(self, offset):
        return self.chip(offset) * 2 + 1 - self.core

    def partners(self):
        return [{"dp": self.ahead}, {"dp": self.behind}, {"dp": self.sibling}]


def gather_slots(half):
    return 2 * half


def side_slots(half):
    return 2 * half


class RingGather:
    def __init__(self, ring, place, rows, sends, recvs, side_sends, side_recvs, base, side_base):
        self.ring, self.place, self.rows, self.cut = ring, place, rows, rows // 2
        self.sends, self.recvs = sends, recvs
        self.side_sends, self.side_recvs = side_sends, side_recvs
        self.base, self.side_base = base, side_base
        self.hops, self.sides = {}, 0

    def hop_copy(self, source, target, device, slot):
        return remote(source, target, "dp", device, self.sends, self.recvs, self.base + slot)

    def side_copy(self, source, target, slot):
        return remote(
            source,
            target,
            "dp",
            self.ring.sibling,
            self.side_sends,
            self.side_recvs,
            self.side_base + slot,
        )

    def hop(self, source, target, device, slot, size):
        self.hop_copy(source, target, device, slot).start()
        self.hops[slot] = size

    def share(self, source, target):
        self.side_copy(source, target, self.sides).start()
        self.sides += 1

    def begin(self, source):
        ring = self.ring
        target = self.place(ring.me, 0, self.rows)
        self.hop(source, target, ring.ahead, 0, self.rows)
        self.hop(source, target, ring.behind, ring.half, self.rows)
        self.share(source, target)

    def wait_hop(self, slot):
        block = self.place(self.ring.me, 0, self.hops[slot])
        self.hop_copy(block, block, self.ring.ahead, slot).wait_recv()

    def step(self, number):
        ring = self.ring
        for which, sign in enumerate((-1, 1)):
            owner = ring.device(sign * number)
            onward = (ring.ahead, ring.behind)[which]
            self.wait_hop(which * ring.half + number - 1)
            if number < ring.half:
                block = self.place(owner, 0, self.rows)
                size = self.rows
                part = block
                if number == ring.half - 1:
                    size = self.cut
                    part = self.place(owner, (0, self.cut)[which], size)
                self.hop(part, part, onward, which * ring.half + number, size)
                self.share(block, block)
        if number == ring.half:
            block = self.place(ring.device(number), 0, self.rows)
            self.share(block, block)

    def wait_side(self, index):
        block = self.place(self.ring.me, 0, self.rows)
        self.side_copy(block, block, index).wait_recv()

    def sent(self):
        for slot, size in self.hops.items():
            block = self.place(self.ring.me, 0, size)
            self.hop_copy(block, block, self.ring.ahead, slot).wait_send()
        for index in range(self.sides):
            block = self.place(self.ring.me, 0, self.rows)
            self.side_copy(block, block, index).wait_send()

    def finish(self):
        self.sent()
        for index in range(self.sides):
            self.wait_side(index)


def near_first(peers):
    order = [0]
    for step in range(1, peers // 2 + 1):
        order.append(step)
        if peers - step != step:
            order.append(peers - step)
    return order


STRIP = 64
OUT_DUE, NORM_DUE = 10, 15


def strips(rows, body):
    strip = min(STRIP, rows)

    def step(index, carry):
        body(pl.ds(pl.multiple_of(index * strip, strip), strip), index * strip, strip)
        return carry

    lax.fori_loop(0, rows // strip, step, 0)


HIDDEN_TILE, OUT_TILE, BACK_TILE = 1024, 1024, 1024


def matmul(left, right):
    return lax.dot_general(
        left, right, (((1,), (0,)), ((), ())), preferred_element_type=jnp.float32
    )


def matmul_last(left, right):
    return lax.dot_general(
        left, right, (((1,), (1,)), ((), ())), preferred_element_type=jnp.float32
    )


def tiles(width, tile, body):
    def step(index, carry):
        body(pl.ds(pl.multiple_of(index * tile, tile), tile))
        return carry

    lax.fori_loop(0, width // tile, step, 0)


class Layout:
    def __init__(self, local_experts, expert_hidden, shared_own, expert_count):
        self.local_experts = local_experts
        self.expert_hidden = expert_hidden
        self.shared_own = shared_own
        self.expert_count = expert_count
        self.part = -(-expert_hidden // 128) * 128
        self.shared_at = local_experts * self.part
        self.router_at = self.shared_at + shared_own
        self.last = -(-(shared_own + expert_count + 1) // 128) * 128
        self.hidden = self.shared_at + self.last
        self.router_tile = self.router_at // 128 * 128
        self.router_lane = self.router_at - self.router_tile
        self.tile = next(size for size in (HIDDEN_TILE, 256, 128) if self.hidden % size == 0)


def hidden_tiles(layout, x_ref, gates, ups, pre_gate, pre_up):
    def body(spot):
        pre_gate[:, spot] = matmul_last(x_ref[...], gates[spot, :])
        pre_up[:, spot] = matmul_last(x_ref[...], ups[spot, :])

    tiles(layout.hidden, layout.tile, body)


def cot_tiles(layout, cot_ref, downs, cot_hidden):
    def body(spot):
        cot_hidden[:, spot] = matmul_last(cot_ref[...], downs[spot, :]).astype(cot_hidden.dtype)

    tiles(layout.hidden, layout.tile, body)


def gate_strips(layout, first_expert, chosen, pre_gate, pre_up, cot_hidden, scaled, grads):
    rows = pre_gate.shape[0]
    count, lane0 = layout.expert_count, layout.router_lane
    router = slice(layout.router_tile, layout.router_tile + 128)
    bounds = [(j * layout.part, (j + 1) * layout.part) for j in range(layout.local_experts)]
    bounds.append((layout.shared_at, layout.hidden))
    low = scaled.dtype

    def body(spot, start, size):
        lane = lax.broadcasted_iota(jnp.int32, (size, 128), 1)
        logits = pre_gate[spot, router]
        is_router = (lane >= lane0) & (lane < lane0 + count)
        is_switch = lane == lane0 + count
        power = jnp.where(is_router, jnp.exp(jnp.where(is_router, logits, 0.0)), 0.0)
        probs = power / jnp.sum(power, axis=-1, keepdims=True)
        raw = jnp.sum(jnp.where(is_switch, logits, 0.0), axis=-1, keepdims=True)
        switch = 1.0 / (1.0 + jnp.exp(-raw))
        mask = chosen[spot, :].astype(jnp.float32)
        scales = []
        for j in range(layout.local_experts):
            spotted = lane == lane0 + first_expert + j
            scales.append(jnp.sum(jnp.where(spotted, probs * mask, 0.0), axis=-1, keepdims=True))
        scales.append(switch)
        totals = []
        for (begin, end), scale in zip(bounds, scales):
            shared = begin == layout.shared_at
            columns = slice(begin, end)
            gate, up = pre_gate[spot, columns], pre_up[spot, columns]
            through = cot_hidden[spot, columns].astype(jnp.float32)
            sig = 1.0 / (1.0 + jnp.exp(-gate))
            act = gate * sig
            state = act * up
            grad = scale * through
            totals.append(jnp.sum(state * through, axis=-1, keepdims=True))
            scaled[spot, columns] = (scale * state).astype(low)
            grad_gate = grad * up * sig * (1.0 + gate * (1.0 - sig))
            grads[spot, columns] = grad_gate.astype(low)
            grads[spot, layout.hidden + begin : layout.hidden + end] = (grad * act).astype(low)
        choice = jnp.zeros_like(probs)
        for j in range(layout.local_experts):
            spotted = lane == lane0 + first_expert + j
            choice = choice + jnp.where(spotted, mask * totals[j], 0.0)
        small = probs * (choice - jnp.sum(probs * choice, axis=-1, keepdims=True))
        small = jnp.where(is_switch, totals[-1] * switch * (1.0 - switch), small)
        kept = grads[spot, router].astype(jnp.float32)
        kept = jnp.where(is_router | is_switch, small, kept)
        grads[spot, router] = kept.astype(low)

    strips(rows, body)


def out_tiles(width, scaled, downs, out):
    def body(spot):
        out[:, spot] = matmul(scaled[...], downs[:, spot]).astype(out.dtype)

    tiles(width, OUT_TILE, body)


def back_tiles(layout, width, grads, gates, ups, back):
    hidden = layout.hidden

    def body(spot):
        total = matmul(grads[:, :hidden], gates[:, spot])
        total = total + matmul(grads[:, hidden:], ups[:, spot])
        back[:, spot] = total.astype(back.dtype)

    tiles(width, BACK_TILE, body)


def rope(values, cosine, sine, sign):
    return values * cosine + pltpu.roll(values, HEAD_DIM // 2, 1) * (sine * sign)


def attend(heads, qkv, allowed_ref, cos_ref, sin_ref, queries, keys, values, probs_ref, context):
    cosine, sine = cos_ref[...], sin_ref[...]
    allowed = allowed_ref[...] > 0.5
    low = queries.dtype
    for head in range(heads):
        columns = slice(head * HEAD_DIM, (head + 1) * HEAD_DIM)
        query = rope(qkv(head), cosine, sine, 1.0).astype(low)
        key = rope(qkv(heads + head), cosine, sine, 1.0).astype(low)
        value = qkv(2 * heads + head).astype(low)
        queries[:, columns], keys[:, columns], values[:, columns] = query, key, value
        scores = matmul_last(query, key) * HEAD_DIM ** (-0.5)
        power = jnp.where(allowed, jnp.exp(jnp.where(allowed, scores, 0.0)), 0.0)
        probs = power / jnp.sum(power, axis=-1, keepdims=True)
        probs_ref[head] = probs
        context[:, columns] = matmul(probs.astype(low), value).astype(low)


def layer_kernel(
    layout,
    ranks,
    peers,
    query_ref,
    key_ref,
    value_ref,
    chosen_own_ref,
    proj_ref,
    router_ref,
    vectors_ref,
    tokens_ref,
    cot_ref,
    allowed_ref,
    cos_ref,
    sin_ref,
    expert_gate_ref,
    expert_up_ref,
    expert_down_ref,
    shared_gate_ref,
    shared_up_ref,
    shared_down_ref,
    rows_all,
    columns_all,
    attn_in,
    queries,
    keys,
    values,
    context,
    probs_ref,
    x_all,
    cot_all,
    middle_ref,
    scaled_ref,
    grads_ref,
    out_ref,
    back_ref,
    row_stage,
    column_stage,
    rows_full,
    columns_full,
    qkv_raw,
    part_ref,
    gates,
    ups,
    downs,
    shared_got,
    own,
    got,
    x_block,
    cot_block,
    pre_gate,
    pre_up,
    cot_hidden,
    scaled,
    grads,
    out,
    back,
    chosen,
    local_sem,
    gather_sem,
    a_sends,
    a_recvs,
    a_side_sends,
    a_side_recvs,
    block_sem,
    store_sem,
    shared_sends,
    shared_recvs,
    z_sends,
    z_recvs,
    x_sends,
    x_recvs,
    sends,
    recvs,
    side_sends,
    side_recvs,
    c_sends,
    c_recvs,
    c_side_sends,
    c_side_recvs,
):
    ring = Ring(ranks)
    here = lax.axis_index("tensor")
    block, width = tokens_ref.shape
    rows = block // peers
    depth = width // ranks
    half = ring.half
    away = [(here + k) % peers for k in range(peers)]
    others = [(ring.me + k) % ranks for k in range(ranks)]

    count, lane0 = layout.expert_count, layout.router_lane
    head_width = query_ref.shape[1]
    heads = head_width // HEAD_DIM
    lot, wide = row_stage.shape
    height = column_stage.shape[0]
    small_rows = height - head_width
    low = gates.dtype
    loads, start = [], 0
    for index, source in enumerate((query_ref, key_ref, value_ref, chosen_own_ref)):
        size = source.shape[1]
        loads.append(
            pltpu.make_async_copy(source, row_stage.at[:, pl.ds(start, size)], gather_sem.at[index])
        )
        start += size
    loads.append(
        pltpu.make_async_copy(
            proj_ref, column_stage.at[pl.ds(small_rows, head_width)], gather_sem.at[4]
        )
    )
    for load in loads:
        load.start()
    small = jnp.concatenate(
        [
            router_ref[...].astype(jnp.float32),
            vectors_ref[...].astype(jnp.float32),
            jnp.zeros((small_rows - count - vectors_ref.shape[0], depth), jnp.float32),
        ],
        axis=0,
    )
    column_stage[:small_rows, :] = small.astype(low)
    greet(
        [{"dp": others[k]} for k in range(1, ranks)] + [{"tensor": away[k]} for k in range(1, peers)]
    )
    order = near_first(peers)

    def row_place(device, first, size):
        return rows_all.at[pl.ds(device * lot + first, size)]

    def column_place(device, first, size):
        place = pl.ds(pl.multiple_of(device * depth, depth), depth)
        return columns_all.at[pl.ds(first, size), place]

    for load in loads:
        load.wait()
    gathers = [
        RingGather(ring, row_place, lot, a_sends, a_recvs, a_side_sends, a_side_recvs, 0, 0),
        RingGather(
            ring,
            column_place,
            height,
            a_sends,
            a_recvs,
            a_side_sends,
            a_side_recvs,
            gather_slots(half),
            side_slots(half),
        ),
    ]
    stores_own = []
    for index, (gather, stage) in enumerate(zip(gathers, (row_stage, column_stage))):
        gather.begin(stage)
        store = pltpu.make_async_copy(
            stage, gather.place(ring.me, 0, gather.rows), gather_sem.at[5 + index]
        )
        store.start()
        stores_own.append(store)
    for number in range(1, half):
        for gather in gathers:
            gather.step(number)

    experts, hid = layout.local_experts, layout.expert_hidden
    wides = (gates, ups, downs)
    loads = []
    for which, (target, source) in enumerate(
        zip(wides, (expert_gate_ref, expert_up_ref, expert_down_ref))
    ):
        for j in range(experts):
            load = pltpu.make_async_copy(
                source.at[j],
                target.at[pl.ds(j * layout.part, hid)],
                local_sem.at[5 + which * experts + j],
            )
            load.start()
            loads.append(load)
            if layout.part > hid:
                target[j * layout.part + hid : (j + 1) * layout.part, :] = jnp.zeros(
                    (layout.part - hid, width), low
                )
        target[layout.router_at :, :] = jnp.zeros((layout.hidden - layout.router_at, width), low)

    for gather in gathers:
        gather.step(half)

    shared_refs = (shared_gate_ref, shared_up_ref, shared_down_ref)
    handed, kept = [], []
    for k in range(1, ranks):
        for which, source in enumerate(shared_refs):
            copy = remote(
                source.at[others[k]],
                shared_got.at[which, ring.me],
                "dp",
                others[k],
                shared_sends,
                shared_recvs,
                which * (ranks - 1) + ranks - k - 1,
            )
            copy.start()
            handed.append(copy)
    for which, source in enumerate(shared_refs):
        copy = pltpu.make_async_copy(
            source.at[ring.me], shared_got.at[which, ring.me], local_sem.at[which]
        )
        copy.start()
        kept.append(copy)

    def cot_place(device, start, size):
        return cot_all.at[pl.ds(device * block + start, size)]

    cots = RingGather(
        ring, cot_place, block, c_sends, c_recvs, c_side_sends, c_side_recvs, 0, 0
    )
    cots.begin(cot_ref)
    kept_cot = pltpu.make_async_copy(cot_ref, cot_place(ring.me, 0, block), local_sem.at[3])
    kept_cot.start()

    for store in stores_own:
        store.wait()
    for gather in gathers:
        for index in range(gather.sides):
            gather.wait_side(index)
    fetches = [
        pltpu.make_async_copy(rows_all, rows_full, gather_sem.at[7]),
        pltpu.make_async_copy(columns_all, columns_full, gather_sem.at[8]),
    ]
    for fetch in fetches:
        fetch.start()
    fetches[1].wait()
    gates[layout.router_at : layout.router_at + count + 1, :] = columns_full[: count + 1, :]
    vectors = columns_full[:small_rows, :].astype(jnp.float32)
    attn_gain = vectors[count + 1 : count + 2, :]
    ffn_gain = vectors[count + 2 : count + 3, :]

    def norm_in(spot, start, size):
        value = tokens_ref[spot, :].astype(jnp.float32)
        inverse = lax.rsqrt(jnp.mean(value * value, axis=-1, keepdims=True) + EPSILON)
        attn_in[spot, :] = ((value * inverse) * attn_gain).astype(low)

    strips(block, norm_in)
    fetches[0].wait()

    def project(spot):
        qkv_raw[:, spot] = matmul(attn_in[...], rows_full[:, spot])

    tiles(3 * head_width, 256, project)

    def qkv(index):
        return qkv_raw[:, index * HEAD_DIM : (index + 1) * HEAD_DIM]

    attend(heads, qkv, allowed_ref, cos_ref, sin_ref, queries, keys, values, probs_ref, context)

    def project_out(spot):
        part_ref[:, spot] = matmul(context[...], columns_full[small_rows:, spot]).astype(low)

    tiles(width, 256, project_out)

    exchanged = []
    for k in reversed(order[1:]):
        copy = remote(
            part_ref.at[pl.ds(away[k] * rows, rows)],
            got.at[peers - k - 1],
            "tensor",
            away[k],
            z_sends,
            z_recvs,
            peers - k - 1,
        )
        copy.start()
        exchanged.append(copy)

    for copy in kept + loads:
        copy.wait()
    for copy in handed:
        copy.wait_recv()
    for which, target in enumerate(wides):
        for source in range(ranks):
            columns = slice(source * depth, (source + 1) * depth)
            target[layout.shared_at : layout.router_at, columns] = shared_got[which, source]

    chip_rows = 2 * block

    def chip_spot(turn):
        offset = (1 - 2 * (turn % 2)) * ((turn + 1) // 2)
        return pl.ds(pl.multiple_of(ring.chip(offset) * chip_rows, chip_rows), chip_rows)

    def cot_turn(turn, slot):
        cots.wait_side(turn)
        load_cot = pltpu.make_async_copy(cot_all.at[chip_spot(turn)], cot_block, block_sem.at[0])
        load_cot.start()
        load_cot.wait()
        cot_tiles(layout, cot_block, downs, cot_hidden.at[slot])

    kept_cot.wait()
    cot_turn(0, 0)

    for copy in exchanged:
        copy.wait()
    first = here * rows

    def norm(spot, start, size):
        mine = pl.ds(pl.multiple_of(first + start, size), size)
        total = part_ref[mine, :].astype(jnp.float32)
        for k in range(peers - 1):
            total = total + got[k, spot, :].astype(jnp.float32)
        middle = tokens_ref[mine, :].astype(jnp.float32) + total
        middle_ref[spot, :] = middle
        inverse = lax.rsqrt(jnp.mean(middle * middle, axis=-1, keepdims=True) + EPSILON)
        own[spot, :] = ((middle * inverse) * ffn_gain).astype(own.dtype)

    strips(rows, norm)

    def place_of(k):
        def place(device, start, size):
            return x_all.at[pl.ds(device * block + away[k] * rows + start, size)]

        return place

    mine = place_of(0)(ring.me, 0, rows)
    forwards = []
    for k in order[1:]:
        copy = remote(own, mine, "tensor", away[k], x_sends, x_recvs, peers - k - 1)
        copy.start()
        forwards.append(copy)
    works = [
        RingGather(
            ring,
            place_of(k),
            rows,
            sends,
            recvs,
            side_sends,
            side_recvs,
            k * gather_slots(half),
            k * side_slots(half),
        )
        for k in range(peers)
    ]
    works[0].begin(own)
    store = pltpu.make_async_copy(own, mine, local_sem.at[4])
    store.start()

    for index, k in enumerate(order[1:]):
        spot = place_of(k)(ring.me, 0, rows)
        remote(own, spot, "tensor", away[k], x_sends, x_recvs, k - 1).wait_recv()
        works[k].begin(spot)
        if index == 0:
            cots.step(1)
            cot_turn(1, 1)
        if index == 1:
            cot_turn(2, 2)
    store.wait()
    passing = [works[k] for k in order]
    cuts = [part * len(passing) // 4 for part in range(5)]
    first_expert = ring.me * experts

    def stores(spot):
        return [
            pltpu.make_async_copy(source, target.at[spot], store_sem.at[slot])
            for slot, (source, target) in enumerate(
                ((scaled, scaled_ref), (grads, grads_ref), (out, out_ref), (back, back_ref))
            )
        ]

    def chip_step(turn, carry):
        offset = (1 - 2 * (turn % 2)) * ((turn + 1) // 2)
        spot = chip_spot(turn)
        slot = turn - turn // 4 * (turn - 3)

        def pass_on(part):
            for number in range(1, half + 1):

                @pl.when(turn == 2 * number - 2)
                def _(number=number):
                    if part == 0 and number > 1:
                        cots.step(number)
                    for work in passing[cuts[part] : cuts[part + 1]]:
                        work.step(number)

        for device in range(2):
            for fold in range(block // lot):
                there = ring.chip(offset) * 2 * lot + device * lot
                first_lane = 3 * head_width + fold * 128
                chosen[device * block + fold * lot : device * block + (fold + 1) * lot, :] = rows_full[
                    pl.ds(pl.multiple_of(there, lot), lot), first_lane : first_lane + 128
                ]
        for work in works:
            work.wait_side(turn)
        load_x = pltpu.make_async_copy(x_all.at[spot], x_block, block_sem.at[1])
        load_x.start()
        load_x.wait()
        hidden_tiles(layout, x_block, gates, ups, pre_gate, pre_up)
        pass_on(0)

        @pl.when(turn > 2)
        def _():
            cot_turn(turn, 3)

        pending = stores(spot)

        @pl.when(turn > 0)
        def _():
            pending[0].wait()
            pending[1].wait()

        gate_strips(
            layout,
            first_expert,
            chosen,
            pre_gate,
            pre_up,
            cot_hidden.at[slot],
            scaled,
            grads,
        )
        pending[0].start()
        pending[1].start()
        pass_on(1)

        @pl.when(turn > 0)
        def _():
            pending[2].wait()
            pending[3].wait()

        out_tiles(width, scaled, downs, out)
        pending[2].start()
        pass_on(2)
        back_tiles(layout, width, grads, gates, ups, back)
        pending[3].start()
        pass_on(3)
        return carry

    lax.fori_loop(0, ring.chips, chip_step, 0)
    for copy in stores(pl.ds(0, chip_rows)):
        copy.wait()
    for copy in forwards + handed:
        copy.wait_send()
    for gather in gathers:
        gather.sent()
    cots.sent()
    for work in works:
        work.sent()


def layer_forward_back(
    layout,
    query,
    key,
    value,
    chosen,
    proj,
    router,
    vectors,
    tokens,
    cot,
    allowed,
    cosine,
    sine,
    expert_gate,
    expert_up,
    expert_down,
    shared_gate,
    shared_up,
    shared_down,
    small_rows,
    ranks,
    peers,
    identity,
):
    half = ranks // 4
    block, width = tokens.shape
    rows = block // peers
    total = ranks * block
    depth = width // ranks
    hidden = layout.hidden
    chip = 2 * block
    head_width = query.shape[1]
    wide = 3 * head_width + chosen.shape[1]
    height = small_rows + head_width
    low = tokens.dtype
    vmem = pl.BlockSpec(memory_space=pltpu.VMEM)
    hbm = pl.BlockSpec(memory_space=pl.ANY)
    dma = pltpu.SemaphoreType.DMA
    f32 = jnp.float32
    heads = head_width // HEAD_DIM
    small_ones = [jax.ShapeDtypeStruct((block, head_width), low)] * 4
    return pl.pallas_call(
        functools.partial(layer_kernel, layout, ranks, peers),
        out_shape=(
            jax.ShapeDtypeStruct((width, wide), low),
            jax.ShapeDtypeStruct((height, width), low),
            jax.ShapeDtypeStruct((block, width), low),
            *small_ones,
            jax.ShapeDtypeStruct((heads, block, block), f32),
            jax.ShapeDtypeStruct((total, width), low),
            jax.ShapeDtypeStruct((total, width), low),
            jax.ShapeDtypeStruct((rows, width), f32),
            jax.ShapeDtypeStruct((total, hidden), low),
            jax.ShapeDtypeStruct((total, 2 * hidden), low),
            jax.ShapeDtypeStruct((total, width), low),
            jax.ShapeDtypeStruct((total, width), low),
        ),
        in_specs=[hbm] * 5 + [vmem] * 7 + [hbm] * 6,
        out_specs=(hbm, hbm, *[vmem] * 6, hbm, hbm, vmem, hbm, hbm, hbm, hbm),
        scratch_shapes=[
            pltpu.VMEM((depth, wide), low),
            pltpu.VMEM((height, depth), low),
            pltpu.VMEM((width, wide), low),
            pltpu.VMEM((height, width), low),
            pltpu.VMEM((block, 3 * head_width), f32),
            pltpu.VMEM((block, width), low),
            pltpu.VMEM((hidden, width), low),
            pltpu.VMEM((hidden, width), low),
            pltpu.VMEM((hidden, width), low),
            pltpu.VMEM((3, ranks, layout.shared_own, depth), low),
            pltpu.VMEM((rows, width), low),
            pltpu.VMEM((peers - 1, rows, width), low),
            pltpu.VMEM((chip, width), low),
            pltpu.VMEM((chip, width), low),
            pltpu.VMEM((chip, hidden), f32),
            pltpu.VMEM((chip, hidden), f32),
            pltpu.VMEM((4, chip, hidden), low),
            pltpu.VMEM((chip, hidden), low),
            pltpu.VMEM((chip, 2 * hidden), low),
            pltpu.VMEM((chip, width), low),
            pltpu.VMEM((chip, width), low),
            pltpu.VMEM((chip, 128), low),
            dma((5 + 3 * layout.local_experts,)),
            dma((9,)),
            dma((2 * gather_slots(half),)),
            dma((2 * gather_slots(half),)),
            dma((2 * side_slots(half),)),
            dma((2 * side_slots(half),)),
            dma((2,)),
            dma((4,)),
            dma((3 * (ranks - 1),)),
            dma((3 * (ranks - 1),)),
            dma((peers - 1,)),
            dma((peers - 1,)),
            dma((peers - 1,)),
            dma((peers - 1,)),
            dma((peers * gather_slots(half),)),
            dma((peers * gather_slots(half),)),
            dma((peers * side_slots(half),)),
            dma((peers * side_slots(half),)),
            dma((gather_slots(half),)),
            dma((gather_slots(half),)),
            dma((side_slots(half),)),
            dma((side_slots(half),)),
        ],
        compiler_params=pltpu.CompilerParams(
            collective_id=identity, has_side_effects=True, vmem_limit_bytes=62 << 20
        ),
        name="layer_forward_back",
    )(
        query,
        key,
        value,
        chosen,
        proj,
        router,
        vectors,
        tokens,
        cot,
        allowed,
        cosine,
        sine,
        expert_gate,
        expert_up,
        expert_down,
        shared_gate,
        shared_up,
        shared_down,
    )


class RingReduce:
    def __init__(self, ring, source_at, rows, buffers, sems, slot):
        self.ring, self.source_at, self.rows, self.cut = ring, source_at, rows, rows // 2
        self.mine, self.side, self.got = [buffer.at[slot] for buffer in buffers]
        self.loads, self.sends, self.recvs, self.side_sends, self.side_recvs = sems
        self.base, self.side_base = slot * 2 * ring.half, slot * ring.chips
        half = ring.half
        self.order = [half]
        for distance in range(half - 1, 0, -1):
            self.order += [distance, ring.chips - distance]
        self.order.append(0)

    def load(self, offset):
        return pltpu.make_async_copy(
            self.source_at(self.ring.device(offset)),
            self.mine.at[offset],
            self.loads.at[self.side_base + offset],
        )

    def side_copy(self, offset):
        return remote(
            self.source_at(self.ring.other(offset)),
            self.side.at[offset],
            "dp",
            self.ring.sibling,
            self.side_sends,
            self.side_recvs,
            self.side_base + offset,
        )

    def hand_over(self, offset):
        self.side_copy(offset).start()
        self.load(offset).start()

    def ready(self, offset):
        self.load(offset).wait()
        self.side_copy(offset).wait_recv()

    def hop(self, which, number):
        ring, half, cut = self.ring, self.ring.half, self.cut
        distance = half - number
        offset = distance if which == 0 else ring.chips - distance
        place = pl.ds((0, cut)[which], cut) if number == 0 else pl.ds(0, self.rows)
        return remote(
            self.mine.at[offset, place],
            self.got.at[which * half + number, place],
            "dp",
            (ring.ahead, ring.behind)[which],
            self.sends,
            self.recvs,
            self.base + which * half + number,
        )

    def add(self, offset, extra, first, size):
        def total(spot):
            mine = self.mine[offset, spot, :].astype(jnp.float32)
            return mine + self.side[offset, spot, :].astype(jnp.float32)

        def more(spot, start, count):
            here = pl.ds(pl.multiple_of(first + start, count), count)
            value = total(here) + extra[here, :].astype(jnp.float32)
            self.mine[offset, here, :] = value.astype(self.mine.dtype)

        rest, begin = self.rows - size, 0 if first else size

        def plain(spot, start, count):
            here = pl.ds(pl.multiple_of(begin + start, count), count)
            self.mine[offset, here, :] = total(here).astype(self.mine.dtype)

        if size:
            strips(size, more)
        if rest:
            strips(rest, plain)

    def step(self, number):
        ring, half, cut = self.ring, self.ring.half, self.cut
        if number == 0:
            self.ready(half)
            self.add(half, None, 0, 0)
            self.hop(0, 0).start()
            self.hop(1, 0).start()
            return
        for which in range(2):
            distance = half - number
            offset = distance if which == 0 else ring.chips - distance
            self.ready(offset)
            self.hop(which, number - 1).wait_recv()
            extra = self.got.at[which * half + number - 1]
            if number == 1:
                self.add(offset, extra, (0, cut)[which], cut)
            else:
                self.add(offset, extra, 0, self.rows)
            self.hop(which, number).start()

    def total(self, emit):
        half = self.ring.half
        self.ready(0)
        self.hop(0, half - 1).wait_recv()
        self.hop(1, half - 1).wait_recv()

        def body(spot, start, size):
            value = self.mine[0, spot, :].astype(jnp.float32) + self.side[0, spot, :].astype(jnp.float32)
            value = value + self.got[half - 1, spot, :].astype(jnp.float32)
            value = value + self.got[2 * half - 1, spot, :].astype(jnp.float32)
            emit(spot, start, size, value)

        strips(self.rows, body)

    def finish(self):
        for offset in range(self.ring.chips):
            self.side_copy(offset).wait_send()
        for number in range(self.ring.half):
            for which in range(2):
                self.hop(which, number).wait_send()


def reduce_buffers(pieces, chips, rows, width, low):
    return [pltpu.VMEM((pieces, chips, rows, width), low)] * 3


def reduce_sems(pieces, chips):
    dma = pltpu.SemaphoreType.DMA
    return [dma((pieces * chips,))] * 5


def attend_back(heads, queries, keys, values, probs_ref, grad_context, cos_ref, sin_ref, grads):
    cosine, sine = cos_ref[...], sin_ref[...]
    low = grads.dtype
    scale = HEAD_DIM ** (-0.5)
    for head in range(heads):
        columns = slice(head * HEAD_DIM, (head + 1) * HEAD_DIM)
        probs, through = probs_ref[head], grad_context[:, columns]
        grad_probs = matmul_last(through, values[:, columns])
        inner = jnp.sum(probs * grad_probs, axis=-1, keepdims=True)
        grad_scores = (probs * (grad_probs - inner)).astype(low)
        parts = (
            rope(matmul(grad_scores, keys[:, columns]) * scale, cosine, sine, -1.0),
            rope(matmul(grad_scores.T, queries[:, columns]) * scale, cosine, sine, -1.0),
            matmul(probs.astype(low).T, through),
        )
        for index, part in enumerate(parts):
            first = (index * heads + head) * HEAD_DIM
            grads[:, first : first + HEAD_DIM] = part.astype(low)


def rear_kernel(
    layout,
    ranks,
    peers,
    with_out,
    part_ref,
    out_part_ref,
    x_ref,
    cots_ref,
    grads_ref,
    scaled_ref,
    rows_all,
    columns_all,
    middle_ref,
    cot_ref,
    tokens_ref,
    attn_in,
    queries,
    keys,
    values,
    context,
    probs_ref,
    cos_ref,
    sin_ref,
    input_ref,
    output_ref,
    qkv_sum_ref,
    proj_sum_ref,
    small_sum_ref,
    gate_grads_ref,
    up_grads_ref,
    down_grads_ref,
    shared_grads_ref,
    shared_got_ref,
    cot_rows,
    token_rows,
    small_vec,
    grad_ref,
    small_own,
    small_got,
    small_part,
    small_z,
    z_stage,
    z_got,
    a_got,
    o_got,
    low_ref,
    gm_all,
    right,
    left,
    turned,
    product,
    shared_low,
    gain_grad,
    qkv_full,
    grad_context,
    grad_rows,
    attn_part,
    out_sum,
    kept,
    z_sends,
    z_recvs,
    m_sends,
    m_recvs,
    a_sends,
    a_recvs,
    o_sends,
    o_recvs,
    x_sends,
    x_recvs,
    y_sends,
    y_recvs,
    h_sends,
    h_recvs,
    g_sends,
    g_recvs,
    s_sends,
    s_recvs,
    local_sem,
    left_sem,
    right_sem,
    product_sem,
    reuse_sem,
    *refs,
):
    buffers = refs[0:3]
    back_sems, qkv_sems, proj_buffers, proj_sems = refs[3:8], refs[8:13], refs[13:16], refs[16:21]
    out_buffers, out_sems = refs[21:24], refs[24:]
    out_low = z_stage.at[0]
    ring = Ring(ranks)
    here = lax.axis_index("tensor")
    block, width = cot_ref.shape
    rows = block // peers
    half = ring.half
    low = low_ref.dtype
    columns = width // ranks
    hidden = layout.hidden
    head_width = queries.shape[1]
    heads = head_width // HEAD_DIM
    small_rows = small_vec.shape[0]
    away = [(here + k) % peers for k in range(peers)]
    others = [(ring.me + k) % ranks for k in range(ranks)]
    greet(
        [{"dp": others[k]} for k in range(1, ranks)] + [{"tensor": away[k]} for k in range(1, peers)]
    )
    first = here * rows
    order = list(reversed(near_first(peers)))
    far_first = order[:-1]

    def slice_of(device):
        return pl.ds(pl.multiple_of(device * columns, columns), columns)

    def to_peers(source_of, target_of, sends, recvs):
        return [
            remote(
                source_of(k),
                target_of(peers - k - 1),
                "tensor",
                away[k],
                sends,
                recvs,
                peers - k - 1,
            )
            for k in far_first
        ]

    def reducer(source, where, sems, k):
        def source_at(device):
            return source.at[pl.ds(device * block + away[k] * rows, rows)]

        return RingReduce(ring, source_at, rows, where, sems, k)

    backs = {k: reducer(part_ref, buffers, back_sems, k) for k in order}
    outs = {}
    if with_out:
        outs = {k: reducer(out_part_ref, out_buffers, out_sems, k) for k in order}
    for offset in backs[0].order:
        for k in order:
            backs[k].hand_over(offset)

    tile = right.shape[2]
    blocks = width // tile
    steps = 3 * blocks

    def fetch_left(wide):
        source = scaled_ref if wide == 2 else grads_ref.at[:, pl.ds(wide * hidden, hidden)]
        return pltpu.make_async_copy(source, left, left_sem)

    def fetch_right(step, late):
        spot = pl.ds(pl.multiple_of(step % blocks * tile, tile), tile)
        source = cots_ref if late else x_ref
        return pltpu.make_async_copy(source.at[:, spot], right.at[step % 2], right_sem.at[step % 2])

    fetch_right(0, False).start()
    fetch_left(0).start()
    vec_load = pltpu.make_async_copy(columns_all.at[pl.ds(0, small_rows)], small_vec, local_sem.at[0])
    vec_load.start()
    row_loads = [
        pltpu.make_async_copy(source.at[pl.ds(first, rows)], target, local_sem.at[slot])
        for source, target, slot in ((cot_ref, cot_rows, 5), (tokens_ref, token_rows, 6))
    ]
    for load in row_loads:
        load.start()
    qkv_load = pltpu.make_async_copy(
        rows_all.at[:, pl.ds(0, 3 * head_width)], qkv_full, local_sem.at[1]
    )
    qkv_load.start()
    if not with_out:
        out_load = pltpu.make_async_copy(out_part_ref, out_sum, local_sem.at[2])
        out_load.start()
    for number in range(half):
        for k in order:
            backs[k].step(number)
    for offset in backs[0].order:
        for k in outs:
            outs[k].hand_over(offset)
    vec_load.wait()
    for load in row_loads:
        load.wait()
    count = layout.expert_count
    vectors = small_vec[...].astype(jnp.float32)
    attn_gain = vectors[count + 1 : count + 2, :]
    ffn_gain = vectors[count + 2 : count + 3, :]

    def z_copy(k):
        slot = peers - k - 1
        return remote(z_stage.at[k], z_got.at[slot], "tensor", away[k], z_sends, z_recvs, slot)

    def pass_z(k):
        def emit(spot, start, size, value):
            z_stage[k, spot, :] = value.astype(low)

        backs[k].total(emit)
        z_copy(k).start()

    def results(step, wide):
        slot = step % 2
        spot = pl.ds(pl.multiple_of(step % blocks * tile, tile), tile)
        base = slot * (layout.local_experts + 1)
        copies = [
            pltpu.make_async_copy(
                product.at[slot, pl.ds(j * layout.part, layout.expert_hidden)],
                (gate_grads_ref, up_grads_ref, down_grads_ref)[wide].at[j, :, spot],
                product_sem.at[base + j],
            )
            for j in range(layout.local_experts)
        ]
        copies.append(
            pltpu.make_async_copy(
                shared_low.at[slot],
                shared_grads_ref.at[wide, :, spot],
                product_sem.at[base + layout.local_experts],
            )
        )
        return copies

    gain_grad[...] = jnp.zeros_like(gain_grad)

    def norm_middle(spot, start, size, value):
        for k in range(peers - 1):
            value = value + z_got[k, spot, :].astype(jnp.float32)
        middle = middle_ref[spot, :]
        inverse = lax.rsqrt(jnp.mean(middle * middle, axis=-1, keepdims=True) + EPSILON)
        normed = middle * inverse
        scaled = value * ffn_gain
        back = inverse * (scaled - normed * jnp.mean(scaled * normed, axis=-1, keepdims=True))
        mine = pl.ds(pl.multiple_of(first + start, size), size)
        grad = cot_rows[spot, :].astype(jnp.float32) + back
        grad_ref[spot, :] = grad
        low_ref[spot, :] = grad.astype(low)
        gm_all[mine, :] = grad.astype(low)
        gain_grad[...] += jnp.sum(value * normed, axis=0, keepdims=True)

    def spread():
        mine = gm_all.at[pl.ds(first, rows)]
        return to_peers(lambda k: low_ref, lambda slot: mine, m_sends, m_recvs)

    def finish_norm():
        for k in far_first:
            z_copy(k).wait_recv()
        backs[0].total(norm_middle)
        for copy in spread():
            copy.start()

    gap = 12 // (peers - 1)
    events = [(3 + gap * index, functools.partial(pass_z, k)) for index, k in enumerate(far_first)]
    for number in range(half):
        for k in outs:
            events.append((OUT_DUE + 3 * number, functools.partial(outs[k].step, number)))
    events.append((NORM_DUE, finish_norm))

    def grad_step(step, carry):
        wide, slot = step // blocks, step % 2
        for number in range(3):

            @pl.when(step == number * blocks)
            def _(number=number):
                fetch_left(number).wait()

                def turn_over(index, carry):
                    spot = pl.ds(pl.multiple_of(index * 256, 256), 256)
                    turned[:, spot] = left[spot, :].T
                    return carry

                lax.fori_loop(0, left.shape[0] // 256, turn_over, 0)
                if number < 2:
                    fetch_left(number + 1).start()

        fetch_right(step, False).wait()

        @pl.when(step + 1 < 2 * blocks)
        def _():
            fetch_right(step + 1, False).start()

        @pl.when((step + 1 >= 2 * blocks) & (step + 1 < steps))
        def _():
            fetch_right(step + 1, True).start()

        @pl.when(step > 1)
        def _():
            for copy in results(step, 0):
                copy.wait()

        value = matmul(turned[...], right[slot])
        product[slot] = value[: layout.shared_at].astype(low)
        shared_low[slot] = value[layout.shared_at : layout.router_at].astype(low)

        @pl.when(wide == 0)
        def _():
            spot = pl.ds(pl.multiple_of(step % blocks * tile, tile), tile)
            small_own[:, spot] = value[layout.router_at : layout.router_at + small_rows]

        for number in range(3):

            @pl.when(wide == number)
            def _(number=number):
                for copy in results(step, number):
                    copy.start()

        for due, event in events:

            @pl.when(step == due)
            def _(event=event):
                event()

        return carry

    lax.fori_loop(0, steps, grad_step, 0)
    proj_load = pltpu.make_async_copy(
        columns_all.at[pl.ds(small_rows, head_width)],
        turned.at[pl.ds(head_width, head_width), pl.ds(0, width)],
        local_sem.at[3],
    )
    proj_load.start()
    for step in (steps - 2, steps - 1):
        for copy in results(step, 0):
            copy.wait()
    small_own[count + 1 : count + 2, :] = jnp.zeros((1, width), jnp.float32)
    small_own[count + 2 : count + 3, :] = gain_grad[...]

    if not with_out:
        out_load.wait()
    for k in outs:

        def emit_out(spot, start, size, value, k=k):
            there = pl.ds(pl.multiple_of(away[k] * rows + start, size), size)
            out_sum[there, :] = value.astype(low)

        outs[k].total(emit_out)
    summed = to_peers(
        lambda k: out_sum.at[pl.ds(away[k] * rows, rows)], lambda slot: o_got.at[slot], o_sends, o_recvs
    )
    for copy in summed:
        copy.start()

    for copy in spread():
        copy.wait()
    proj_load.wait()
    out_weights = turned.at[pl.ds(head_width, head_width), pl.ds(0, width)]
    grad_context[...] = matmul_last(gm_all[...], out_weights[...]).astype(low)
    attend_back(heads, queries, keys, values, probs_ref, grad_context, cos_ref, sin_ref, grad_rows)
    qkv_load.wait()

    def through_qkv(spot):
        attn_part[:, spot] = matmul_last(grad_rows[...], qkv_full[spot, :]).astype(low)

    tiles(width, 256, through_qkv)
    exchanged = to_peers(
        lambda k: attn_part.at[pl.ds(away[k] * rows, rows)], lambda slot: a_got.at[slot], a_sends, a_recvs
    )
    for copy in exchanged:
        copy.start()

    def weight_tiles(spot):
        qkv_full[spot, :] = matmul(attn_in[:, spot].T, grad_rows[...]).astype(low)

    tiles(width, 256, weight_tiles)

    def proj_tiles(spot):
        turned[:head_width, spot] = matmul(context[...].T, gm_all[:, spot]).astype(low)

    tiles(width, 256, proj_tiles)

    for k in order:
        backs[k].finish()
    for partner in ring.partners():
        pl.semaphore_signal(reuse_sem, inc=1, device_id=partner, device_id_type=MESH)
    pl.semaphore_wait(reuse_sem, 3)
    pieces = proj_buffers[0].shape[0]
    lot, size = qkv_sum_ref.shape[0], qkv_sum_ref.shape[0] // pieces
    proj_size = proj_buffers[0].shape[2]
    narrow = [
        buffer.at[pl.ds(0, pieces), :, pl.ds(0, size), pl.ds(0, 3 * head_width)] for buffer in buffers
    ]
    works = []
    for piece in range(pieces):

        def qkv_at(device, piece=piece):
            return qkv_full.at[pl.ds(device * lot + piece * size, size)]

        def proj_at(device, piece=piece):
            return turned.at[pl.ds(piece * proj_size, proj_size), slice_of(device)]

        works.append(RingReduce(ring, qkv_at, size, narrow, qkv_sems, piece))
        works.append(RingReduce(ring, proj_at, proj_size, proj_buffers, proj_sems, piece))
    for offset in works[0].order:
        for work in works:
            work.hand_over(offset)
    for number in range(half):
        for work in works:
            work.step(number)

    spot_row = count + 1

    def norm_tokens(spot, start, size):
        mine = pl.ds(pl.multiple_of(first + start, size), size)
        value = attn_part[mine, :].astype(jnp.float32)
        for k in range(peers - 1):
            value = value + a_got[k, spot, :].astype(jnp.float32)
        inputs = token_rows[spot, :].astype(jnp.float32)
        inverse = lax.rsqrt(jnp.mean(inputs * inputs, axis=-1, keepdims=True) + EPSILON)
        normed = inputs * inverse
        scaled = value * attn_gain
        back = inverse * (scaled - normed * jnp.mean(scaled * normed, axis=-1, keepdims=True))
        low_ref[spot, :] = (grad_ref[spot, :] + back).astype(low)
        small_own[spot_row : spot_row + 1, :] += jnp.sum(value * normed, axis=0, keepdims=True)

    for copy in exchanged:
        copy.wait_recv()
    strips(rows, norm_tokens)
    mine = input_ref.at[pl.ds(first, rows)]
    inputs_out = to_peers(lambda k: low_ref, lambda slot: mine, x_sends, x_recvs)
    for copy in inputs_out:
        copy.start()
    stores = [pltpu.make_async_copy(low_ref, mine, local_sem.at[5])]
    stores[0].start()
    handed = []
    for k in range(1, ranks):
        copy = remote(
            small_own.at[:, slice_of(others[k])],
            small_got.at[ranks - k - 1],
            "dp",
            others[k],
            g_sends,
            g_recvs,
            ranks - k - 1,
        )
        copy.start()
        handed.append(copy)

    shared = []
    for k in range(1, ranks):
        copy = remote(
            shared_grads_ref.at[:, :, slice_of(others[k])],
            shared_got_ref.at[ring.me],
            "dp",
            others[k],
            s_sends,
            s_recvs,
            ranks - k - 1,
        )
        copy.start()
        shared.append(copy)
    keep = pltpu.make_async_copy(
        shared_grads_ref.at[:, :, slice_of(ring.me)], kept, local_sem.at[4]
    )
    keep.start()

    def finish_rows(spot, start, size):
        there = pl.ds(pl.multiple_of(first + start, size), size)
        value = out_sum[there, :].astype(jnp.float32)
        for k in range(peers - 1):
            value = value + o_got[k, spot, :].astype(jnp.float32)
        out_low[spot, :] = (middle_ref[spot, :] + value).astype(low)

    for copy in summed:
        copy.wait_recv()
    strips(rows, finish_rows)
    keep.wait()
    keep = pltpu.make_async_copy(kept, shared_got_ref.at[ring.me], local_sem.at[4])
    keep.start()
    for copy in handed:
        copy.wait_recv()
    value = small_own[:, slice_of(ring.me)]
    for k in range(ranks - 1):
        value = value + small_got[k]
    small_part[...] = value
    last = to_peers(lambda k: small_part, lambda slot: small_z.at[slot], h_sends, h_recvs)
    for copy in last:
        copy.start()
    out_mine = output_ref.at[pl.ds(first, rows)]
    outputs_out = to_peers(lambda k: out_low, lambda slot: out_mine, y_sends, y_recvs)
    for copy in outputs_out:
        copy.start()
    stores.append(pltpu.make_async_copy(out_low, out_mine, local_sem.at[6]))
    stores[1].start()
    for piece in range(pieces):

        def emit_qkv(spot, start, count, value, piece=piece):
            qkv_sum_ref[pl.ds(pl.multiple_of(piece * size + start, count), count), :] = value

        def emit_proj(spot, start, count, value, piece=piece):
            proj_sum_ref[pl.ds(pl.multiple_of(piece * proj_size + start, count), count), :] = value

        works[2 * piece].total(emit_qkv)
        works[2 * piece + 1].total(emit_proj)
    for copy in last:
        copy.wait_recv()
    value = small_part[...]
    for k in range(peers - 1):
        value = value + small_z[k]
    small_sum_ref[...] = value
    keep.wait()
    for copy in stores:
        copy.wait()
    for k in far_first:
        z_copy(k).wait_send()
    for copy in exchanged + summed + handed + last:
        copy.wait_send()
    for copy in shared + inputs_out + outputs_out:
        copy.wait()
    for k in outs:
        outs[k].finish()
    for work in works:
        work.finish()


def rear(
    layout,
    back_part,
    out_part,
    x_all,
    cot_all,
    grads,
    scaled,
    rows_all,
    columns_all,
    middle,
    cotangent,
    tokens,
    attn_in,
    queries,
    keys,
    values,
    context,
    probs,
    cosine,
    sine,
    small_rows,
    with_out,
    ranks,
    peers,
    identity,
):
    chips = ranks // 2
    block, width = tokens.shape
    total = x_all.shape[0]
    rows = block // peers
    hidden, own = layout.hidden, layout.shared_own
    experts, units = layout.local_experts, layout.expert_hidden
    head_width = queries.shape[1]
    columns = width // ranks
    pieces = 4
    tile = 256
    vmem = pl.BlockSpec(memory_space=pltpu.VMEM)
    hbm = pl.BlockSpec(memory_space=pl.ANY)
    dma = pltpu.SemaphoreType.DMA
    low, f32 = tokens.dtype, jnp.float32
    shape = jax.ShapeDtypeStruct
    return pl.pallas_call(
        functools.partial(rear_kernel, layout, ranks, peers, with_out),
        out_shape=(
            shape((block, width), low),
            shape((block, width), low),
            shape((columns, 3 * head_width), f32),
            shape((head_width, columns), f32),
            shape((small_rows, columns), f32),
            *[shape((experts, units, width), low)] * 3,
            shape((3, own, width), low),
            shape((ranks, 3, own, columns), low),
        ),
        in_specs=[hbm] * 8 + [vmem] + [hbm] * 2 + [vmem] * 8,
        out_specs=(hbm, hbm, vmem, vmem, vmem, hbm, hbm, hbm, hbm, hbm),
        scratch_shapes=[
            pltpu.VMEM((rows, width), low),
            pltpu.VMEM((rows, width), low),
            pltpu.VMEM((small_rows, width), low),
            pltpu.VMEM((rows, width), f32),
            pltpu.VMEM((small_rows, width), f32),
            pltpu.VMEM((ranks - 1, small_rows, columns), f32),
            pltpu.VMEM((small_rows, columns), f32),
            pltpu.VMEM((peers - 1, small_rows, columns), f32),
            pltpu.VMEM((peers, rows, width), low),
            pltpu.VMEM((peers - 1, rows, width), low),
            pltpu.VMEM((peers - 1, rows, width), low),
            pltpu.VMEM((peers - 1, rows, width), low),
            pltpu.VMEM((rows, width), low),
            pltpu.VMEM((block, width), low),
            pltpu.VMEM((2, total, tile), low),
            pltpu.VMEM((total, hidden), low),
            pltpu.VMEM((hidden, total), low),
            pltpu.VMEM((2, layout.shared_at, tile), low),
            pltpu.VMEM((2, own, tile), low),
            pltpu.VMEM((1, width), f32),
            pltpu.VMEM((width, 3 * head_width), low),
            pltpu.VMEM((block, head_width), low),
            pltpu.VMEM((block, 3 * head_width), low),
            pltpu.VMEM((block, width), low),
            pltpu.VMEM((block, width), low),
            pltpu.VMEM((3, own, columns), low),
        ]
        + [dma((peers - 1,))] * 14
        + [dma((ranks - 1,))] * 4
        + [
            dma((7,)),
            dma,
            dma((2,)),
            dma((2 * (experts + 1),)),
            pltpu.SemaphoreType.REGULAR,
        ]
        + reduce_buffers(peers, chips, rows, width, low)
        + reduce_sems(peers, chips)
        + reduce_sems(pieces, chips)
        + reduce_buffers(pieces, chips, head_width // pieces, columns, low)
        + reduce_sems(pieces, chips)
        + (reduce_buffers(peers, chips, rows, width, low) + reduce_sems(peers, chips)) * with_out,
        compiler_params=pltpu.CompilerParams(
            collective_id=identity, has_side_effects=True, vmem_limit_bytes=67043328
        ),
        name="rear",
    )(
        back_part,
        out_part,
        x_all,
        cot_all,
        grads,
        scaled,
        rows_all,
        columns_all,
        middle,
        cotangent,
        tokens,
        attn_in,
        queries,
        keys,
        values,
        context,
        probs,
        cosine,
        sine,
    )


def rope_tables():
    half_dim = HEAD_DIM // 2
    exponent = np.arange(half_dim, dtype=np.float32) * np.float32(2.0 / HEAD_DIM)
    inverse_freq = np.exp(-exponent * np.log(np.float32(1000000.0)))
    angles = np.arange(SEQ, dtype=np.float32)[:, None] * inverse_freq[None, :]
    cosine, sine = np.cos(angles), np.sin(angles)
    return (
        jnp.asarray(np.concatenate([cosine, cosine], axis=1)),
        jnp.asarray(np.concatenate([-sine, sine], axis=1)),
    )


def scatter_rows(values):
    return lax.psum_scatter(values, "dp", scatter_dimension=0, tiled=True)


def shards(
    tokens,
    w_query,
    w_key,
    w_value,
    w_out,
    gain_attn,
    gain_ffn,
    w_router,
    shared_gate,
    shared_up,
    shared_down,
    shared_switch,
    expert_gate,
    expert_up_weight,
    expert_down,
    routes,
    segments,
    cotangent,
):
    low = jnp.bfloat16
    ranks = lax.axis_size("dp")
    peers = lax.axis_size("tensor")
    token_count, width = tokens.shape
    local_experts, _, expert_hidden = expert_gate.shape
    expert_count = local_experts * ranks
    block = width // ranks
    head_width = w_query.shape[1]
    shared_width = shared_gate.shape[1]
    shared_own = shared_width // ranks
    small_pad = 128
    layout = Layout(local_experts, expert_hidden, shared_own, expert_count)
    lane0 = layout.router_lane

    small_rows = -(-(expert_count + 3) // 16) * 16
    spots = jnp.arange(small_pad, dtype=jnp.int32)[None, None, :] - lane0
    chosen = jnp.sum((routes[:, :, None] == spots).astype(jnp.float32), axis=1).astype(low)
    fold = token_count // block
    chosen = chosen.reshape(fold, block, small_pad).transpose(1, 0, 2).reshape(block, fold * small_pad)
    vectors = jnp.stack([shared_switch, gain_attn, gain_ffn])
    cosine, sine = rope_tables()
    spots = jnp.arange(SEQ, dtype=jnp.int32)
    allowed = (spots[None, :] <= spots[:, None]) & (segments[0][None, :] == segments[0][:, None])

    (
        qkv_full,
        columns_full,
        attn_in,
        queries,
        key_rows,
        value_rows,
        context_flat,
        probs,
        x_all,
        cot_all,
        middle,
        scaled_hidden,
        grads_wide,
        out_part,
        back_part,
    ) = layer_forward_back(
        layout,
        w_query,
        w_key,
        w_value,
        chosen,
        w_out,
        w_router.T,
        vectors,
        tokens,
        cotangent,
        allowed.astype(jnp.float32),
        cosine,
        sine,
        expert_gate.swapaxes(1, 2),
        expert_up_weight.swapaxes(1, 2),
        expert_down,
        shared_gate.T.reshape(ranks, shared_own, block),
        shared_up.T.reshape(ranks, shared_own, block),
        shared_down.reshape(ranks, shared_own, block),
        small_rows,
        ranks,
        peers,
        1,
    )
    with_out = ranks == 8
    grad_input, output, grad_qkv, grad_proj, grad_small, *grad_experts, _, grad_shared = rear(
        layout,
        back_part,
        out_part if with_out else scatter_rows(out_part),
        x_all,
        cot_all,
        grads_wide,
        scaled_hidden,
        qkv_full,
        columns_full,
        middle,
        cotangent,
        tokens,
        attn_in,
        queries,
        key_rows,
        value_rows,
        context_flat,
        probs,
        cosine,
        sine,
        small_rows,
        with_out,
        ranks,
        peers,
        2,
    )
    grad_experts = [grads.astype(jnp.float32) for grads in grad_experts]
    grad_shared = grad_shared.astype(jnp.float32)
    return (
        output,
        grad_input.astype(jnp.float32),
        grad_qkv[:, :head_width],
        grad_qkv[:, head_width : 2 * head_width],
        grad_qkv[:, 2 * head_width :],
        grad_proj,
        grad_small[expert_count + 1],
        grad_small[expert_count + 2],
        grad_small[:expert_count].T,
        grad_shared[:, 0].reshape(shared_width, block).T,
        grad_shared[:, 1].reshape(shared_width, block).T,
        grad_shared[:, 2].reshape(shared_width, block),
        grad_small[expert_count],
        grad_experts[0].swapaxes(1, 2),
        grad_experts[1].swapaxes(1, 2),
        grad_experts[2],
    )


def solution(mesh):
    in_specs = (
        P("dp", None),
        P("dp", "tensor"),
        P("dp", "tensor"),
        P("dp", "tensor"),
        P("tensor", "dp"),
        P("dp"),
        P("dp"),
        P("dp", None),
        P("dp", "tensor"),
        P("dp", "tensor"),
        P("tensor", "dp"),
        P("dp"),
        P("dp", None, "tensor"),
        P("dp", None, "tensor"),
        P("dp", "tensor", None),
        P("dp", None),
        P("dp", None),
        P("dp", None),
    )
    out_specs = (
        P("dp", None),
        P("dp", None),
        P("dp", "tensor"),
        P("dp", "tensor"),
        P("dp", "tensor"),
        P("tensor", "dp"),
        P("dp"),
        P("dp"),
        P("dp", None),
        P("dp", "tensor"),
        P("dp", "tensor"),
        P("tensor", "dp"),
        P("dp"),
        P("dp", None, "tensor"),
        P("dp", None, "tensor"),
        P("dp", "tensor", None),
    )
    return jax.shard_map(shards, mesh=mesh, in_specs=in_specs, out_specs=out_specs, check_vma=False)
```

```python
import functools

import jax
import jax.numpy as jnp
import numpy as np
from jax import lax
from jax.experimental import pallas as pl
from jax.experimental.pallas import tpu as pltpu
from jax.sharding import PartitionSpec as P

HEAD_DIM = 128
TOP = 4
SEQ = 256


EPSILON = 1e-06
MESH = pl.DeviceIdType.MESH


def ring_chip(position, chips):
    half = chips // 2
    upper = position // half
    return position + upper * (chips - 1 + half - 2 * position)


def ring_spot(chip, chips):
    return ring_chip(chip, chips)


def greet(partners):
    barrier = pltpu.get_barrier_semaphore()
    for partner in partners:
        pl.semaphore_signal(barrier, inc=1, device_id=partner, device_id_type=MESH)
    pl.semaphore_wait(barrier, len(partners))


def remote(source, target, axis, device, sends, recvs, slot):
    return pltpu.make_async_remote_copy(
        src_ref=source,
        dst_ref=target,
        send_sem=sends.at[slot],
        recv_sem=recvs.at[slot],
        device_id={axis: device},
        device_id_type=MESH,
    )


class Ring:
    def __init__(self, ranks):
        self.ranks = ranks
        self.chips = ranks // 2
        self.half = self.chips // 2
        self.me = lax.axis_index("dp")
        self.core = self.me % 2
        self.position = ring_spot(self.me // 2, self.chips)
        self.sibling = self.me + 1 - 2 * self.core
        self.ahead = self.device(1)
        self.behind = self.device(-1)

    def chip(self, offset):
        return ring_chip((self.position + offset + self.chips) % self.chips, self.chips)

    def device(self, offset):
        return self.chip(offset) * 2 + self.core

    def other(self, offset):
        return self.chip(offset) * 2 + 1 - self.core

    def partners(self):
        return [{"dp": self.ahead}, {"dp": self.behind}, {"dp": self.sibling}]


def gather_slots(half):
    return 2 * half


def side_slots(half):
    return 2 * half


class RingGather:
    def __init__(self, ring, place, rows, sends, recvs, side_sends, side_recvs, base, side_base):
        self.ring, self.place, self.rows, self.cut = ring, place, rows, rows // 2
        self.sends, self.recvs = sends, recvs
        self.side_sends, self.side_recvs = side_sends, side_recvs
        self.base, self.side_base = base, side_base
        self.sides = side_slots(ring.half)

    def hop_copy(self, source, target, device, slot):
        return remote(source, target, "dp", device, self.sends, self.recvs, self.base + slot)

    def side_copy(self, source, target, slot):
        return remote(
            source,
            target,
            "dp",
            self.ring.sibling,
            self.side_sends,
            self.side_recvs,
            self.side_base + slot,
        )

    def hop_size(self, slot):
        number = slot % self.ring.half
        return self.cut if number and number == self.ring.half - 1 else self.rows

    def begin(self, source):
        ring = self.ring
        target = self.place(ring.me, 0, self.rows)
        self.hop_copy(source, target, ring.ahead, 0).start()
        self.hop_copy(source, target, ring.behind, ring.half).start()
        self.side_copy(source, target, 0).start()

    def wait_hop(self, slot):
        block = self.place(self.ring.me, 0, self.hop_size(slot))
        self.hop_copy(block, block, self.ring.ahead, slot).wait_recv()

    def step(self, number):
        ring = self.ring
        for which, sign in enumerate((-1, 1)):
            owner = ring.device(sign * number)
            onward = (ring.ahead, ring.behind)[which]
            self.wait_hop(which * ring.half + number - 1)
            if number < ring.half:
                block = self.place(owner, 0, self.rows)
                slot = which * ring.half + number
                size = self.hop_size(slot)
                part = block if size == self.rows else self.place(owner, (0, self.cut)[which], size)
                self.hop_copy(part, part, onward, slot).start()
                self.side_copy(block, block, 2 * number - 1 + which).start()
        if number == ring.half:
            block = self.place(ring.device(number), 0, self.rows)
            self.side_copy(block, block, 2 * ring.half - 1).start()

    def wait_side(self, index):
        block = self.place(self.ring.me, 0, self.rows)
        self.side_copy(block, block, index).wait_recv()

    def sent(self):
        for slot in range(2 * self.ring.half):
            block = self.place(self.ring.me, 0, self.hop_size(slot))
            self.hop_copy(block, block, self.ring.ahead, slot).wait_send()
        for index in range(self.sides):
            block = self.place(self.ring.me, 0, self.rows)
            self.side_copy(block, block, index).wait_send()


def near_first(peers):
    order = [0]
    for step in range(1, peers // 2 + 1):
        order.append(step)
        if peers - step != step:
            order.append(peers - step)
    return order


STRIP = 64
BACK_DUE = (0, 5, 11, 11, 17)


def strips(rows, body):
    strip = min(STRIP, rows)

    def step(index, carry):
        body(pl.ds(pl.multiple_of(index * strip, strip), strip), index * strip, strip)
        return carry

    lax.fori_loop(0, rows // strip, step, 0)


HIDDEN_TILE, OUT_TILE, BACK_TILE = 1024, 1024, 1024


def matmul(left, right):
    return lax.dot_general(
        left, right, (((1,), (0,)), ((), ())), preferred_element_type=jnp.float32
    )


def matmul_last(left, right):
    return lax.dot_general(
        left, right, (((1,), (1,)), ((), ())), preferred_element_type=jnp.float32
    )


def tiles(width, tile, body):
    def step(index, carry):
        body(pl.ds(pl.multiple_of(index * tile, tile), tile))
        return carry

    lax.fori_loop(0, width // tile, step, 0)


class Layout:
    def __init__(self, local_experts, expert_hidden, shared_own, expert_count):
        self.local_experts = local_experts
        self.expert_hidden = expert_hidden
        self.shared_own = shared_own
        self.expert_count = expert_count
        self.part = -(-expert_hidden // 128) * 128
        self.shared_at = local_experts * self.part
        self.router_at = self.shared_at + shared_own
        self.last = -(-(shared_own + expert_count + 1) // 128) * 128
        self.hidden = self.shared_at + self.last
        self.router_tile = self.router_at // 128 * 128
        self.router_lane = self.router_at - self.router_tile
        self.tile = next(size for size in (HIDDEN_TILE, 256, 128) if self.hidden % size == 0)


def hidden_tiles(layout, x_ref, gates, ups, pre_gate, pre_up):
    def body(spot):
        pre_gate[:, spot] = matmul_last(x_ref[...], gates[spot, :])
        pre_up[:, spot] = matmul_last(x_ref[...], ups[spot, :])

    tiles(layout.hidden, layout.tile, body)


def cot_tiles(layout, cot_ref, downs, cot_hidden):
    def body(spot):
        cot_hidden[:, spot] = matmul_last(cot_ref[...], downs[spot, :]).astype(cot_hidden.dtype)

    tiles(layout.hidden, layout.tile, body)


def gate_strips(layout, first_expert, chosen, pre_gate, pre_up, cot_hidden, scaled, grads):
    rows = pre_gate.shape[0]
    count, lane0 = layout.expert_count, layout.router_lane
    router = slice(layout.router_tile, layout.router_tile + 128)
    bounds = [(j * layout.part, (j + 1) * layout.part) for j in range(layout.local_experts)]
    bounds.append((layout.shared_at, layout.hidden))
    low = scaled.dtype

    def body(spot, start, size):
        lane = lax.broadcasted_iota(jnp.int32, (size, 128), 1)
        logits = pre_gate[spot, router]
        is_router = (lane >= lane0) & (lane < lane0 + count)
        is_switch = lane == lane0 + count
        power = jnp.where(is_router, jnp.exp(jnp.where(is_router, logits, 0.0)), 0.0)
        probs = power / jnp.sum(power, axis=-1, keepdims=True)
        raw = jnp.sum(jnp.where(is_switch, logits, 0.0), axis=-1, keepdims=True)
        switch = 1.0 / (1.0 + jnp.exp(-raw))
        mask = chosen[spot, :].astype(jnp.float32)
        scales = []
        for j in range(layout.local_experts):
            spotted = lane == lane0 + first_expert + j
            scales.append(jnp.sum(jnp.where(spotted, probs * mask, 0.0), axis=-1, keepdims=True))
        scales.append(switch)
        totals = []
        for (begin, end), scale in zip(bounds, scales):
            shared = begin == layout.shared_at
            columns = slice(begin, end)
            gate, up = pre_gate[spot, columns], pre_up[spot, columns]
            through = cot_hidden[spot, columns].astype(jnp.float32)
            sig = 1.0 / (1.0 + jnp.exp(-gate))
            act = gate * sig
            state = act * up
            grad = scale * through
            totals.append(jnp.sum(state * through, axis=-1, keepdims=True))
            scaled[spot, columns] = (scale * state).astype(low)
            grad_gate = grad * up * sig * (1.0 + gate * (1.0 - sig))
            grads[spot, columns] = grad_gate.astype(low)
            grads[spot, layout.hidden + begin : layout.hidden + end] = (grad * act).astype(low)
        choice = jnp.zeros_like(probs)
        for j in range(layout.local_experts):
            spotted = lane == lane0 + first_expert + j
            choice = choice + jnp.where(spotted, mask * totals[j], 0.0)
        small = probs * (choice - jnp.sum(probs * choice, axis=-1, keepdims=True))
        small = jnp.where(is_switch, totals[-1] * switch * (1.0 - switch), small)
        kept = grads[spot, router].astype(jnp.float32)
        kept = jnp.where(is_router | is_switch, small, kept)
        grads[spot, router] = kept.astype(low)

    strips(rows, body)


def out_tiles(width, scaled, downs, out):
    def body(spot):
        out[:, spot] = matmul(scaled[...], downs[:, spot]).astype(out.dtype)

    tiles(width, OUT_TILE, body)


def back_tiles(layout, width, grads, gates, ups, back):
    hidden = layout.hidden

    def body(spot):
        total = matmul(grads[:, :hidden], gates[:, spot])
        total = total + matmul(grads[:, hidden:], ups[:, spot])
        back[:, spot] = total.astype(back.dtype)

    tiles(width, BACK_TILE, body)


def rope(values, cosine, sine, sign):
    return values * cosine + pltpu.roll(values, HEAD_DIM // 2, 1) * (sine * sign)


def attend(heads, qkv, allowed_ref, cos_ref, sin_ref, queries, keys, values, probs_ref, context):
    cosine, sine = cos_ref[...], sin_ref[...]
    allowed = allowed_ref[...] > 0.5
    low = queries.dtype
    for head in range(heads):
        columns = slice(head * HEAD_DIM, (head + 1) * HEAD_DIM)
        query = rope(qkv(head), cosine, sine, 1.0).astype(low)
        key = rope(qkv(heads + head), cosine, sine, 1.0).astype(low)
        value = qkv(2 * heads + head).astype(low)
        queries[:, columns], keys[:, columns], values[:, columns] = query, key, value
        scores = matmul_last(query, key) * HEAD_DIM ** (-0.5)
        power = jnp.where(allowed, jnp.exp(jnp.where(allowed, scores, 0.0)), 0.0)
        probs = power / jnp.sum(power, axis=-1, keepdims=True)
        probs_ref[head] = probs
        context[:, columns] = matmul(probs.astype(low), value).astype(low)


def layer_kernel(
    layout,
    ranks,
    peers,
    query_ref,
    key_ref,
    value_ref,
    chosen_own_ref,
    proj_ref,
    router_ref,
    vectors_ref,
    tokens_ref,
    cot_ref,
    allowed_ref,
    cos_ref,
    sin_ref,
    expert_gate_ref,
    expert_up_ref,
    expert_down_ref,
    shared_gate_ref,
    shared_up_ref,
    shared_down_ref,
    rows_all,
    columns_all,
    attn_in,
    queries,
    keys,
    values,
    context,
    probs_ref,
    x_all,
    cot_all,
    middle_ref,
    scaled_ref,
    grads_ref,
    out_ref,
    back_ref,
    row_stage,
    column_stage,
    rows_full,
    columns_full,
    qkv_raw,
    part_ref,
    gates,
    ups,
    downs,
    shared_got,
    own,
    got,
    x_block,
    cot_block,
    pre_gate,
    pre_up,
    cot_hidden,
    scaled,
    grads,
    out,
    back,
    chosen,
    local_sem,
    gather_sem,
    a_sends,
    a_recvs,
    a_side_sends,
    a_side_recvs,
    block_sem,
    x_sem,
    store_sem,
    shared_sends,
    shared_recvs,
    z_sends,
    z_recvs,
    x_sends,
    x_recvs,
    sends,
    recvs,
    side_sends,
    side_recvs,
    c_sends,
    c_recvs,
    c_side_sends,
    c_side_recvs,
):
    ring = Ring(ranks)
    here = lax.axis_index("tensor")
    block, width = tokens_ref.shape
    rows = block // peers
    depth = width // ranks
    half = ring.half
    away = [(here + k) % peers for k in range(peers)]
    others = [(ring.me + k) % ranks for k in range(ranks)]

    count, lane0 = layout.expert_count, layout.router_lane
    head_width = query_ref.shape[1]
    heads = head_width // HEAD_DIM
    lot, wide = row_stage.shape
    height = column_stage.shape[0]
    small_rows = height - head_width
    low = gates.dtype
    loads, start = [], 0
    for index, source in enumerate((query_ref, key_ref, value_ref, chosen_own_ref)):
        size = source.shape[1]
        loads.append(
            pltpu.make_async_copy(source, row_stage.at[:, pl.ds(start, size)], gather_sem.at[index])
        )
        start += size
    loads.append(
        pltpu.make_async_copy(
            proj_ref, column_stage.at[pl.ds(small_rows, head_width)], gather_sem.at[4]
        )
    )
    for load in loads:
        load.start()
    small = jnp.concatenate(
        [
            router_ref[...].astype(jnp.float32),
            vectors_ref[...].astype(jnp.float32),
            jnp.zeros((small_rows - count - vectors_ref.shape[0], depth), jnp.float32),
        ],
        axis=0,
    )
    column_stage[:small_rows, :] = small.astype(low)
    greet(
        [{"dp": others[k]} for k in range(1, ranks)] + [{"tensor": away[k]} for k in range(1, peers)]
    )
    order = near_first(peers)

    def row_place(device, first, size):
        return rows_all.at[pl.ds(device * lot + first, size)]

    def column_place(device, first, size):
        place = pl.ds(pl.multiple_of(device * depth, depth), depth)
        return columns_all.at[pl.ds(first, size), place]

    for load in loads:
        load.wait()
    gathers = [
        RingGather(ring, row_place, lot, a_sends, a_recvs, a_side_sends, a_side_recvs, 0, 0),
        RingGather(
            ring,
            column_place,
            height,
            a_sends,
            a_recvs,
            a_side_sends,
            a_side_recvs,
            gather_slots(half),
            side_slots(half),
        ),
    ]
    stores_own = []
    for index, (gather, stage) in enumerate(zip(gathers, (row_stage, column_stage))):
        gather.begin(stage)
        store = pltpu.make_async_copy(
            stage, gather.place(ring.me, 0, gather.rows), gather_sem.at[5 + index]
        )
        store.start()
        stores_own.append(store)
    for number in range(1, half):
        for gather in gathers:
            gather.step(number)

    experts, hid = layout.local_experts, layout.expert_hidden
    wides = (gates, ups, downs)
    loads = []
    for which, (target, source) in enumerate(
        zip(wides, (expert_gate_ref, expert_up_ref, expert_down_ref))
    ):
        for j in range(experts):
            load = pltpu.make_async_copy(
                source.at[j],
                target.at[pl.ds(j * layout.part, hid)],
                local_sem.at[5 + which * experts + j],
            )
            load.start()
            loads.append(load)
            if layout.part > hid:
                target[j * layout.part + hid : (j + 1) * layout.part, :] = jnp.zeros(
                    (layout.part - hid, width), low
                )
        target[layout.router_at :, :] = jnp.zeros((layout.hidden - layout.router_at, width), low)

    for gather in gathers:
        gather.step(half)

    shared_refs = (shared_gate_ref, shared_up_ref, shared_down_ref)
    handed, kept = [], []
    for k in range(1, ranks):
        for which, source in enumerate(shared_refs):
            copy = remote(
                source.at[others[k]],
                shared_got.at[which, ring.me],
                "dp",
                others[k],
                shared_sends,
                shared_recvs,
                which * (ranks - 1) + ranks - k - 1,
            )
            copy.start()
            handed.append(copy)
    for which, source in enumerate(shared_refs):
        copy = pltpu.make_async_copy(
            source.at[ring.me], shared_got.at[which, ring.me], local_sem.at[which]
        )
        copy.start()
        kept.append(copy)

    def cot_place(device, start, size):
        return cot_all.at[pl.ds(device * block + start, size)]

    cots = RingGather(
        ring, cot_place, block, c_sends, c_recvs, c_side_sends, c_side_recvs, 0, 0
    )
    cots.begin(cot_ref)
    kept_cot = pltpu.make_async_copy(cot_ref, cot_place(ring.me, 0, block), local_sem.at[3])
    kept_cot.start()

    for store in stores_own:
        store.wait()
    for gather in gathers:
        for index in range(gather.sides):
            gather.wait_side(index)
    fetches = [
        pltpu.make_async_copy(rows_all, rows_full, gather_sem.at[7]),
        pltpu.make_async_copy(
            columns_all.at[pl.ds(small_rows, head_width)],
            columns_full.at[pl.ds(small_rows, head_width)],
            gather_sem.at[8],
        ),
    ]
    first_rows = pltpu.make_async_copy(
        columns_all.at[pl.ds(0, small_rows)],
        columns_full.at[pl.ds(0, small_rows)],
        gather_sem.at[9],
    )
    first_rows.start()
    for fetch in fetches:
        fetch.start()
    first_rows.wait()
    gates[layout.router_at : layout.router_at + count + 1, :] = columns_full[: count + 1, :]
    vectors = columns_full[:small_rows, :].astype(jnp.float32)
    attn_gain = vectors[count + 1 : count + 2, :]
    ffn_gain = vectors[count + 2 : count + 3, :]

    def norm_in(spot, start, size):
        value = tokens_ref[spot, :].astype(jnp.float32)
        inverse = lax.rsqrt(jnp.mean(value * value, axis=-1, keepdims=True) + EPSILON)
        attn_in[spot, :] = ((value * inverse) * attn_gain).astype(low)

    strips(block, norm_in)
    fetches[0].wait()

    def project(spot):
        qkv_raw[:, spot] = matmul(attn_in[...], rows_full[:, spot])

    tiles(3 * head_width, 256, project)

    def qkv(index):
        return qkv_raw[:, index * HEAD_DIM : (index + 1) * HEAD_DIM]

    attend(heads, qkv, allowed_ref, cos_ref, sin_ref, queries, keys, values, probs_ref, context)

    fetches[1].wait()

    def project_out(spot):
        part_ref[:, spot] = matmul(context[...], columns_full[small_rows:, spot]).astype(low)

    tiles(width, 256, project_out)

    exchanged = []
    for k in reversed(order[1:]):
        copy = remote(
            part_ref.at[pl.ds(away[k] * rows, rows)],
            got.at[peers - k - 1],
            "tensor",
            away[k],
            z_sends,
            z_recvs,
            peers - k - 1,
        )
        copy.start()
        exchanged.append(copy)

    for copy in kept + loads:
        copy.wait()
    for copy in handed:
        copy.wait_recv()
    for which, target in enumerate(wides):
        for source in range(ranks):
            columns = slice(source * depth, (source + 1) * depth)
            target[layout.shared_at : layout.router_at, columns] = shared_got[which, source]

    chip_rows = 2 * block

    def chip_spot(turn):
        offset = (1 - 2 * (turn % 2)) * ((turn + 1) // 2)
        return pl.ds(pl.multiple_of(ring.chip(offset) * chip_rows, chip_rows), chip_rows)

    def cot_turn(turn, slot):
        cots.wait_side(turn)
        load_cot = pltpu.make_async_copy(cot_all.at[chip_spot(turn)], cot_block, block_sem.at[0])
        load_cot.start()
        load_cot.wait()
        cot_tiles(layout, cot_block, downs, cot_hidden.at[slot])

    kept_cot.wait()
    cot_turn(0, 0)

    for copy in exchanged:
        copy.wait()
    first = here * rows

    def norm(spot, start, size):
        mine = pl.ds(pl.multiple_of(first + start, size), size)
        total = part_ref[mine, :].astype(jnp.float32)
        for k in range(peers - 1):
            total = total + got[k, spot, :].astype(jnp.float32)
        middle = tokens_ref[mine, :].astype(jnp.float32) + total
        middle_ref[spot, :] = middle
        inverse = lax.rsqrt(jnp.mean(middle * middle, axis=-1, keepdims=True) + EPSILON)
        own[spot, :] = ((middle * inverse) * ffn_gain).astype(own.dtype)

    strips(rows, norm)

    def place_of(k):
        def place(device, start, size):
            return x_all.at[pl.ds(device * block + away[k] * rows + start, size)]

        return place

    mine = place_of(0)(ring.me, 0, rows)

    def peer_place(device, start, size):
        return x_all.at[pl.ds(ring.me * block + device * rows + start, size)]

    forwards = TensorGather(peers, own, peer_place, rows, x_sends, x_recvs)
    forwards.begin()
    works = [
        RingGather(
            ring,
            place_of(k),
            rows,
            sends,
            recvs,
            side_sends,
            side_recvs,
            k * gather_slots(half),
            k * side_slots(half),
        )
        for k in range(peers)
    ]
    works[0].begin(own)
    store = pltpu.make_async_copy(own, mine, local_sem.at[4])
    store.start()

    half_peers = peers // 2
    for number in range(1, half_peers + 1):
        forwards.step(number)
        for k in sorted({peers - number, number}):
            works[k].begin(place_of(k)(ring.me, 0, rows))
        if number == 1:
            cots.step(1)
    store.wait()
    passing = [works[k] for k in order]
    cuts = [part * len(passing) // 4 for part in range(5)]
    first_expert = ring.me * experts

    def stores(spot):
        return [
            pltpu.make_async_copy(source, target.at[spot], store_sem.at[slot])
            for slot, (source, target) in enumerate(
                ((scaled, scaled_ref), (grads, grads_ref), (out, out_ref), (back, back_ref))
            )
        ]

    def fetch_x(turn):
        return pltpu.make_async_copy(
            x_all.at[chip_spot(turn)], x_block.at[turn % 2], x_sem.at[turn % 2]
        )

    for work in works:
        work.wait_side(0)
    fetch_x(0).start()

    def chip_step(turn, carry):
        offset = (1 - 2 * (turn % 2)) * ((turn + 1) // 2)
        spot = chip_spot(turn)
        slot = turn - turn // 4 * (turn - 3)

        def pass_on(part):
            @pl.when(turn == 0)
            def _():
                for work in passing[cuts[part] : cuts[part + 1]]:
                    work.step(1)

        def pass_on_far():
            for number in range(2, half + 1):

                @pl.when(turn == 2 * number - 2)
                def _(number=number):
                    for work in [cots] + passing:
                        work.step(number)

        def fetch_next():
            for work in works:
                work.wait_side(turn + 1)
            fetch_x(turn + 1).start()

        for device in range(2):
            for fold in range(block // lot):
                there = ring.chip(offset) * 2 * lot + device * lot
                first_lane = 3 * head_width + fold * 128
                chosen[device * block + fold * lot : device * block + (fold + 1) * lot, :] = rows_full[
                    pl.ds(pl.multiple_of(there, lot), lot), first_lane : first_lane + 128
                ]
        fetch_x(turn).wait()
        hidden_tiles(layout, x_block.at[turn % 2], gates, ups, pre_gate, pre_up)
        pass_on(0)
        pass_on_far()

        @pl.when(turn == 0)
        def _():
            cot_turn(1, 1)

        @pl.when(turn > 2)
        def _():
            cot_turn(turn, 3)

        pending = stores(spot)

        @pl.when(turn > 0)
        def _():
            pending[0].wait()
            pending[1].wait()

        gate_strips(
            layout,
            first_expert,
            chosen,
            pre_gate,
            pre_up,
            cot_hidden.at[slot],
            scaled,
            grads,
        )
        pending[0].start()
        pending[1].start()
        pass_on(1)

        @pl.when(turn > 0)
        def _():
            pending[2].wait()
            pending[3].wait()

        out_tiles(width, scaled, downs, out)
        pending[2].start()

        @pl.when(turn == 0)
        def _():
            cot_turn(2, 2)

        pass_on(2)

        @pl.when((turn > 0) & (turn + 1 < ring.chips))
        def _():
            fetch_next()

        back_tiles(layout, width, grads, gates, ups, back)
        pending[3].start()
        pass_on(3)

        @pl.when(turn == 0)
        def _():
            fetch_next()

        return carry

    lax.fori_loop(0, ring.chips, chip_step, 0)
    for copy in stores(pl.ds(0, chip_rows)):
        copy.wait()
    forwards.sent()
    for copy in handed:
        copy.wait_send()
    for gather in gathers:
        gather.sent()
    cots.sent()
    for work in works:
        work.sent()


def layer_forward_back(
    layout,
    query,
    key,
    value,
    chosen,
    proj,
    router,
    vectors,
    tokens,
    cot,
    allowed,
    cosine,
    sine,
    expert_gate,
    expert_up,
    expert_down,
    shared_gate,
    shared_up,
    shared_down,
    small_rows,
    ranks,
    peers,
    identity,
):
    half = ranks // 4
    block, width = tokens.shape
    rows = block // peers
    total = ranks * block
    depth = width // ranks
    hidden = layout.hidden
    chip = 2 * block
    head_width = query.shape[1]
    wide = 3 * head_width + chosen.shape[1]
    height = small_rows + head_width
    low = tokens.dtype
    vmem = pl.BlockSpec(memory_space=pltpu.VMEM)
    hbm = pl.BlockSpec(memory_space=pl.ANY)
    dma = pltpu.SemaphoreType.DMA
    f32 = jnp.float32
    heads = head_width // HEAD_DIM
    small_ones = [jax.ShapeDtypeStruct((block, head_width), low)] * 4
    return pl.pallas_call(
        functools.partial(layer_kernel, layout, ranks, peers),
        out_shape=(
            jax.ShapeDtypeStruct((width, wide), low),
            jax.ShapeDtypeStruct((height, width), low),
            jax.ShapeDtypeStruct((block, width), low),
            *small_ones,
            jax.ShapeDtypeStruct((heads, block, block), f32),
            jax.ShapeDtypeStruct((total, width), low),
            jax.ShapeDtypeStruct((total, width), low),
            jax.ShapeDtypeStruct((rows, width), f32),
            jax.ShapeDtypeStruct((total, hidden), low),
            jax.ShapeDtypeStruct((total, 2 * hidden), low),
            jax.ShapeDtypeStruct((total, width), low),
            jax.ShapeDtypeStruct((total, width), low),
        ),
        in_specs=[hbm] * 5 + [vmem] * 7 + [hbm] * 6,
        out_specs=(hbm, hbm, *[vmem] * 6, hbm, hbm, vmem, hbm, hbm, hbm, hbm),
        scratch_shapes=[
            pltpu.VMEM((depth, wide), low),
            pltpu.VMEM((height, depth), low),
            pltpu.VMEM((width, wide), low),
            pltpu.VMEM((height, width), low),
            pltpu.VMEM((block, 3 * head_width), f32),
            pltpu.VMEM((block, width), low),
            pltpu.VMEM((hidden, width), low),
            pltpu.VMEM((hidden, width), low),
            pltpu.VMEM((hidden, width), low),
            pltpu.VMEM((3, ranks, layout.shared_own, depth), low),
            pltpu.VMEM((rows, width), low),
            pltpu.VMEM((peers - 1, rows, width), low),
            pltpu.VMEM((2, chip, width), low),
            pltpu.VMEM((chip, width), low),
            pltpu.VMEM((chip, hidden), f32),
            pltpu.VMEM((chip, hidden), f32),
            pltpu.VMEM((4, chip, hidden), low),
            pltpu.VMEM((chip, hidden), low),
            pltpu.VMEM((chip, 2 * hidden), low),
            pltpu.VMEM((chip, width), low),
            pltpu.VMEM((chip, width), low),
            pltpu.VMEM((chip, 128), low),
            dma((5 + 3 * layout.local_experts,)),
            dma((10,)),
            dma((2 * gather_slots(half),)),
            dma((2 * gather_slots(half),)),
            dma((2 * side_slots(half),)),
            dma((2 * side_slots(half),)),
            dma((2,)),
            dma((2,)),
            dma((4,)),
            dma((3 * (ranks - 1),)),
            dma((3 * (ranks - 1),)),
            dma((peers - 1,)),
            dma((peers - 1,)),
            dma((peers,)),
            dma((peers,)),
            dma((peers * gather_slots(half),)),
            dma((peers * gather_slots(half),)),
            dma((peers * side_slots(half),)),
            dma((peers * side_slots(half),)),
            dma((gather_slots(half),)),
            dma((gather_slots(half),)),
            dma((side_slots(half),)),
            dma((side_slots(half),)),
        ],
        compiler_params=pltpu.CompilerParams(
            collective_id=identity, has_side_effects=True, vmem_limit_bytes=62 << 20
        ),
        name="layer_forward_back",
    )(
        query,
        key,
        value,
        chosen,
        proj,
        router,
        vectors,
        tokens,
        cot,
        allowed,
        cosine,
        sine,
        expert_gate,
        expert_up,
        expert_down,
        shared_gate,
        shared_up,
        shared_down,
    )


class RingReduce:
    def __init__(self, ring, source_at, rows, buffers, sems, slot):
        self.ring, self.source_at, self.rows, self.cut = ring, source_at, rows, rows // 2
        self.mine, self.side, self.got = [buffer.at[slot] for buffer in buffers]
        self.loads, self.sends, self.recvs, self.side_sends, self.side_recvs = sems
        self.base, self.side_base = slot * 2 * ring.half, slot * ring.chips
        half = ring.half
        self.order = [half]
        for distance in range(half - 1, 0, -1):
            self.order += [distance, ring.chips - distance]
        self.order.append(0)

    def load(self, offset):
        return pltpu.make_async_copy(
            self.source_at(self.ring.device(offset)),
            self.mine.at[offset],
            self.loads.at[self.side_base + offset],
        )

    def side_copy(self, offset):
        return remote(
            self.source_at(self.ring.other(offset)),
            self.side.at[offset],
            "dp",
            self.ring.sibling,
            self.side_sends,
            self.side_recvs,
            self.side_base + offset,
        )

    def hand_over(self, offset):
        self.side_copy(offset).start()
        self.load(offset).start()

    def ready(self, offset):
        self.load(offset).wait()
        self.side_copy(offset).wait_recv()

    def hop(self, which, number):
        ring, half, cut = self.ring, self.ring.half, self.cut
        distance = half - number
        offset = distance if which == 0 else ring.chips - distance
        place = pl.ds((0, cut)[which], cut) if number == 0 else pl.ds(0, self.rows)
        return remote(
            self.mine.at[offset, place],
            self.got.at[which * half + number, place],
            "dp",
            (ring.ahead, ring.behind)[which],
            self.sends,
            self.recvs,
            self.base + which * half + number,
        )

    def add(self, offset, extra, first, size):
        def total(spot):
            mine = self.mine[offset, spot, :].astype(jnp.float32)
            return mine + self.side[offset, spot, :].astype(jnp.float32)

        def more(spot, start, count):
            here = pl.ds(pl.multiple_of(first + start, count), count)
            value = total(here) + extra[here, :].astype(jnp.float32)
            self.mine[offset, here, :] = value.astype(self.mine.dtype)

        rest, begin = self.rows - size, 0 if first else size

        def plain(spot, start, count):
            here = pl.ds(pl.multiple_of(begin + start, count), count)
            self.mine[offset, here, :] = total(here).astype(self.mine.dtype)

        if size:
            strips(size, more)
        if rest:
            strips(rest, plain)

    def step(self, number):
        ring, half, cut = self.ring, self.ring.half, self.cut
        if number == 0:
            self.ready(half)
            self.add(half, None, 0, 0)
            self.hop(0, 0).start()
            self.hop(1, 0).start()
            return
        for which in range(2):
            distance = half - number
            offset = distance if which == 0 else ring.chips - distance
            self.ready(offset)
            self.hop(which, number - 1).wait_recv()
            extra = self.got.at[which * half + number - 1]
            if number == 1:
                self.add(offset, extra, (0, cut)[which], cut)
            else:
                self.add(offset, extra, 0, self.rows)
            self.hop(which, number).start()

    def total(self, emit):
        half = self.ring.half
        self.ready(0)
        self.hop(0, half - 1).wait_recv()
        self.hop(1, half - 1).wait_recv()

        def body(spot, start, size):
            value = self.mine[0, spot, :].astype(jnp.float32) + self.side[0, spot, :].astype(jnp.float32)
            value = value + self.got[half - 1, spot, :].astype(jnp.float32)
            value = value + self.got[2 * half - 1, spot, :].astype(jnp.float32)
            emit(spot, start, size, value)

        strips(self.rows, body)

    def finish(self):
        for offset in range(self.ring.chips):
            self.side_copy(offset).wait_send()
        for number in range(self.ring.half):
            for which in range(2):
                self.hop(which, number).wait_send()


def reduce_buffers(pieces, chips, rows, width, low):
    return [pltpu.VMEM((pieces, chips, rows, width), low)] * 3


def reduce_sems(pieces, chips):
    dma = pltpu.SemaphoreType.DMA
    return [dma((pieces * chips,))] * 5


class TensorSum:
    def __init__(self, peers, own_at, got, sends, recvs):
        self.peers, self.half = peers, peers // 2
        self.here = lax.axis_index("tensor")
        self.own_at, self.got, self.sends, self.recvs = own_at, got, sends, recvs
        self.rows = got.shape[1]

    def hop(self, which, number):
        peers, half = self.peers, self.half
        cut = self.rows // 2
        distance = half - number
        k = distance if which == 0 else peers - distance
        if number == 0:
            place, slot = pl.ds((0, cut)[which], cut), 0
        else:
            place, slot = pl.ds(0, self.rows), which * (half - 1) + number
        device = (self.here + (1, peers - 1)[which]) % peers
        return remote(
            self.own_at(k).at[place],
            self.got.at[slot, place],
            "tensor",
            device,
            self.sends,
            self.recvs,
            which * half + number,
        )

    def begin(self):
        self.hop(0, 0).start()
        self.hop(1, 0).start()

    def send(self, k):
        half = self.half
        if k == half:
            self.begin()
            return
        which = 0 if k < half else 1
        number = half - (k if which == 0 else self.peers - k)
        self.hop(which, number - 1).wait_recv()
        own = self.own_at(k)
        cut = self.rows // 2
        first, size, slot = 0, self.rows, which * (half - 1) + number - 1
        if number == 1:
            first, size, slot = (0, cut)[which], cut, 0
        place = slice(first, first + size)
        value = own[place, :].astype(jnp.float32) + self.got[slot, place, :].astype(jnp.float32)
        own[place, :] = value.astype(own.dtype)
        self.hop(which, number).start()

    def arrived(self):
        self.hop(0, self.half - 1).wait_recv()
        self.hop(1, self.half - 1).wait_recv()

    def rest(self, spot):
        half = self.half
        if half == 1:
            return self.got[0, spot, :].astype(jnp.float32)
        value = self.got[half - 1, spot, :].astype(jnp.float32)
        return value + self.got[2 * half - 2, spot, :].astype(jnp.float32)

    def sent(self):
        for number in range(self.half):
            for which in range(2):
                self.hop(which, number).wait_send()


class TensorGather:
    def __init__(self, peers, source, place, rows, sends, recvs):
        self.peers, self.half = peers, peers // 2
        self.here = lax.axis_index("tensor")
        self.source, self.place, self.rows = source, place, rows
        self.sends, self.recvs = sends, recvs

    def hop(self, which, number):
        peers, half = self.peers, self.half
        cut = self.rows // 2
        owner = (self.here + (peers - number, number)[which]) % peers
        first, size = 0, self.rows
        if number and number == half - 1:
            first, size = (0, cut)[which], cut
        target = self.place(owner, first, size)
        source = self.source if number == 0 else target
        device = (self.here + (1, peers - 1)[which]) % peers
        return remote(
            source, target, "tensor", device, self.sends, self.recvs, which * half + number
        )

    def begin(self):
        self.hop(0, 0).start()
        self.hop(1, 0).start()

    def step(self, number):
        for which in range(2):
            self.hop(which, number - 1).wait_recv()
            if number < self.half:
                self.hop(which, number).start()

    def sent(self):
        for number in range(self.half):
            for which in range(2):
                self.hop(which, number).wait_send()


def attend_back(heads, queries, keys, values, probs_ref, grad_context, cos_ref, sin_ref, grads):
    cosine, sine = cos_ref[...], sin_ref[...]
    low = grads.dtype
    scale = HEAD_DIM ** (-0.5)
    for head in range(heads):
        columns = slice(head * HEAD_DIM, (head + 1) * HEAD_DIM)
        probs, through = probs_ref[head], grad_context[:, columns]
        grad_probs = matmul_last(through, values[:, columns])
        inner = jnp.sum(probs * grad_probs, axis=-1, keepdims=True)
        grad_scores = (probs * (grad_probs - inner)).astype(low)
        parts = (
            rope(matmul(grad_scores, keys[:, columns]) * scale, cosine, sine, -1.0),
            rope(matmul(grad_scores.T, queries[:, columns]) * scale, cosine, sine, -1.0),
            matmul(probs.astype(low).T, through),
        )
        for index, part in enumerate(parts):
            first = (index * heads + head) * HEAD_DIM
            grads[:, first : first + HEAD_DIM] = part.astype(low)


def rear_kernel(
    layout,
    ranks,
    peers,
    with_out,
    part_ref,
    out_part_ref,
    x_ref,
    cots_ref,
    grads_ref,
    scaled_ref,
    rows_all,
    columns_all,
    middle_ref,
    cot_ref,
    tokens_ref,
    attn_in,
    queries,
    keys,
    values,
    context,
    probs_ref,
    cos_ref,
    sin_ref,
    input_ref,
    output_ref,
    qkv_sum_ref,
    proj_sum_ref,
    small_sum_ref,
    gate_grads_ref,
    up_grads_ref,
    down_grads_ref,
    shared_grads_ref,
    shared_got_ref,
    cot_rows,
    token_rows,
    small_vec,
    grad_ref,
    small_own,
    small_got,
    small_part,
    small_z,
    z_stage,
    z_got,
    a_got,
    o_got,
    low_ref,
    gm_all,
    right,
    left,
    turned,
    product,
    shared_low,
    gain_grad,
    qkv_full,
    grad_context,
    grad_rows,
    attn_part,
    out_sum,
    kept,
    z_sends,
    z_recvs,
    m_sends,
    m_recvs,
    a_sends,
    a_recvs,
    o_sends,
    o_recvs,
    x_sends,
    x_recvs,
    y_sends,
    y_recvs,
    h_sends,
    h_recvs,
    g_sends,
    g_recvs,
    s_sends,
    s_recvs,
    local_sem,
    left_sem,
    right_sem,
    product_sem,
    reuse_sem,
    *refs,
):
    buffers = refs[0:3]
    back_sems, qkv_sems, proj_buffers, proj_sems = refs[3:8], refs[8:13], refs[13:16], refs[16:21]
    out_buffers, out_sems = refs[21:24], refs[24:]
    out_low = z_stage.at[0]
    ring = Ring(ranks)
    here = lax.axis_index("tensor")
    block, width = cot_ref.shape
    rows = block // peers
    half = ring.half
    low = low_ref.dtype
    columns = width // ranks
    hidden = layout.hidden
    head_width = queries.shape[1]
    heads = head_width // HEAD_DIM
    small_rows = small_vec.shape[0]
    away = [(here + k) % peers for k in range(peers)]
    others = [(ring.me + k) % ranks for k in range(ranks)]
    greet(
        [{"dp": others[k]} for k in range(1, ranks)] + [{"tensor": away[k]} for k in range(1, peers)]
    )
    first = here * rows
    order = list(reversed(near_first(peers)))
    far_first = order[:-1]

    def slice_of(device):
        return pl.ds(pl.multiple_of(device * columns, columns), columns)

    def to_peers(source_of, target_of, sends, recvs):
        return [
            remote(
                source_of(k),
                target_of(peers - k - 1),
                "tensor",
                away[k],
                sends,
                recvs,
                peers - k - 1,
            )
            for k in far_first
        ]

    def reducer(source, where, sems, k):
        def source_at(device):
            return source.at[pl.ds(device * block + away[k] * rows, rows)]

        return RingReduce(ring, source_at, rows, where, sems, k)

    backs = {k: reducer(part_ref, buffers, back_sems, k) for k in order}
    outs = {}
    if with_out:
        outs = {k: reducer(out_part_ref, out_buffers, out_sems, k) for k in order}
    for offset in backs[0].order:
        for k in order:
            backs[k].hand_over(offset)

    tile = right.shape[2]
    blocks = width // tile
    steps = 3 * blocks

    def fetch_left(wide):
        source = scaled_ref if wide == 2 else grads_ref.at[:, pl.ds(wide * hidden, hidden)]
        return pltpu.make_async_copy(source, left, left_sem)

    def fetch_right(step, late):
        spot = pl.ds(pl.multiple_of(step % blocks * tile, tile), tile)
        source = cots_ref if late else x_ref
        return pltpu.make_async_copy(source.at[:, spot], right.at[step % 2], right_sem.at[step % 2])

    fetch_right(0, False).start()
    fetch_left(0).start()
    vec_load = pltpu.make_async_copy(columns_all.at[pl.ds(0, small_rows)], small_vec, local_sem.at[0])
    vec_load.start()
    row_loads = [
        pltpu.make_async_copy(source.at[pl.ds(first, rows)], target, local_sem.at[slot])
        for source, target, slot in ((cot_ref, cot_rows, 5), (tokens_ref, token_rows, 6))
    ]
    for load in row_loads:
        load.start()
    qkv_load = pltpu.make_async_copy(
        rows_all.at[:, pl.ds(0, 3 * head_width)], qkv_full, local_sem.at[1]
    )
    qkv_load.start()
    if not with_out:
        out_load = pltpu.make_async_copy(out_part_ref, out_sum, local_sem.at[2])
        out_load.start()
    for k in order:
        backs[k].step(0)

    def hand_outs():
        for offset in backs[0].order:
            for k in outs:
                outs[k].hand_over(offset)

    vec_load.wait()
    for load in row_loads:
        load.wait()
    count = layout.expert_count
    vectors = small_vec[...].astype(jnp.float32)
    attn_gain = vectors[count + 1 : count + 2, :]
    ffn_gain = vectors[count + 2 : count + 3, :]

    z_sum = TensorSum(peers, lambda k: z_stage.at[k], z_got, z_sends, z_recvs)
    def pass_z(k):
        def emit(spot, start, size, value):
            z_stage[k, spot, :] = value.astype(low)

        backs[k].total(emit)
        z_sum.send(k)

    def results(step, wide):
        slot = step % 2
        spot = pl.ds(pl.multiple_of(step % blocks * tile, tile), tile)
        base = slot * (layout.local_experts + 1)
        copies = [
            pltpu.make_async_copy(
                product.at[slot, pl.ds(j * layout.part, layout.expert_hidden)],
                (gate_grads_ref, up_grads_ref, down_grads_ref)[wide].at[j, :, spot],
                product_sem.at[base + j],
            )
            for j in range(layout.local_experts)
        ]
        copies.append(
            pltpu.make_async_copy(
                shared_low.at[slot],
                shared_grads_ref.at[wide, :, spot],
                product_sem.at[base + layout.local_experts],
            )
        )
        return copies

    gain_grad[...] = jnp.zeros_like(gain_grad)

    def norm_middle(spot, start, size, value):
        value = value + z_sum.rest(spot)
        middle = middle_ref[spot, :]
        inverse = lax.rsqrt(jnp.mean(middle * middle, axis=-1, keepdims=True) + EPSILON)
        normed = middle * inverse
        scaled = value * ffn_gain
        back = inverse * (scaled - normed * jnp.mean(scaled * normed, axis=-1, keepdims=True))
        mine = pl.ds(pl.multiple_of(first + start, size), size)
        grad = cot_rows[spot, :].astype(jnp.float32) + back
        grad_ref[spot, :] = grad
        low_ref[spot, :] = grad.astype(low)
        gm_all[mine, :] = grad.astype(low)
        gain_grad[...] += jnp.sum(value * normed, axis=0, keepdims=True)

    def rows_in(target):
        def place(device, start, size):
            return target.at[pl.ds(device * rows + start, size)]

        return place

    def spread(source, target, sends, recvs):
        return TensorGather(peers, source, rows_in(target), rows, sends, recvs)

    gm_spread = spread(low_ref, gm_all, m_sends, m_recvs)

    def finish_norm():
        z_sum.arrived()
        backs[0].total(norm_middle)
        gm_spread.begin()

    events = []
    for number in range(1, half):
        for index, k in enumerate(order):
            events.append((BACK_DUE[0] + number - 1 + index, functools.partial(backs[k].step, number)))
    events.append((BACK_DUE[1], hand_outs))
    gap = 6 // (peers - 2)
    for index, k in enumerate(far_first):
        events.append((BACK_DUE[2] + gap * index, functools.partial(pass_z, k)))
    for number in range(half):
        for index, k in enumerate(outs):
            due = BACK_DUE[3 + number] + number * index
            events.append((due, functools.partial(outs[k].step, number)))

    def grad_step(step, carry):
        wide, slot = step // blocks, step % 2
        for number in range(3):

            @pl.when(step == number * blocks)
            def _(number=number):
                fetch_left(number).wait()

                def turn_over(index, carry):
                    spot = pl.ds(pl.multiple_of(index * 256, 256), 256)
                    turned[:, spot] = left[spot, :].T
                    return carry

                lax.fori_loop(0, left.shape[0] // 256, turn_over, 0)
                if number < 2:
                    fetch_left(number + 1).start()

        fetch_right(step, False).wait()

        @pl.when(step + 1 < 2 * blocks)
        def _():
            fetch_right(step + 1, False).start()

        @pl.when((step + 1 >= 2 * blocks) & (step + 1 < steps))
        def _():
            fetch_right(step + 1, True).start()

        @pl.when(step > 1)
        def _():
            for copy in results(step, 0):
                copy.wait()

        value = matmul(turned[...], right[slot])
        product[slot] = value[: layout.shared_at].astype(low)
        shared_low[slot] = value[layout.shared_at : layout.router_at].astype(low)

        @pl.when(wide == 0)
        def _():
            spot = pl.ds(pl.multiple_of(step % blocks * tile, tile), tile)
            small_own[:, spot] = value[layout.router_at : layout.router_at + small_rows]

        for number in range(3):

            @pl.when(wide == number)
            def _(number=number):
                for copy in results(step, number):
                    copy.start()

        for due, event in events:

            @pl.when(step == due)
            def _(event=event):
                event()

        return carry

    lax.fori_loop(0, steps, grad_step, 0)
    proj_load = pltpu.make_async_copy(
        columns_all.at[pl.ds(small_rows, head_width)],
        turned.at[pl.ds(head_width, head_width), pl.ds(0, width)],
        local_sem.at[3],
    )
    proj_load.start()
    for step in (steps - 2, steps - 1):
        for copy in results(step, 0):
            copy.wait()

    finish_norm()
    small_own[count + 1 : count + 2, :] = jnp.zeros((1, width), jnp.float32)
    small_own[count + 2 : count + 3, :] = gain_grad[...]
    shared = []
    for k in range(1, ranks):
        copy = remote(
            shared_grads_ref.at[:, :, slice_of(others[k])],
            shared_got_ref.at[ring.me],
            "dp",
            others[k],
            s_sends,
            s_recvs,
            ranks - k - 1,
        )
        copy.start()
        shared.append(copy)
    keep = pltpu.make_async_copy(
        shared_grads_ref.at[:, :, slice_of(ring.me)], kept, local_sem.at[4]
    )
    keep.start()
    half_peers = peers // 2
    for number in range(1, half_peers):
        gm_spread.step(number)

    def chunk_of(source):
        return lambda k: source.at[pl.ds(away[k] * rows, rows)]

    if not with_out:
        out_load.wait()
    for k in outs:

        def emit_out(spot, start, size, value, k=k):
            there = pl.ds(pl.multiple_of(away[k] * rows + start, size), size)
            out_sum[there, :] = value.astype(low)

        outs[k].total(emit_out)
    out_total = TensorSum(peers, chunk_of(out_sum), o_got, o_sends, o_recvs)
    out_total.begin()

    gm_spread.step(half_peers)
    proj_load.wait()
    out_weights = turned.at[pl.ds(head_width, head_width), pl.ds(0, width)]
    grad_context[...] = matmul_last(gm_all[...], out_weights[...]).astype(low)
    attend_back(heads, queries, keys, values, probs_ref, grad_context, cos_ref, sin_ref, grad_rows)
    qkv_load.wait()

    def through_qkv(spot):
        attn_part[:, spot] = matmul_last(grad_rows[...], qkv_full[spot, :]).astype(low)

    tiles(width, 256, through_qkv)
    attn_total = TensorSum(peers, chunk_of(attn_part), a_got, a_sends, a_recvs)
    attn_total.begin()
    def weight_tiles(spot):
        qkv_full[spot, :] = matmul(attn_in[:, spot].T, grad_rows[...]).astype(low)

    tiles(width, 256, weight_tiles)
    for k in far_first[1:]:
        attn_total.send(k)
    for k in far_first[1:]:
        out_total.send(k)

    def proj_tiles(spot):
        turned[:head_width, spot] = matmul(context[...].T, gm_all[:, spot]).astype(low)

    tiles(width, 256, proj_tiles)

    for k in order:
        backs[k].finish()
    for partner in ring.partners():
        pl.semaphore_signal(reuse_sem, inc=1, device_id=partner, device_id_type=MESH)
    pl.semaphore_wait(reuse_sem, 3)
    pieces = proj_buffers[0].shape[0]
    lot, size = qkv_sum_ref.shape[0], qkv_sum_ref.shape[0] // pieces
    proj_size = proj_buffers[0].shape[2]
    narrow = [
        buffer.at[pl.ds(0, pieces), :, pl.ds(0, size), pl.ds(0, 3 * head_width)] for buffer in buffers
    ]
    works = []
    for piece in range(pieces):

        def qkv_at(device, piece=piece):
            return qkv_full.at[pl.ds(device * lot + piece * size, size)]

        def proj_at(device, piece=piece):
            return turned.at[pl.ds(piece * proj_size, proj_size), slice_of(device)]

        works.append(RingReduce(ring, qkv_at, size, narrow, qkv_sems, piece))
        works.append(RingReduce(ring, proj_at, proj_size, proj_buffers, proj_sems, piece))
    for offset in works[0].order:
        for work in works:
            work.hand_over(offset)
    for work in works:
        work.step(0)

    spot_row = count + 1

    def norm_tokens(spot, start, size):
        mine = pl.ds(pl.multiple_of(first + start, size), size)
        value = attn_part[mine, :].astype(jnp.float32)
        value = value + attn_total.rest(spot)
        inputs = token_rows[spot, :].astype(jnp.float32)
        inverse = lax.rsqrt(jnp.mean(inputs * inputs, axis=-1, keepdims=True) + EPSILON)
        normed = inputs * inverse
        scaled = value * attn_gain
        back = inverse * (scaled - normed * jnp.mean(scaled * normed, axis=-1, keepdims=True))
        low_ref[spot, :] = (grad_ref[spot, :] + back).astype(low)
        small_own[spot_row : spot_row + 1, :] += jnp.sum(value * normed, axis=0, keepdims=True)

    attn_total.arrived()
    gm_spread.sent()
    strips(rows, norm_tokens)
    mine = input_ref.at[pl.ds(first, rows)]
    input_spread = spread(low_ref, input_ref, x_sends, x_recvs)
    input_spread.begin()
    stores = [pltpu.make_async_copy(low_ref, mine, local_sem.at[5])]
    stores[0].start()
    handed = []
    for k in range(1, ranks):
        copy = remote(
            small_own.at[:, slice_of(others[k])],
            small_got.at[ranks - k - 1],
            "dp",
            others[k],
            g_sends,
            g_recvs,
            ranks - k - 1,
        )
        copy.start()
        handed.append(copy)

    for number in range(1, half):
        for work in works:
            work.step(number)

    def finish_rows(spot, start, size):
        there = pl.ds(pl.multiple_of(first + start, size), size)
        value = out_sum[there, :].astype(jnp.float32)
        value = value + out_total.rest(spot)
        out_low[spot, :] = (middle_ref[spot, :] + value).astype(low)

    out_total.arrived()
    strips(rows, finish_rows)
    out_mine = output_ref.at[pl.ds(first, rows)]
    output_spread = spread(out_low, output_ref, y_sends, y_recvs)
    output_spread.begin()
    for number in range(1, half_peers):
        input_spread.step(number)
    keep.wait()
    keep = pltpu.make_async_copy(kept, shared_got_ref.at[ring.me], local_sem.at[4])
    keep.start()
    for copy in handed:
        copy.wait_recv()
    value = small_own[:, slice_of(ring.me)]
    for k in range(ranks - 1):
        value = value + small_got[k]
    small_part[...] = value
    last = to_peers(lambda k: small_part, lambda slot: small_z.at[slot], h_sends, h_recvs)
    for copy in last:
        copy.start()
    stores.append(pltpu.make_async_copy(out_low, out_mine, local_sem.at[6]))
    stores[1].start()
    for piece in range(pieces):

        def emit_qkv(spot, start, count, value, piece=piece):
            qkv_sum_ref[pl.ds(pl.multiple_of(piece * size + start, count), count), :] = value

        def emit_proj(spot, start, count, value, piece=piece):
            proj_sum_ref[pl.ds(pl.multiple_of(piece * proj_size + start, count), count), :] = value

        works[2 * piece].total(emit_qkv)
        works[2 * piece + 1].total(emit_proj)
    for number in range(1, half_peers):
        output_spread.step(number)
    for copy in last:
        copy.wait_recv()
    value = small_part[...]
    for k in range(peers - 1):
        value = value + small_z[k]
    small_sum_ref[...] = value
    keep.wait()
    for copy in stores:
        copy.wait()
    input_spread.step(half_peers)
    output_spread.step(half_peers)
    for work in (z_sum, out_total, attn_total, input_spread, output_spread):
        work.sent()
    for copy in handed + last:
        copy.wait_send()
    for copy in shared:
        copy.wait()
    for k in outs:
        outs[k].finish()
    for work in works:
        work.finish()


def rear(
    layout,
    back_part,
    out_part,
    x_all,
    cot_all,
    grads,
    scaled,
    rows_all,
    columns_all,
    middle,
    cotangent,
    tokens,
    attn_in,
    queries,
    keys,
    values,
    context,
    probs,
    cosine,
    sine,
    small_rows,
    with_out,
    ranks,
    peers,
    identity,
):
    chips = ranks // 2
    block, width = tokens.shape
    total = x_all.shape[0]
    rows = block // peers
    hidden, own = layout.hidden, layout.shared_own
    experts, units = layout.local_experts, layout.expert_hidden
    head_width = queries.shape[1]
    columns = width // ranks
    pieces = 4
    tile = 256
    vmem = pl.BlockSpec(memory_space=pltpu.VMEM)
    hbm = pl.BlockSpec(memory_space=pl.ANY)
    dma = pltpu.SemaphoreType.DMA
    low, f32 = tokens.dtype, jnp.float32
    shape = jax.ShapeDtypeStruct
    return pl.pallas_call(
        functools.partial(rear_kernel, layout, ranks, peers, with_out),
        out_shape=(
            shape((block, width), low),
            shape((block, width), low),
            shape((columns, 3 * head_width), f32),
            shape((head_width, columns), f32),
            shape((small_rows, columns), f32),
            *[shape((experts, units, width), low)] * 3,
            shape((3, own, width), low),
            shape((ranks, 3, own, columns), low),
        ),
        in_specs=[hbm] * 8 + [vmem] + [hbm] * 2 + [vmem] * 8,
        out_specs=(hbm, hbm, vmem, vmem, vmem, hbm, hbm, hbm, hbm, hbm),
        scratch_shapes=[
            pltpu.VMEM((rows, width), low),
            pltpu.VMEM((rows, width), low),
            pltpu.VMEM((small_rows, width), low),
            pltpu.VMEM((rows, width), f32),
            pltpu.VMEM((small_rows, width), f32),
            pltpu.VMEM((ranks - 1, small_rows, columns), f32),
            pltpu.VMEM((small_rows, columns), f32),
            pltpu.VMEM((peers - 1, small_rows, columns), f32),
            pltpu.VMEM((peers, rows, width), low),
            pltpu.VMEM((peers - 1, rows, width), low),
            pltpu.VMEM((peers - 1, rows, width), low),
            pltpu.VMEM((peers - 1, rows, width), low),
            pltpu.VMEM((rows, width), low),
            pltpu.VMEM((block, width), low),
            pltpu.VMEM((2, total, tile), low),
            pltpu.VMEM((total, hidden), low),
            pltpu.VMEM((hidden, total), low),
            pltpu.VMEM((2, layout.shared_at, tile), low),
            pltpu.VMEM((2, own, tile), low),
            pltpu.VMEM((1, width), f32),
            pltpu.VMEM((width, 3 * head_width), low),
            pltpu.VMEM((block, head_width), low),
            pltpu.VMEM((block, 3 * head_width), low),
            pltpu.VMEM((block, width), low),
            pltpu.VMEM((block, width), low),
            pltpu.VMEM((3, own, columns), low),
        ]
        + [dma((peers,))] * 14
        + [dma((ranks - 1,))] * 4
        + [
            dma((7,)),
            dma,
            dma((2,)),
            dma((2 * (experts + 1),)),
            pltpu.SemaphoreType.REGULAR,
        ]
        + reduce_buffers(peers, chips, rows, width, low)
        + reduce_sems(peers, chips)
        + reduce_sems(pieces, chips)
        + reduce_buffers(pieces, chips, head_width // pieces, columns, low)
        + reduce_sems(pieces, chips)
        + (reduce_buffers(peers, chips, rows, width, low) + reduce_sems(peers, chips)) * with_out,
        compiler_params=pltpu.CompilerParams(
            collective_id=identity, has_side_effects=True, vmem_limit_bytes=67043328
        ),
        name="rear",
    )(
        back_part,
        out_part,
        x_all,
        cot_all,
        grads,
        scaled,
        rows_all,
        columns_all,
        middle,
        cotangent,
        tokens,
        attn_in,
        queries,
        keys,
        values,
        context,
        probs,
        cosine,
        sine,
    )


def rope_tables():
    half_dim = HEAD_DIM // 2
    exponent = np.arange(half_dim, dtype=np.float32) * np.float32(2.0 / HEAD_DIM)
    inverse_freq = np.exp(-exponent * np.log(np.float32(1000000.0)))
    angles = np.arange(SEQ, dtype=np.float32)[:, None] * inverse_freq[None, :]
    cosine, sine = np.cos(angles), np.sin(angles)
    return (
        jnp.asarray(np.concatenate([cosine, cosine], axis=1)),
        jnp.asarray(np.concatenate([-sine, sine], axis=1)),
    )


def scatter_rows(values):
    return lax.psum_scatter(values, "dp", scatter_dimension=0, tiled=True)


def shards(
    tokens,
    w_query,
    w_key,
    w_value,
    w_out,
    gain_attn,
    gain_ffn,
    w_router,
    shared_gate,
    shared_up,
    shared_down,
    shared_switch,
    expert_gate,
    expert_up_weight,
    expert_down,
    routes,
    segments,
    cotangent,
):
    low = jnp.bfloat16
    ranks = lax.axis_size("dp")
    peers = lax.axis_size("tensor")
    token_count, width = tokens.shape
    local_experts, _, expert_hidden = expert_gate.shape
    expert_count = local_experts * ranks
    block = width // ranks
    head_width = w_query.shape[1]
    shared_width = shared_gate.shape[1]
    shared_own = shared_width // ranks
    small_pad = 128
    layout = Layout(local_experts, expert_hidden, shared_own, expert_count)
    lane0 = layout.router_lane

    small_rows = -(-(expert_count + 3) // 16) * 16
    spots = jnp.arange(small_pad, dtype=jnp.int32)[None, None, :] - lane0
    chosen = jnp.sum((routes[:, :, None] == spots).astype(jnp.float32), axis=1).astype(low)
    fold = token_count // block
    chosen = chosen.reshape(fold, block, small_pad).transpose(1, 0, 2).reshape(block, fold * small_pad)
    vectors = jnp.stack([shared_switch, gain_attn, gain_ffn])
    cosine, sine = rope_tables()
    spots = jnp.arange(SEQ, dtype=jnp.int32)
    allowed = (spots[None, :] <= spots[:, None]) & (segments[0][None, :] == segments[0][:, None])

    (
        qkv_full,
        columns_full,
        attn_in,
        queries,
        key_rows,
        value_rows,
        context_flat,
        probs,
        x_all,
        cot_all,
        middle,
        scaled_hidden,
        grads_wide,
        out_part,
        back_part,
    ) = layer_forward_back(
        layout,
        w_query,
        w_key,
        w_value,
        chosen,
        w_out,
        w_router.T,
        vectors,
        tokens,
        cotangent,
        allowed.astype(jnp.float32),
        cosine,
        sine,
        expert_gate.swapaxes(1, 2),
        expert_up_weight.swapaxes(1, 2),
        expert_down,
        shared_gate.T.reshape(ranks, shared_own, block),
        shared_up.T.reshape(ranks, shared_own, block),
        shared_down.reshape(ranks, shared_own, block),
        small_rows,
        ranks,
        peers,
        1,
    )
    with_out = ranks == 8
    grad_input, output, grad_qkv, grad_proj, grad_small, *grad_experts, _, grad_shared = rear(
        layout,
        back_part,
        out_part if with_out else scatter_rows(out_part),
        x_all,
        cot_all,
        grads_wide,
        scaled_hidden,
        qkv_full,
        columns_full,
        middle,
        cotangent,
        tokens,
        attn_in,
        queries,
        key_rows,
        value_rows,
        context_flat,
        probs,
        cosine,
        sine,
        small_rows,
        with_out,
        ranks,
        peers,
        2,
    )
    grad_experts = [grads.astype(jnp.float32) for grads in grad_experts]
    grad_shared = grad_shared.astype(jnp.float32)
    return (
        output,
        grad_input.astype(jnp.float32),
        grad_qkv[:, :head_width],
        grad_qkv[:, head_width : 2 * head_width],
        grad_qkv[:, 2 * head_width :],
        grad_proj,
        grad_small[expert_count + 1],
        grad_small[expert_count + 2],
        grad_small[:expert_count].T,
        grad_shared[:, 0].reshape(shared_width, block).T,
        grad_shared[:, 1].reshape(shared_width, block).T,
        grad_shared[:, 2].reshape(shared_width, block),
        grad_small[expert_count],
        grad_experts[0].swapaxes(1, 2),
        grad_experts[1].swapaxes(1, 2),
        grad_experts[2],
    )


def solution(mesh):
    in_specs = (
        P("dp", None),
        P("dp", "tensor"),
        P("dp", "tensor"),
        P("dp", "tensor"),
        P("tensor", "dp"),
        P("dp"),
        P("dp"),
        P("dp", None),
        P("dp", "tensor"),
        P("dp", "tensor"),
        P("tensor", "dp"),
        P("dp"),
        P("dp", None, "tensor"),
        P("dp", None, "tensor"),
        P("dp", "tensor", None),
        P("dp", None),
        P("dp", None),
        P("dp", None),
    )
    out_specs = (
        P("dp", None),
        P("dp", None),
        P("dp", "tensor"),
        P("dp", "tensor"),
        P("dp", "tensor"),
        P("tensor", "dp"),
        P("dp"),
        P("dp"),
        P("dp", None),
        P("dp", "tensor"),
        P("dp", "tensor"),
        P("tensor", "dp"),
        P("dp"),
        P("dp", None, "tensor"),
        P("dp", None, "tensor"),
        P("dp", "tensor", None),
    )
    return jax.shard_map(shards, mesh=mesh, in_specs=in_specs, out_specs=out_specs, check_vma=False)
```

```python
import functools

import jax
import jax.numpy as jnp
import numpy as np
from jax import lax
from jax.experimental import pallas as pl
from jax.experimental.pallas import tpu as pltpu
from jax.sharding import PartitionSpec as P

HEAD_DIM = 128
TOP = 4
SEQ = 256


EPSILON = 1e-06
MESH = pl.DeviceIdType.MESH


def ring_chip(position, chips):
    half = chips // 2
    upper = position // half
    return position + upper * (chips - 1 + half - 2 * position)


def ring_spot(chip, chips):
    return ring_chip(chip, chips)


def greet(partners):
    barrier = pltpu.get_barrier_semaphore()
    for partner in partners:
        pl.semaphore_signal(barrier, inc=1, device_id=partner, device_id_type=MESH)
    pl.semaphore_wait(barrier, len(partners))


def remote(source, target, axis, device, sends, recvs, slot):
    return pltpu.make_async_remote_copy(
        src_ref=source,
        dst_ref=target,
        send_sem=sends.at[slot],
        recv_sem=recvs.at[slot],
        device_id={axis: device},
        device_id_type=MESH,
    )


class Ring:
    def __init__(self, ranks):
        self.ranks = ranks
        self.chips = ranks // 2
        self.half = self.chips // 2
        self.me = lax.axis_index("dp")
        self.core = self.me % 2
        self.position = ring_spot(self.me // 2, self.chips)
        self.sibling = self.me + 1 - 2 * self.core
        self.ahead = self.device(1)
        self.behind = self.device(-1)

    def chip(self, offset):
        return ring_chip((self.position + offset + self.chips) % self.chips, self.chips)

    def device(self, offset):
        return self.chip(offset) * 2 + self.core

    def other(self, offset):
        return self.chip(offset) * 2 + 1 - self.core

    def partners(self):
        return [{"dp": self.ahead}, {"dp": self.behind}, {"dp": self.sibling}]


def gather_slots(half):
    return 2 * half


def side_slots(half):
    return 2 * half


class RingGather:
    def __init__(self, ring, place, rows, sends, recvs, side_sends, side_recvs, base, side_base):
        self.ring, self.place, self.rows, self.cut = ring, place, rows, rows // 2
        self.sends, self.recvs = sends, recvs
        self.side_sends, self.side_recvs = side_sends, side_recvs
        self.base, self.side_base = base, side_base
        self.sides = side_slots(ring.half)

    def hop_copy(self, source, target, device, slot):
        return remote(source, target, "dp", device, self.sends, self.recvs, self.base + slot)

    def side_copy(self, source, target, slot):
        return remote(
            source,
            target,
            "dp",
            self.ring.sibling,
            self.side_sends,
            self.side_recvs,
            self.side_base + slot,
        )

    def hop_size(self, slot):
        number = slot % self.ring.half
        return self.cut if number and number == self.ring.half - 1 else self.rows

    def begin(self, source):
        ring = self.ring
        target = self.place(ring.me, 0, self.rows)
        self.hop_copy(source, target, ring.ahead, 0).start()
        self.hop_copy(source, target, ring.behind, ring.half).start()
        self.side_copy(source, target, 0).start()

    def wait_hop(self, slot):
        block = self.place(self.ring.me, 0, self.hop_size(slot))
        self.hop_copy(block, block, self.ring.ahead, slot).wait_recv()

    def step(self, number):
        ring = self.ring
        for which, sign in enumerate((-1, 1)):
            owner = ring.device(sign * number)
            onward = (ring.ahead, ring.behind)[which]
            self.wait_hop(which * ring.half + number - 1)
            if number < ring.half:
                block = self.place(owner, 0, self.rows)
                slot = which * ring.half + number
                size = self.hop_size(slot)
                part = block if size == self.rows else self.place(owner, (0, self.cut)[which], size)
                self.hop_copy(part, part, onward, slot).start()
                self.side_copy(block, block, 2 * number - 1 + which).start()
        if number == ring.half:
            block = self.place(ring.device(number), 0, self.rows)
            self.side_copy(block, block, 2 * ring.half - 1).start()

    def wait_side(self, index):
        block = self.place(self.ring.me, 0, self.rows)
        self.side_copy(block, block, index).wait_recv()

    def sent(self):
        for slot in range(2 * self.ring.half):
            block = self.place(self.ring.me, 0, self.hop_size(slot))
            self.hop_copy(block, block, self.ring.ahead, slot).wait_send()
        for index in range(self.sides):
            block = self.place(self.ring.me, 0, self.rows)
            self.side_copy(block, block, index).wait_send()


def near_first(peers):
    order = [0]
    for step in range(1, peers // 2 + 1):
        order.append(step)
        if peers - step != step:
            order.append(peers - step)
    return order


STRIP = 64
BACK_DUE = (0, 5, 11, 11, 17)


def strips(rows, body):
    strip = min(STRIP, rows)

    def step(index, carry):
        body(pl.ds(pl.multiple_of(index * strip, strip), strip), index * strip, strip)
        return carry

    lax.fori_loop(0, rows // strip, step, 0)


HIDDEN_TILE, OUT_TILE, BACK_TILE = 1024, 1024, 1024


def matmul(left, right):
    return lax.dot_general(
        left, right, (((1,), (0,)), ((), ())), preferred_element_type=jnp.float32
    )


def matmul_last(left, right):
    return lax.dot_general(
        left, right, (((1,), (1,)), ((), ())), preferred_element_type=jnp.float32
    )


def tiles(width, tile, body):
    def step(index, carry):
        body(pl.ds(pl.multiple_of(index * tile, tile), tile))
        return carry

    lax.fori_loop(0, width // tile, step, 0)


class Layout:
    def __init__(self, local_experts, expert_hidden, shared_own, expert_count):
        self.local_experts = local_experts
        self.expert_hidden = expert_hidden
        self.shared_own = shared_own
        self.expert_count = expert_count
        self.part = -(-expert_hidden // 128) * 128
        self.shared_at = local_experts * self.part
        self.router_at = self.shared_at + shared_own
        self.last = -(-(shared_own + expert_count + 1) // 128) * 128
        self.hidden = self.shared_at + self.last
        self.router_tile = self.router_at // 128 * 128
        self.router_lane = self.router_at - self.router_tile
        self.tile = next(size for size in (HIDDEN_TILE, 256, 128) if self.hidden % size == 0)


def hidden_tiles(layout, x_ref, gates, ups, pre_gate, pre_up):
    def body(spot):
        pre_gate[:, spot] = matmul_last(x_ref[...], gates[spot, :])
        pre_up[:, spot] = matmul_last(x_ref[...], ups[spot, :])

    tiles(layout.hidden, layout.tile, body)


def cot_tiles(layout, cot_ref, downs, cot_hidden):
    def body(spot):
        cot_hidden[:, spot] = matmul_last(cot_ref[...], downs[spot, :]).astype(cot_hidden.dtype)

    tiles(layout.hidden, layout.tile, body)


def gate_strips(layout, first_expert, chosen, pre_gate, pre_up, cot_hidden, scaled, grads):
    rows = pre_gate.shape[0]
    count, lane0 = layout.expert_count, layout.router_lane
    router = slice(layout.router_tile, layout.router_tile + 128)
    bounds = [(j * layout.part, (j + 1) * layout.part) for j in range(layout.local_experts)]
    bounds.append((layout.shared_at, layout.hidden))
    low = scaled.dtype

    def body(spot, start, size):
        lane = lax.broadcasted_iota(jnp.int32, (size, 128), 1)
        logits = pre_gate[spot, router]
        is_router = (lane >= lane0) & (lane < lane0 + count)
        is_switch = lane == lane0 + count
        power = jnp.where(is_router, jnp.exp(jnp.where(is_router, logits, 0.0)), 0.0)
        probs = power / jnp.sum(power, axis=-1, keepdims=True)
        raw = jnp.sum(jnp.where(is_switch, logits, 0.0), axis=-1, keepdims=True)
        switch = 1.0 / (1.0 + jnp.exp(-raw))
        mask = chosen[spot, :].astype(jnp.float32)
        scales = []
        for j in range(layout.local_experts):
            spotted = lane == lane0 + first_expert + j
            scales.append(jnp.sum(jnp.where(spotted, probs * mask, 0.0), axis=-1, keepdims=True))
        scales.append(switch)
        totals = []
        for (begin, end), scale in zip(bounds, scales):
            shared = begin == layout.shared_at
            columns = slice(begin, end)
            gate, up = pre_gate[spot, columns], pre_up[spot, columns]
            through = cot_hidden[spot, columns].astype(jnp.float32)
            sig = 1.0 / (1.0 + jnp.exp(-gate))
            act = gate * sig
            state = act * up
            grad = scale * through
            totals.append(jnp.sum(state * through, axis=-1, keepdims=True))
            scaled[spot, columns] = (scale * state).astype(low)
            grad_gate = grad * up * sig * (1.0 + gate * (1.0 - sig))
            grads[spot, columns] = grad_gate.astype(low)
            grads[spot, layout.hidden + begin : layout.hidden + end] = (grad * act).astype(low)
        choice = jnp.zeros_like(probs)
        for j in range(layout.local_experts):
            spotted = lane == lane0 + first_expert + j
            choice = choice + jnp.where(spotted, mask * totals[j], 0.0)
        small = probs * (choice - jnp.sum(probs * choice, axis=-1, keepdims=True))
        small = jnp.where(is_switch, totals[-1] * switch * (1.0 - switch), small)
        kept = grads[spot, router].astype(jnp.float32)
        kept = jnp.where(is_router | is_switch, small, kept)
        grads[spot, router] = kept.astype(low)

    strips(rows, body)


def out_tiles(width, scaled, downs, out):
    def body(spot):
        out[:, spot] = matmul(scaled[...], downs[:, spot]).astype(out.dtype)

    tiles(width, OUT_TILE, body)


def back_tiles(layout, width, grads, gates, ups, back):
    hidden = layout.hidden

    def body(spot):
        total = matmul(grads[:, :hidden], gates[:, spot])
        total = total + matmul(grads[:, hidden:], ups[:, spot])
        back[:, spot] = total.astype(back.dtype)

    tiles(width, BACK_TILE, body)


def rope(values, cosine, sine, sign):
    return values * cosine + pltpu.roll(values, HEAD_DIM // 2, 1) * (sine * sign)


def attend(heads, qkv, segments_ref, cos_ref, sin_ref, queries, keys, values, probs_ref, context):
    cosine, sine = cos_ref[...], sin_ref[...]
    length = queries.shape[0]
    segments = jnp.broadcast_to(segments_ref[...].astype(jnp.float32), (length, length))
    row = lax.broadcasted_iota(jnp.int32, (length, length), 0)
    column = lax.broadcasted_iota(jnp.int32, (length, length), 1)
    allowed = (segments == segments.T) & (column <= row)
    low = queries.dtype
    for head in range(heads):
        columns = slice(head * HEAD_DIM, (head + 1) * HEAD_DIM)
        query = rope(qkv(head), cosine, sine, 1.0).astype(low)
        key = rope(qkv(heads + head), cosine, sine, 1.0).astype(low)
        value = qkv(2 * heads + head).astype(low)
        queries[:, columns], keys[:, columns], values[:, columns] = query, key, value
        scores = matmul_last(query, key) * HEAD_DIM ** (-0.5)
        power = jnp.where(allowed, jnp.exp(jnp.where(allowed, scores, 0.0)), 0.0)
        probs = power / jnp.sum(power, axis=-1, keepdims=True)
        probs_ref[head] = probs
        context[:, columns] = matmul(probs.astype(low), value).astype(low)


def layer_kernel(
    layout,
    ranks,
    peers,
    query_ref,
    key_ref,
    value_ref,
    proj_ref,
    router_ref,
    routes_ref,
    switch_ref,
    attn_gain_ref,
    ffn_gain_ref,
    tokens_ref,
    cot_ref,
    segments_ref,
    cos_ref,
    sin_ref,
    expert_gate_ref,
    expert_up_ref,
    expert_down_ref,
    shared_gate_ref,
    shared_up_ref,
    shared_down_ref,
    rows_all,
    columns_all,
    attn_in,
    queries,
    keys,
    values,
    context,
    probs_ref,
    x_all,
    cot_all,
    middle_ref,
    scaled_ref,
    grads_ref,
    out_ref,
    back_ref,
    row_stage,
    column_stage,
    rows_full,
    columns_full,
    qkv_raw,
    part_ref,
    gates,
    ups,
    downs,
    shared_got,
    shared_rows,
    own,
    got,
    x_block,
    cot_block,
    pre_gate,
    pre_up,
    cot_hidden,
    scaled,
    grads,
    out,
    back,
    chosen,
    local_sem,
    gather_sem,
    a_sends,
    a_recvs,
    a_side_sends,
    a_side_recvs,
    block_sem,
    x_sem,
    store_sem,
    shared_sends,
    shared_recvs,
    z_sends,
    z_recvs,
    x_sends,
    x_recvs,
    sends,
    recvs,
    side_sends,
    side_recvs,
    c_sends,
    c_recvs,
    c_side_sends,
    c_side_recvs,
):
    ring = Ring(ranks)
    here = lax.axis_index("tensor")
    block, width = tokens_ref.shape
    rows = block // peers
    depth = width // ranks
    half = ring.half
    away = [(here + k) % peers for k in range(peers)]
    others = [(ring.me + k) % ranks for k in range(ranks)]

    count, lane0 = layout.expert_count, layout.router_lane
    head_width = query_ref.shape[1]
    heads = head_width // HEAD_DIM
    lot, wide = row_stage.shape
    height = column_stage.shape[0]
    small_rows = height - head_width
    low = gates.dtype
    loads, start = [], 0
    for index, source in enumerate((query_ref, key_ref, value_ref)):
        size = source.shape[1]
        loads.append(
            pltpu.make_async_copy(source, row_stage.at[:, pl.ds(start, size)], gather_sem.at[index])
        )
        start += size
    loads.append(
        pltpu.make_async_copy(
            proj_ref, column_stage.at[pl.ds(small_rows, head_width)], gather_sem.at[4]
        )
    )
    for load in loads:
        load.start()
    small = jnp.concatenate(
        [
            router_ref[...].astype(jnp.float32),
            switch_ref[...].astype(jnp.float32).reshape(1, depth),
            attn_gain_ref[...].astype(jnp.float32).reshape(1, depth),
            ffn_gain_ref[...].astype(jnp.float32).reshape(1, depth),
            jnp.zeros((small_rows - count - 3, depth), jnp.float32),
        ],
        axis=0,
    )
    column_stage[:small_rows, :] = small.astype(low)
    top = routes_ref.shape[0]
    routes = routes_ref[...].astype(jnp.float32)
    routes = jnp.concatenate([routes, jnp.zeros((8 - top, block), jnp.float32)], axis=0).T
    for fold in range(block // lot):
        lane = lax.broadcasted_iota(jnp.int32, (lot, 128), 1).astype(jnp.float32) - lane0
        mark = jnp.zeros((lot, 128), jnp.float32)
        for k in range(top):
            route = routes[fold * lot : (fold + 1) * lot, k : k + 1]
            mark = jnp.where(lane == route, 1.0, mark)
        row_stage[:, start + fold * 128 : start + (fold + 1) * 128] = mark.astype(low)
    aligned = layout.shared_own % 16 == 0
    shared_loads = []
    if aligned:
        shared_wide = ranks * layout.shared_own
        for which, source in enumerate((shared_gate_ref, shared_up_ref)):
            load = pltpu.make_async_copy(
                source,
                x_block.at[which, pl.ds(0, depth), pl.ds(0, shared_wide)],
                gather_sem.at[10 + which],
            )
            load.start()
            shared_loads.append(load)
    greet(
        [{"dp": others[k]} for k in range(1, ranks)] + [{"tensor": away[k]} for k in range(1, peers)]
    )
    order = near_first(peers)

    def row_place(device, first, size):
        return rows_all.at[pl.ds(device * lot + first, size)]

    def column_place(device, first, size):
        place = pl.ds(pl.multiple_of(device * depth, depth), depth)
        return columns_all.at[pl.ds(first, size), place]

    for load in loads:
        load.wait()
    gathers = [
        RingGather(ring, row_place, lot, a_sends, a_recvs, a_side_sends, a_side_recvs, 0, 0),
        RingGather(
            ring,
            column_place,
            height,
            a_sends,
            a_recvs,
            a_side_sends,
            a_side_recvs,
            gather_slots(half),
            side_slots(half),
        ),
    ]
    stores_own = []
    for index, (gather, stage) in enumerate(zip(gathers, (row_stage, column_stage))):
        gather.begin(stage)
        store = pltpu.make_async_copy(
            stage, gather.place(ring.me, 0, gather.rows), gather_sem.at[5 + index]
        )
        store.start()
        stores_own.append(store)
    if aligned:
        for which, load in enumerate(shared_loads):
            load.wait()
            for first in range(0, shared_wide, 128):
                size = min(128, shared_wide - first)
                part = x_block[which, :depth, first : first + size]
                shared_rows[which, first : first + size, :] = part.T
    for number in range(1, half):
        for gather in gathers:
            gather.step(number)

    experts, hid = layout.local_experts, layout.expert_hidden
    wides = (gates, ups, downs)
    loads = []
    for which, (target, source) in enumerate(
        zip(wides, (expert_gate_ref, expert_up_ref, expert_down_ref))
    ):
        for j in range(experts):
            load = pltpu.make_async_copy(
                source.at[j],
                target.at[pl.ds(j * layout.part, hid)],
                local_sem.at[5 + which * experts + j],
            )
            load.start()
            loads.append(load)
            if layout.part > hid:
                target[j * layout.part + hid : (j + 1) * layout.part, :] = jnp.zeros(
                    (layout.part - hid, width), low
                )
        target[layout.router_at :, :] = jnp.zeros((layout.hidden - layout.router_at, width), low)

    for gather in gathers:
        gather.step(half)

    def shared_source(which, device):
        if which < 2 and aligned:
            place = pl.ds(pl.multiple_of(device * layout.shared_own, 16), layout.shared_own)
            return shared_rows.at[which, place]
        return (shared_gate_ref, shared_up_ref, shared_down_ref)[which].at[device]

    handed, kept = [], []
    for k in range(1, ranks):
        for which in range(3):
            copy = remote(
                shared_source(which, others[k]),
                shared_got.at[which, ring.me],
                "dp",
                others[k],
                shared_sends,
                shared_recvs,
                which * (ranks - 1) + ranks - k - 1,
            )
            copy.start()
            handed.append(copy)
    for which in range(3):
        copy = pltpu.make_async_copy(
            shared_source(which, ring.me), shared_got.at[which, ring.me], local_sem.at[which]
        )
        copy.start()
        kept.append(copy)

    def cot_place(device, start, size):
        return cot_all.at[pl.ds(device * block + start, size)]

    cots = RingGather(
        ring, cot_place, block, c_sends, c_recvs, c_side_sends, c_side_recvs, 0, 0
    )
    cots.begin(cot_ref)
    kept_cot = pltpu.make_async_copy(cot_ref, cot_place(ring.me, 0, block), local_sem.at[3])
    kept_cot.start()

    for store in stores_own:
        store.wait()
    for gather in gathers:
        for index in range(gather.sides):
            gather.wait_side(index)
    fetches = [
        pltpu.make_async_copy(rows_all, rows_full, gather_sem.at[7]),
        pltpu.make_async_copy(
            columns_all.at[pl.ds(small_rows, head_width)],
            columns_full.at[pl.ds(small_rows, head_width)],
            gather_sem.at[8],
        ),
    ]
    first_rows = pltpu.make_async_copy(
        columns_all.at[pl.ds(0, small_rows)],
        columns_full.at[pl.ds(0, small_rows)],
        gather_sem.at[9],
    )
    first_rows.start()
    for fetch in fetches:
        fetch.start()
    first_rows.wait()
    gates[layout.router_at : layout.router_at + count + 1, :] = columns_full[: count + 1, :]
    vectors = columns_full[:small_rows, :].astype(jnp.float32)
    attn_gain = vectors[count + 1 : count + 2, :]
    ffn_gain = vectors[count + 2 : count + 3, :]

    def norm_in(spot, start, size):
        value = tokens_ref[spot, :].astype(jnp.float32)
        inverse = lax.rsqrt(jnp.mean(value * value, axis=-1, keepdims=True) + EPSILON)
        attn_in[spot, :] = ((value * inverse) * attn_gain).astype(low)

    strips(block, norm_in)
    fetches[0].wait()

    def project(spot):
        qkv_raw[:, spot] = matmul(attn_in[...], rows_full[:, spot])

    tiles(3 * head_width, 256, project)

    def qkv(index):
        return qkv_raw[:, index * HEAD_DIM : (index + 1) * HEAD_DIM]

    attend(heads, qkv, segments_ref, cos_ref, sin_ref, queries, keys, values, probs_ref, context)

    fetches[1].wait()

    def project_out(spot):
        part_ref[:, spot] = matmul(context[...], columns_full[small_rows:, spot]).astype(low)

    tiles(width, 256, project_out)

    exchanged = []
    for k in reversed(order[1:]):
        copy = remote(
            part_ref.at[pl.ds(away[k] * rows, rows)],
            got.at[peers - k - 1],
            "tensor",
            away[k],
            z_sends,
            z_recvs,
            peers - k - 1,
        )
        copy.start()
        exchanged.append(copy)

    for copy in kept + loads:
        copy.wait()
    for copy in handed:
        copy.wait_recv()
    for which, target in enumerate(wides):
        for source in range(ranks):
            columns = slice(source * depth, (source + 1) * depth)
            target[layout.shared_at : layout.router_at, columns] = shared_got[which, source]

    chip_rows = 2 * block

    def chip_spot(turn):
        offset = (1 - 2 * (turn % 2)) * ((turn + 1) // 2)
        return pl.ds(pl.multiple_of(ring.chip(offset) * chip_rows, chip_rows), chip_rows)

    def cot_turn(turn, slot):
        cots.wait_side(turn)
        load_cot = pltpu.make_async_copy(cot_all.at[chip_spot(turn)], cot_block, block_sem.at[0])
        load_cot.start()
        load_cot.wait()
        cot_tiles(layout, cot_block, downs, cot_hidden.at[slot])

    kept_cot.wait()
    cot_turn(0, 0)

    for copy in exchanged:
        copy.wait()
    first = here * rows

    def norm(spot, start, size):
        mine = pl.ds(pl.multiple_of(first + start, size), size)
        total = part_ref[mine, :].astype(jnp.float32)
        for k in range(peers - 1):
            total = total + got[k, spot, :].astype(jnp.float32)
        middle = tokens_ref[mine, :].astype(jnp.float32) + total
        middle_ref[spot, :] = middle
        inverse = lax.rsqrt(jnp.mean(middle * middle, axis=-1, keepdims=True) + EPSILON)
        own[spot, :] = ((middle * inverse) * ffn_gain).astype(own.dtype)

    strips(rows, norm)

    def place_of(k):
        def place(device, start, size):
            return x_all.at[pl.ds(device * block + away[k] * rows + start, size)]

        return place

    mine = place_of(0)(ring.me, 0, rows)

    def peer_place(device, start, size):
        return x_all.at[pl.ds(ring.me * block + device * rows + start, size)]

    forwards = TensorGather(peers, own, peer_place, rows, x_sends, x_recvs)
    forwards.begin()
    works = [
        RingGather(
            ring,
            place_of(k),
            rows,
            sends,
            recvs,
            side_sends,
            side_recvs,
            k * gather_slots(half),
            k * side_slots(half),
        )
        for k in range(peers)
    ]
    works[0].begin(own)
    store = pltpu.make_async_copy(own, mine, local_sem.at[4])
    store.start()

    half_peers = peers // 2
    for number in range(1, half_peers + 1):
        forwards.step(number)
        for k in sorted({peers - number, number}):
            works[k].begin(place_of(k)(ring.me, 0, rows))
        if number == 1:
            cots.step(1)
    store.wait()
    passing = [works[k] for k in order]
    cuts = [part * len(passing) // 4 for part in range(5)]
    first_expert = ring.me * experts

    def stores(spot):
        return [
            pltpu.make_async_copy(source, target.at[spot], store_sem.at[slot])
            for slot, (source, target) in enumerate(
                ((scaled, scaled_ref), (grads, grads_ref), (out, out_ref), (back, back_ref))
            )
        ]

    def fetch_x(turn):
        return pltpu.make_async_copy(
            x_all.at[chip_spot(turn)], x_block.at[turn % 2], x_sem.at[turn % 2]
        )

    for work in works:
        work.wait_side(0)
    fetch_x(0).start()

    def chip_step(turn, carry):
        offset = (1 - 2 * (turn % 2)) * ((turn + 1) // 2)
        spot = chip_spot(turn)
        slot = turn - turn // 4 * (turn - 3)

        def pass_on(part):
            @pl.when(turn == 0)
            def _():
                for work in passing[cuts[part] : cuts[part + 1]]:
                    work.step(1)

        def pass_on_far():
            for number in range(2, half + 1):

                @pl.when(turn == 2 * number - 2)
                def _(number=number):
                    for work in [cots] + passing:
                        work.step(number)

        def fetch_next():
            for work in works:
                work.wait_side(turn + 1)
            fetch_x(turn + 1).start()

        for device in range(2):
            for fold in range(block // lot):
                there = ring.chip(offset) * 2 * lot + device * lot
                first_lane = 3 * head_width + fold * 128
                chosen[device * block + fold * lot : device * block + (fold + 1) * lot, :] = rows_full[
                    pl.ds(pl.multiple_of(there, lot), lot), first_lane : first_lane + 128
                ]
        fetch_x(turn).wait()
        hidden_tiles(layout, x_block.at[turn % 2], gates, ups, pre_gate, pre_up)
        pass_on(0)
        pass_on_far()

        @pl.when(turn == 0)
        def _():
            cot_turn(1, 1)

        @pl.when(turn > 2)
        def _():
            cot_turn(turn, 3)

        pending = stores(spot)

        @pl.when(turn > 0)
        def _():
            pending[0].wait()
            pending[1].wait()

        gate_strips(
            layout,
            first_expert,
            chosen,
            pre_gate,
            pre_up,
            cot_hidden.at[slot],
            scaled,
            grads,
        )
        pending[0].start()
        pending[1].start()
        pass_on(1)

        @pl.when(turn > 0)
        def _():
            pending[2].wait()
            pending[3].wait()

        out_tiles(width, scaled, downs, out)
        pending[2].start()

        @pl.when(turn == 0)
        def _():
            cot_turn(2, 2)

        pass_on(2)

        @pl.when((turn > 0) & (turn + 1 < ring.chips))
        def _():
            fetch_next()

        back_tiles(layout, width, grads, gates, ups, back)
        pending[3].start()
        pass_on(3)

        @pl.when(turn == 0)
        def _():
            fetch_next()

        return carry

    lax.fori_loop(0, ring.chips, chip_step, 0)
    for copy in stores(pl.ds(0, chip_rows)):
        copy.wait()
    forwards.sent()
    for copy in handed:
        copy.wait_send()
    for gather in gathers:
        gather.sent()
    cots.sent()
    for work in works:
        work.sent()


def layer_forward_back(
    layout,
    query,
    key,
    value,
    proj,
    router,
    routes,
    switch,
    attn_gain,
    ffn_gain,
    tokens,
    cot,
    segments,
    cosine,
    sine,
    expert_gate,
    expert_up,
    expert_down,
    shared_gate,
    shared_up,
    shared_down,
    small_rows,
    ranks,
    peers,
    identity,
):
    half = ranks // 4
    block, width = tokens.shape
    rows = block // peers
    total = ranks * block
    depth = width // ranks
    hidden = layout.hidden
    chip = 2 * block
    head_width = query.shape[1]
    wide = 3 * head_width + block // depth * 128
    aligned = layout.shared_own % 16 == 0
    height = small_rows + head_width
    low = tokens.dtype
    vmem = pl.BlockSpec(memory_space=pltpu.VMEM)
    hbm = pl.BlockSpec(memory_space=pl.ANY)
    dma = pltpu.SemaphoreType.DMA
    f32 = jnp.float32
    heads = head_width // HEAD_DIM
    small_ones = [jax.ShapeDtypeStruct((block, head_width), low)] * 4
    return pl.pallas_call(
        functools.partial(layer_kernel, layout, ranks, peers),
        out_shape=(
            jax.ShapeDtypeStruct((width, wide), low),
            jax.ShapeDtypeStruct((height, width), low),
            jax.ShapeDtypeStruct((block, width), low),
            *small_ones,
            jax.ShapeDtypeStruct((heads, block, block), f32),
            jax.ShapeDtypeStruct((total, width), low),
            jax.ShapeDtypeStruct((total, width), low),
            jax.ShapeDtypeStruct((rows, width), f32),
            jax.ShapeDtypeStruct((total, hidden), low),
            jax.ShapeDtypeStruct((total, 2 * hidden), low),
            jax.ShapeDtypeStruct((total, width), low),
            jax.ShapeDtypeStruct((total, width), low),
        ),
        in_specs=[hbm] * 4 + [vmem] * 10 + [hbm] * 6,
        out_specs=(hbm, hbm, *[vmem] * 6, hbm, hbm, vmem, hbm, hbm, hbm, hbm),
        scratch_shapes=[
            pltpu.VMEM((depth, wide), low),
            pltpu.VMEM((height, depth), low),
            pltpu.VMEM((width, wide), low),
            pltpu.VMEM((height, width), low),
            pltpu.VMEM((block, 3 * head_width), f32),
            pltpu.VMEM((block, width), low),
            pltpu.VMEM((hidden, width), low),
            pltpu.VMEM((hidden, width), low),
            pltpu.VMEM((hidden, width), low),
            pltpu.VMEM((3, ranks, layout.shared_own, depth), low),
            pltpu.VMEM((2, ranks * layout.shared_own if aligned else 16, depth), low),
            pltpu.VMEM((rows, width), low),
            pltpu.VMEM((peers - 1, rows, width), low),
            pltpu.VMEM((2, chip, width), low),
            pltpu.VMEM((chip, width), low),
            pltpu.VMEM((chip, hidden), f32),
            pltpu.VMEM((chip, hidden), f32),
            pltpu.VMEM((4, chip, hidden), low),
            pltpu.VMEM((chip, hidden), low),
            pltpu.VMEM((chip, 2 * hidden), low),
            pltpu.VMEM((chip, width), low),
            pltpu.VMEM((chip, width), low),
            pltpu.VMEM((chip, 128), low),
            dma((5 + 3 * layout.local_experts,)),
            dma((12,)),
            dma((2 * gather_slots(half),)),
            dma((2 * gather_slots(half),)),
            dma((2 * side_slots(half),)),
            dma((2 * side_slots(half),)),
            dma((2,)),
            dma((2,)),
            dma((4,)),
            dma((3 * (ranks - 1),)),
            dma((3 * (ranks - 1),)),
            dma((peers - 1,)),
            dma((peers - 1,)),
            dma((peers,)),
            dma((peers,)),
            dma((peers * gather_slots(half),)),
            dma((peers * gather_slots(half),)),
            dma((peers * side_slots(half),)),
            dma((peers * side_slots(half),)),
            dma((gather_slots(half),)),
            dma((gather_slots(half),)),
            dma((side_slots(half),)),
            dma((side_slots(half),)),
        ],
        compiler_params=pltpu.CompilerParams(
            collective_id=identity, has_side_effects=True, vmem_limit_bytes=62 << 20
        ),
        name="layer_forward_back",
    )(
        query,
        key,
        value,
        proj,
        router,
        routes,
        switch,
        attn_gain,
        ffn_gain,
        tokens,
        cot,
        segments,
        cosine,
        sine,
        expert_gate,
        expert_up,
        expert_down,
        shared_gate,
        shared_up,
        shared_down,
    )


class RingReduce:
    def __init__(self, ring, source_at, rows, buffers, sems, slot):
        self.ring, self.source_at, self.rows, self.cut = ring, source_at, rows, rows // 2
        self.mine, self.side, self.got = [buffer.at[slot] for buffer in buffers]
        self.loads, self.sends, self.recvs, self.side_sends, self.side_recvs = sems
        self.base, self.side_base = slot * 2 * ring.half, slot * ring.chips
        half = ring.half
        self.order = [half]
        for distance in range(half - 1, 0, -1):
            self.order += [distance, ring.chips - distance]
        self.order.append(0)

    def load(self, offset):
        return pltpu.make_async_copy(
            self.source_at(self.ring.device(offset)),
            self.mine.at[offset],
            self.loads.at[self.side_base + offset],
        )

    def side_copy(self, offset):
        return remote(
            self.source_at(self.ring.other(offset)),
            self.side.at[offset],
            "dp",
            self.ring.sibling,
            self.side_sends,
            self.side_recvs,
            self.side_base + offset,
        )

    def hand_over(self, offset):
        self.side_copy(offset).start()
        self.load(offset).start()

    def ready(self, offset):
        self.load(offset).wait()
        self.side_copy(offset).wait_recv()

    def hop(self, which, number):
        ring, half, cut = self.ring, self.ring.half, self.cut
        distance = half - number
        offset = distance if which == 0 else ring.chips - distance
        place = pl.ds((0, cut)[which], cut) if number == 0 else pl.ds(0, self.rows)
        return remote(
            self.mine.at[offset, place],
            self.got.at[which * half + number, place],
            "dp",
            (ring.ahead, ring.behind)[which],
            self.sends,
            self.recvs,
            self.base + which * half + number,
        )

    def add(self, offset, extra, first, size):
        def total(spot):
            mine = self.mine[offset, spot, :].astype(jnp.float32)
            return mine + self.side[offset, spot, :].astype(jnp.float32)

        def more(spot, start, count):
            here = pl.ds(pl.multiple_of(first + start, count), count)
            value = total(here) + extra[here, :].astype(jnp.float32)
            self.mine[offset, here, :] = value.astype(self.mine.dtype)

        rest, begin = self.rows - size, 0 if first else size

        def plain(spot, start, count):
            here = pl.ds(pl.multiple_of(begin + start, count), count)
            self.mine[offset, here, :] = total(here).astype(self.mine.dtype)

        if size:
            strips(size, more)
        if rest:
            strips(rest, plain)

    def step(self, number):
        ring, half, cut = self.ring, self.ring.half, self.cut
        if number == 0:
            self.ready(half)
            self.add(half, None, 0, 0)
            self.hop(0, 0).start()
            self.hop(1, 0).start()
            return
        for which in range(2):
            distance = half - number
            offset = distance if which == 0 else ring.chips - distance
            self.ready(offset)
            self.hop(which, number - 1).wait_recv()
            extra = self.got.at[which * half + number - 1]
            if number == 1:
                self.add(offset, extra, (0, cut)[which], cut)
            else:
                self.add(offset, extra, 0, self.rows)
            self.hop(which, number).start()

    def total(self, emit):
        half = self.ring.half
        self.ready(0)
        self.hop(0, half - 1).wait_recv()
        self.hop(1, half - 1).wait_recv()

        def body(spot, start, size):
            value = self.mine[0, spot, :].astype(jnp.float32) + self.side[0, spot, :].astype(jnp.float32)
            value = value + self.got[half - 1, spot, :].astype(jnp.float32)
            value = value + self.got[2 * half - 1, spot, :].astype(jnp.float32)
            emit(spot, start, size, value)

        strips(self.rows, body)

    def finish(self):
        for offset in range(self.ring.chips):
            self.side_copy(offset).wait_send()
        for number in range(self.ring.half):
            for which in range(2):
                self.hop(which, number).wait_send()


def reduce_buffers(pieces, chips, rows, width, low):
    return [pltpu.VMEM((pieces, chips, rows, width), low)] * 3


def reduce_sems(pieces, chips):
    dma = pltpu.SemaphoreType.DMA
    return [dma((pieces * chips,))] * 5


class TensorSum:
    def __init__(self, peers, own_at, got, sends, recvs):
        self.peers, self.half = peers, peers // 2
        self.here = lax.axis_index("tensor")
        self.own_at, self.got, self.sends, self.recvs = own_at, got, sends, recvs
        self.rows = got.shape[1]

    def hop(self, which, number):
        peers, half = self.peers, self.half
        cut = self.rows // 2
        distance = half - number
        k = distance if which == 0 else peers - distance
        if number == 0:
            place, slot = pl.ds((0, cut)[which], cut), 0
        else:
            place, slot = pl.ds(0, self.rows), which * (half - 1) + number
        device = (self.here + (1, peers - 1)[which]) % peers
        return remote(
            self.own_at(k).at[place],
            self.got.at[slot, place],
            "tensor",
            device,
            self.sends,
            self.recvs,
            which * half + number,
        )

    def begin(self):
        self.hop(0, 0).start()
        self.hop(1, 0).start()

    def send(self, k):
        half = self.half
        if k == half:
            self.begin()
            return
        which = 0 if k < half else 1
        number = half - (k if which == 0 else self.peers - k)
        self.hop(which, number - 1).wait_recv()
        own = self.own_at(k)
        cut = self.rows // 2
        first, size, slot = 0, self.rows, which * (half - 1) + number - 1
        if number == 1:
            first, size, slot = (0, cut)[which], cut, 0
        place = slice(first, first + size)
        value = own[place, :].astype(jnp.float32) + self.got[slot, place, :].astype(jnp.float32)
        own[place, :] = value.astype(own.dtype)
        self.hop(which, number).start()

    def arrived(self):
        self.hop(0, self.half - 1).wait_recv()
        self.hop(1, self.half - 1).wait_recv()

    def rest(self, spot):
        half = self.half
        if half == 1:
            return self.got[0, spot, :].astype(jnp.float32)
        value = self.got[half - 1, spot, :].astype(jnp.float32)
        return value + self.got[2 * half - 2, spot, :].astype(jnp.float32)

    def sent(self):
        for number in range(self.half):
            for which in range(2):
                self.hop(which, number).wait_send()


class TensorGather:
    def __init__(self, peers, source, place, rows, sends, recvs):
        self.peers, self.half = peers, peers // 2
        self.here = lax.axis_index("tensor")
        self.source, self.place, self.rows = source, place, rows
        self.sends, self.recvs = sends, recvs

    def hop(self, which, number):
        peers, half = self.peers, self.half
        cut = self.rows // 2
        owner = (self.here + (peers - number, number)[which]) % peers
        first, size = 0, self.rows
        if number and number == half - 1:
            first, size = (0, cut)[which], cut
        target = self.place(owner, first, size)
        source = self.source if number == 0 else target
        device = (self.here + (1, peers - 1)[which]) % peers
        return remote(
            source, target, "tensor", device, self.sends, self.recvs, which * half + number
        )

    def begin(self):
        self.hop(0, 0).start()
        self.hop(1, 0).start()

    def step(self, number):
        for which in range(2):
            self.hop(which, number - 1).wait_recv()
            if number < self.half:
                self.hop(which, number).start()

    def sent(self):
        for number in range(self.half):
            for which in range(2):
                self.hop(which, number).wait_send()


def attend_back(heads, queries, keys, values, probs_ref, grad_context, cos_ref, sin_ref, grads):
    cosine, sine = cos_ref[...], sin_ref[...]
    low = grads.dtype
    scale = HEAD_DIM ** (-0.5)
    for head in range(heads):
        columns = slice(head * HEAD_DIM, (head + 1) * HEAD_DIM)
        probs, through = probs_ref[head], grad_context[:, columns]
        grad_probs = matmul_last(through, values[:, columns])
        inner = jnp.sum(probs * grad_probs, axis=-1, keepdims=True)
        grad_scores = (probs * (grad_probs - inner)).astype(low)
        parts = (
            rope(matmul(grad_scores, keys[:, columns]) * scale, cosine, sine, -1.0),
            rope(matmul(grad_scores.T, queries[:, columns]) * scale, cosine, sine, -1.0),
            matmul(probs.astype(low).T, through),
        )
        for index, part in enumerate(parts):
            first = (index * heads + head) * HEAD_DIM
            grads[:, first : first + HEAD_DIM] = part.astype(low)


def rear_kernel(
    layout,
    ranks,
    peers,
    with_out,
    part_ref,
    out_part_ref,
    x_ref,
    cots_ref,
    grads_ref,
    scaled_ref,
    rows_all,
    columns_all,
    middle_ref,
    cot_ref,
    tokens_ref,
    attn_in,
    queries,
    keys,
    values,
    context,
    probs_ref,
    cos_ref,
    sin_ref,
    input_ref,
    output_ref,
    qkv_sum_ref,
    proj_sum_ref,
    small_sum_ref,
    gate_grads_ref,
    up_grads_ref,
    down_grads_ref,
    shared_grads_ref,
    shared_got_ref,
    cot_rows,
    token_rows,
    small_vec,
    grad_ref,
    small_own,
    small_got,
    small_part,
    small_z,
    z_stage,
    z_got,
    a_got,
    o_got,
    low_ref,
    gm_all,
    right,
    left,
    turned,
    product,
    shared_low,
    gain_grad,
    qkv_full,
    grad_context,
    grad_rows,
    attn_part,
    out_sum,
    kept,
    z_sends,
    z_recvs,
    m_sends,
    m_recvs,
    a_sends,
    a_recvs,
    o_sends,
    o_recvs,
    x_sends,
    x_recvs,
    y_sends,
    y_recvs,
    h_sends,
    h_recvs,
    g_sends,
    g_recvs,
    s_sends,
    s_recvs,
    local_sem,
    left_sem,
    right_sem,
    product_sem,
    reuse_sem,
    *refs,
):
    buffers = refs[0:3]
    back_sems, qkv_sems, proj_buffers, proj_sems = refs[3:8], refs[8:13], refs[13:16], refs[16:21]
    out_buffers, out_sems = refs[21:24], refs[24:]
    out_low = z_stage.at[0]
    ring = Ring(ranks)
    here = lax.axis_index("tensor")
    block, width = cot_ref.shape
    rows = block // peers
    half = ring.half
    low = low_ref.dtype
    columns = width // ranks
    hidden = layout.hidden
    head_width = queries.shape[1]
    heads = head_width // HEAD_DIM
    small_rows = small_vec.shape[0]
    away = [(here + k) % peers for k in range(peers)]
    others = [(ring.me + k) % ranks for k in range(ranks)]
    greet(
        [{"dp": others[k]} for k in range(1, ranks)] + [{"tensor": away[k]} for k in range(1, peers)]
    )
    first = here * rows
    order = list(reversed(near_first(peers)))
    far_first = order[:-1]

    def slice_of(device):
        return pl.ds(pl.multiple_of(device * columns, columns), columns)

    def to_peers(source_of, target_of, sends, recvs):
        return [
            remote(
                source_of(k),
                target_of(peers - k - 1),
                "tensor",
                away[k],
                sends,
                recvs,
                peers - k - 1,
            )
            for k in far_first
        ]

    def reducer(source, where, sems, k):
        def source_at(device):
            return source.at[pl.ds(device * block + away[k] * rows, rows)]

        return RingReduce(ring, source_at, rows, where, sems, k)

    backs = {k: reducer(part_ref, buffers, back_sems, k) for k in order}
    outs = {}
    if with_out:
        outs = {k: reducer(out_part_ref, out_buffers, out_sems, k) for k in order}
    for offset in backs[0].order:
        for k in order:
            backs[k].hand_over(offset)

    tile = right.shape[2]
    blocks = width // tile
    steps = 3 * blocks

    def fetch_left(wide):
        source = scaled_ref if wide == 2 else grads_ref.at[:, pl.ds(wide * hidden, hidden)]
        return pltpu.make_async_copy(source, left, left_sem)

    def fetch_right(step, late):
        spot = pl.ds(pl.multiple_of(step % blocks * tile, tile), tile)
        source = cots_ref if late else x_ref
        return pltpu.make_async_copy(source.at[:, spot], right.at[step % 2], right_sem.at[step % 2])

    fetch_right(0, False).start()
    fetch_left(0).start()
    vec_load = pltpu.make_async_copy(columns_all.at[pl.ds(0, small_rows)], small_vec, local_sem.at[0])
    vec_load.start()
    row_loads = [
        pltpu.make_async_copy(source.at[pl.ds(first, rows)], target, local_sem.at[slot])
        for source, target, slot in ((cot_ref, cot_rows, 5), (tokens_ref, token_rows, 6))
    ]
    for load in row_loads:
        load.start()
    qkv_load = pltpu.make_async_copy(
        rows_all.at[:, pl.ds(0, 3 * head_width)], qkv_full, local_sem.at[1]
    )
    qkv_load.start()
    if not with_out:
        out_load = pltpu.make_async_copy(out_part_ref, out_sum, local_sem.at[2])
        out_load.start()
    for k in order:
        backs[k].step(0)

    def hand_outs():
        for offset in backs[0].order:
            for k in outs:
                outs[k].hand_over(offset)

    vec_load.wait()
    for load in row_loads:
        load.wait()
    count = layout.expert_count
    vectors = small_vec[...].astype(jnp.float32)
    attn_gain = vectors[count + 1 : count + 2, :]
    ffn_gain = vectors[count + 2 : count + 3, :]

    z_sum = TensorSum(peers, lambda k: z_stage.at[k], z_got, z_sends, z_recvs)
    def pass_z(k):
        def emit(spot, start, size, value):
            z_stage[k, spot, :] = value.astype(low)

        backs[k].total(emit)
        z_sum.send(k)

    def results(step, wide):
        slot = step % 2
        spot = pl.ds(pl.multiple_of(step % blocks * tile, tile), tile)
        base = slot * (layout.local_experts + 1)
        copies = [
            pltpu.make_async_copy(
                product.at[slot, pl.ds(j * layout.part, layout.expert_hidden)],
                (gate_grads_ref, up_grads_ref, down_grads_ref)[wide].at[j, :, spot],
                product_sem.at[base + j],
            )
            for j in range(layout.local_experts)
        ]
        copies.append(
            pltpu.make_async_copy(
                shared_low.at[slot],
                shared_grads_ref.at[wide, :, spot],
                product_sem.at[base + layout.local_experts],
            )
        )
        return copies

    gain_grad[...] = jnp.zeros_like(gain_grad)

    def norm_middle(spot, start, size, value):
        value = value + z_sum.rest(spot)
        middle = middle_ref[spot, :]
        inverse = lax.rsqrt(jnp.mean(middle * middle, axis=-1, keepdims=True) + EPSILON)
        normed = middle * inverse
        scaled = value * ffn_gain
        back = inverse * (scaled - normed * jnp.mean(scaled * normed, axis=-1, keepdims=True))
        mine = pl.ds(pl.multiple_of(first + start, size), size)
        grad = cot_rows[spot, :].astype(jnp.float32) + back
        grad_ref[spot, :] = grad
        low_ref[spot, :] = grad.astype(low)
        gm_all[mine, :] = grad.astype(low)
        gain_grad[...] += jnp.sum(value * normed, axis=0, keepdims=True)

    def rows_in(target):
        def place(device, start, size):
            return target.at[pl.ds(device * rows + start, size)]

        return place

    def spread(source, target, sends, recvs):
        return TensorGather(peers, source, rows_in(target), rows, sends, recvs)

    gm_spread = spread(low_ref, gm_all, m_sends, m_recvs)

    def finish_norm():
        z_sum.arrived()
        backs[0].total(norm_middle)
        gm_spread.begin()

    events = []
    for number in range(1, half):
        for index, k in enumerate(order):
            events.append((BACK_DUE[0] + number - 1 + index, functools.partial(backs[k].step, number)))
    events.append((BACK_DUE[1], hand_outs))
    gap = 6 // (peers - 2)
    for index, k in enumerate(far_first):
        events.append((BACK_DUE[2] + gap * index, functools.partial(pass_z, k)))
    for number in range(half):
        for index, k in enumerate(outs):
            due = BACK_DUE[3 + number] + number * index
            events.append((due, functools.partial(outs[k].step, number)))

    def grad_step(step, carry):
        wide, slot = step // blocks, step % 2
        for number in range(3):

            @pl.when(step == number * blocks)
            def _(number=number):
                fetch_left(number).wait()

                def turn_over(index, carry):
                    spot = pl.ds(pl.multiple_of(index * 256, 256), 256)
                    turned[:, spot] = left[spot, :].T
                    return carry

                lax.fori_loop(0, left.shape[0] // 256, turn_over, 0)
                if number < 2:
                    fetch_left(number + 1).start()

        fetch_right(step, False).wait()

        @pl.when(step + 1 < 2 * blocks)
        def _():
            fetch_right(step + 1, False).start()

        @pl.when((step + 1 >= 2 * blocks) & (step + 1 < steps))
        def _():
            fetch_right(step + 1, True).start()

        @pl.when(step > 1)
        def _():
            for copy in results(step, 0):
                copy.wait()

        value = matmul(turned[...], right[slot])
        product[slot] = value[: layout.shared_at].astype(low)
        shared_low[slot] = value[layout.shared_at : layout.router_at].astype(low)

        @pl.when(wide == 0)
        def _():
            spot = pl.ds(pl.multiple_of(step % blocks * tile, tile), tile)
            small_own[:, spot] = value[layout.router_at : layout.router_at + small_rows]

        for number in range(3):

            @pl.when(wide == number)
            def _(number=number):
                for copy in results(step, number):
                    copy.start()

        for due, event in events:

            @pl.when(step == due)
            def _(event=event):
                event()

        return carry

    lax.fori_loop(0, steps, grad_step, 0)
    proj_load = pltpu.make_async_copy(
        columns_all.at[pl.ds(small_rows, head_width)],
        turned.at[pl.ds(head_width, head_width), pl.ds(0, width)],
        local_sem.at[3],
    )
    proj_load.start()
    for step in (steps - 2, steps - 1):
        for copy in results(step, 0):
            copy.wait()

    finish_norm()
    small_own[count + 1 : count + 2, :] = jnp.zeros((1, width), jnp.float32)
    small_own[count + 2 : count + 3, :] = gain_grad[...]
    shared = []
    for k in range(1, ranks):
        copy = remote(
            shared_grads_ref.at[:, :, slice_of(others[k])],
            shared_got_ref.at[ring.me],
            "dp",
            others[k],
            s_sends,
            s_recvs,
            ranks - k - 1,
        )
        copy.start()
        shared.append(copy)
    keep = pltpu.make_async_copy(
        shared_grads_ref.at[:, :, slice_of(ring.me)], kept, local_sem.at[4]
    )
    keep.start()
    half_peers = peers // 2
    for number in range(1, half_peers):
        gm_spread.step(number)

    def chunk_of(source):
        return lambda k: source.at[pl.ds(away[k] * rows, rows)]

    if not with_out:
        out_load.wait()
    for k in outs:

        def emit_out(spot, start, size, value, k=k):
            there = pl.ds(pl.multiple_of(away[k] * rows + start, size), size)
            out_sum[there, :] = value.astype(low)

        outs[k].total(emit_out)
    out_total = TensorSum(peers, chunk_of(out_sum), o_got, o_sends, o_recvs)
    out_total.begin()

    gm_spread.step(half_peers)
    proj_load.wait()
    out_weights = turned.at[pl.ds(head_width, head_width), pl.ds(0, width)]
    grad_context[...] = matmul_last(gm_all[...], out_weights[...]).astype(low)
    attend_back(heads, queries, keys, values, probs_ref, grad_context, cos_ref, sin_ref, grad_rows)
    qkv_load.wait()

    def through_qkv(spot):
        attn_part[:, spot] = matmul_last(grad_rows[...], qkv_full[spot, :]).astype(low)

    tiles(width, 256, through_qkv)
    attn_total = TensorSum(peers, chunk_of(attn_part), a_got, a_sends, a_recvs)
    attn_total.begin()
    def weight_tiles(spot):
        qkv_full[spot, :] = matmul(attn_in[:, spot].T, grad_rows[...]).astype(low)

    tiles(width, 256, weight_tiles)
    for k in far_first[1:]:
        attn_total.send(k)
    for k in far_first[1:]:
        out_total.send(k)

    def proj_tiles(spot):
        turned[:head_width, spot] = matmul(context[...].T, gm_all[:, spot]).astype(low)

    tiles(width, 256, proj_tiles)

    for k in order:
        backs[k].finish()
    for partner in ring.partners():
        pl.semaphore_signal(reuse_sem, inc=1, device_id=partner, device_id_type=MESH)
    pl.semaphore_wait(reuse_sem, 3)
    pieces = proj_buffers[0].shape[0]
    lot, size = qkv_sum_ref.shape[0], qkv_sum_ref.shape[0] // pieces
    proj_size = proj_buffers[0].shape[2]
    narrow = [
        buffer.at[pl.ds(0, pieces), :, pl.ds(0, size), pl.ds(0, 3 * head_width)] for buffer in buffers
    ]
    works = []
    for piece in range(pieces):

        def qkv_at(device, piece=piece):
            return qkv_full.at[pl.ds(device * lot + piece * size, size)]

        def proj_at(device, piece=piece):
            return turned.at[pl.ds(piece * proj_size, proj_size), slice_of(device)]

        works.append(RingReduce(ring, qkv_at, size, narrow, qkv_sems, piece))
        works.append(RingReduce(ring, proj_at, proj_size, proj_buffers, proj_sems, piece))
    for offset in works[0].order:
        for work in works:
            work.hand_over(offset)
    for work in works:
        work.step(0)

    spot_row = count + 1

    def norm_tokens(spot, start, size):
        mine = pl.ds(pl.multiple_of(first + start, size), size)
        value = attn_part[mine, :].astype(jnp.float32)
        value = value + attn_total.rest(spot)
        inputs = token_rows[spot, :].astype(jnp.float32)
        inverse = lax.rsqrt(jnp.mean(inputs * inputs, axis=-1, keepdims=True) + EPSILON)
        normed = inputs * inverse
        scaled = value * attn_gain
        back = inverse * (scaled - normed * jnp.mean(scaled * normed, axis=-1, keepdims=True))
        low_ref[spot, :] = (grad_ref[spot, :] + back).astype(low)
        small_own[spot_row : spot_row + 1, :] += jnp.sum(value * normed, axis=0, keepdims=True)

    attn_total.arrived()
    gm_spread.sent()
    strips(rows, norm_tokens)
    mine = input_ref.at[pl.ds(first, rows)]
    input_spread = spread(low_ref, input_ref, x_sends, x_recvs)
    input_spread.begin()
    stores = [pltpu.make_async_copy(low_ref, mine, local_sem.at[5])]
    stores[0].start()
    handed = []
    for k in range(1, ranks):
        copy = remote(
            small_own.at[:, slice_of(others[k])],
            small_got.at[ranks - k - 1],
            "dp",
            others[k],
            g_sends,
            g_recvs,
            ranks - k - 1,
        )
        copy.start()
        handed.append(copy)

    for number in range(1, half):
        for work in works:
            work.step(number)

    def finish_rows(spot, start, size):
        there = pl.ds(pl.multiple_of(first + start, size), size)
        value = out_sum[there, :].astype(jnp.float32)
        value = value + out_total.rest(spot)
        out_low[spot, :] = (middle_ref[spot, :] + value).astype(low)

    out_total.arrived()
    strips(rows, finish_rows)
    out_mine = output_ref.at[pl.ds(first, rows)]
    output_spread = spread(out_low, output_ref, y_sends, y_recvs)
    output_spread.begin()
    for number in range(1, half_peers):
        input_spread.step(number)
    keep.wait()
    keep = pltpu.make_async_copy(kept, shared_got_ref.at[ring.me], local_sem.at[4])
    keep.start()
    for copy in handed:
        copy.wait_recv()
    value = small_own[:, slice_of(ring.me)]
    for k in range(ranks - 1):
        value = value + small_got[k]
    small_part[...] = value
    last = to_peers(lambda k: small_part, lambda slot: small_z.at[slot], h_sends, h_recvs)
    for copy in last:
        copy.start()
    stores.append(pltpu.make_async_copy(out_low, out_mine, local_sem.at[6]))
    stores[1].start()
    for piece in range(pieces):

        def emit_qkv(spot, start, count, value, piece=piece):
            qkv_sum_ref[pl.ds(pl.multiple_of(piece * size + start, count), count), :] = value

        def emit_proj(spot, start, count, value, piece=piece):
            proj_sum_ref[pl.ds(pl.multiple_of(piece * proj_size + start, count), count), :] = value

        works[2 * piece].total(emit_qkv)
        works[2 * piece + 1].total(emit_proj)
    for number in range(1, half_peers):
        output_spread.step(number)
    for copy in last:
        copy.wait_recv()
    value = small_part[...]
    for k in range(peers - 1):
        value = value + small_z[k]
    small_sum_ref[...] = value
    keep.wait()
    for copy in stores:
        copy.wait()
    input_spread.step(half_peers)
    output_spread.step(half_peers)
    for work in (z_sum, out_total, attn_total, input_spread, output_spread):
        work.sent()
    for copy in handed + last:
        copy.wait_send()
    for copy in shared:
        copy.wait()
    for k in outs:
        outs[k].finish()
    for work in works:
        work.finish()


def rear(
    layout,
    back_part,
    out_part,
    x_all,
    cot_all,
    grads,
    scaled,
    rows_all,
    columns_all,
    middle,
    cotangent,
    tokens,
    attn_in,
    queries,
    keys,
    values,
    context,
    probs,
    cosine,
    sine,
    small_rows,
    with_out,
    ranks,
    peers,
    identity,
):
    chips = ranks // 2
    block, width = tokens.shape
    total = x_all.shape[0]
    rows = block // peers
    hidden, own = layout.hidden, layout.shared_own
    experts, units = layout.local_experts, layout.expert_hidden
    head_width = queries.shape[1]
    columns = width // ranks
    pieces = 4
    tile = 256
    vmem = pl.BlockSpec(memory_space=pltpu.VMEM)
    hbm = pl.BlockSpec(memory_space=pl.ANY)
    dma = pltpu.SemaphoreType.DMA
    low, f32 = tokens.dtype, jnp.float32
    shape = jax.ShapeDtypeStruct
    return pl.pallas_call(
        functools.partial(rear_kernel, layout, ranks, peers, with_out),
        out_shape=(
            shape((block, width), low),
            shape((block, width), low),
            shape((columns, 3 * head_width), f32),
            shape((head_width, columns), f32),
            shape((small_rows, columns), f32),
            *[shape((experts, units, width), low)] * 3,
            shape((3, own, width), low),
            shape((ranks, 3, own, columns), low),
        ),
        in_specs=[hbm] * 8 + [vmem] + [hbm] * 2 + [vmem] * 8,
        out_specs=(hbm, hbm, vmem, vmem, vmem, hbm, hbm, hbm, hbm, hbm),
        scratch_shapes=[
            pltpu.VMEM((rows, width), low),
            pltpu.VMEM((rows, width), low),
            pltpu.VMEM((small_rows, width), low),
            pltpu.VMEM((rows, width), f32),
            pltpu.VMEM((small_rows, width), f32),
            pltpu.VMEM((ranks - 1, small_rows, columns), f32),
            pltpu.VMEM((small_rows, columns), f32),
            pltpu.VMEM((peers - 1, small_rows, columns), f32),
            pltpu.VMEM((peers, rows, width), low),
            pltpu.VMEM((peers - 1, rows, width), low),
            pltpu.VMEM((peers - 1, rows, width), low),
            pltpu.VMEM((peers - 1, rows, width), low),
            pltpu.VMEM((rows, width), low),
            pltpu.VMEM((block, width), low),
            pltpu.VMEM((2, total, tile), low),
            pltpu.VMEM((total, hidden), low),
            pltpu.VMEM((hidden, total), low),
            pltpu.VMEM((2, layout.shared_at, tile), low),
            pltpu.VMEM((2, own, tile), low),
            pltpu.VMEM((1, width), f32),
            pltpu.VMEM((width, 3 * head_width), low),
            pltpu.VMEM((block, head_width), low),
            pltpu.VMEM((block, 3 * head_width), low),
            pltpu.VMEM((block, width), low),
            pltpu.VMEM((block, width), low),
            pltpu.VMEM((3, own, columns), low),
        ]
        + [dma((peers,))] * 14
        + [dma((ranks - 1,))] * 4
        + [
            dma((7,)),
            dma,
            dma((2,)),
            dma((2 * (experts + 1),)),
            pltpu.SemaphoreType.REGULAR,
        ]
        + reduce_buffers(peers, chips, rows, width, low)
        + reduce_sems(peers, chips)
        + reduce_sems(pieces, chips)
        + reduce_buffers(pieces, chips, head_width // pieces, columns, low)
        + reduce_sems(pieces, chips)
        + (reduce_buffers(peers, chips, rows, width, low) + reduce_sems(peers, chips)) * with_out,
        compiler_params=pltpu.CompilerParams(
            collective_id=identity, has_side_effects=True, vmem_limit_bytes=67043328
        ),
        name="rear",
    )(
        back_part,
        out_part,
        x_all,
        cot_all,
        grads,
        scaled,
        rows_all,
        columns_all,
        middle,
        cotangent,
        tokens,
        attn_in,
        queries,
        keys,
        values,
        context,
        probs,
        cosine,
        sine,
    )


def widen_kernel(ranks, experts_in, with_shared, *refs):
    ins, refs = refs[:8], refs[8:]
    gate_in, up_in, down_in, input_in, output_in, qkv_in, proj_in, shared_in = ins
    amount = 12 if with_shared else 9
    outs, refs = refs[:amount], refs[amount:]
    lows, wides, input_low, input_wide, output_low, qkv, proj, shared, rows, turned, sems, out_sems = refs
    loads = []

    def load(source, target):
        copy = pltpu.make_async_copy(source, target, sems.at[len(loads)])
        copy.start()
        loads.append(copy)
        return copy

    stores = []

    def store(source, target):
        copy = pltpu.make_async_copy(source, target, out_sems.at[len(stores)])
        copy.start()
        stores.append(copy)

    parts = []
    for which, source in enumerate((gate_in, up_in, down_in)):
        for j in range(experts_in):
            parts.append((which, j, load(source.at[j], lows.at[which, j])))
    rest = [
        load(input_in, input_low),
        load(output_in, output_low),
        load(qkv_in, qkv),
        load(proj_in, proj),
    ]
    if with_shared:
        rest.append(load(shared_in, shared))

    def convert(source, target):
        size = 32 if source.shape[0] % 32 == 0 else 16

        def step(index, carry):
            spot = pl.ds(pl.multiple_of(index * size, size), size)
            target[spot, :] = source[spot, :].astype(target.dtype)
            return carry

        lax.fori_loop(0, source.shape[0] // size, step, 0)

    for which, j, copy in parts:
        copy.wait()
        convert(lows.at[which, j], wides.at[which, j])
        store(wides.at[which, j], outs[which].at[j])
    rest[0].wait()
    convert(input_low, input_wide)
    store(input_wide, outs[3])
    rest[1].wait()
    store(output_low, outs[4])
    rest[2].wait()
    head_width = qkv.shape[1] // 3
    for which in range(3):
        store(qkv.at[:, pl.ds(which * head_width, head_width)], outs[5 + which])
    rest[3].wait()
    store(proj, outs[8])
    if with_shared:
        rest[4].wait()
        own = shared.shape[2]
        for which in range(3):
            for source in range(ranks):
                rows[which, source * own : (source + 1) * own, :] = shared[source, which].astype(
                    rows.dtype
                )
        for which in range(2):
            for tile in range(rows.shape[1] // 128):
                spot = slice(tile * 128, (tile + 1) * 128)
                turned[which, :, spot] = rows[which, spot, :].T
            store(turned.at[which], outs[9 + which])
        store(rows.at[2], outs[11])
    for copy in stores:
        copy.wait()


def widen(gate, up, down, grad_input, output, qkv, proj, shared):
    experts, units, width = gate.shape
    block = grad_input.shape[0]
    lot, wide = qkv.shape
    ranks, _, own, columns = shared.shape
    with_shared = (ranks * own) % 128 == 0 and own % 16 == 0
    hbm = pl.BlockSpec(memory_space=pl.ANY)
    dma = pltpu.SemaphoreType.DMA
    low, f32 = gate.dtype, jnp.float32
    shape = jax.ShapeDtypeStruct
    outs = [shape((experts, units, width), f32)] * 3
    outs += [shape((block, width), f32), shape((block, width), low)]
    outs += [shape((lot, wide // 3), f32)] * 3
    outs.append(shape(proj.shape, f32))
    if with_shared:
        outs += [shape((columns, ranks * own), f32)] * 2
        outs.append(shape((ranks * own, columns), f32))
    results = pl.pallas_call(
        functools.partial(widen_kernel, ranks, experts, with_shared),
        out_shape=tuple(outs),
        in_specs=[hbm] * 8,
        out_specs=(hbm,) * len(outs),
        scratch_shapes=[
            pltpu.VMEM((3, experts, units, width), low),
            pltpu.VMEM((3, experts, units, width), f32),
            pltpu.VMEM((block, width), low),
            pltpu.VMEM((block, width), f32),
            pltpu.VMEM((block, width), low),
            pltpu.VMEM((lot, wide), f32),
            pltpu.VMEM(proj.shape, f32),
            pltpu.VMEM(shared.shape, low),
            pltpu.VMEM((3, ranks * own, columns), f32),
            pltpu.VMEM((2, columns, ranks * own), f32),
            dma((3 * experts + 5,)),
            dma((3 * experts + 9,)),
        ],
        compiler_params=pltpu.CompilerParams(vmem_limit_bytes=60 << 20),
        name="widen",
    )(gate, up, down, grad_input, output, qkv, proj, shared)
    if with_shared:
        return results
    shared = shared.astype(f32)
    whole = [shared[:, which].reshape(ranks * own, columns) for which in range(3)]
    return (*results, whole[0].T, whole[1].T, whole[2])


def rope_tables():
    half_dim = HEAD_DIM // 2
    exponent = np.arange(half_dim, dtype=np.float32) * np.float32(2.0 / HEAD_DIM)
    inverse_freq = np.exp(-exponent * np.log(np.float32(1000000.0)))
    angles = np.arange(SEQ, dtype=np.float32)[:, None] * inverse_freq[None, :]
    cosine, sine = np.cos(angles), np.sin(angles)
    return (
        jnp.asarray(np.concatenate([cosine, cosine], axis=1)),
        jnp.asarray(np.concatenate([-sine, sine], axis=1)),
    )


def scatter_rows(values):
    return lax.psum_scatter(values, "dp", scatter_dimension=0, tiled=True)


def shards(
    tokens,
    w_query,
    w_key,
    w_value,
    w_out,
    gain_attn,
    gain_ffn,
    w_router,
    shared_gate,
    shared_up,
    shared_down,
    shared_switch,
    expert_gate,
    expert_up_weight,
    expert_down,
    routes,
    segments,
    cotangent,
):
    low = jnp.bfloat16
    ranks = lax.axis_size("dp")
    peers = lax.axis_size("tensor")
    token_count, width = tokens.shape
    local_experts, _, expert_hidden = expert_gate.shape
    expert_count = local_experts * ranks
    block = width // ranks
    head_width = w_query.shape[1]
    shared_own = shared_gate.shape[1] // ranks
    layout = Layout(local_experts, expert_hidden, shared_own, expert_count)

    small_rows = -(-(expert_count + 3) // 16) * 16
    cosine, sine = rope_tables()
    gate_rows, up_rows = shared_gate, shared_up
    if shared_own % 16:
        gate_rows, up_rows = [
            part.T.reshape(ranks, shared_own, block) for part in (shared_gate, shared_up)
        ]

    (
        qkv_full,
        columns_full,
        attn_in,
        queries,
        key_rows,
        value_rows,
        context_flat,
        probs,
        x_all,
        cot_all,
        middle,
        scaled_hidden,
        grads_wide,
        out_part,
        back_part,
    ) = layer_forward_back(
        layout,
        w_query,
        w_key,
        w_value,
        w_out,
        w_router.T,
        routes.T,
        shared_switch,
        gain_attn,
        gain_ffn,
        tokens,
        cotangent,
        segments,
        cosine,
        sine,
        expert_gate.swapaxes(1, 2),
        expert_up_weight.swapaxes(1, 2),
        expert_down,
        gate_rows,
        up_rows,
        shared_down.reshape(ranks, shared_own, block),
        small_rows,
        ranks,
        peers,
        1,
    )
    with_out = ranks == 8
    grad_input, output, grad_qkv, grad_proj, grad_small, *grad_experts, _, grad_shared = rear(
        layout,
        back_part,
        out_part if with_out else scatter_rows(out_part),
        x_all,
        cot_all,
        grads_wide,
        scaled_hidden,
        qkv_full,
        columns_full,
        middle,
        cotangent,
        tokens,
        attn_in,
        queries,
        key_rows,
        value_rows,
        context_flat,
        probs,
        cosine,
        sine,
        small_rows,
        with_out,
        ranks,
        peers,
        2,
    )
    (
        grad_gate,
        grad_up,
        grad_down,
        grad_input,
        output,
        grad_query,
        grad_key,
        grad_value,
        grad_proj,
        grad_shared_gate,
        grad_shared_up,
        grad_shared_down,
    ) = widen(*grad_experts, grad_input, output, grad_qkv, grad_proj, grad_shared)
    return (
        output,
        grad_input,
        grad_query,
        grad_key,
        grad_value,
        grad_proj,
        grad_small[expert_count + 1],
        grad_small[expert_count + 2],
        grad_small[:expert_count].T,
        grad_shared_gate,
        grad_shared_up,
        grad_shared_down,
        grad_small[expert_count],
        grad_gate.swapaxes(1, 2),
        grad_up.swapaxes(1, 2),
        grad_down,
    )


def solution(mesh):
    in_specs = (
        P("dp", None),
        P("dp", "tensor"),
        P("dp", "tensor"),
        P("dp", "tensor"),
        P("tensor", "dp"),
        P("dp"),
        P("dp"),
        P("dp", None),
        P("dp", "tensor"),
        P("dp", "tensor"),
        P("tensor", "dp"),
        P("dp"),
        P("dp", None, "tensor"),
        P("dp", None, "tensor"),
        P("dp", "tensor", None),
        P("dp", None),
        P("dp", None),
        P("dp", None),
    )
    out_specs = (
        P("dp", None),
        P("dp", None),
        P("dp", "tensor"),
        P("dp", "tensor"),
        P("dp", "tensor"),
        P("tensor", "dp"),
        P("dp"),
        P("dp"),
        P("dp", None),
        P("dp", "tensor"),
        P("dp", "tensor"),
        P("tensor", "dp"),
        P("dp"),
        P("dp", None, "tensor"),
        P("dp", None, "tensor"),
        P("dp", "tensor", None),
    )
    return jax.shard_map(shards, mesh=mesh, in_specs=in_specs, out_specs=out_specs, check_vma=False)
```

```python
import functools

import jax
import jax.numpy as jnp
import numpy as np
from jax import lax
from jax.experimental import pallas as pl
from jax.experimental.pallas import tpu as pltpu
from jax.sharding import PartitionSpec as P

HEAD_DIM = 128
TOP = 4
SEQ = 256


EPSILON = 1e-06
MESH = pl.DeviceIdType.MESH


def ring_chip(position, chips):
    half = chips // 2
    upper = position // half
    return position + upper * (chips - 1 + half - 2 * position)


def ring_spot(chip, chips):
    return ring_chip(chip, chips)


def greet(partners):
    barrier = pltpu.get_barrier_semaphore()
    for partner in partners:
        pl.semaphore_signal(barrier, inc=1, device_id=partner, device_id_type=MESH)
    pl.semaphore_wait(barrier, len(partners))


def remote(source, target, axis, device, sends, recvs, slot):
    return pltpu.make_async_remote_copy(
        src_ref=source,
        dst_ref=target,
        send_sem=sends.at[slot],
        recv_sem=recvs.at[slot],
        device_id={axis: device},
        device_id_type=MESH,
    )


class Ring:
    def __init__(self, ranks):
        self.ranks = ranks
        self.chips = ranks // 2
        self.half = self.chips // 2
        self.me = lax.axis_index("dp")
        self.core = self.me % 2
        self.position = ring_spot(self.me // 2, self.chips)
        self.sibling = self.me + 1 - 2 * self.core
        self.ahead = self.device(1)
        self.behind = self.device(-1)

    def chip(self, offset):
        return ring_chip((self.position + offset + self.chips) % self.chips, self.chips)

    def device(self, offset):
        return self.chip(offset) * 2 + self.core

    def other(self, offset):
        return self.chip(offset) * 2 + 1 - self.core

    def partners(self):
        return [{"dp": self.ahead}, {"dp": self.behind}, {"dp": self.sibling}]


def gather_slots(half):
    return 2 * half


def side_slots(half):
    return 2 * half


class RingGather:
    def __init__(self, ring, place, rows, sends, recvs, side_sends, side_recvs, base, side_base):
        self.ring, self.place, self.rows, self.cut = ring, place, rows, rows // 2
        self.sends, self.recvs = sends, recvs
        self.side_sends, self.side_recvs = side_sends, side_recvs
        self.base, self.side_base = base, side_base
        self.sides = side_slots(ring.half)

    def hop_copy(self, source, target, device, slot):
        return remote(source, target, "dp", device, self.sends, self.recvs, self.base + slot)

    def side_copy(self, source, target, slot):
        return remote(
            source,
            target,
            "dp",
            self.ring.sibling,
            self.side_sends,
            self.side_recvs,
            self.side_base + slot,
        )

    def hop_size(self, slot):
        number = slot % self.ring.half
        return self.cut if number and number == self.ring.half - 1 else self.rows

    def begin(self, source):
        ring = self.ring
        target = self.place(ring.me, 0, self.rows)
        self.hop_copy(source, target, ring.ahead, 0).start()
        self.hop_copy(source, target, ring.behind, ring.half).start()
        self.side_copy(source, target, 0).start()

    def wait_hop(self, slot):
        block = self.place(self.ring.me, 0, self.hop_size(slot))
        self.hop_copy(block, block, self.ring.ahead, slot).wait_recv()

    def step(self, number):
        ring = self.ring
        for which, sign in enumerate((-1, 1)):
            owner = ring.device(sign * number)
            onward = (ring.ahead, ring.behind)[which]
            self.wait_hop(which * ring.half + number - 1)
            if number < ring.half:
                block = self.place(owner, 0, self.rows)
                slot = which * ring.half + number
                size = self.hop_size(slot)
                part = block if size == self.rows else self.place(owner, (0, self.cut)[which], size)
                self.hop_copy(part, part, onward, slot).start()
                self.side_copy(block, block, 2 * number - 1 + which).start()
        if number == ring.half:
            block = self.place(ring.device(number), 0, self.rows)
            self.side_copy(block, block, 2 * ring.half - 1).start()

    def wait_side(self, index):
        block = self.place(self.ring.me, 0, self.rows)
        self.side_copy(block, block, index).wait_recv()

    def sent(self):
        for slot in range(2 * self.ring.half):
            block = self.place(self.ring.me, 0, self.hop_size(slot))
            self.hop_copy(block, block, self.ring.ahead, slot).wait_send()
        for index in range(self.sides):
            block = self.place(self.ring.me, 0, self.rows)
            self.side_copy(block, block, index).wait_send()


def near_first(peers):
    order = [0]
    for step in range(1, peers // 2 + 1):
        order.append(step)
        if peers - step != step:
            order.append(peers - step)
    return order


STRIP = 64
BACK_DUE = (0, 5, 11, 11, 17)
NORM_DUE = 19


def strips(rows, body):
    strip = min(STRIP, rows)

    def step(index, carry):
        body(pl.ds(pl.multiple_of(index * strip, strip), strip), index * strip, strip)
        return carry

    lax.fori_loop(0, rows // strip, step, 0)


HIDDEN_TILE, OUT_TILE, BACK_TILE = 1024, 1024, 1024


def matmul(left, right):
    return lax.dot_general(
        left, right, (((1,), (0,)), ((), ())), preferred_element_type=jnp.float32
    )


def matmul_last(left, right):
    return lax.dot_general(
        left, right, (((1,), (1,)), ((), ())), preferred_element_type=jnp.float32
    )


def tiles(width, tile, body):
    def step(index, carry):
        body(pl.ds(pl.multiple_of(index * tile, tile), tile))
        return carry

    lax.fori_loop(0, width // tile, step, 0)


class Layout:
    def __init__(self, local_experts, expert_hidden, shared_own, expert_count):
        self.local_experts = local_experts
        self.expert_hidden = expert_hidden
        self.shared_own = shared_own
        self.expert_count = expert_count
        self.part = -(-expert_hidden // 128) * 128
        self.shared_at = local_experts * self.part
        self.router_at = self.shared_at + shared_own
        self.last = -(-(shared_own + expert_count + 1) // 128) * 128
        self.hidden = self.shared_at + self.last
        self.router_tile = self.router_at // 128 * 128
        self.router_lane = self.router_at - self.router_tile
        self.tile = next(size for size in (HIDDEN_TILE, 256, 128) if self.hidden % size == 0)


def hidden_tiles(layout, x_ref, gates, ups, pre_gate, pre_up):
    def body(spot):
        pre_gate[:, spot] = matmul_last(x_ref[...], gates[spot, :])
        pre_up[:, spot] = matmul_last(x_ref[...], ups[spot, :])

    tiles(layout.hidden, layout.tile, body)


def cot_tiles(layout, cot_ref, downs, cot_hidden):
    def body(spot):
        cot_hidden[:, spot] = matmul_last(cot_ref[...], downs[spot, :]).astype(cot_hidden.dtype)

    tiles(layout.hidden, layout.tile, body)


def gate_strips(layout, first_expert, chosen, pre_gate, pre_up, cot_hidden, scaled, grads):
    rows = pre_gate.shape[0]
    count, lane0 = layout.expert_count, layout.router_lane
    router = slice(layout.router_tile, layout.router_tile + 128)
    bounds = [(j * layout.part, (j + 1) * layout.part) for j in range(layout.local_experts)]
    bounds.append((layout.shared_at, layout.hidden))
    low = scaled.dtype

    def body(spot, start, size):
        lane = lax.broadcasted_iota(jnp.int32, (size, 128), 1)
        logits = pre_gate[spot, router]
        is_router = (lane >= lane0) & (lane < lane0 + count)
        is_switch = lane == lane0 + count
        power = jnp.where(is_router, jnp.exp(jnp.where(is_router, logits, 0.0)), 0.0)
        probs = power / jnp.sum(power, axis=-1, keepdims=True)
        raw = jnp.sum(jnp.where(is_switch, logits, 0.0), axis=-1, keepdims=True)
        switch = 1.0 / (1.0 + jnp.exp(-raw))
        mask = chosen[spot, :].astype(jnp.float32)
        scales = []
        for j in range(layout.local_experts):
            spotted = lane == lane0 + first_expert + j
            scales.append(jnp.sum(jnp.where(spotted, probs * mask, 0.0), axis=-1, keepdims=True))
        scales.append(switch)
        totals = []
        for (begin, end), scale in zip(bounds, scales):
            shared = begin == layout.shared_at
            columns = slice(begin, end)
            gate, up = pre_gate[spot, columns], pre_up[spot, columns]
            through = cot_hidden[spot, columns].astype(jnp.float32)
            sig = 1.0 / (1.0 + jnp.exp(-gate))
            act = gate * sig
            state = act * up
            grad = scale * through
            totals.append(jnp.sum(state * through, axis=-1, keepdims=True))
            scaled[spot, columns] = (scale * state).astype(low)
            grad_gate = grad * up * sig * (1.0 + gate * (1.0 - sig))
            grads[spot, columns] = grad_gate.astype(low)
            grads[spot, layout.hidden + begin : layout.hidden + end] = (grad * act).astype(low)
        choice = jnp.zeros_like(probs)
        for j in range(layout.local_experts):
            spotted = lane == lane0 + first_expert + j
            choice = choice + jnp.where(spotted, mask * totals[j], 0.0)
        small = probs * (choice - jnp.sum(probs * choice, axis=-1, keepdims=True))
        small = jnp.where(is_switch, totals[-1] * switch * (1.0 - switch), small)
        kept = grads[spot, router].astype(jnp.float32)
        kept = jnp.where(is_router | is_switch, small, kept)
        grads[spot, router] = kept.astype(low)

    strips(rows, body)


def out_tiles(width, scaled, downs, out):
    def body(spot):
        out[:, spot] = matmul(scaled[...], downs[:, spot]).astype(out.dtype)

    tiles(width, OUT_TILE, body)


def back_tiles(layout, width, grads, gates, ups, back):
    hidden = layout.hidden

    def body(spot):
        total = matmul(grads[:, :hidden], gates[:, spot])
        total = total + matmul(grads[:, hidden:], ups[:, spot])
        back[:, spot] = total.astype(back.dtype)

    tiles(width, BACK_TILE, body)


def rope(values, cosine, sine, sign):
    return values * cosine + pltpu.roll(values, HEAD_DIM // 2, 1) * (sine * sign)


def attend(heads, qkv, segments_ref, cos_ref, sin_ref, queries, keys, values, probs_ref, context):
    cosine, sine = cos_ref[...], sin_ref[...]
    length = queries.shape[0]
    segments = jnp.broadcast_to(segments_ref[...].astype(jnp.float32), (length, length))
    row = lax.broadcasted_iota(jnp.int32, (length, length), 0)
    column = lax.broadcasted_iota(jnp.int32, (length, length), 1)
    allowed = (segments == segments.T) & (column <= row)
    low = queries.dtype
    for head in range(heads):
        columns = slice(head * HEAD_DIM, (head + 1) * HEAD_DIM)
        query = rope(qkv(head), cosine, sine, 1.0).astype(low)
        key = rope(qkv(heads + head), cosine, sine, 1.0).astype(low)
        value = qkv(2 * heads + head).astype(low)
        queries[:, columns], keys[:, columns], values[:, columns] = query, key, value
        scores = matmul_last(query, key) * HEAD_DIM ** (-0.5)
        power = jnp.where(allowed, jnp.exp(jnp.where(allowed, scores, 0.0)), 0.0)
        probs = power / jnp.sum(power, axis=-1, keepdims=True)
        probs_ref[head] = probs
        context[:, columns] = matmul(probs.astype(low), value).astype(low)


def layer_kernel(
    layout,
    ranks,
    peers,
    query_ref,
    key_ref,
    value_ref,
    proj_ref,
    router_ref,
    routes_ref,
    switch_ref,
    attn_gain_ref,
    ffn_gain_ref,
    tokens_ref,
    cot_ref,
    segments_ref,
    cos_ref,
    sin_ref,
    expert_gate_ref,
    expert_up_ref,
    expert_down_ref,
    shared_gate_ref,
    shared_up_ref,
    shared_down_ref,
    rows_all,
    columns_all,
    attn_in,
    queries,
    keys,
    values,
    context,
    probs_ref,
    x_all,
    cot_all,
    middle_ref,
    scaled_ref,
    grads_ref,
    out_ref,
    back_ref,
    row_stage,
    column_stage,
    rows_full,
    columns_full,
    qkv_raw,
    part_ref,
    gates,
    ups,
    downs,
    shared_got,
    shared_rows,
    own,
    got,
    x_block,
    cot_block,
    pre_gate,
    pre_up,
    cot_hidden,
    scaled,
    grads,
    out,
    back,
    chosen,
    local_sem,
    gather_sem,
    a_sends,
    a_recvs,
    a_side_sends,
    a_side_recvs,
    block_sem,
    x_sem,
    store_sem,
    shared_sends,
    shared_recvs,
    z_sends,
    z_recvs,
    x_sends,
    x_recvs,
    sends,
    recvs,
    side_sends,
    side_recvs,
    c_sends,
    c_recvs,
    c_side_sends,
    c_side_recvs,
):
    ring = Ring(ranks)
    here = lax.axis_index("tensor")
    block, width = tokens_ref.shape
    rows = block // peers
    depth = width // ranks
    half = ring.half
    away = [(here + k) % peers for k in range(peers)]
    others = [(ring.me + k) % ranks for k in range(ranks)]

    count, lane0 = layout.expert_count, layout.router_lane
    head_width = query_ref.shape[1]
    heads = head_width // HEAD_DIM
    lot, wide = row_stage.shape
    height = column_stage.shape[0]
    small_rows = height - head_width
    low = gates.dtype
    loads, start = [], 0
    for index, source in enumerate((query_ref, key_ref, value_ref)):
        size = source.shape[1]
        loads.append(
            pltpu.make_async_copy(source, row_stage.at[:, pl.ds(start, size)], gather_sem.at[index])
        )
        start += size
    loads.append(
        pltpu.make_async_copy(
            proj_ref, column_stage.at[pl.ds(small_rows, head_width)], gather_sem.at[4]
        )
    )
    for load in loads:
        load.start()
    small = jnp.concatenate(
        [
            router_ref[...].astype(jnp.float32),
            switch_ref[...].astype(jnp.float32).reshape(1, depth),
            attn_gain_ref[...].astype(jnp.float32).reshape(1, depth),
            ffn_gain_ref[...].astype(jnp.float32).reshape(1, depth),
            jnp.zeros((small_rows - count - 3, depth), jnp.float32),
        ],
        axis=0,
    )
    column_stage[:small_rows, :] = small.astype(low)
    top = routes_ref.shape[0]
    routes = routes_ref[...].astype(jnp.float32)
    routes = jnp.concatenate([routes, jnp.zeros((8 - top, block), jnp.float32)], axis=0).T
    for fold in range(block // lot):
        lane = lax.broadcasted_iota(jnp.int32, (lot, 128), 1).astype(jnp.float32) - lane0
        mark = jnp.zeros((lot, 128), jnp.float32)
        for k in range(top):
            route = routes[fold * lot : (fold + 1) * lot, k : k + 1]
            mark = jnp.where(lane == route, 1.0, mark)
        row_stage[:, start + fold * 128 : start + (fold + 1) * 128] = mark.astype(low)
    aligned = layout.shared_own % 16 == 0
    shared_loads = []
    if aligned:
        shared_wide = ranks * layout.shared_own
        for which, source in enumerate((shared_gate_ref, shared_up_ref)):
            load = pltpu.make_async_copy(
                source,
                x_block.at[which, pl.ds(0, depth), pl.ds(0, shared_wide)],
                gather_sem.at[10 + which],
            )
            load.start()
            shared_loads.append(load)
    greet(
        [{"dp": others[k]} for k in range(1, ranks)] + [{"tensor": away[k]} for k in range(1, peers)]
    )
    order = near_first(peers)

    def row_place(device, first, size):
        return rows_all.at[pl.ds(device * lot + first, size)]

    def column_place(device, first, size):
        place = pl.ds(pl.multiple_of(device * depth, depth), depth)
        return columns_all.at[pl.ds(first, size), place]

    for load in loads:
        load.wait()
    gathers = [
        RingGather(ring, row_place, lot, a_sends, a_recvs, a_side_sends, a_side_recvs, 0, 0),
        RingGather(
            ring,
            column_place,
            height,
            a_sends,
            a_recvs,
            a_side_sends,
            a_side_recvs,
            gather_slots(half),
            side_slots(half),
        ),
    ]
    stores_own = []
    for index, (gather, stage) in enumerate(zip(gathers, (row_stage, column_stage))):
        gather.begin(stage)
        store = pltpu.make_async_copy(
            stage, gather.place(ring.me, 0, gather.rows), gather_sem.at[5 + index]
        )
        store.start()
        stores_own.append(store)
    if aligned:
        for which, load in enumerate(shared_loads):
            load.wait()
            for first in range(0, shared_wide, 128):
                size = min(128, shared_wide - first)
                part = x_block[which, :depth, first : first + size]
                shared_rows[which, first : first + size, :] = part.T
    for number in range(1, half):
        for gather in gathers:
            gather.step(number)

    experts, hid = layout.local_experts, layout.expert_hidden
    wides = (gates, ups, downs)
    loads = []
    for which, (target, source) in enumerate(
        zip(wides, (expert_gate_ref, expert_up_ref, expert_down_ref))
    ):
        for j in range(experts):
            load = pltpu.make_async_copy(
                source.at[j],
                target.at[pl.ds(j * layout.part, hid)],
                local_sem.at[5 + which * experts + j],
            )
            load.start()
            loads.append(load)
            if layout.part > hid:
                target[j * layout.part + hid : (j + 1) * layout.part, :] = jnp.zeros(
                    (layout.part - hid, width), low
                )
        target[layout.router_at :, :] = jnp.zeros((layout.hidden - layout.router_at, width), low)

    for gather in gathers:
        gather.step(half)

    def shared_source(which, device):
        if which < 2 and aligned:
            place = pl.ds(pl.multiple_of(device * layout.shared_own, 16), layout.shared_own)
            return shared_rows.at[which, place]
        return (shared_gate_ref, shared_up_ref, shared_down_ref)[which].at[device]

    handed, kept = [], []
    for k in range(1, ranks):
        for which in range(3):
            copy = remote(
                shared_source(which, others[k]),
                shared_got.at[which, ring.me],
                "dp",
                others[k],
                shared_sends,
                shared_recvs,
                which * (ranks - 1) + ranks - k - 1,
            )
            copy.start()
            handed.append(copy)
    for which in range(3):
        copy = pltpu.make_async_copy(
            shared_source(which, ring.me), shared_got.at[which, ring.me], local_sem.at[which]
        )
        copy.start()
        kept.append(copy)

    def cot_place(device, start, size):
        return cot_all.at[pl.ds(device * block + start, size)]

    cots = RingGather(
        ring, cot_place, block, c_sends, c_recvs, c_side_sends, c_side_recvs, 0, 0
    )
    cots.begin(cot_ref)
    kept_cot = pltpu.make_async_copy(cot_ref, cot_place(ring.me, 0, block), local_sem.at[3])
    kept_cot.start()

    for store in stores_own:
        store.wait()
    for gather in gathers:
        for index in range(gather.sides):
            gather.wait_side(index)
    fetches = [
        pltpu.make_async_copy(rows_all, rows_full, gather_sem.at[7]),
        pltpu.make_async_copy(
            columns_all.at[pl.ds(small_rows, head_width)],
            columns_full.at[pl.ds(small_rows, head_width)],
            gather_sem.at[8],
        ),
    ]
    first_rows = pltpu.make_async_copy(
        columns_all.at[pl.ds(0, small_rows)],
        columns_full.at[pl.ds(0, small_rows)],
        gather_sem.at[9],
    )
    first_rows.start()
    for fetch in fetches:
        fetch.start()
    first_rows.wait()
    gates[layout.router_at : layout.router_at + count + 1, :] = columns_full[: count + 1, :]
    vectors = columns_full[:small_rows, :].astype(jnp.float32)
    attn_gain = vectors[count + 1 : count + 2, :]
    ffn_gain = vectors[count + 2 : count + 3, :]

    def norm_in(spot, start, size):
        value = tokens_ref[spot, :].astype(jnp.float32)
        inverse = lax.rsqrt(jnp.mean(value * value, axis=-1, keepdims=True) + EPSILON)
        attn_in[spot, :] = ((value * inverse) * attn_gain).astype(low)

    strips(block, norm_in)
    fetches[0].wait()

    def project(spot):
        qkv_raw[:, spot] = matmul(attn_in[...], rows_full[:, spot])

    tiles(3 * head_width, 256, project)

    def qkv(index):
        return qkv_raw[:, index * HEAD_DIM : (index + 1) * HEAD_DIM]

    attend(heads, qkv, segments_ref, cos_ref, sin_ref, queries, keys, values, probs_ref, context)

    fetches[1].wait()

    def project_out(spot):
        part_ref[:, spot] = matmul(context[...], columns_full[small_rows:, spot]).astype(low)

    tiles(width, 256, project_out)

    exchanged = []
    for k in reversed(order[1:]):
        copy = remote(
            part_ref.at[pl.ds(away[k] * rows, rows)],
            got.at[peers - k - 1],
            "tensor",
            away[k],
            z_sends,
            z_recvs,
            peers - k - 1,
        )
        copy.start()
        exchanged.append(copy)

    for copy in kept + loads:
        copy.wait()
    for copy in handed:
        copy.wait_recv()
    for which, target in enumerate(wides):
        for source in range(ranks):
            columns = slice(source * depth, (source + 1) * depth)
            target[layout.shared_at : layout.router_at, columns] = shared_got[which, source]

    chip_rows = 2 * block

    def chip_spot(turn):
        offset = (1 - 2 * (turn % 2)) * ((turn + 1) // 2)
        return pl.ds(pl.multiple_of(ring.chip(offset) * chip_rows, chip_rows), chip_rows)

    def cot_turn(turn, slot):
        cots.wait_side(turn)
        load_cot = pltpu.make_async_copy(cot_all.at[chip_spot(turn)], cot_block, block_sem.at[0])
        load_cot.start()
        load_cot.wait()
        cot_tiles(layout, cot_block, downs, cot_hidden.at[slot])

    kept_cot.wait()
    cot_turn(0, 0)

    for copy in exchanged:
        copy.wait()
    first = here * rows

    def norm(spot, start, size):
        mine = pl.ds(pl.multiple_of(first + start, size), size)
        total = part_ref[mine, :].astype(jnp.float32)
        for k in range(peers - 1):
            total = total + got[k, spot, :].astype(jnp.float32)
        middle = tokens_ref[mine, :].astype(jnp.float32) + total
        middle_ref[spot, :] = middle
        inverse = lax.rsqrt(jnp.mean(middle * middle, axis=-1, keepdims=True) + EPSILON)
        own[spot, :] = ((middle * inverse) * ffn_gain).astype(own.dtype)

    strips(rows, norm)

    def place_of(k):
        def place(device, start, size):
            return x_all.at[pl.ds(device * block + away[k] * rows + start, size)]

        return place

    mine = place_of(0)(ring.me, 0, rows)

    def peer_place(device, start, size):
        return x_all.at[pl.ds(ring.me * block + device * rows + start, size)]

    forwards = TensorGather(peers, own, peer_place, rows, x_sends, x_recvs)
    forwards.begin()
    works = [
        RingGather(
            ring,
            place_of(k),
            rows,
            sends,
            recvs,
            side_sends,
            side_recvs,
            k * gather_slots(half),
            k * side_slots(half),
        )
        for k in range(peers)
    ]
    works[0].begin(own)
    store = pltpu.make_async_copy(own, mine, local_sem.at[4])
    store.start()

    half_peers = peers // 2
    for number in range(1, half_peers + 1):
        forwards.step(number)
        for k in sorted({peers - number, number}):
            works[k].begin(place_of(k)(ring.me, 0, rows))
        if number == 1:
            cots.step(1)
    store.wait()
    passing = [works[k] for k in order]
    cuts = [part * len(passing) // 4 for part in range(5)]
    first_expert = ring.me * experts

    def stores(spot):
        return [
            pltpu.make_async_copy(source, target.at[spot], store_sem.at[slot])
            for slot, (source, target) in enumerate(
                ((scaled, scaled_ref), (grads, grads_ref), (out, out_ref), (back, back_ref))
            )
        ]

    def fetch_x(turn):
        return pltpu.make_async_copy(
            x_all.at[chip_spot(turn)], x_block.at[turn % 2], x_sem.at[turn % 2]
        )

    for work in works:
        work.wait_side(0)
    fetch_x(0).start()

    def chip_step(turn, carry):
        offset = (1 - 2 * (turn % 2)) * ((turn + 1) // 2)
        spot = chip_spot(turn)
        slot = turn - turn // 4 * (turn - 3)

        def pass_on(part):
            @pl.when(turn == 0)
            def _():
                for work in passing[cuts[part] : cuts[part + 1]]:
                    work.step(1)

        def pass_on_far():
            for number in range(2, half + 1):

                @pl.when(turn == 2 * number - 2)
                def _(number=number):
                    for work in [cots] + passing:
                        work.step(number)

        def fetch_next():
            for work in works:
                work.wait_side(turn + 1)
            fetch_x(turn + 1).start()

        for device in range(2):
            for fold in range(block // lot):
                there = ring.chip(offset) * 2 * lot + device * lot
                first_lane = 3 * head_width + fold * 128
                chosen[device * block + fold * lot : device * block + (fold + 1) * lot, :] = rows_full[
                    pl.ds(pl.multiple_of(there, lot), lot), first_lane : first_lane + 128
                ]
        fetch_x(turn).wait()
        hidden_tiles(layout, x_block.at[turn % 2], gates, ups, pre_gate, pre_up)
        pass_on(0)
        pass_on_far()

        @pl.when(turn == 0)
        def _():
            cot_turn(1, 1)

        @pl.when(turn > 2)
        def _():
            cot_turn(turn, 3)

        pending = stores(spot)

        @pl.when(turn > 0)
        def _():
            pending[0].wait()
            pending[1].wait()

        gate_strips(
            layout,
            first_expert,
            chosen,
            pre_gate,
            pre_up,
            cot_hidden.at[slot],
            scaled,
            grads,
        )
        pending[0].start()
        pending[1].start()
        pass_on(1)

        @pl.when(turn > 0)
        def _():
            pending[2].wait()
            pending[3].wait()

        out_tiles(width, scaled, downs, out)
        pending[2].start()

        @pl.when(turn == 0)
        def _():
            cot_turn(2, 2)

        pass_on(2)

        @pl.when((turn > 0) & (turn + 1 < ring.chips))
        def _():
            fetch_next()

        back_tiles(layout, width, grads, gates, ups, back)
        pending[3].start()
        pass_on(3)

        @pl.when(turn == 0)
        def _():
            fetch_next()

        return carry

    lax.fori_loop(0, ring.chips, chip_step, 0)
    for copy in stores(pl.ds(0, chip_rows)):
        copy.wait()
    forwards.sent()
    for copy in handed:
        copy.wait_send()
    for gather in gathers:
        gather.sent()
    cots.sent()
    for work in works:
        work.sent()


def layer_forward_back(
    layout,
    query,
    key,
    value,
    proj,
    router,
    routes,
    switch,
    attn_gain,
    ffn_gain,
    tokens,
    cot,
    segments,
    cosine,
    sine,
    expert_gate,
    expert_up,
    expert_down,
    shared_gate,
    shared_up,
    shared_down,
    small_rows,
    ranks,
    peers,
    identity,
):
    half = ranks // 4
    block, width = tokens.shape
    rows = block // peers
    total = ranks * block
    depth = width // ranks
    hidden = layout.hidden
    chip = 2 * block
    head_width = query.shape[1]
    wide = 3 * head_width + block // depth * 128
    aligned = layout.shared_own % 16 == 0
    height = small_rows + head_width
    low = tokens.dtype
    vmem = pl.BlockSpec(memory_space=pltpu.VMEM)
    hbm = pl.BlockSpec(memory_space=pl.ANY)
    dma = pltpu.SemaphoreType.DMA
    f32 = jnp.float32
    heads = head_width // HEAD_DIM
    small_ones = [jax.ShapeDtypeStruct((block, head_width), low)] * 4
    return pl.pallas_call(
        functools.partial(layer_kernel, layout, ranks, peers),
        out_shape=(
            jax.ShapeDtypeStruct((width, wide), low),
            jax.ShapeDtypeStruct((height, width), low),
            jax.ShapeDtypeStruct((block, width), low),
            *small_ones,
            jax.ShapeDtypeStruct((heads, block, block), f32),
            jax.ShapeDtypeStruct((total, width), low),
            jax.ShapeDtypeStruct((total, width), low),
            jax.ShapeDtypeStruct((rows, width), f32),
            jax.ShapeDtypeStruct((total, hidden), low),
            jax.ShapeDtypeStruct((total, 2 * hidden), low),
            jax.ShapeDtypeStruct((total, width), low),
            jax.ShapeDtypeStruct((total, width), low),
        ),
        in_specs=[hbm] * 4 + [vmem] * 10 + [hbm] * 6,
        out_specs=(hbm, hbm, *[vmem] * 6, hbm, hbm, vmem, hbm, hbm, hbm, hbm),
        scratch_shapes=[
            pltpu.VMEM((depth, wide), low),
            pltpu.VMEM((height, depth), low),
            pltpu.VMEM((width, wide), low),
            pltpu.VMEM((height, width), low),
            pltpu.VMEM((block, 3 * head_width), f32),
            pltpu.VMEM((block, width), low),
            pltpu.VMEM((hidden, width), low),
            pltpu.VMEM((hidden, width), low),
            pltpu.VMEM((hidden, width), low),
            pltpu.VMEM((3, ranks, layout.shared_own, depth), low),
            pltpu.VMEM((2, ranks * layout.shared_own if aligned else 16, depth), low),
            pltpu.VMEM((rows, width), low),
            pltpu.VMEM((peers - 1, rows, width), low),
            pltpu.VMEM((2, chip, width), low),
            pltpu.VMEM((chip, width), low),
            pltpu.VMEM((chip, hidden), f32),
            pltpu.VMEM((chip, hidden), f32),
            pltpu.VMEM((4, chip, hidden), low),
            pltpu.VMEM((chip, hidden), low),
            pltpu.VMEM((chip, 2 * hidden), low),
            pltpu.VMEM((chip, width), low),
            pltpu.VMEM((chip, width), low),
            pltpu.VMEM((chip, 128), low),
            dma((5 + 3 * layout.local_experts,)),
            dma((12,)),
            dma((2 * gather_slots(half),)),
            dma((2 * gather_slots(half),)),
            dma((2 * side_slots(half),)),
            dma((2 * side_slots(half),)),
            dma((2,)),
            dma((2,)),
            dma((4,)),
            dma((3 * (ranks - 1),)),
            dma((3 * (ranks - 1),)),
            dma((peers - 1,)),
            dma((peers - 1,)),
            dma((peers,)),
            dma((peers,)),
            dma((peers * gather_slots(half),)),
            dma((peers * gather_slots(half),)),
            dma((peers * side_slots(half),)),
            dma((peers * side_slots(half),)),
            dma((gather_slots(half),)),
            dma((gather_slots(half),)),
            dma((side_slots(half),)),
            dma((side_slots(half),)),
        ],
        compiler_params=pltpu.CompilerParams(
            collective_id=identity, has_side_effects=True, vmem_limit_bytes=62 << 20
        ),
        name="layer_forward_back",
    )(
        query,
        key,
        value,
        proj,
        router,
        routes,
        switch,
        attn_gain,
        ffn_gain,
        tokens,
        cot,
        segments,
        cosine,
        sine,
        expert_gate,
        expert_up,
        expert_down,
        shared_gate,
        shared_up,
        shared_down,
    )


class RingReduce:
    def __init__(self, ring, source_at, rows, buffers, sems, slot):
        self.ring, self.source_at, self.rows, self.cut = ring, source_at, rows, rows // 2
        self.mine, self.side, self.got = [buffer.at[slot] for buffer in buffers]
        self.loads, self.sends, self.recvs, self.side_sends, self.side_recvs = sems
        self.base, self.side_base = slot * 2 * ring.half, slot * ring.chips
        half = ring.half
        self.order = [half]
        for distance in range(half - 1, 0, -1):
            self.order += [distance, ring.chips - distance]
        self.order.append(0)

    def load(self, offset):
        return pltpu.make_async_copy(
            self.source_at(self.ring.device(offset)),
            self.mine.at[offset],
            self.loads.at[self.side_base + offset],
        )

    def side_copy(self, offset):
        return remote(
            self.source_at(self.ring.other(offset)),
            self.side.at[offset],
            "dp",
            self.ring.sibling,
            self.side_sends,
            self.side_recvs,
            self.side_base + offset,
        )

    def hand_over(self, offset):
        self.side_copy(offset).start()
        self.load(offset).start()

    def ready(self, offset):
        self.load(offset).wait()
        self.side_copy(offset).wait_recv()

    def hop(self, which, number):
        ring, half, cut = self.ring, self.ring.half, self.cut
        distance = half - number
        offset = distance if which == 0 else ring.chips - distance
        place = pl.ds((0, cut)[which], cut) if number == 0 else pl.ds(0, self.rows)
        return remote(
            self.mine.at[offset, place],
            self.got.at[which * half + number, place],
            "dp",
            (ring.ahead, ring.behind)[which],
            self.sends,
            self.recvs,
            self.base + which * half + number,
        )

    def add(self, offset, extra, first, size):
        def total(spot):
            mine = self.mine[offset, spot, :].astype(jnp.float32)
            return mine + self.side[offset, spot, :].astype(jnp.float32)

        def more(spot, start, count):
            here = pl.ds(pl.multiple_of(first + start, count), count)
            value = total(here) + extra[here, :].astype(jnp.float32)
            self.mine[offset, here, :] = value.astype(self.mine.dtype)

        rest, begin = self.rows - size, 0 if first else size

        def plain(spot, start, count):
            here = pl.ds(pl.multiple_of(begin + start, count), count)
            self.mine[offset, here, :] = total(here).astype(self.mine.dtype)

        if size:
            strips(size, more)
        if rest:
            strips(rest, plain)

    def step(self, number):
        ring, half, cut = self.ring, self.ring.half, self.cut
        if number == 0:
            self.ready(half)
            self.add(half, None, 0, 0)
            self.hop(0, 0).start()
            self.hop(1, 0).start()
            return
        for which in range(2):
            distance = half - number
            offset = distance if which == 0 else ring.chips - distance
            self.ready(offset)
            self.hop(which, number - 1).wait_recv()
            extra = self.got.at[which * half + number - 1]
            if number == 1:
                self.add(offset, extra, (0, cut)[which], cut)
            else:
                self.add(offset, extra, 0, self.rows)
            self.hop(which, number).start()

    def total(self, emit):
        half = self.ring.half
        self.ready(0)
        self.hop(0, half - 1).wait_recv()
        self.hop(1, half - 1).wait_recv()

        def body(spot, start, size):
            value = self.mine[0, spot, :].astype(jnp.float32) + self.side[0, spot, :].astype(jnp.float32)
            value = value + self.got[half - 1, spot, :].astype(jnp.float32)
            value = value + self.got[2 * half - 1, spot, :].astype(jnp.float32)
            emit(spot, start, size, value)

        strips(self.rows, body)

    def finish(self):
        for offset in range(self.ring.chips):
            self.side_copy(offset).wait_send()
        for number in range(self.ring.half):
            for which in range(2):
                self.hop(which, number).wait_send()


def reduce_buffers(pieces, chips, rows, width, low):
    return [pltpu.VMEM((pieces, chips, rows, width), low)] * 3


def reduce_sems(pieces, chips):
    dma = pltpu.SemaphoreType.DMA
    return [dma((pieces * chips,))] * 5


class TensorSum:
    def __init__(self, peers, own_at, got, sends, recvs):
        self.peers, self.half = peers, peers // 2
        self.here = lax.axis_index("tensor")
        self.own_at, self.got, self.sends, self.recvs = own_at, got, sends, recvs
        self.rows = got.shape[1]

    def hop(self, which, number):
        peers, half = self.peers, self.half
        cut = self.rows // 2
        distance = half - number
        k = distance if which == 0 else peers - distance
        if number == 0:
            place, slot = pl.ds((0, cut)[which], cut), 0
        else:
            place, slot = pl.ds(0, self.rows), which * (half - 1) + number
        device = (self.here + (1, peers - 1)[which]) % peers
        return remote(
            self.own_at(k).at[place],
            self.got.at[slot, place],
            "tensor",
            device,
            self.sends,
            self.recvs,
            which * half + number,
        )

    def begin(self):
        self.hop(0, 0).start()
        self.hop(1, 0).start()

    def send(self, k):
        half = self.half
        if k == half:
            self.begin()
            return
        which = 0 if k < half else 1
        number = half - (k if which == 0 else self.peers - k)
        self.hop(which, number - 1).wait_recv()
        own = self.own_at(k)
        cut = self.rows // 2
        first, size, slot = 0, self.rows, which * (half - 1) + number - 1
        if number == 1:
            first, size, slot = (0, cut)[which], cut, 0
        place = slice(first, first + size)
        value = own[place, :].astype(jnp.float32) + self.got[slot, place, :].astype(jnp.float32)
        own[place, :] = value.astype(own.dtype)
        self.hop(which, number).start()

    def arrived(self):
        self.hop(0, self.half - 1).wait_recv()
        self.hop(1, self.half - 1).wait_recv()

    def rest(self, spot):
        half = self.half
        if half == 1:
            return self.got[0, spot, :].astype(jnp.float32)
        value = self.got[half - 1, spot, :].astype(jnp.float32)
        return value + self.got[2 * half - 2, spot, :].astype(jnp.float32)

    def sent(self):
        for number in range(self.half):
            for which in range(2):
                self.hop(which, number).wait_send()


class TensorGather:
    def __init__(self, peers, source, place, rows, sends, recvs):
        self.peers, self.half = peers, peers // 2
        self.here = lax.axis_index("tensor")
        self.source, self.place, self.rows = source, place, rows
        self.sends, self.recvs = sends, recvs

    def hop(self, which, number):
        peers, half = self.peers, self.half
        cut = self.rows // 2
        owner = (self.here + (peers - number, number)[which]) % peers
        first, size = 0, self.rows
        if number and number == half - 1:
            first, size = (0, cut)[which], cut
        target = self.place(owner, first, size)
        source = self.source if number == 0 else target
        device = (self.here + (1, peers - 1)[which]) % peers
        return remote(
            source, target, "tensor", device, self.sends, self.recvs, which * half + number
        )

    def begin(self):
        self.hop(0, 0).start()
        self.hop(1, 0).start()

    def step(self, number):
        for which in range(2):
            self.hop(which, number - 1).wait_recv()
            if number < self.half:
                self.hop(which, number).start()

    def sent(self):
        for number in range(self.half):
            for which in range(2):
                self.hop(which, number).wait_send()


def attend_back(heads, queries, keys, values, probs_ref, grad_context, cos_ref, sin_ref, grads):
    cosine, sine = cos_ref[...], sin_ref[...]
    low = grads.dtype
    scale = HEAD_DIM ** (-0.5)
    for head in range(heads):
        columns = slice(head * HEAD_DIM, (head + 1) * HEAD_DIM)
        probs, through = probs_ref[head], grad_context[:, columns]
        grad_probs = matmul_last(through, values[:, columns])
        inner = jnp.sum(probs * grad_probs, axis=-1, keepdims=True)
        grad_scores = (probs * (grad_probs - inner)).astype(low)
        parts = (
            rope(matmul(grad_scores, keys[:, columns]) * scale, cosine, sine, -1.0),
            rope(matmul(grad_scores.T, queries[:, columns]) * scale, cosine, sine, -1.0),
            matmul(probs.astype(low).T, through),
        )
        for index, part in enumerate(parts):
            first = (index * heads + head) * HEAD_DIM
            grads[:, first : first + HEAD_DIM] = part.astype(low)


def rear_kernel(
    layout,
    ranks,
    peers,
    with_out,
    part_ref,
    out_part_ref,
    x_ref,
    cots_ref,
    grads_ref,
    scaled_ref,
    rows_all,
    columns_all,
    middle_ref,
    cot_ref,
    tokens_ref,
    attn_in,
    queries,
    keys,
    values,
    context,
    probs_ref,
    cos_ref,
    sin_ref,
    input_ref,
    output_ref,
    qkv_sum_ref,
    proj_sum_ref,
    small_sum_ref,
    gate_grads_ref,
    up_grads_ref,
    down_grads_ref,
    shared_grads_ref,
    shared_got_ref,
    cot_rows,
    token_rows,
    small_vec,
    grad_ref,
    small_own,
    small_got,
    small_part,
    small_z,
    z_stage,
    z_got,
    a_got,
    o_got,
    low_ref,
    gm_all,
    right,
    left,
    turned,
    product,
    shared_low,
    gain_grad,
    qkv_full,
    grad_context,
    grad_rows,
    attn_part,
    out_sum,
    kept,
    z_sends,
    z_recvs,
    m_sends,
    m_recvs,
    a_sends,
    a_recvs,
    o_sends,
    o_recvs,
    x_sends,
    x_recvs,
    y_sends,
    y_recvs,
    h_sends,
    h_recvs,
    g_sends,
    g_recvs,
    s_sends,
    s_recvs,
    local_sem,
    left_sem,
    right_sem,
    product_sem,
    reuse_sem,
    *refs,
):
    buffers = refs[0:3]
    back_sems, qkv_sems, proj_buffers, proj_sems = refs[3:8], refs[8:13], refs[13:16], refs[16:21]
    out_buffers, out_sems = refs[21:24], refs[24:]
    out_low = z_stage.at[0]
    ring = Ring(ranks)
    here = lax.axis_index("tensor")
    block, width = cot_ref.shape
    rows = block // peers
    half = ring.half
    low = low_ref.dtype
    columns = width // ranks
    hidden = layout.hidden
    head_width = queries.shape[1]
    heads = head_width // HEAD_DIM
    small_rows = small_vec.shape[0]
    away = [(here + k) % peers for k in range(peers)]
    others = [(ring.me + k) % ranks for k in range(ranks)]
    greet(
        [{"dp": others[k]} for k in range(1, ranks)] + [{"tensor": away[k]} for k in range(1, peers)]
    )
    first = here * rows
    order = list(reversed(near_first(peers)))
    far_first = order[:-1]

    def slice_of(device):
        return pl.ds(pl.multiple_of(device * columns, columns), columns)

    def to_peers(source_of, target_of, sends, recvs):
        return [
            remote(
                source_of(k),
                target_of(peers - k - 1),
                "tensor",
                away[k],
                sends,
                recvs,
                peers - k - 1,
            )
            for k in far_first
        ]

    def reducer(source, where, sems, k):
        def source_at(device):
            return source.at[pl.ds(device * block + away[k] * rows, rows)]

        return RingReduce(ring, source_at, rows, where, sems, k)

    backs = {k: reducer(part_ref, buffers, back_sems, k) for k in order}
    outs = {}
    if with_out:
        outs = {k: reducer(out_part_ref, out_buffers, out_sems, k) for k in order}
    for offset in backs[0].order:
        for k in order:
            backs[k].hand_over(offset)

    tile = right.shape[2]
    blocks = width // tile
    steps = 3 * blocks

    def fetch_left(wide):
        source = scaled_ref if wide == 2 else grads_ref.at[:, pl.ds(wide * hidden, hidden)]
        return pltpu.make_async_copy(source, left, left_sem)

    def fetch_right(step, late):
        spot = pl.ds(pl.multiple_of(step % blocks * tile, tile), tile)
        source = cots_ref if late else x_ref
        return pltpu.make_async_copy(source.at[:, spot], right.at[step % 2], right_sem.at[step % 2])

    fetch_right(0, False).start()
    fetch_left(0).start()
    vec_load = pltpu.make_async_copy(columns_all.at[pl.ds(0, small_rows)], small_vec, local_sem.at[0])
    vec_load.start()
    row_loads = [
        pltpu.make_async_copy(source.at[pl.ds(first, rows)], target, local_sem.at[slot])
        for source, target, slot in ((cot_ref, cot_rows, 5), (tokens_ref, token_rows, 6))
    ]
    for load in row_loads:
        load.start()
    qkv_load = pltpu.make_async_copy(
        rows_all.at[:, pl.ds(0, 3 * head_width)], qkv_full, local_sem.at[1]
    )
    qkv_load.start()
    if not with_out:
        out_load = pltpu.make_async_copy(out_part_ref, out_sum, local_sem.at[2])
        out_load.start()
    for k in order:
        backs[k].step(0)

    def hand_outs():
        for offset in backs[0].order:
            for k in outs:
                outs[k].hand_over(offset)

    vec_load.wait()
    for load in row_loads:
        load.wait()
    count = layout.expert_count
    vectors = small_vec[...].astype(jnp.float32)
    attn_gain = vectors[count + 1 : count + 2, :]
    ffn_gain = vectors[count + 2 : count + 3, :]

    z_sum = TensorSum(peers, lambda k: z_stage.at[k], z_got, z_sends, z_recvs)
    def pass_z(k):
        def emit(spot, start, size, value):
            z_stage[k, spot, :] = value.astype(low)

        backs[k].total(emit)
        z_sum.send(k)

    def results(step, wide):
        slot = step % 2
        spot = pl.ds(pl.multiple_of(step % blocks * tile, tile), tile)
        base = slot * (layout.local_experts + 1)
        copies = [
            pltpu.make_async_copy(
                product.at[slot, pl.ds(j * layout.part, layout.expert_hidden)],
                (gate_grads_ref, up_grads_ref, down_grads_ref)[wide].at[j, :, spot],
                product_sem.at[base + j],
            )
            for j in range(layout.local_experts)
        ]
        copies.append(
            pltpu.make_async_copy(
                shared_low.at[slot],
                shared_grads_ref.at[wide, :, spot],
                product_sem.at[base + layout.local_experts],
            )
        )
        return copies

    gain_grad[...] = jnp.zeros_like(gain_grad)

    def norm_middle(spot, start, size, value):
        value = value + z_sum.rest(spot)
        middle = middle_ref[spot, :]
        inverse = lax.rsqrt(jnp.mean(middle * middle, axis=-1, keepdims=True) + EPSILON)
        normed = middle * inverse
        scaled = value * ffn_gain
        back = inverse * (scaled - normed * jnp.mean(scaled * normed, axis=-1, keepdims=True))
        mine = pl.ds(pl.multiple_of(first + start, size), size)
        grad = cot_rows[spot, :].astype(jnp.float32) + back
        grad_ref[spot, :] = grad
        low_ref[spot, :] = grad.astype(low)
        gm_all[mine, :] = grad.astype(low)
        gain_grad[...] += jnp.sum(value * normed, axis=0, keepdims=True)

    def rows_in(target):
        def place(device, start, size):
            return target.at[pl.ds(device * rows + start, size)]

        return place

    def spread(source, target, sends, recvs):
        return TensorGather(peers, source, rows_in(target), rows, sends, recvs)

    gm_spread = spread(low_ref, gm_all, m_sends, m_recvs)

    def finish_norm():
        z_sum.arrived()
        backs[0].total(norm_middle)
        gm_spread.begin()

    events = []
    for number in range(1, half):
        for index, k in enumerate(order):
            events.append((BACK_DUE[0] + number - 1 + index, functools.partial(backs[k].step, number)))
    events.append((BACK_DUE[1], hand_outs))
    gap = 6 // (peers - 2)
    for index, k in enumerate(far_first):
        events.append((BACK_DUE[2] + gap * index, functools.partial(pass_z, k)))
    for number in range(half):
        for index, k in enumerate(outs):
            due = BACK_DUE[3 + number] + number * index
            events.append((due, functools.partial(outs[k].step, number)))

    events.append((NORM_DUE, finish_norm))

    def grad_step(step, carry):
        wide, slot = step // blocks, step % 2
        for number in range(3):

            @pl.when(step == number * blocks)
            def _(number=number):
                fetch_left(number).wait()

                def turn_over(index, carry):
                    spot = pl.ds(pl.multiple_of(index * 256, 256), 256)
                    turned[:, spot] = left[spot, :].T
                    return carry

                lax.fori_loop(0, left.shape[0] // 256, turn_over, 0)
                if number < 2:
                    fetch_left(number + 1).start()

        fetch_right(step, False).wait()

        @pl.when(step + 1 < 2 * blocks)
        def _():
            fetch_right(step + 1, False).start()

        @pl.when((step + 1 >= 2 * blocks) & (step + 1 < steps))
        def _():
            fetch_right(step + 1, True).start()

        @pl.when(step > 1)
        def _():
            for copy in results(step, 0):
                copy.wait()

        value = matmul(turned[...], right[slot])
        product[slot] = value[: layout.shared_at].astype(low)
        shared_low[slot] = value[layout.shared_at : layout.router_at].astype(low)

        @pl.when(wide == 0)
        def _():
            spot = pl.ds(pl.multiple_of(step % blocks * tile, tile), tile)
            small_own[:, spot] = value[layout.router_at : layout.router_at + small_rows]

        for number in range(3):

            @pl.when(wide == number)
            def _(number=number):
                for copy in results(step, number):
                    copy.start()

        for due, event in events:

            @pl.when(step == due)
            def _(event=event):
                event()

        return carry

    lax.fori_loop(0, steps, grad_step, 0)
    proj_load = pltpu.make_async_copy(
        columns_all.at[pl.ds(small_rows, head_width)],
        turned.at[pl.ds(head_width, head_width), pl.ds(0, width)],
        local_sem.at[3],
    )
    proj_load.start()
    for step in (steps - 2, steps - 1):
        for copy in results(step, 0):
            copy.wait()

    small_own[count + 1 : count + 2, :] = jnp.zeros((1, width), jnp.float32)
    small_own[count + 2 : count + 3, :] = gain_grad[...]
    shared = []
    for k in range(1, ranks):
        copy = remote(
            shared_grads_ref.at[:, :, slice_of(others[k])],
            shared_got_ref.at[ring.me],
            "dp",
            others[k],
            s_sends,
            s_recvs,
            ranks - k - 1,
        )
        copy.start()
        shared.append(copy)
    keep = pltpu.make_async_copy(
        shared_grads_ref.at[:, :, slice_of(ring.me)], kept, local_sem.at[4]
    )
    keep.start()
    half_peers = peers // 2
    for number in range(1, half_peers):
        gm_spread.step(number)

    def chunk_of(source):
        return lambda k: source.at[pl.ds(away[k] * rows, rows)]

    if not with_out:
        out_load.wait()
    for k in outs:

        def emit_out(spot, start, size, value, k=k):
            there = pl.ds(pl.multiple_of(away[k] * rows + start, size), size)
            out_sum[there, :] = value.astype(low)

        outs[k].total(emit_out)
    out_total = TensorSum(peers, chunk_of(out_sum), o_got, o_sends, o_recvs)
    out_total.begin()

    gm_spread.step(half_peers)
    proj_load.wait()
    out_weights = turned.at[pl.ds(head_width, head_width), pl.ds(0, width)]
    grad_context[...] = matmul_last(gm_all[...], out_weights[...]).astype(low)
    attend_back(heads, queries, keys, values, probs_ref, grad_context, cos_ref, sin_ref, grad_rows)
    qkv_load.wait()

    def through_qkv(spot):
        attn_part[:, spot] = matmul_last(grad_rows[...], qkv_full[spot, :]).astype(low)

    tiles(width, 256, through_qkv)
    attn_total = TensorSum(peers, chunk_of(attn_part), a_got, a_sends, a_recvs)
    attn_total.begin()
    def weight_tiles(spot):
        qkv_full[spot, :] = matmul(attn_in[:, spot].T, grad_rows[...]).astype(low)

    tiles(width, 256, weight_tiles)
    for k in far_first[1:]:
        attn_total.send(k)
    for k in far_first[1:]:
        out_total.send(k)

    def proj_tiles(spot):
        turned[:head_width, spot] = matmul(context[...].T, gm_all[:, spot]).astype(low)

    tiles(width, 256, proj_tiles)

    for k in order:
        backs[k].finish()
    for partner in ring.partners():
        pl.semaphore_signal(reuse_sem, inc=1, device_id=partner, device_id_type=MESH)
    pl.semaphore_wait(reuse_sem, 3)
    pieces = proj_buffers[0].shape[0]
    lot, size = qkv_sum_ref.shape[0], qkv_sum_ref.shape[0] // pieces
    proj_size = proj_buffers[0].shape[2]
    narrow = [
        buffer.at[pl.ds(0, pieces), :, pl.ds(0, size), pl.ds(0, 3 * head_width)] for buffer in buffers
    ]
    works = []
    for piece in range(pieces):

        def qkv_at(device, piece=piece):
            return qkv_full.at[pl.ds(device * lot + piece * size, size)]

        def proj_at(device, piece=piece):
            return turned.at[pl.ds(piece * proj_size, proj_size), slice_of(device)]

        works.append(RingReduce(ring, qkv_at, size, narrow, qkv_sems, piece))
        works.append(RingReduce(ring, proj_at, proj_size, proj_buffers, proj_sems, piece))
    for offset in works[0].order:
        for work in works:
            work.hand_over(offset)
    for work in works:
        work.step(0)

    spot_row = count + 1

    def norm_tokens(spot, start, size):
        mine = pl.ds(pl.multiple_of(first + start, size), size)
        value = attn_part[mine, :].astype(jnp.float32)
        value = value + attn_total.rest(spot)
        inputs = token_rows[spot, :].astype(jnp.float32)
        inverse = lax.rsqrt(jnp.mean(inputs * inputs, axis=-1, keepdims=True) + EPSILON)
        normed = inputs * inverse
        scaled = value * attn_gain
        back = inverse * (scaled - normed * jnp.mean(scaled * normed, axis=-1, keepdims=True))
        low_ref[spot, :] = (grad_ref[spot, :] + back).astype(low)
        small_own[spot_row : spot_row + 1, :] += jnp.sum(value * normed, axis=0, keepdims=True)

    attn_total.arrived()
    gm_spread.sent()
    strips(rows, norm_tokens)
    mine = input_ref.at[pl.ds(first, rows)]
    input_spread = spread(low_ref, input_ref, x_sends, x_recvs)
    input_spread.begin()
    stores = [pltpu.make_async_copy(low_ref, mine, local_sem.at[5])]
    stores[0].start()
    handed = []
    for k in range(1, ranks):
        copy = remote(
            small_own.at[:, slice_of(others[k])],
            small_got.at[ranks - k - 1],
            "dp",
            others[k],
            g_sends,
            g_recvs,
            ranks - k - 1,
        )
        copy.start()
        handed.append(copy)

    for number in range(1, half):
        for work in works:
            work.step(number)

    def finish_rows(spot, start, size):
        there = pl.ds(pl.multiple_of(first + start, size), size)
        value = out_sum[there, :].astype(jnp.float32)
        value = value + out_total.rest(spot)
        out_low[spot, :] = (middle_ref[spot, :] + value).astype(low)

    out_total.arrived()
    strips(rows, finish_rows)
    out_mine = output_ref.at[pl.ds(first, rows)]
    output_spread = spread(out_low, output_ref, y_sends, y_recvs)
    output_spread.begin()
    for number in range(1, half_peers):
        input_spread.step(number)
    keep.wait()
    keep = pltpu.make_async_copy(kept, shared_got_ref.at[ring.me], local_sem.at[4])
    keep.start()
    for copy in handed:
        copy.wait_recv()
    value = small_own[:, slice_of(ring.me)]
    for k in range(ranks - 1):
        value = value + small_got[k]
    small_part[...] = value
    last = to_peers(lambda k: small_part, lambda slot: small_z.at[slot], h_sends, h_recvs)
    for copy in last:
        copy.start()
    stores.append(pltpu.make_async_copy(out_low, out_mine, local_sem.at[6]))
    stores[1].start()
    for piece in range(pieces):

        def emit_qkv(spot, start, count, value, piece=piece):
            qkv_sum_ref[pl.ds(pl.multiple_of(piece * size + start, count), count), :] = value

        def emit_proj(spot, start, count, value, piece=piece):
            proj_sum_ref[pl.ds(pl.multiple_of(piece * proj_size + start, count), count), :] = value

        works[2 * piece].total(emit_qkv)
        works[2 * piece + 1].total(emit_proj)
    for number in range(1, half_peers):
        output_spread.step(number)
    for copy in last:
        copy.wait_recv()
    value = small_part[...]
    for k in range(peers - 1):
        value = value + small_z[k]
    small_sum_ref[...] = value
    keep.wait()
    for copy in stores:
        copy.wait()
    input_spread.step(half_peers)
    output_spread.step(half_peers)
    for work in (z_sum, out_total, attn_total, input_spread, output_spread):
        work.sent()
    for copy in handed + last:
        copy.wait_send()
    for copy in shared:
        copy.wait()
    for k in outs:
        outs[k].finish()
    for work in works:
        work.finish()


def rear(
    layout,
    back_part,
    out_part,
    x_all,
    cot_all,
    grads,
    scaled,
    rows_all,
    columns_all,
    middle,
    cotangent,
    tokens,
    attn_in,
    queries,
    keys,
    values,
    context,
    probs,
    cosine,
    sine,
    small_rows,
    with_out,
    ranks,
    peers,
    identity,
):
    chips = ranks // 2
    block, width = tokens.shape
    total = x_all.shape[0]
    rows = block // peers
    hidden, own = layout.hidden, layout.shared_own
    experts, units = layout.local_experts, layout.expert_hidden
    head_width = queries.shape[1]
    columns = width // ranks
    pieces = 4
    tile = 256
    vmem = pl.BlockSpec(memory_space=pltpu.VMEM)
    hbm = pl.BlockSpec(memory_space=pl.ANY)
    dma = pltpu.SemaphoreType.DMA
    low, f32 = tokens.dtype, jnp.float32
    shape = jax.ShapeDtypeStruct
    return pl.pallas_call(
        functools.partial(rear_kernel, layout, ranks, peers, with_out),
        out_shape=(
            shape((block, width), low),
            shape((block, width), low),
            shape((columns, 3 * head_width), f32),
            shape((head_width, columns), f32),
            shape((small_rows, columns), f32),
            *[shape((experts, units, width), low)] * 3,
            shape((3, own, width), low),
            shape((ranks, 3, own, columns), low),
        ),
        in_specs=[hbm] * 8 + [vmem] + [hbm] * 2 + [vmem] * 8,
        out_specs=(hbm, hbm, vmem, vmem, vmem, hbm, hbm, hbm, hbm, hbm),
        scratch_shapes=[
            pltpu.VMEM((rows, width), low),
            pltpu.VMEM((rows, width), low),
            pltpu.VMEM((small_rows, width), low),
            pltpu.VMEM((rows, width), f32),
            pltpu.VMEM((small_rows, width), f32),
            pltpu.VMEM((ranks - 1, small_rows, columns), f32),
            pltpu.VMEM((small_rows, columns), f32),
            pltpu.VMEM((peers - 1, small_rows, columns), f32),
            pltpu.VMEM((peers, rows, width), low),
            pltpu.VMEM((peers - 1, rows, width), low),
            pltpu.VMEM((peers - 1, rows, width), low),
            pltpu.VMEM((peers - 1, rows, width), low),
            pltpu.VMEM((rows, width), low),
            pltpu.VMEM((block, width), low),
            pltpu.VMEM((2, total, tile), low),
            pltpu.VMEM((total, hidden), low),
            pltpu.VMEM((hidden, total), low),
            pltpu.VMEM((2, layout.shared_at, tile), low),
            pltpu.VMEM((2, own, tile), low),
            pltpu.VMEM((1, width), f32),
            pltpu.VMEM((width, 3 * head_width), low),
            pltpu.VMEM((block, head_width), low),
            pltpu.VMEM((block, 3 * head_width), low),
            pltpu.VMEM((block, width), low),
            pltpu.VMEM((block, width), low),
            pltpu.VMEM((3, own, columns), low),
        ]
        + [dma((peers,))] * 14
        + [dma((ranks - 1,))] * 4
        + [
            dma((7,)),
            dma,
            dma((2,)),
            dma((2 * (experts + 1),)),
            pltpu.SemaphoreType.REGULAR,
        ]
        + reduce_buffers(peers, chips, rows, width, low)
        + reduce_sems(peers, chips)
        + reduce_sems(pieces, chips)
        + reduce_buffers(pieces, chips, head_width // pieces, columns, low)
        + reduce_sems(pieces, chips)
        + (reduce_buffers(peers, chips, rows, width, low) + reduce_sems(peers, chips)) * with_out,
        compiler_params=pltpu.CompilerParams(
            collective_id=identity, has_side_effects=True, vmem_limit_bytes=67043328
        ),
        name="rear",
    )(
        back_part,
        out_part,
        x_all,
        cot_all,
        grads,
        scaled,
        rows_all,
        columns_all,
        middle,
        cotangent,
        tokens,
        attn_in,
        queries,
        keys,
        values,
        context,
        probs,
        cosine,
        sine,
    )


def widen_kernel(ranks, experts_in, with_shared, *refs):
    ins, refs = refs[:8], refs[8:]
    gate_in, up_in, down_in, input_in, output_in, qkv_in, proj_in, shared_in = ins
    amount = 12 if with_shared else 9
    outs, refs = refs[:amount], refs[amount:]
    lows, wides, input_low, input_wide, output_low, qkv, proj, shared, rows, turned, sems, out_sems = refs
    loads = []

    def load(source, target):
        copy = pltpu.make_async_copy(source, target, sems.at[len(loads)])
        copy.start()
        loads.append(copy)
        return copy

    stores = []

    def store(source, target):
        copy = pltpu.make_async_copy(source, target, out_sems.at[len(stores)])
        copy.start()
        stores.append(copy)

    parts = []
    for which, source in enumerate((gate_in, up_in, down_in)):
        for j in range(experts_in):
            parts.append((which, j, load(source.at[j], lows.at[which, j])))
    rest = [
        load(input_in, input_low),
        load(output_in, output_low),
        load(qkv_in, qkv),
        load(proj_in, proj),
    ]
    if with_shared:
        rest.append(load(shared_in, shared))

    def convert(source, target):
        size = 32 if source.shape[0] % 32 == 0 else 16

        def step(index, carry):
            spot = pl.ds(pl.multiple_of(index * size, size), size)
            target[spot, :] = source[spot, :].astype(target.dtype)
            return carry

        lax.fori_loop(0, source.shape[0] // size, step, 0)

    for which, j, copy in parts:
        copy.wait()
        convert(lows.at[which, j], wides.at[which, j])
        store(wides.at[which, j], outs[which].at[j])
    rest[0].wait()
    convert(input_low, input_wide)
    store(input_wide, outs[3])
    rest[1].wait()
    store(output_low, outs[4])
    rest[2].wait()
    head_width = qkv.shape[1] // 3
    for which in range(3):
        store(qkv.at[:, pl.ds(which * head_width, head_width)], outs[5 + which])
    rest[3].wait()
    store(proj, outs[8])
    if with_shared:
        rest[4].wait()
        own = shared.shape[2]
        for which in range(3):
            for source in range(ranks):
                rows[which, source * own : (source + 1) * own, :] = shared[source, which].astype(
                    rows.dtype
                )
        for which in range(2):
            for tile in range(rows.shape[1] // 128):
                spot = slice(tile * 128, (tile + 1) * 128)
                turned[which, :, spot] = rows[which, spot, :].T
            store(turned.at[which], outs[9 + which])
        store(rows.at[2], outs[11])
    for copy in stores:
        copy.wait()


def widen(gate, up, down, grad_input, output, qkv, proj, shared):
    experts, units, width = gate.shape
    block = grad_input.shape[0]
    lot, wide = qkv.shape
    ranks, _, own, columns = shared.shape
    with_shared = (ranks * own) % 128 == 0 and own % 16 == 0
    hbm = pl.BlockSpec(memory_space=pl.ANY)
    dma = pltpu.SemaphoreType.DMA
    low, f32 = gate.dtype, jnp.float32
    shape = jax.ShapeDtypeStruct
    outs = [shape((experts, units, width), f32)] * 3
    outs += [shape((block, width), f32), shape((block, width), low)]
    outs += [shape((lot, wide // 3), f32)] * 3
    outs.append(shape(proj.shape, f32))
    if with_shared:
        outs += [shape((columns, ranks * own), f32)] * 2
        outs.append(shape((ranks * own, columns), f32))
    results = pl.pallas_call(
        functools.partial(widen_kernel, ranks, experts, with_shared),
        out_shape=tuple(outs),
        in_specs=[hbm] * 8,
        out_specs=(hbm,) * len(outs),
        scratch_shapes=[
            pltpu.VMEM((3, experts, units, width), low),
            pltpu.VMEM((3, experts, units, width), f32),
            pltpu.VMEM((block, width), low),
            pltpu.VMEM((block, width), f32),
            pltpu.VMEM((block, width), low),
            pltpu.VMEM((lot, wide), f32),
            pltpu.VMEM(proj.shape, f32),
            pltpu.VMEM(shared.shape, low),
            pltpu.VMEM((3, ranks * own, columns), f32),
            pltpu.VMEM((2, columns, ranks * own), f32),
            dma((3 * experts + 5,)),
            dma((3 * experts + 9,)),
        ],
        compiler_params=pltpu.CompilerParams(vmem_limit_bytes=60 << 20),
        name="widen",
    )(gate, up, down, grad_input, output, qkv, proj, shared)
    if with_shared:
        return results
    shared = shared.astype(f32)
    whole = [shared[:, which].reshape(ranks * own, columns) for which in range(3)]
    return (*results, whole[0].T, whole[1].T, whole[2])


def rope_tables():
    half_dim = HEAD_DIM // 2
    exponent = np.arange(half_dim, dtype=np.float32) * np.float32(2.0 / HEAD_DIM)
    inverse_freq = np.exp(-exponent * np.log(np.float32(1000000.0)))
    angles = np.arange(SEQ, dtype=np.float32)[:, None] * inverse_freq[None, :]
    cosine, sine = np.cos(angles), np.sin(angles)
    return (
        jnp.asarray(np.concatenate([cosine, cosine], axis=1)),
        jnp.asarray(np.concatenate([-sine, sine], axis=1)),
    )


def scatter_rows(values):
    return lax.psum_scatter(values, "dp", scatter_dimension=0, tiled=True)


def shards(
    tokens,
    w_query,
    w_key,
    w_value,
    w_out,
    gain_attn,
    gain_ffn,
    w_router,
    shared_gate,
    shared_up,
    shared_down,
    shared_switch,
    expert_gate,
    expert_up_weight,
    expert_down,
    routes,
    segments,
    cotangent,
):
    low = jnp.bfloat16
    ranks = lax.axis_size("dp")
    peers = lax.axis_size("tensor")
    token_count, width = tokens.shape
    local_experts, _, expert_hidden = expert_gate.shape
    expert_count = local_experts * ranks
    block = width // ranks
    head_width = w_query.shape[1]
    shared_own = shared_gate.shape[1] // ranks
    layout = Layout(local_experts, expert_hidden, shared_own, expert_count)

    small_rows = -(-(expert_count + 3) // 16) * 16
    cosine, sine = rope_tables()
    gate_rows, up_rows = shared_gate, shared_up
    if shared_own % 16:
        gate_rows, up_rows = [
            part.T.reshape(ranks, shared_own, block) for part in (shared_gate, shared_up)
        ]

    (
        qkv_full,
        columns_full,
        attn_in,
        queries,
        key_rows,
        value_rows,
        context_flat,
        probs,
        x_all,
        cot_all,
        middle,
        scaled_hidden,
        grads_wide,
        out_part,
        back_part,
    ) = layer_forward_back(
        layout,
        w_query,
        w_key,
        w_value,
        w_out,
        w_router.T,
        routes.T,
        shared_switch,
        gain_attn,
        gain_ffn,
        tokens,
        cotangent,
        segments,
        cosine,
        sine,
        expert_gate.swapaxes(1, 2),
        expert_up_weight.swapaxes(1, 2),
        expert_down,
        gate_rows,
        up_rows,
        shared_down.reshape(ranks, shared_own, block),
        small_rows,
        ranks,
        peers,
        1,
    )
    with_out = ranks == 8
    grad_input, output, grad_qkv, grad_proj, grad_small, *grad_experts, _, grad_shared = rear(
        layout,
        back_part,
        out_part if with_out else scatter_rows(out_part),
        x_all,
        cot_all,
        grads_wide,
        scaled_hidden,
        qkv_full,
        columns_full,
        middle,
        cotangent,
        tokens,
        attn_in,
        queries,
        key_rows,
        value_rows,
        context_flat,
        probs,
        cosine,
        sine,
        small_rows,
        with_out,
        ranks,
        peers,
        2,
    )
    (
        grad_gate,
        grad_up,
        grad_down,
        grad_input,
        output,
        grad_query,
        grad_key,
        grad_value,
        grad_proj,
        grad_shared_gate,
        grad_shared_up,
        grad_shared_down,
    ) = widen(*grad_experts, grad_input, output, grad_qkv, grad_proj, grad_shared)
    return (
        output,
        grad_input,
        grad_query,
        grad_key,
        grad_value,
        grad_proj,
        grad_small[expert_count + 1],
        grad_small[expert_count + 2],
        grad_small[:expert_count].T,
        grad_shared_gate,
        grad_shared_up,
        grad_shared_down,
        grad_small[expert_count],
        grad_gate.swapaxes(1, 2),
        grad_up.swapaxes(1, 2),
        grad_down,
    )


def solution(mesh):
    in_specs = (
        P("dp", None),
        P("dp", "tensor"),
        P("dp", "tensor"),
        P("dp", "tensor"),
        P("tensor", "dp"),
        P("dp"),
        P("dp"),
        P("dp", None),
        P("dp", "tensor"),
        P("dp", "tensor"),
        P("tensor", "dp"),
        P("dp"),
        P("dp", None, "tensor"),
        P("dp", None, "tensor"),
        P("dp", "tensor", None),
        P("dp", None),
        P("dp", None),
        P("dp", None),
    )
    out_specs = (
        P("dp", None),
        P("dp", None),
        P("dp", "tensor"),
        P("dp", "tensor"),
        P("dp", "tensor"),
        P("tensor", "dp"),
        P("dp"),
        P("dp"),
        P("dp", None),
        P("dp", "tensor"),
        P("dp", "tensor"),
        P("tensor", "dp"),
        P("dp"),
        P("dp", None, "tensor"),
        P("dp", None, "tensor"),
        P("dp", "tensor", None),
    )
    return jax.shard_map(shards, mesh=mesh, in_specs=in_specs, out_specs=out_specs, check_vma=False)
```
